32 devices in a mesh: conf: 2 (over y), res: 4 (over z), vec: 4 (over x, core).
Axes of the slice: x: 2, y: 2, z: 4, core: 2. Of those that a mesh axis runs over, the one named last changes fastest.
Arguments:
- start_block: float32 [256, 64, 128], P(('conf', 'res')), parts along dimension 0, may hold values from -6 to 6
- diagonal: float32 [256, 128], P(('conf', 'res')), parts along dimension 0, may hold values from 0.3 to 3
- hess_tiles: float32 [8, 4, 44, 128, 128], P(('conf', 'res'), 'vec'), parts along dimension 0, may hold values from -0.15625 to 0.15625
- tile_rows: int32 [8, 4, 44], P(('conf', 'res'), 'vec'), parts along dimension 0, may hold values from 0 to 31
- tile_cols: int32 [8, 4, 44], P(('conf', 'res'), 'vec'), parts along dimension 0, may hold values from 0 to 31
- slot_counts: int32 [8, 4, 3], P(('conf', 'res'), 'vec'), parts along dimension 0, may hold values from 0 to 8, as said below
Outputs:
- next_block: float32 [256, 64, 128], P(('conf', 'res')), parts along dimension 0
- coefficients: float32 [8, 64, 64], P('conf'), parts along dimension 0
The draws below stay inside these ranges and needn't reach their ends.
There are 2 independent parts, one for each index of `conf`. The reference program is written for one: setup_inputs(seed, part) draws one part's arguments, and reference() takes and returns one part's arrays. A program takes and returns all parts, laid end to end along the dimension named above; each array names one. Nothing has to cross between parts.
Inputs may be any that keep to these rules, and one draw needn't show every extreme that they name: slot_counts[r, v, d - 1] is 0 exactly where r + d >= 4 and 1 or more elsewhere; for every hop d some shard has 8 on all of its devices.
All inputs are finite; a program needn't handle non-finite values.
Results may differ from the reference program's by a relative error of at most 0.0003.
Values sent between devices are 32-bit elements; how exact they have to be, the bound alone decides.
No kernel may reach another device: no remote copies, remote signals or barrier semaphores. Data moves between devices by JAX's collectives and lax.ppermute only.
A program may use at most 64 MiB of HBM per device.

```python
import math
import jax
import jax.numpy as jnp
from jax import lax

K = 64
TILE = 128
OWN_SLOTS = 20
HOPS = 3
CAP = 8
RT = 32
NT = 128
N = 16384
SLOTS = 44
N_RES = 4
N_VEC = 4


def draw_slot_counts(key, part):
    count_key = jax.random.fold_in(key, 11)
    full_key = jax.random.fold_in(key, 23)
    counts = jax.random.randint(count_key, (N_RES, N_VEC, HOPS), 1, CAP + 1, dtype=jnp.int32)
    full_at = jax.random.randint(full_key, (HOPS,), 0, N_RES - HOPS, dtype=jnp.int32)
    shard = jnp.arange(N_RES, dtype=jnp.int32)[:, None, None]
    hop = jnp.arange(1, HOPS + 1, dtype=jnp.int32)[None, None, :]
    counts = jnp.where(shard == full_at[None, None, :], CAP, counts)
    counts = jnp.where(shard + hop < N_RES, counts, 0)
    return counts.astype(jnp.int32)


def touch_ends(array, rng, low, largest):
    shape = array.shape
    spot = [jax.random.randint(jax.random.fold_in(rng, axis), (), 0, shape[axis]) for axis in range(len(shape))]
    array = array.at[tuple(spot)].set(low)
    longest = shape.index(max(shape))
    spot[longest] = (spot[longest] + 1) % shape[longest]
    return array.at[tuple(spot)].set(largest)


def block_levels(key, extent, shards, smallest, largest):
    loudness = 1.0
    for position, parts in shards:
        heights = jax.random.uniform(jax.random.fold_in(jax.random.fold_in(key, 6), position), (parts,), jnp.float32, smallest / len(shards), largest / len(shards))
        loudness = loudness * jnp.repeat(jnp.exp(heights), extent[position] // parts).reshape((-1,) + (1,) * (len(extent) - 1 - position))
    return loudness


def noise(key, extent, deviation, bound, pieces=(), kind=jnp.bfloat16):
    level = block_levels(key, extent, pieces, -0.22, 0.18) if pieces else 1.0
    drawn = jax.random.normal(key, extent, jnp.float32) * deviation * level
    return jnp.minimum(jnp.maximum(drawn, -bound), bound).astype(kind)


def setup_inputs(seed: int = 0, part: int = 0) -> dict:
    key_list = jax.random.split(jax.random.key(seed), 7)
    part_splits = jax.random.split(jax.random.fold_in(key_list[6], part), 7)
    return {
        "start_block": noise(part_splits[0], (NT, K, TILE), 1.0, 6.0, ((0, 4),), jnp.float32),
        "diagonal": jnp.clip(jnp.exp(math.log(3.0) - 2.3025851 * jax.random.uniform(part_splits[1], (NT, TILE), jnp.float32) ** block_levels(part_splits[1], (NT, TILE), ((0, 4),), -0.2, 0.2)), 0.3, 3.0),
        "hess_tiles": noise(part_splits[2], (N_RES, N_VEC, SLOTS, TILE, TILE), (TILE * 2 * SLOTS * N_VEC // RT) ** -0.5, 0.15625, ((0, 4), (1, 4)), jnp.float32),
        "tile_rows": touch_ends(jax.random.randint(part_splits[3], (N_RES, N_VEC, SLOTS), 0, RT), jax.random.fold_in(part_splits[3], 1), 0, RT - 1).astype(jnp.int32),
        "tile_cols": touch_ends(jax.random.randint(part_splits[4], (N_RES, N_VEC, SLOTS), 0, RT), jax.random.fold_in(part_splits[4], 1), 0, RT - 1).astype(jnp.int32),
        "slot_counts": draw_slot_counts(jax.random.fold_in(jax.random.fold_in(key_list[6], part), 71), part),
    }


PRECISE = lax.Precision.HIGHEST

def gram_of(left, right):
    return jnp.einsum('nkt,nlt->kl', left, right, precision=PRECISE)

def combine_rows(matrix, vectors):
    return jnp.einsum('kl,nlt->nkt', matrix, vectors, precision=PRECISE)

def factor_of(gram):
    lower = jnp.linalg.cholesky(gram)
    identity = jnp.eye(gram.shape[0], dtype=gram.dtype)
    inverse = lax.linalg.triangular_solve(lower, identity, left_side=True, lower=True)
    return (lower, inverse)

def apply_hessian(vectors, diagonal, hess_tiles, tile_rows, tile_cols, slot_counts):
    device_total = N_RES * N_VEC
    flat_tiles = hess_tiles.reshape(device_total, SLOTS, TILE, TILE)
    flat_rows = tile_rows.reshape(device_total, SLOTS)
    flat_cols = tile_cols.reshape(device_total, SLOTS)
    flat_counts = slot_counts.reshape(device_total, HOPS)
    shard_ids = (jnp.arange(device_total, dtype=jnp.int32) // N_VEC).astype(jnp.int32)
    slot_ids = jnp.arange(SLOTS, dtype=jnp.int32)
    remote = slot_ids >= OWN_SLOTS
    hop_ids = jnp.where(remote, (slot_ids - OWN_SLOTS) // CAP + 1, 0).astype(jnp.int32)
    places = jnp.where(remote, (slot_ids - OWN_SLOTS) % CAP, 0).astype(jnp.int32)
    count_index = jnp.maximum(hop_ids - 1, 0).astype(jnp.int32)

    def one_device(summed, inputs):
        shard_id, tile_set, row_local, col_local, counts = inputs
        live = jnp.where(remote, places < counts[count_index], True).astype(vectors.dtype)
        peers = jnp.minimum(shard_id + hop_ids, N_RES - 1).astype(jnp.int32)
        glob_rows = (shard_id * RT + row_local).astype(jnp.int32)
        glob_cols = (peers * RT + col_local).astype(jnp.int32)
        direct = jnp.einsum('skb,sab->ska', vectors[glob_cols], tile_set, precision=PRECISE) * live[:, None, None]
        mirror = jnp.einsum('ska,sab->skb', vectors[glob_rows], tile_set, precision=PRECISE) * live[:, None, None]
        summed = summed.at[glob_rows].add(direct)
        summed = summed.at[glob_cols].add(mirror)
        return (summed, None)
    summed, _ = lax.scan(one_device, jnp.zeros_like(vectors), (shard_ids, flat_tiles, flat_rows, flat_cols, flat_counts))
    return summed + diagonal[:, None, :] * vectors

def reference(start_block, diagonal, hess_tiles, tile_rows, tile_cols, slot_counts):

    def hessian(vectors):
        return apply_hessian(vectors, diagonal, hess_tiles, tile_rows, tile_cols, slot_counts)
    first_lower, first_inverse = factor_of(gram_of(start_block, start_block))
    first_block = combine_rows(first_inverse, start_block)
    first_applied = hessian(first_block)
    first_cross = gram_of(first_applied, first_block)
    first_residual = first_applied - combine_rows(first_cross, first_block)
    second_lower, second_inverse = factor_of(gram_of(first_residual, first_residual))
    second_block = combine_rows(second_inverse, first_residual)
    second_applied = hessian(second_block) - combine_rows(second_lower, first_block)
    second_cross = gram_of(second_applied, second_block)
    second_residual = second_applied - combine_rows(second_cross, second_block)
    third_lower, third_inverse = factor_of(gram_of(second_residual, second_residual))
    next_block = combine_rows(third_inverse, second_residual) * math.sqrt(N)
    coefficients = jnp.stack([first_cross, second_lower, second_cross, third_lower])
    return (next_block, coefficients)
```

```python
import math

import jax
import jax.numpy as jnp
from jax import lax
from jax.experimental import pallas as pl
from jax.experimental.pallas import tpu as pltpu
from jax.sharding import PartitionSpec as P

OWN_SLOTS = 20
HOPS = 3
CAP = 8
SHIFT = 1.65


def dot(a, b, ta=False, tb=False):
    dims = (((0 if ta else 1,), (1 if tb else 0,)), ((), ()))
    return lax.dot_general(
        a, b, dims, precision=lax.Precision.HIGHEST, preferred_element_type=jnp.float32
    )


VMEM = pl.BlockSpec(memory_space=pltpu.VMEM)
SMEM = pl.BlockSpec(memory_space=pltpu.SMEM)


def call(body, outs, in_specs, scratch=(), name=None):
    shapes = [jax.ShapeDtypeStruct(s, jnp.float32) for s in outs]
    return pl.pallas_call(
        body,
        out_shape=shapes,
        in_specs=in_specs,
        out_specs=[VMEM] * len(outs),
        scratch_shapes=list(scratch),
        compiler_params=pltpu.CompilerParams(vmem_limit_bytes=40 << 20),
        name=name,
    )


def pairings(size):
    rounds = []
    for hop in range(1, HOPS + 1):
        for parity in range(2):
            pairs = [
                (i, i + hop) for i in range(size - hop) if (i // hop) % 2 == parity
            ]
            if not pairs:
                continue
            used = {i for pair in pairs for i in pair}
            for entry in rounds:
                if not entry["used"] & used:
                    entry["used"] |= used
                    entry["pairs"] += pairs
                    entry["kinds"].append((hop, parity))
                    break
            else:
                rounds.append({"used": used, "pairs": pairs, "kinds": [(hop, parity)]})
    return rounds


def exchange(block, axis, pairs):
    return lax.ppermute(block, axis, [(a, b) for a, b in pairs] + [(b, a) for a, b in pairs])


def role_of(entry, rank, size):
    role = jnp.int32(0)
    for hop, parity in entry["kinds"]:
        lower = (rank + hop < size) & ((rank // hop) % 2 == parity)
        upper = (rank >= hop) & ((jnp.maximum(rank - hop, 0) // hop) % 2 == parity)
        role = jnp.where(lower, hop, jnp.where(upper, -hop, role))
    return role


def all_sum(block, axis):
    size = lax.axis_size(axis)
    if size & (size - 1):
        return lax.psum(block, axis)
    step = 1
    while step < size:
        masks = [step] if step * 2 >= size else [step, 2 * step, 3 * step]
        got = [
            lax.ppermute(block, axis, [(i, i ^ mask) for i in range(size)]) for mask in masks
        ]
        if len(got) == 1:
            block = block + got[0]
            step *= 2
        else:
            block = (block + got[0]) + (got[1] + got[2])
            step *= 4
    return block


def factor(gram):
    size = gram.shape[0]
    row_id = lax.broadcasted_iota(jnp.int32, (size, size), 0)
    col_id = lax.broadcasted_iota(jnp.int32, (size, size), 1)
    work = jnp.concatenate([gram, (row_id == col_id).astype(jnp.float32)], axis=1)
    blocks = [work[8 * b : 8 * b + 8] for b in range(size // 8)]
    sub = lax.broadcasted_iota(jnp.int32, (8, 2 * size), 0)
    for j in range(size):
        b, s = divmod(j, 8)
        row = blocks[b][s : s + 1]
        scaled = row / row[:, j : j + 1]
        scaled = jnp.broadcast_to(scaled, (8, 2 * size))
        for other in range(b, size // 8):
            col = jnp.broadcast_to(blocks[other][:, j : j + 1], (8, 2 * size))
            if other == b:
                col = jnp.where(sub > s, col, 0.0)
            blocks[other] = blocks[other] - col * scaled
    work = jnp.concatenate(blocks, axis=0)
    pivots = jnp.sum(jnp.where(row_id == col_id, work[:, :size], 0.0), axis=1, keepdims=True)
    work = work / jnp.sqrt(pivots)
    upper = jnp.where(col_id >= row_id, work[:, :size], 0.0)
    inverse = jnp.where(col_id <= row_id, work[:, size:], 0.0)
    return upper, inverse


def local(start_block, diagonal, hess_tiles, tile_rows, tile_cols, slot_counts):
    peers = lax.axis_size("res")
    lanes = lax.axis_size("vec")
    rows, width, length = start_block.shape
    half = rows // 2
    rounds = pairings(peers)
    count = len(rounds)
    full = (rows, width, length)
    halfshape = (half, width, length)
    packet = (CAP, width, length)
    square = (width, width)

    place = jnp.stack(
        [lax.axis_index("vec")]
        + [role_of(entry, lax.axis_index("res"), peers) for entry in rounds]
    ).astype(jnp.int32)

    asked = [exchange(tile_cols, "res", entry["pairs"]) for entry in rounds]

    def send_body(place_ref, rows_ref, counts_ref, *refs):
        asked_refs, (x_ref, tiles_ref), out_refs = refs[:count], refs[count : count + 2], refs[count + 2 :]
        for p in range(count):
            role = place_ref[1 + p]

            @pl.when(role > 0)
            def _():
                base = OWN_SLOTS + (role - 1) * CAP
                for c in range(CAP):
                    term = dot(x_ref[rows_ref[0, 0, base + c]], tiles_ref[0, 0, base + c])
                    out_refs[p][c] = jnp.where(c < counts_ref[0, 0, role - 1], term, 0.0)

            @pl.when(role < 0)
            def _():
                base = OWN_SLOTS + (-role - 1) * CAP
                for c in range(CAP):
                    out_refs[p][c] = x_ref[asked_refs[p][0, 0, base + c]]

            @pl.when(role == 0)
            def _():
                out_refs[p][...] = jnp.zeros(packet, jnp.float32)

    def own_body(place_ref, rows_ref, cols_ref, x_ref, diag_ref, tiles_ref, acc_ref):
        first = (place_ref[0] == 0).astype(jnp.float32)
        acc_ref[...] = x_ref[...] * ((diag_ref[...] - SHIFT) * first)[:, None, :]
        for s in range(OWN_SLOTS):
            i, j, tile = rows_ref[0, 0, s], cols_ref[0, 0, s], tiles_ref[0, 0, s]
            direct = dot(x_ref[j], tile, tb=True)
            mirror = dot(x_ref[i], tile)
            acc_ref[i] += direct
            acc_ref[j] += mirror

    def join_body(place_ref, rows_ref, counts_ref, *refs):
        asked_refs, got_refs = refs[:count], refs[count : 2 * count]
        tiles_ref, part_ref, keep_ref, give_ref, acc_ref = refs[2 * count :]
        acc_ref[...] = part_ref[...]
        for p in range(count):
            role = place_ref[1 + p]

            @pl.when(role > 0)
            def _():
                base = OWN_SLOTS + (role - 1) * CAP
                for c in range(CAP):
                    term = dot(got_refs[p][c], tiles_ref[0, 0, base + c], tb=True)
                    acc_ref[rows_ref[0, 0, base + c]] += jnp.where(
                        c < counts_ref[0, 0, role - 1], term, 0.0
                    )

            @pl.when(role < 0)
            def _():
                base = OWN_SLOTS + (-role - 1) * CAP
                for c in range(CAP):
                    acc_ref[asked_refs[p][0, 0, base + c]] += got_refs[p][c]

        core = place_ref[0] % 2
        keep_ref[...] = acc_ref[pl.ds(core * half, half)]
        give_ref[...] = acc_ref[pl.ds((1 - core) * half, half)]

    def gram_body(x_ref, out_ref):
        total = jnp.zeros(square, jnp.float32)
        for n in range(rows):
            total += dot(x_ref[n], x_ref[n], tb=True)
        out_ref[...] = total

    def settle_body(place_ref, mine_ref, other_ref, x_ref, y_ref, out_ref):
        core = place_ref[0] % 2
        y_ref[pl.ds(core * half, half)] = mine_ref[...]
        y_ref[pl.ds((1 - core) * half, half)] = other_ref[...]
        total = jnp.zeros((width, 2 * width), jnp.float32)
        for n in range(rows):
            y = y_ref[n]
            total += dot(y, jnp.concatenate([x_ref[n], y], axis=0), tb=True)
        out_ref[...] = total

    def first_body(gram_ref, inverse_ref):
        _, inverse_ref[...] = factor(gram_ref[...])

    def second_body(gram_ref, inverse_ref, cross_ref, lower_ref, coef_ref):
        start_inv = inverse_ref[...]
        cross = dot(dot(start_inv, gram_ref[:, :width]), start_inv, tb=True)
        applied = dot(dot(start_inv, gram_ref[:, width:]), start_inv, tb=True)
        upper, inverse = factor(applied - dot(cross, cross, tb=True))
        lower = upper.T
        eye = lax.broadcasted_iota(jnp.int32, square, 0) == lax.broadcasted_iota(jnp.int32, square, 1)
        cross_ref[...] = cross + jnp.where(eye, SHIFT, 0.0)
        lower_ref[...] = lower
        coef_ref[:, :width] = -dot(lower, start_inv)
        coef_ref[:, width : 2 * width] = -dot(dot(inverse, cross), start_inv)
        coef_ref[:, 2 * width :] = dot(inverse, start_inv)

    def third_body(place_ref, mine_ref, other_ref, x_ref, y_ref, coef_ref, w_ref, q_ref, out_ref, z_ref):
        core = place_ref[0] % 2
        z_ref[pl.ds(core * half, half)] = mine_ref[...]
        z_ref[pl.ds((1 - core) * half, half)] = other_ref[...]
        total = jnp.zeros((width, 2 * width), jnp.float32)
        for n in range(rows):
            stack = jnp.concatenate([x_ref[n], y_ref[n], z_ref[n]], axis=0)
            w = dot(coef_ref[...], stack)
            q = dot(coef_ref[:, width:], stack[: 2 * width])
            w_ref[n] = w
            q_ref[n] = q
            total += dot(w, jnp.concatenate([q, w], axis=0), tb=True)
        out_ref[...] = total

    def fourth_body(gram_ref, cross_ref, lower_ref, coef_ref):
        cross = gram_ref[:, :width]
        upper, inverse = factor(gram_ref[:, width:] - dot(cross, cross, tb=True))
        eye = lax.broadcasted_iota(jnp.int32, square, 0) == lax.broadcasted_iota(jnp.int32, square, 1)
        cross_ref[...] = cross + jnp.where(eye, SHIFT, 0.0)
        lower_ref[...] = upper.T
        scale = math.sqrt(rows * length * peers)
        coef_ref[:, :width] = inverse * scale
        coef_ref[:, width:] = -dot(inverse, cross) * scale

    def last_body(w_ref, q_ref, coef_ref, out_ref):
        for n in range(rows):
            out_ref[n] = dot(coef_ref[...], jnp.concatenate([w_ref[n], q_ref[n]], axis=0))

    def apply_shifted(x):
        sent = call(
            send_body, [packet] * count, [SMEM] * (3 + count) + [VMEM] * 2, name="send"
        )(place, tile_rows, slot_counts, *asked, x, hess_tiles)
        got = [exchange(s, "res", entry["pairs"]) for s, entry in zip(sent, rounds)]
        (part,) = call(own_body, [full], [SMEM] * 3 + [VMEM] * 3, name="own")(
            place, tile_rows, tile_cols, x, diagonal, hess_tiles
        )
        keep, give = call(
            join_body,
            [halfshape] * 2,
            [SMEM] * (3 + count) + [VMEM] * (count + 2),
            [pltpu.VMEM(full, jnp.float32)],
            name="join",
        )(place, tile_rows, slot_counts, *asked, *got, hess_tiles, part)
        swap = [(i, i ^ 1) for i in range(lanes)]
        mine = keep + lax.ppermute(give, "vec", swap)
        step = 2
        while step < lanes:
            mine = mine + lax.ppermute(mine, "vec", [(i, i ^ step) for i in range(lanes)])
            step *= 2
        return mine, lax.ppermute(mine, "vec", swap)

    (start_gram,) = call(gram_body, [square], [VMEM], name="gram")(start_block)
    start_gram = all_sum(start_gram, "res")
    (start_inv,) = call(first_body, [square], [VMEM], name="first")(start_gram)

    mine, other = apply_shifted(start_block)
    y, gram = call(settle_body, [full, (width, 2 * width)], [SMEM] + [VMEM] * 3, name="settle")(
        place, mine, other, start_block
    )
    gram = all_sum(gram, "res")
    cross1, lower1, coef = call(
        second_body, [square, square, (width, 3 * width)], [VMEM] * 2, name="second"
    )(gram, start_inv)
    mine, other = apply_shifted(y)
    w, q, gram = call(
        third_body,
        [full, full, (width, 2 * width)],
        [SMEM] + [VMEM] * 5,
        [pltpu.VMEM(full, jnp.float32)],
        name="third",
    )(place, mine, other, start_block, y, coef)
    gram = all_sum(gram, "res")
    cross2, lower2, coef = call(
        fourth_body, [square, square, (width, 2 * width)], [VMEM], name="fourth"
    )(gram)
    (next_block,) = call(last_body, [full], [VMEM] * 3, name="last")(w, q, coef)
    return next_block, jnp.stack([cross1, lower1, cross2, lower2])


def solution(mesh):
    in_specs = (
        P(("conf", "res"), None, None),
        P(("conf", "res"), None),
        P(("conf", "res"), "vec", None, None, None),
        P(("conf", "res"), "vec", None),
        P(("conf", "res"), "vec", None),
        P(("conf", "res"), "vec", None),
    )
    out_specs = (P(("conf", "res"), None, None), P("conf", None, None))
    return jax.shard_map(local, mesh=mesh, in_specs=in_specs, out_specs=out_specs, check_vma=False)
```

```python
import math

import jax
import jax.numpy as jnp
from jax import lax
from jax.experimental import pallas as pl
from jax.experimental.pallas import tpu as pltpu
from jax.sharding import PartitionSpec as P

OWN_SLOTS = 20
HOPS = 3
CAP = 8
SHIFT = 1.65
BF16 = jnp.bfloat16
F32 = jnp.float32

VMEM = pl.BlockSpec(memory_space=pltpu.VMEM)
SMEM = pl.BlockSpec(memory_space=pltpu.SMEM)
ANY = pl.BlockSpec(memory_space=pl.ANY)


def contract(a, b, ta=False, tb=False, precision=None):
    dims = (((0 if ta else 1,), (1 if tb else 0,)), ((), ()))
    return lax.dot_general(a, b, dims, precision=precision, preferred_element_type=F32)


def dot(a, b, ta=False, tb=False):
    return contract(a, b, ta, tb, lax.Precision.HIGHEST)


def pieces(x, count):
    out = []
    for _ in range(count):
        out.append(x.astype(BF16))
        x = x - out[-1].astype(F32)
    return out


def tile_product(x, tile_ref, slot, transposed):
    x1, x2 = pieces(x, 2)
    m1, m2 = tile_ref[slot, 0], tile_ref[slot, 1]
    axis = 1 if transposed else 0
    left = jnp.concatenate([x1, x2, x1], axis=1)
    return contract(left, jnp.concatenate([m1, m1, m2], axis=axis), tb=transposed)


def wide_product(coef, blocks):
    c1, c2, c3 = pieces(coef, 3)
    z1, z2, z3 = pieces(jnp.concatenate(blocks, axis=1), 3)
    left = jnp.concatenate([c1, c1, c1, c2, c2, c3], axis=1)
    out = contract(left, jnp.concatenate([z1, z2, z3, z1, z2, z1], axis=0))
    width = blocks[0].shape[1]
    return [out[:, n * width : (n + 1) * width] for n in range(len(blocks))]


def gram_step(left, right):
    a = jnp.concatenate(pieces(jnp.concatenate(left, axis=1), 2), axis=0)
    b = jnp.concatenate(
        [p for group in right for p in pieces(jnp.concatenate(group, axis=1), 2)], axis=0
    )
    out = contract(a, b, tb=True)
    size = left[0].shape[0]
    out = out[:size] + out[size:]
    return jnp.concatenate(
        [
            out[:, 2 * g * size : (2 * g + 1) * size] + out[:, (2 * g + 1) * size : (2 * g + 2) * size]
            for g in range(len(right))
        ],
        axis=1,
    )


def call(body, outs, in_specs, scratch=(), name=None, aliases=None):
    shapes = [
        o if isinstance(o, jax.ShapeDtypeStruct) else jax.ShapeDtypeStruct(o, F32) for o in outs
    ]
    return pl.pallas_call(
        body,
        out_shape=shapes,
        in_specs=in_specs,
        out_specs=[VMEM] * len(outs),
        scratch_shapes=list(scratch),
        compiler_params=pltpu.CompilerParams(vmem_limit_bytes=40 << 20),
        input_output_aliases=aliases or {},
        name=name,
    )


def after(value, *tokens):
    return lax.optimization_barrier((value,) + tokens)[0]


def pairings(size):
    rounds = []
    for hop in range(1, HOPS + 1):
        for parity in range(2):
            pairs = [(i, i + hop) for i in range(size - hop) if (i // hop) % 2 == parity]
            if not pairs:
                continue
            used = {i for pair in pairs for i in pair}
            for entry in rounds:
                if not entry["used"] & used:
                    entry["used"] |= used
                    entry["pairs"] += pairs
                    entry["kinds"].append((hop, parity))
                    break
            else:
                rounds.append({"used": used, "pairs": pairs, "kinds": [(hop, parity)]})
    return rounds


def exchange(block, axis, pairs):
    return lax.ppermute(block, axis, [(a, b) for a, b in pairs] + [(b, a) for a, b in pairs])


def role_table(rounds, size):
    table = [[0] * size for _ in rounds]
    for p, entry in enumerate(rounds):
        for a, b in entry["pairs"]:
            table[p][a] = b - a
            table[p][b] = a - b
    return jnp.array(table, jnp.int32)


def all_sum(block, axis):
    size = lax.axis_size(axis)
    if size & (size - 1):
        return lax.psum(block, axis)
    step = 1
    while step < size:
        masks = [step] if step * 2 >= size else [step, 2 * step, 3 * step]
        got = [lax.ppermute(block, axis, [(i, i ^ mask) for i in range(size)]) for mask in masks]
        if len(got) == 1:
            block = block + got[0]
            step *= 2
        else:
            block = (block + got[0]) + (got[1] + got[2])
            step *= 4
    return block


def factor(gram):
    size = gram.shape[0]
    row_id = lax.broadcasted_iota(jnp.int32, (size, size), 0)
    col_id = lax.broadcasted_iota(jnp.int32, (size, size), 1)
    work = jnp.concatenate([gram, (row_id == col_id).astype(F32)], axis=1)
    blocks = [work[8 * b : 8 * b + 8] for b in range(size // 8)]
    sub = lax.broadcasted_iota(jnp.int32, (8, 2 * size), 0)
    for j in range(size):
        b, s = divmod(j, 8)
        row = blocks[b][s : s + 1]
        scaled = row / row[:, j : j + 1]
        scaled = jnp.broadcast_to(scaled, (8, 2 * size))
        for other in range(b, size // 8):
            col = jnp.broadcast_to(blocks[other][:, j : j + 1], (8, 2 * size))
            if other == b:
                col = jnp.where(sub > s, col, 0.0)
            blocks[other] = blocks[other] - col * scaled
    work = jnp.concatenate(blocks, axis=0)
    pivots = jnp.sum(jnp.where(row_id == col_id, work[:, :size], 0.0), axis=1, keepdims=True)
    work = work / jnp.sqrt(pivots)
    upper = jnp.where(col_id >= row_id, work[:, :size], 0.0)
    inverse = jnp.where(col_id <= row_id, work[:, size:], 0.0)
    return upper, inverse


def local(start_block, diagonal, hess_tiles, tile_rows, tile_cols, slot_counts):
    peers = lax.axis_size("res")
    lanes = lax.axis_size("vec")
    rows, width, length = start_block.shape
    slots = hess_tiles.shape[2]
    half = rows // 2
    part = width // 2
    rounds = pairings(peers)
    count = len(rounds)
    full = (rows, width, length)
    chunk = (rows, part, length)
    halfchunk = (half, part, length)
    packet = (CAP, part, length)
    square = (width, width)
    split_shape = jax.ShapeDtypeStruct((slots, 2, length, length), BF16)

    table = role_table(rounds, peers)
    place = jnp.concatenate(
        [lax.axis_index("vec").reshape(1), table[:, lax.axis_index("res")]]
    ).astype(jnp.int32)

    def own_sum(acc_refs, x_of, split_ref, rows_ref, cols_ref):
        for s in range(OWN_SLOTS):
            i, j = rows_ref[0, 0, s], cols_ref[0, 0, s]
            direct = tile_product(x_of(j), split_ref, s, True)
            mirror = tile_product(x_of(i), split_ref, s, False)
            for n, acc_ref in enumerate(acc_refs):
                acc_ref[i] += direct[n * part : (n + 1) * part]
                acc_ref[j] += mirror[n * part : (n + 1) * part]

    def prepare_body(place_ref, rows_ref, cols_ref, x_ref, diag_ref, tiles_ref, split_ref, a_ref, b_ref, raw_ref, sem):
        size = slots // 4
        copies = [
            pltpu.make_async_copy(
                tiles_ref.at[0, 0, pl.ds(n * size, size)], raw_ref.at[pl.ds(n * size, size)], sem.at[n]
            )
            for n in range(4)
        ]
        for c in copies:
            c.start()
        first = (place_ref[0] == 0).astype(F32)
        d = ((diag_ref[...] - SHIFT) * first)[:, None, :]
        a_ref[...] = x_ref[:, :part] * d
        b_ref[...] = x_ref[:, part:] * d
        for n in range(4):
            copies[n].wait()
            for s in range(n * size, (n + 1) * size):
                split_ref[s, 0], split_ref[s, 1] = pieces(raw_ref[s], 2)
        own_sum([a_ref, b_ref], lambda i: x_ref[i], split_ref, rows_ref, cols_ref)

    def own_body(place_ref, rows_ref, cols_ref, x_ref, diag_ref, split_ref, acc_ref):
        first = (place_ref[0] == 0).astype(F32)
        acc_ref[...] = x_ref[...] * ((diag_ref[...] - SHIFT) * first)[:, None, :]
        own_sum([acc_ref], lambda i: x_ref[i], split_ref, rows_ref, cols_ref)

    def pack(place_ref, rows_ref, counts_ref, asked_refs, x_ref, split_ref, outs):
        for p in range(count):
            role = place_ref[1 + p]

            def put(c, value, p=p):
                for n, ref in enumerate(outs[p]):
                    ref[c] = value[n * part : (n + 1) * part]

            @pl.when(role > 0)
            def _():
                base = OWN_SLOTS + (role - 1) * CAP
                for c in range(CAP):
                    term = tile_product(x_ref[rows_ref[0, 0, base + c]], split_ref, base + c, False)
                    put(c, jnp.where(c < counts_ref[0, 0, role - 1], term, 0.0))

            @pl.when(role < 0)
            def _():
                base = OWN_SLOTS + (-role - 1) * CAP
                for c in range(CAP):
                    put(c, x_ref[asked_refs[p][0, 0, base + c]])

    def send_body(place_ref, rows_ref, counts_ref, *refs):
        asked_refs, (x_ref, split_ref), outs = refs[:count], refs[count : count + 2], refs[count + 2 :]
        pack(
            place_ref, rows_ref, counts_ref, asked_refs, x_ref, split_ref,
            [(outs[p], outs[count + p]) for p in range(count)],
        )

    def settle(place_ref, mine_ref, other_ref, y_ref):
        core = place_ref[0] % 2
        y_ref[pl.ds(core * half, half)] = mine_ref[...]
        y_ref[pl.ds((1 - core) * half, half)] = other_ref[...]

    def resend_body(place_ref, rows_ref, counts_ref, *refs):
        asked_refs = refs[:count]
        mine_ref, other_ref, split_ref, y_ref = refs[count : count + 4]
        outs = refs[count + 4 :]
        settle(place_ref, mine_ref, other_ref, y_ref)
        pack(
            place_ref, rows_ref, counts_ref, asked_refs, y_ref, split_ref,
            [(outs[p],) for p in range(count)],
        )

    def join_body(place_ref, rows_ref, counts_ref, *refs):
        asked_refs, got_refs = refs[:count], refs[count : 2 * count]
        split_ref, part_ref, keep_ref, give_ref, acc_ref = refs[2 * count :]
        acc_ref[...] = part_ref[...]
        for p in range(count):
            role = place_ref[1 + p]

            @pl.when(role > 0)
            def _():
                base = OWN_SLOTS + (role - 1) * CAP
                for c in range(CAP):
                    term = tile_product(got_refs[p][c], split_ref, base + c, True)
                    acc_ref[rows_ref[0, 0, base + c]] += jnp.where(
                        c < counts_ref[0, 0, role - 1], term, 0.0
                    )

            @pl.when(role < 0)
            def _():
                base = OWN_SLOTS + (-role - 1) * CAP
                for c in range(CAP):
                    acc_ref[asked_refs[p][0, 0, base + c]] += got_refs[p][c]

        core = place_ref[0] % 2
        keep_ref[...] = acc_ref[pl.ds(core * half, half)]
        give_ref[...] = acc_ref[pl.ds((1 - core) * half, half)]

    def gram_body(x_ref, out_ref):
        total = jnp.zeros(square, F32)
        for n in range(0, rows, 2):
            pair = [x_ref[n], x_ref[n + 1]]
            total += gram_step(pair, [pair])
        out_ref[...] = total

    def cross_body(x_ref, a_ref, b_ref, out_ref):
        total = jnp.zeros((width, 2 * width), F32)
        for n in range(0, rows, 2):
            y = [jnp.concatenate([a_ref[m], b_ref[m]], axis=0) for m in (n, n + 1)]
            total += gram_step(y, [[x_ref[n], x_ref[n + 1]], y])
        out_ref[...] = total

    def first_body(gram_ref, inverse_ref):
        _, inverse_ref[...] = factor(gram_ref[...])

    def identity():
        eye = lax.broadcasted_iota(jnp.int32, square, 0) == lax.broadcasted_iota(jnp.int32, square, 1)
        return eye.astype(F32)

    def second_body(gram_ref, inverse_ref, cross_ref, lower_ref, coef_ref, gain_ref):
        start_inv = inverse_ref[...]
        cross = dot(dot(start_inv, gram_ref[:, :width]), start_inv, tb=True)
        applied = dot(dot(start_inv, gram_ref[:, width:]), start_inv, tb=True)
        upper, inverse = factor(applied - dot(cross, cross, tb=True))
        lower = upper.T
        cross_ref[...] = cross + SHIFT * identity()
        lower_ref[...] = lower
        gain = dot(inverse, start_inv)
        back = -dot(dot(inverse, cross), start_inv)
        gain_ref[...] = gain
        coef_ref[:width, :width] = -dot(lower, start_inv)
        coef_ref[:width, width:] = back
        coef_ref[width:, :width] = back
        coef_ref[width:, width:] = gain

    def blend_body(x_ref, a_ref, b_ref, coef_ref, w_ref, q_ref, out_ref):
        total = jnp.zeros(square, F32)
        for n in range(0, rows, 2):
            qs = []
            stacks = [
                jnp.concatenate([x_ref[m], a_ref[m], b_ref[m]], axis=0) for m in (n, n + 1)
            ]
            for m, both in zip((n, n + 1), wide_product(coef_ref[...], stacks)):
                w_ref[m] = both[:width]
                q_ref[m] = both[width:]
                qs.append(both[width:])
            total += gram_step(qs, [qs])
        out_ref[...] = total

    def third_body(place_ref, *refs):
        mine_refs, other_refs = refs[0:2], refs[2:4]
        prior_ref, q_ref, gain_ref, norm_ref, w_ref, out_ref = refs[4:10]
        z_refs = refs[10:12]
        for n in range(2):
            settle(place_ref, mine_refs[n], other_refs[n], z_refs[n])
        total = jnp.zeros((width, 2 * width), F32)
        for n in range(0, rows, 2):
            zs = [jnp.concatenate([z_refs[0][m], z_refs[1][m]], axis=0) for m in (n, n + 1)]
            ws = []
            for m, w in zip((n, n + 1), wide_product(gain_ref[...], zs)):
                w = w + prior_ref[m]
                w_ref[m] = w
                ws.append(w)
            total += gram_step(ws, [[q_ref[n], q_ref[n + 1]], ws])
        out_ref[:, : 2 * width] = total
        out_ref[:, 2 * width : 3 * width] = norm_ref[...]
        out_ref[:, 3 * width :] = jnp.zeros(square, F32)

    def fourth_body(gram_ref, cross_ref, lower_ref, coef_ref):
        cross = gram_ref[:, :width]
        norm = gram_ref[:, 2 * width : 3 * width]
        taken = cross + SHIFT * (norm - identity())
        mixed = dot(taken, cross, tb=True)
        squared = gram_ref[:, width : 2 * width] - mixed - mixed.T + dot(dot(taken, norm), taken, tb=True)
        upper, inverse = factor(squared)
        cross_ref[...] = taken + SHIFT * identity()
        lower_ref[...] = upper.T
        scale = math.sqrt(rows * length * peers)
        coef_ref[:, :width] = inverse * scale
        coef_ref[:, width:] = -dot(inverse, taken) * scale

    def last_body(w_ref, q_ref, coef_ref, a1_ref, l1_ref, a2_ref, l2_ref, out_ref, pack_ref):
        for n, ref in enumerate((a1_ref, l1_ref, a2_ref, l2_ref)):
            pack_ref[n] = ref[...]
        for n in range(0, rows, 2):
            stacks = [jnp.concatenate([w_ref[m], q_ref[m]], axis=0) for m in (n, n + 1)]
            for m, out in zip((n, n + 1), wide_product(coef_ref[...], stacks)):
                out_ref[m] = out

    swap = [(i, i ^ 1) for i in range(lanes)]

    def spread(sent):
        return [exchange(s, "res", entry["pairs"]) for s, entry in zip(sent, rounds)]

    def join(got, prior, token):
        return call(
            join_body,
            [halfchunk] * 2,
            [SMEM] * (3 + count) + [VMEM] * (count + 2),
            [pltpu.VMEM(chunk, F32)],
            name="join",
        )(place, tile_rows, slot_counts, *asked, *got, split, after(prior, token))

    def vec_sum(keep, give, token=None):
        mine = keep + lax.ppermute(give, "vec", swap)
        step = 2
        while step < lanes:
            got = lax.ppermute(mine, "vec", [(i, i ^ step) for i in range(lanes)])
            if token is not None:
                got = after(got, token)
            mine = mine + got
            step *= 2
        return mine, lax.ppermute(mine, "vec", swap)

    def resend(mine, other, token):
        y, *sent = call(
            resend_body, [chunk] + [packet] * count, [SMEM] * (3 + count) + [VMEM] * 3, name="resend"
        )(place, tile_rows, slot_counts, *asked, mine, after(other, token), split)
        return y, sent

    def own(y, token):
        (acc,) = call(own_body, [chunk], [SMEM] * 3 + [VMEM] * 3, name="own")(
            place, tile_rows, tile_cols, after(y, token), diagonal, split
        )
        return acc

    asked = [exchange(tile_cols, "res", entry["pairs"]) for entry in rounds]
    split, prior_a, prior_b = call(
        prepare_body,
        [split_shape, chunk, chunk],
        [SMEM] * 3 + [VMEM] * 2 + [ANY],
        [pltpu.VMEM((slots, length, length), F32), pltpu.SemaphoreType.DMA((4,))],
        name="prepare",
    )(place, tile_rows, tile_cols, start_block, diagonal, hess_tiles)
    sent = call(
        send_body, [packet] * (2 * count), [SMEM] * (3 + count) + [VMEM] * 2, name="send"
    )(place, tile_rows, slot_counts, *asked, start_block, split)
    got_a = spread(sent[:count])
    got_b = spread(sent[count:])
    (start_gram,) = call(gram_body, [square], [VMEM], name="gram")(after(start_block, sent[0]))
    start_total = all_sum(start_gram, "res")
    keep, give = join(got_a, prior_a, start_gram)
    (start_inv,) = call(first_body, [square], [VMEM], name="first")(after(start_total, keep))
    mine, other = vec_sum(keep, give, start_inv)
    y_a, sent = resend(mine, other, start_inv)
    got_a = spread(sent)
    keep, give = join(got_b, prior_b, y_a)
    prior_a = own(y_a, keep)
    mine, other = vec_sum(keep, give, prior_a)
    y_b, sent = resend(mine, other, prior_a)
    got_b = spread(sent)
    (cross_gram,) = call(cross_body, [(width, 2 * width)], [VMEM] * 3, name="cross")(
        start_block, y_a, y_b
    )
    cross_total = all_sum(cross_gram, "res")
    prior_b = own(y_b, cross_gram)
    cross1, lower1, coef, gain = call(
        second_body, [square, square, (2 * width, 2 * width), square], [VMEM] * 2, name="second"
    )(after(cross_total, prior_b), start_inv)
    w_prior, q, norm = call(blend_body, [full, full, square], [VMEM] * 4, name="blend")(
        start_block, y_a, y_b, coef
    )
    keep_a, give_a = join(got_a, prior_a, norm)
    mine_a, other_a = vec_sum(keep_a, give_a)
    keep_b, give_b = join(got_b, prior_b, keep_a)
    mine_b, other_b = vec_sum(keep_b, give_b)
    w, gram = call(
        third_body,
        [full, (width, 4 * width)],
        [SMEM] + [VMEM] * 8,
        [pltpu.VMEM(chunk, F32)] * 2,
        name="third",
    )(place, mine_a, mine_b, other_a, other_b, w_prior, q, gain, norm)
    gram = all_sum(gram, "res")
    cross2, lower2, coef = call(
        fourth_body, [square, square, (width, 2 * width)], [VMEM], name="fourth"
    )(gram)
    return call(last_body, [full, (4, width, width)], [VMEM] * 7, name="last")(
        w, q, coef, cross1, lower1, cross2, lower2
    )


def solution(mesh):
    in_specs = (
        P(("conf", "res"), None, None),
        P(("conf", "res"), None),
        P(("conf", "res"), "vec", None, None, None),
        P(("conf", "res"), "vec", None),
        P(("conf", "res"), "vec", None),
        P(("conf", "res"), "vec", None),
    )
    out_specs = (P(("conf", "res"), None, None), P("conf", None, None))
    return jax.shard_map(local, mesh=mesh, in_specs=in_specs, out_specs=out_specs, check_vma=False)
```

```python
import math

import jax
import jax.numpy as jnp
from jax import lax
from jax.experimental import pallas as pl
from jax.experimental.pallas import tpu as pltpu
from jax.sharding import PartitionSpec as P

OWN_SLOTS = 20
HOPS = 3
CAP = 8
SHIFT = 1.65
BF16 = jnp.bfloat16
F32 = jnp.float32

VMEM = pl.BlockSpec(memory_space=pltpu.VMEM)
SMEM = pl.BlockSpec(memory_space=pltpu.SMEM)
HBM = pl.BlockSpec(memory_space=pltpu.HBM)


def contract(a, b, ta=False, tb=False, precision=None):
    dims = (((0 if ta else 1,), (1 if tb else 0,)), ((), ()))
    return lax.dot_general(a, b, dims, precision=precision, preferred_element_type=F32)


def dot(a, b, ta=False, tb=False):
    return contract(a, b, ta, tb, lax.Precision.HIGHEST)


def pieces(x, count):
    out = []
    for _ in range(count):
        out.append(x.astype(BF16))
        x = x - out[-1].astype(F32)
    return out


def tile_product(x, tile_ref, slot, transposed):
    x1, x2 = pieces(x, 2)
    m1, m2 = tile_ref[slot, 0], tile_ref[slot, 1]
    axis = 1 if transposed else 0
    left = jnp.concatenate([x1, x2, x1], axis=1)
    return contract(left, jnp.concatenate([m1, m1, m2], axis=axis), tb=transposed)


def wide_product(coef, blocks):
    c1, c2, c3 = pieces(coef, 3)
    z1, z2, z3 = pieces(jnp.concatenate(blocks, axis=1), 3)
    left = jnp.concatenate([c1, c1, c1, c2, c2, c3], axis=1)
    out = contract(left, jnp.concatenate([z1, z2, z3, z1, z2, z1], axis=0))
    width = blocks[0].shape[1]
    return [out[:, n * width : (n + 1) * width] for n in range(len(blocks))]


def gram_step(left, right):
    a = jnp.concatenate(pieces(jnp.concatenate(left, axis=1), 2), axis=0)
    b = jnp.concatenate(
        [p for group in right for p in pieces(jnp.concatenate(group, axis=1), 2)], axis=0
    )
    out = contract(a, b, tb=True)
    size = left[0].shape[0]
    out = out[:size] + out[size:]
    return jnp.concatenate(
        [
            out[:, 2 * g * size : (2 * g + 1) * size] + out[:, (2 * g + 1) * size : (2 * g + 2) * size]
            for g in range(len(right))
        ],
        axis=1,
    )


def call(body, outs, in_specs, scratch=(), name=None, aliases=None):
    shapes = [
        o if isinstance(o, jax.ShapeDtypeStruct) else jax.ShapeDtypeStruct(o, F32) for o in outs
    ]
    return pl.pallas_call(
        body,
        out_shape=shapes,
        in_specs=in_specs,
        out_specs=[VMEM] * len(outs),
        scratch_shapes=list(scratch),
        compiler_params=pltpu.CompilerParams(vmem_limit_bytes=40 << 20),
        input_output_aliases=aliases or {},
        name=name,
    )


def after(value, *tokens):
    return lax.optimization_barrier((value,) + tokens)[0]


def pairings(size):
    rounds = []
    for hop in range(1, HOPS + 1):
        for parity in range(2):
            pairs = [(i, i + hop) for i in range(size - hop) if (i // hop) % 2 == parity]
            if not pairs:
                continue
            used = {i for pair in pairs for i in pair}
            for entry in rounds:
                if not entry["used"] & used:
                    entry["used"] |= used
                    entry["pairs"] += pairs
                    entry["kinds"].append((hop, parity))
                    break
            else:
                rounds.append({"used": used, "pairs": pairs, "kinds": [(hop, parity)]})
    return rounds


def exchange(block, axis, pairs):
    return lax.ppermute(block, axis, [(a, b) for a, b in pairs] + [(b, a) for a, b in pairs])


def role_table(rounds, size):
    table = [[0] * size for _ in rounds]
    for p, entry in enumerate(rounds):
        for a, b in entry["pairs"]:
            table[p][a] = b - a
            table[p][b] = a - b
    return jnp.array(table, jnp.int32)


def all_sum(block, axis):
    size = lax.axis_size(axis)
    if size & (size - 1):
        return lax.psum(block, axis)
    step = 1
    while step < size:
        block = block + lax.ppermute(block, axis, [(i, i ^ step) for i in range(size)])
        step *= 2
    return block


def factor(gram):
    size = gram.shape[0]
    row_id = lax.broadcasted_iota(jnp.int32, (size, size), 0)
    col_id = lax.broadcasted_iota(jnp.int32, (size, size), 1)
    work = jnp.concatenate([gram, (row_id == col_id).astype(F32)], axis=1)
    blocks = [work[8 * b : 8 * b + 8] for b in range(size // 8)]
    sub = lax.broadcasted_iota(jnp.int32, (8, 2 * size), 0)
    for j in range(size):
        b, s = divmod(j, 8)
        row = blocks[b][s : s + 1]
        scaled = row / row[:, j : j + 1]
        scaled = jnp.broadcast_to(scaled, (8, 2 * size))
        for other in range(b, size // 8):
            col = jnp.broadcast_to(blocks[other][:, j : j + 1], (8, 2 * size))
            if other == b:
                col = jnp.where(sub > s, col, 0.0)
            blocks[other] = blocks[other] - col * scaled
    work = jnp.concatenate(blocks, axis=0)
    pivots = jnp.sum(jnp.where(row_id == col_id, work[:, :size], 0.0), axis=1, keepdims=True)
    work = work / jnp.sqrt(pivots)
    upper = jnp.where(col_id >= row_id, work[:, :size], 0.0)
    inverse = jnp.where(col_id <= row_id, work[:, size:], 0.0)
    return upper, inverse


def local(start_block, diagonal, hess_tiles, tile_rows, tile_cols, slot_counts):
    peers = lax.axis_size("res")
    lanes = lax.axis_size("vec")
    rows, width, length = start_block.shape
    slots = hess_tiles.shape[2]
    half = rows // 2
    part = width // 2
    rounds = pairings(peers)
    count = len(rounds)
    full = (rows, width, length)
    chunk = (rows, part, length)
    halfchunk = (half, part, length)
    packet = (CAP, part, length)
    square = (width, width)
    split_shape = jax.ShapeDtypeStruct((slots, 2, length, length), BF16)

    table = role_table(rounds, peers)
    place = jnp.concatenate(
        [lax.axis_index("vec").reshape(1), table[:, lax.axis_index("res")]]
    ).astype(jnp.int32)

    def own_sum(acc_refs, x_ref, split_ref, rows_ref, cols_ref):
        for s in range(OWN_SLOTS):
            i, j = rows_ref[0, 0, s], cols_ref[0, 0, s]
            direct = tile_product(x_ref[j], split_ref, s, True)
            mirror = tile_product(x_ref[i], split_ref, s, False)
            for n, acc_ref in enumerate(acc_refs):
                acc_ref[i] += direct[n * part : (n + 1) * part]
                acc_ref[j] += mirror[n * part : (n + 1) * part]

    def prepare_body(rows_hbm, cols_hbm, x_hbm, diag_hbm, tiles_hbm, *refs):
        x_ref, split_ref, a_ref, b_ref, rows_ref, cols_ref, diag_ref, raw_ref, sem = refs
        size = slots // 4
        copies = [
            pltpu.make_async_copy(src, dst, sem.at[n])
            for n, (src, dst) in enumerate(
                [(x_hbm, x_ref), (diag_hbm, diag_ref), (rows_hbm, rows_ref), (cols_hbm, cols_ref)]
            )
        ]
        tile_copies = [
            pltpu.make_async_copy(
                tiles_hbm.at[0, 0, pl.ds(n * size, size)], raw_ref.at[pl.ds(n * size, size)], sem.at[4 + n]
            )
            for n in range(4)
        ]
        for c in copies + tile_copies:
            c.start()
        for n in range(4):
            tile_copies[n].wait()
            for s in range(n * size, (n + 1) * size):
                split_ref[s, 0], split_ref[s, 1] = pieces(raw_ref[s], 2)
        for c in copies:
            c.wait()
        first = (lax.axis_index("vec") == 0).astype(F32)
        d = ((diag_ref[...] - SHIFT) * first)[:, None, :]
        a_ref[...] = x_ref[:, :part] * d
        b_ref[...] = x_ref[:, part:] * d
        own_sum([a_ref, b_ref], x_ref, split_ref, rows_ref, cols_ref)

    def own_body(rows_ref, cols_ref, x_ref, split_ref, prior_ref, acc_ref):
        own_sum([acc_ref], x_ref, split_ref, rows_ref, cols_ref)

    def pack(place_ref, rows_ref, counts_ref, asked_refs, x_ref, split_ref, outs):
        for p in range(count):
            role = place_ref[1 + p]

            def put(c, value, p=p):
                for n, ref in enumerate(outs[p]):
                    ref[c] = value[n * part : (n + 1) * part]

            @pl.when(role > 0)
            def _():
                base = OWN_SLOTS + (role - 1) * CAP
                for c in range(CAP):
                    term = tile_product(x_ref[rows_ref[0, 0, base + c]], split_ref, base + c, False)
                    put(c, jnp.where(c < counts_ref[0, 0, role - 1], term, 0.0))

            @pl.when(role < 0)
            def _():
                base = OWN_SLOTS + (-role - 1) * CAP
                for c in range(CAP):
                    put(c, x_ref[asked_refs[p][0, 0, base + c]])

    def send_body(place_ref, rows_ref, counts_ref, *refs):
        asked_refs, (x_ref, split_ref), outs = refs[:count], refs[count : count + 2], refs[count + 2 :]
        pack(
            place_ref, rows_ref, counts_ref, asked_refs, x_ref, split_ref,
            [(outs[p], outs[count + p]) for p in range(count)],
        )

    def settle(place_ref, mine_ref, other_ref, y_ref):
        core = place_ref[0] % 2
        y_ref[pl.ds(core * half, half)] = mine_ref[...]
        y_ref[pl.ds((1 - core) * half, half)] = other_ref[...]

    def resend_body(place_ref, rows_ref, counts_ref, *refs):
        asked_refs = refs[:count]
        mine_ref, other_ref, diag_ref, split_ref, y_ref, acc_ref = refs[count : count + 6]
        outs = refs[count + 6 :]
        settle(place_ref, mine_ref, other_ref, y_ref)
        pack(
            place_ref, rows_ref, counts_ref, asked_refs, y_ref, split_ref,
            [(outs[p],) for p in range(count)],
        )
        first = (place_ref[0] == 0).astype(F32)
        acc_ref[...] = y_ref[...] * ((diag_ref[...] - SHIFT) * first)[:, None, :]

    def join_rounds(members, place_ref, rows_ref, counts_ref, asked_refs, got_refs, split_ref, acc_ref):
        for n, p in enumerate(members):
            role = place_ref[1 + p]

            @pl.when(role > 0)
            def _():
                base = OWN_SLOTS + (role - 1) * CAP
                for c in range(CAP):
                    term = tile_product(got_refs[n][c], split_ref, base + c, True)
                    acc_ref[rows_ref[0, 0, base + c]] += jnp.where(
                        c < counts_ref[0, 0, role - 1], term, 0.0
                    )

            @pl.when(role < 0)
            def _():
                base = OWN_SLOTS + (-role - 1) * CAP
                for c in range(CAP):
                    acc_ref[asked_refs[n][0, 0, base + c]] += got_refs[n][c]

    def join(acc, got, members, last=False):
        size = len(members)

        def body(place_ref, rows_ref, counts_ref, *refs):
            asked_refs, got_refs = refs[:size], refs[size : 2 * size]
            split_ref, prior_ref = refs[2 * size : 2 * size + 2]
            outs = refs[2 * size + 2 :]
            if last:
                keep_ref, give_ref, acc_ref = outs
                acc_ref[...] = prior_ref[...]
            else:
                (acc_ref,) = outs
            join_rounds(
                members, place_ref, rows_ref, counts_ref, asked_refs, got_refs, split_ref, acc_ref
            )
            if last:
                core = place_ref[0] % 2
                keep_ref[...] = acc_ref[pl.ds(core * half, half)]
                give_ref[...] = acc_ref[pl.ds((1 - core) * half, half)]

        out = call(
            body,
            [halfchunk] * 2 if last else [chunk],
            [SMEM] * (3 + size) + [VMEM] * (size + 2),
            [pltpu.VMEM(chunk, F32)] if last else [],
            name="join",
            aliases=None if last else {3 + 2 * size + 1: 0},
        )(
            place, tile_rows, slot_counts, *[asked[p] for p in members], *[got[p] for p in members], split, acc
        )
        return out if last else out[0]

    def gram_body(x_ref, out_ref):
        total = jnp.zeros(square, F32)
        for n in range(0, rows, 2):
            pair = [x_ref[n], x_ref[n + 1]]
            total += gram_step(pair, [pair])
        out_ref[...] = total

    def cross_body(x_ref, a_ref, b_ref, out_ref):
        total = jnp.zeros((width, 2 * width), F32)
        for n in range(0, rows, 2):
            y = [jnp.concatenate([a_ref[m], b_ref[m]], axis=0) for m in (n, n + 1)]
            total += gram_step(y, [[x_ref[n], x_ref[n + 1]], y])
        out_ref[...] = total

    def first_body(gram_ref, inverse_ref):
        _, inverse_ref[...] = factor(gram_ref[...])

    def identity():
        eye = lax.broadcasted_iota(jnp.int32, square, 0) == lax.broadcasted_iota(jnp.int32, square, 1)
        return eye.astype(F32)

    def second_body(gram_ref, inverse_ref, cross_ref, lower_ref, coef_ref, gain_ref):
        start_inv = inverse_ref[...]
        cross = dot(dot(start_inv, gram_ref[:, :width]), start_inv, tb=True)
        applied = dot(dot(start_inv, gram_ref[:, width:]), start_inv, tb=True)
        upper, inverse = factor(applied - dot(cross, cross, tb=True))
        lower = upper.T
        cross_ref[...] = cross + SHIFT * identity()
        lower_ref[...] = lower
        gain = dot(inverse, start_inv)
        back = -dot(dot(inverse, cross), start_inv)
        gain_ref[...] = gain
        coef_ref[:width, :width] = -dot(lower, start_inv)
        coef_ref[:width, width : 2 * width] = back
        coef_ref[:width, 2 * width :] = gain
        coef_ref[width:, :width] = back
        coef_ref[width:, width : 2 * width] = gain
        coef_ref[width:, 2 * width :] = jnp.zeros(square, F32)

    def blend_body(place_ref, x_ref, a_ref, b_ref, mine_ref, other_ref, coef_ref, w_ref, q_ref, out_ref, z_ref):
        settle(place_ref, mine_ref, other_ref, z_ref)
        total = jnp.zeros(square, F32)
        for n in range(0, rows, 2):
            qs = []
            stacks = [
                jnp.concatenate([x_ref[m], a_ref[m], b_ref[m], z_ref[m]], axis=0) for m in (n, n + 1)
            ]
            for m, both in zip((n, n + 1), wide_product(coef_ref[:, : 2 * width + part], stacks)):
                w_ref[m] = both[:width]
                q_ref[m] = both[width:]
                qs.append(both[width:])
            total += gram_step(qs, [qs])
        out_ref[...] = total

    def third_body(place_ref, mine_ref, other_ref, prior_ref, q_ref, gain_ref, w_ref, out_ref, z_ref):
        settle(place_ref, mine_ref, other_ref, z_ref)
        total = jnp.zeros((width, 2 * width), F32)
        for n in range(0, rows, 2):
            ws = []
            for m, w in zip((n, n + 1), wide_product(gain_ref[:, part:], [z_ref[n], z_ref[n + 1]])):
                w = w + prior_ref[m]
                w_ref[m] = w
                ws.append(w)
            total += gram_step(ws, [[q_ref[n], q_ref[n + 1]], ws])
        out_ref[...] = total

    def fourth_body(gram_ref, norm_ref, cross_ref, lower_ref, coef_ref):
        cross = gram_ref[:, :width]
        norm = norm_ref[...]
        taken = cross + SHIFT * (norm - identity())
        mixed = dot(taken, cross, tb=True)
        squared = gram_ref[:, width:] - mixed - mixed.T + dot(dot(taken, norm), taken, tb=True)
        upper, inverse = factor(squared)
        cross_ref[...] = taken + SHIFT * identity()
        lower_ref[...] = upper.T
        scale = math.sqrt(rows * length * peers)
        coef_ref[:, :width] = inverse * scale
        coef_ref[:, width:] = -dot(inverse, taken) * scale

    def last_body(w_ref, q_ref, coef_ref, a1_ref, l1_ref, a2_ref, l2_ref, out_ref, pack_ref):
        for n, ref in enumerate((a1_ref, l1_ref, a2_ref, l2_ref)):
            pack_ref[n] = ref[...]
        for n in range(0, rows, 2):
            stacks = [jnp.concatenate([w_ref[m], q_ref[m]], axis=0) for m in (n, n + 1)]
            for m, out in zip((n, n + 1), wide_product(coef_ref[...], stacks)):
                out_ref[m] = out

    swap = [(i, i ^ 1) for i in range(lanes)]
    cuts = [count * n // 3 for n in range(4)]
    groups = [list(range(cuts[n], cuts[n + 1])) for n in range(3)]

    def spread(sent):
        return [exchange(s, "res", entry["pairs"]) for s, entry in zip(sent, rounds)]

    def across(mine, *tokens):
        step = 2
        while step < lanes:
            got = lax.ppermute(mine, "vec", [(i, i ^ step) for i in range(lanes)])
            mine = mine + after(got, *tokens)
            step *= 2
        return mine

    def resend(mine, other):
        y, acc, *sent = call(
            resend_body,
            [chunk, chunk] + [packet] * count,
            [SMEM] * (3 + count) + [VMEM] * 4,
            name="resend",
        )(place, tile_rows, slot_counts, *asked, mine, other, diagonal, split)
        return y, acc, spread(sent)

    def own(acc, y):
        return call(own_body, [chunk], [SMEM] * 2 + [VMEM] * 3, name="own", aliases={4: 0})(
            tile_rows, tile_cols, y, split, acc
        )[0]

    asked = [exchange(tile_cols, "res", entry["pairs"]) for entry in rounds]
    x, split, acc_a, acc_b = call(
        prepare_body,
        [full, split_shape, chunk, chunk],
        [HBM] * 5,
        [
            pltpu.SMEM(tile_rows.shape, jnp.int32),
            pltpu.SMEM(tile_cols.shape, jnp.int32),
            pltpu.VMEM(diagonal.shape, F32),
            pltpu.VMEM((slots, length, length), F32),
            pltpu.SemaphoreType.DMA((8,)),
        ],
        name="prepare",
    )(tile_rows, tile_cols, start_block, diagonal, hess_tiles)
    sent = call(
        send_body, [packet] * (2 * count), [SMEM] * (3 + count) + [VMEM] * 2, name="send"
    )(place, tile_rows, slot_counts, *asked, x, split)
    got_a = spread(sent[:count])
    got_b = spread(sent[count:])
    (gram,) = call(gram_body, [square], [VMEM], name="gram")(after(x, sent[0]))
    start_gram = all_sum(gram, "res")
    for n in range(2):
        acc_a = join(after(acc_a, gram), got_a, groups[n])
    keep_a, give_a = join(acc_a, got_a, groups[2], last=True)

    core = lax.ppermute(give_a, "vec", swap)
    acc_b = join(acc_b, got_b, groups[0])
    mine_a = keep_a + after(core, acc_b)
    (start_inv,) = call(first_body, [square], [VMEM], name="first")(after(start_gram, mine_a))
    acc_b = join(after(acc_b, start_inv), got_b, groups[1])
    mine_a = across(mine_a, acc_b)
    other_a = lax.ppermute(mine_a, "vec", swap)
    keep_b, give_b = join(acc_b, got_b, groups[2], last=True)
    y_a, acc_a, got_a = resend(mine_a, after(other_a, keep_b))

    core = lax.ppermute(give_b, "vec", swap)
    acc_a = join(acc_a, got_a, groups[0])
    mine_b = keep_b + after(core, acc_a)
    acc_a = own(after(acc_a, mine_b), y_a)
    acc_a = join(acc_a, got_a, groups[1])
    mine_b = across(mine_b, acc_a)
    other_b = lax.ppermute(mine_b, "vec", swap)
    keep_a, give_a = join(acc_a, got_a, groups[2], last=True)
    y_b, acc_b, got_b = resend(mine_b, after(other_b, keep_a))

    (gram,) = call(cross_body, [(width, 2 * width)], [VMEM] * 3, name="cross")(x, y_a, y_b)
    core = lax.ppermute(give_a, "vec", swap)
    acc_b = own(after(acc_b, gram), y_b)
    acc_b = join(acc_b, got_b, groups[0])
    mine_a = keep_a + after(core, acc_b)
    cross_gram = all_sum(gram, "res")
    cross1, lower1, coef, gain = call(
        second_body, [square, square, (2 * width, 3 * width), square], [VMEM] * 2, name="second"
    )(after(cross_gram, mine_a), start_inv)
    acc_b = join(after(acc_b, gain), got_b, groups[1])
    mine_a = across(mine_a, acc_b)
    other_a = lax.ppermute(mine_a, "vec", swap)
    keep_b, give_b = join(acc_b, got_b, groups[2], last=True)

    core = lax.ppermute(give_b, "vec", swap)
    mine_b = keep_b + core
    w_prior, q, norm = call(
        blend_body,
        [full, full, square],
        [SMEM] + [VMEM] * 6,
        [pltpu.VMEM(chunk, F32)],
        name="blend",
    )(place, x, y_a, y_b, mine_a, other_a, after(coef, mine_b))
    mine_b = across(mine_b, norm)
    other_b = lax.ppermute(mine_b, "vec", swap)
    w, gram = call(
        third_body,
        [full, (width, 2 * width)],
        [SMEM] + [VMEM] * 5,
        [pltpu.VMEM(chunk, F32)],
        name="third",
    )(place, mine_b, other_b, w_prior, q, gain)
    norm = all_sum(norm, "res")
    gram = all_sum(gram, "res")
    cross2, lower2, coef = call(
        fourth_body, [square, square, (width, 2 * width)], [VMEM] * 2, name="fourth"
    )(gram, norm)
    return call(last_body, [full, (4, width, width)], [VMEM] * 7, name="last")(
        w, q, coef, cross1, lower1, cross2, lower2
    )


def solution(mesh):
    in_specs = (
        P(("conf", "res"), None, None),
        P(("conf", "res"), None),
        P(("conf", "res"), "vec", None, None, None),
        P(("conf", "res"), "vec", None),
        P(("conf", "res"), "vec", None),
        P(("conf", "res"), "vec", None),
    )
    out_specs = (P(("conf", "res"), None, None), P("conf", None, None))
    return jax.shard_map(local, mesh=mesh, in_specs=in_specs, out_specs=out_specs, check_vma=False)
```

```python
import math

import jax
import jax.numpy as jnp
from jax import lax
from jax.experimental import pallas as pl
from jax.experimental.pallas import tpu as pltpu
from jax.sharding import PartitionSpec as P

OWN_SLOTS = 20
HOPS = 3
CAP = 8
SHIFT = 1.65
BF16 = jnp.bfloat16
F32 = jnp.float32

VMEM = pl.BlockSpec(memory_space=pltpu.VMEM)
SMEM = pl.BlockSpec(memory_space=pltpu.SMEM)
HBM = pl.BlockSpec(memory_space=pltpu.HBM)


def contract(a, b, ta=False, tb=False, precision=None):
    dims = (((0 if ta else 1,), (1 if tb else 0,)), ((), ()))
    return lax.dot_general(a, b, dims, precision=precision, preferred_element_type=F32)


def dot(a, b, ta=False, tb=False):
    return contract(a, b, ta, tb, lax.Precision.HIGHEST)


def pieces(x, count):
    out = []
    for _ in range(count):
        out.append(x.astype(BF16))
        x = x - out[-1].astype(F32)
    return out


def tile_product(x, tile_ref, slot, transposed):
    x1, x2 = pieces(x, 2)
    m1, m2 = tile_ref[slot, 0], tile_ref[slot, 1]
    axis = 1 if transposed else 0
    left = jnp.concatenate([x1, x2, x1], axis=1)
    return contract(left, jnp.concatenate([m1, m1, m2], axis=axis), tb=transposed)


def wide_product(coef, blocks):
    c1, c2, c3 = pieces(coef, 3)
    z1, z2, z3 = pieces(jnp.concatenate(blocks, axis=1), 3)
    left = jnp.concatenate([c1, c1, c1, c2, c2, c3], axis=1)
    out = contract(left, jnp.concatenate([z1, z2, z3, z1, z2, z1], axis=0))
    width = blocks[0].shape[1]
    return [out[:, n * width : (n + 1) * width] for n in range(len(blocks))]


def gram_step(left, right):
    a = jnp.concatenate(pieces(jnp.concatenate(left, axis=1), 2), axis=0)
    b = jnp.concatenate(
        [p for group in right for p in pieces(jnp.concatenate(group, axis=1), 2)], axis=0
    )
    out = contract(a, b, tb=True)
    size = left[0].shape[0]
    out = out[:size] + out[size:]
    return jnp.concatenate(
        [
            out[:, 2 * g * size : (2 * g + 1) * size] + out[:, (2 * g + 1) * size : (2 * g + 2) * size]
            for g in range(len(right))
        ],
        axis=1,
    )


def call(body, outs, in_specs, scratch=(), name=None, aliases=None, weight=0):
    shapes = [
        o if isinstance(o, jax.ShapeDtypeStruct) else jax.ShapeDtypeStruct(o, F32) for o in outs
    ]
    return pl.pallas_call(
        body,
        out_shape=shapes,
        in_specs=in_specs,
        out_specs=[VMEM] * len(outs),
        scratch_shapes=list(scratch),
        compiler_params=pltpu.CompilerParams(vmem_limit_bytes=40 << 20),
        input_output_aliases=aliases or {},
        cost_estimate=pl.CostEstimate(flops=weight, bytes_accessed=weight, transcendentals=0) if weight else None,
        name=name,
    )


def after(value, *tokens):
    return lax.optimization_barrier((value,) + tokens)[0]


def pairings(size):
    rounds = []
    for hop in range(1, HOPS + 1):
        for parity in range(2):
            pairs = [(i, i + hop) for i in range(size - hop) if (i // hop) % 2 == parity]
            if not pairs:
                continue
            used = {i for pair in pairs for i in pair}
            for entry in rounds:
                if not entry["used"] & used:
                    entry["used"] |= used
                    entry["pairs"] += pairs
                    entry["kinds"].append((hop, parity))
                    break
            else:
                rounds.append({"used": used, "pairs": pairs, "kinds": [(hop, parity)]})
    return rounds


def exchange(block, axis, pairs):
    return lax.ppermute(block, axis, [(a, b) for a, b in pairs] + [(b, a) for a, b in pairs])


def role_table(rounds, size):
    table = [[0] * size for _ in rounds]
    for p, entry in enumerate(rounds):
        for a, b in entry["pairs"]:
            table[p][a] = b - a
            table[p][b] = a - b
    return jnp.array(table, jnp.int32)


def sum_steps(size):
    return [1 << n for n in range(size.bit_length() - 1)]


def start_sum(block, axis):
    size = lax.axis_size(axis)
    if size & (size - 1):
        return block
    for step in sum_steps(size)[:-1]:
        block = block + lax.ppermute(block, axis, [(i, i ^ step) for i in range(size)])
    return block


def end_sum(block, axis, *tokens):
    size = lax.axis_size(axis)
    if size & (size - 1):
        return lax.psum(block, axis)
    for step in sum_steps(size)[-1:]:
        got = lax.ppermute(block, axis, [(i, i ^ step) for i in range(size)])
        block = block + (after(got, *tokens) if tokens else got)
    return block


def all_sum(block, axis, *tokens):
    return end_sum(start_sum(block, axis), axis, *tokens)


def factor(gram):
    size = gram.shape[0]
    row_id = lax.broadcasted_iota(jnp.int32, (size, size), 0)
    col_id = lax.broadcasted_iota(jnp.int32, (size, size), 1)
    work = jnp.concatenate([gram, (row_id == col_id).astype(F32)], axis=1)
    blocks = [work[8 * b : 8 * b + 8] for b in range(size // 8)]
    sub = lax.broadcasted_iota(jnp.int32, (8, 2 * size), 0)
    for j in range(size):
        b, s = divmod(j, 8)
        row = blocks[b][s : s + 1]
        scaled = row / row[:, j : j + 1]
        scaled = jnp.broadcast_to(scaled, (8, 2 * size))
        for other in range(b, size // 8):
            col = jnp.broadcast_to(blocks[other][:, j : j + 1], (8, 2 * size))
            if other == b:
                col = jnp.where(sub > s, col, 0.0)
            blocks[other] = blocks[other] - col * scaled
    work = jnp.concatenate(blocks, axis=0)
    pivots = jnp.sum(jnp.where(row_id == col_id, work[:, :size], 0.0), axis=1, keepdims=True)
    work = work / jnp.sqrt(pivots)
    upper = jnp.where(col_id >= row_id, work[:, :size], 0.0)
    inverse = jnp.where(col_id <= row_id, work[:, size:], 0.0)
    return upper, inverse


def local(start_block, diagonal, hess_tiles, tile_rows, tile_cols, slot_counts):
    peers = lax.axis_size("res")
    lanes = lax.axis_size("vec")
    rows, width, length = start_block.shape
    slots = hess_tiles.shape[2]
    half = rows // 2
    part = width // 2
    rounds = pairings(peers)
    count = len(rounds)
    full = (rows, width, length)
    chunk = (rows, part, length)
    halfchunk = (half, part, length)
    packet = (CAP, part, length)
    square = (width, width)
    split_shape = jax.ShapeDtypeStruct((slots, 2, length, length), BF16)

    table = role_table(rounds, peers)
    place = jnp.concatenate(
        [lax.axis_index("vec").reshape(1), table[:, lax.axis_index("res")]]
    ).astype(jnp.int32)

    def own_sum(acc_refs, x_ref, split_ref, rows_ref, cols_ref):
        for s in range(OWN_SLOTS):
            i, j = rows_ref[0, 0, s], cols_ref[0, 0, s]
            direct = tile_product(x_ref[j], split_ref, s, True)
            mirror = tile_product(x_ref[i], split_ref, s, False)
            for n, acc_ref in enumerate(acc_refs):
                acc_ref[i] += direct[n * part : (n + 1) * part]
                acc_ref[j] += mirror[n * part : (n + 1) * part]

    def prepare_body(rows_hbm, cols_hbm, x_hbm, diag_hbm, tiles_hbm, *refs):
        x_ref, split_ref, a_ref, b_ref, rows_ref, cols_ref, diag_ref, raw_ref, sem = refs
        size = slots // 4
        copies = [
            pltpu.make_async_copy(src, dst, sem.at[n])
            for n, (src, dst) in enumerate(
                [(x_hbm, x_ref), (diag_hbm, diag_ref), (rows_hbm, rows_ref), (cols_hbm, cols_ref)]
            )
        ]
        tile_copies = [
            pltpu.make_async_copy(
                tiles_hbm.at[0, 0, pl.ds(n * size, size)], raw_ref.at[pl.ds(n * size, size)], sem.at[4 + n]
            )
            for n in range(4)
        ]
        for c in copies + tile_copies:
            c.start()
        for n in range(4):
            tile_copies[n].wait()
            for s in range(n * size, (n + 1) * size):
                split_ref[s, 0], split_ref[s, 1] = pieces(raw_ref[s], 2)
        for c in copies:
            c.wait()
        first = (lax.axis_index("vec") == 0).astype(F32)
        d = ((diag_ref[...] - SHIFT) * first)[:, None, :]
        a_ref[...] = x_ref[:, :part] * d
        b_ref[...] = x_ref[:, part:] * d
        own_sum([a_ref, b_ref], x_ref, split_ref, rows_ref, cols_ref)

    def own_body(rows_ref, cols_ref, x_ref, split_ref, prior_ref, acc_ref):
        own_sum([acc_ref], x_ref, split_ref, rows_ref, cols_ref)

    def pack(place_ref, rows_ref, counts_ref, asked_refs, x_ref, split_ref, outs):
        for p in range(count):
            role = place_ref[1 + p]

            def put(c, value, p=p):
                for n, ref in enumerate(outs[p]):
                    ref[c] = value[n * part : (n + 1) * part]

            @pl.when(role > 0)
            def _():
                base = OWN_SLOTS + (role - 1) * CAP
                for c in range(CAP):
                    term = tile_product(x_ref[rows_ref[0, 0, base + c]], split_ref, base + c, False)
                    put(c, jnp.where(c < counts_ref[0, 0, role - 1], term, 0.0))

            @pl.when(role < 0)
            def _():
                base = OWN_SLOTS + (-role - 1) * CAP
                for c in range(CAP):
                    put(c, x_ref[asked_refs[p][0, 0, base + c]])

    def send_body(place_ref, rows_ref, counts_ref, *refs):
        asked_refs, (x_ref, split_ref), outs = refs[:count], refs[count : count + 2], refs[count + 2 :]
        pack(
            place_ref, rows_ref, counts_ref, asked_refs, x_ref, split_ref,
            [(outs[p], outs[count + p]) for p in range(count)],
        )

    def settle(place_ref, mine_ref, other_ref, y_ref):
        core = place_ref[0] % 2
        y_ref[pl.ds(core * half, half)] = mine_ref[...]
        y_ref[pl.ds((1 - core) * half, half)] = other_ref[...]

    def resend_body(place_ref, rows_ref, counts_ref, *refs):
        asked_refs = refs[:count]
        mine_ref, other_ref, diag_ref, split_ref, y_ref, acc_ref = refs[count : count + 6]
        outs = refs[count + 6 :]
        settle(place_ref, mine_ref, other_ref, y_ref)
        pack(
            place_ref, rows_ref, counts_ref, asked_refs, y_ref, split_ref,
            [(outs[p],) for p in range(count)],
        )
        first = (place_ref[0] == 0).astype(F32)
        acc_ref[...] = y_ref[...] * ((diag_ref[...] - SHIFT) * first)[:, None, :]

    def join_rounds(members, place_ref, rows_ref, counts_ref, asked_refs, got_refs, split_ref, acc_ref):
        for n, p in enumerate(members):
            role = place_ref[1 + p]

            @pl.when(role > 0)
            def _():
                base = OWN_SLOTS + (role - 1) * CAP
                for c in range(CAP):
                    term = tile_product(got_refs[n][c], split_ref, base + c, True)
                    acc_ref[rows_ref[0, 0, base + c]] += jnp.where(
                        c < counts_ref[0, 0, role - 1], term, 0.0
                    )

            @pl.when(role < 0)
            def _():
                base = OWN_SLOTS + (-role - 1) * CAP
                for c in range(CAP):
                    acc_ref[asked_refs[n][0, 0, base + c]] += got_refs[n][c]

    def join(acc, got, members, last=False):
        size = len(members)

        def body(place_ref, rows_ref, counts_ref, *refs):
            asked_refs, got_refs = refs[:size], refs[size : 2 * size]
            split_ref, prior_ref = refs[2 * size : 2 * size + 2]
            outs = refs[2 * size + 2 :]
            if last:
                keep_ref, give_ref, acc_ref = outs
                acc_ref[...] = prior_ref[...]
            else:
                (acc_ref,) = outs
            join_rounds(
                members, place_ref, rows_ref, counts_ref, asked_refs, got_refs, split_ref, acc_ref
            )
            if last:
                core = place_ref[0] % 2
                keep_ref[...] = acc_ref[pl.ds(core * half, half)]
                give_ref[...] = acc_ref[pl.ds((1 - core) * half, half)]

        out = call(
            body,
            [halfchunk] * 2 if last else [chunk],
            [SMEM] * (3 + size) + [VMEM] * (size + 2),
            [pltpu.VMEM(chunk, F32)] if last else [],
            name="join",
            weight=10**10,
            aliases=None if last else {3 + 2 * size + 1: 0},
        )(
            place, tile_rows, slot_counts, *[asked[p] for p in members], *[got[p] for p in members], split, acc
        )
        return out if last else out[0]

    def gram_body(x_ref, out_ref):
        total = jnp.zeros(square, F32)
        for n in range(0, rows, 2):
            pair = [x_ref[n], x_ref[n + 1]]
            total += gram_step(pair, [pair])
        out_ref[...] = total

    def cross_body(x_ref, a_ref, b_ref, out_ref):
        total = jnp.zeros((width, 2 * width), F32)
        for n in range(0, rows, 2):
            y = [jnp.concatenate([a_ref[m], b_ref[m]], axis=0) for m in (n, n + 1)]
            total += gram_step(y, [[x_ref[n], x_ref[n + 1]], y])
        out_ref[...] = total

    def first_body(gram_ref, inverse_ref):
        _, inverse_ref[...] = factor(gram_ref[...])

    def identity():
        eye = lax.broadcasted_iota(jnp.int32, square, 0) == lax.broadcasted_iota(jnp.int32, square, 1)
        return eye.astype(F32)

    def second_body(gram_ref, inverse_ref, cross_ref, lower_ref, coef_ref, gain_ref):
        start_inv = inverse_ref[...]
        cross = dot(dot(start_inv, gram_ref[:, :width]), start_inv, tb=True)
        applied = dot(dot(start_inv, gram_ref[:, width:]), start_inv, tb=True)
        upper, inverse = factor(applied - dot(cross, cross, tb=True))
        lower = upper.T
        cross_ref[...] = cross + SHIFT * identity()
        lower_ref[...] = lower
        gain = dot(inverse, start_inv)
        back = -dot(dot(inverse, cross), start_inv)
        gain_ref[...] = gain
        coef_ref[:width, :width] = -dot(lower, start_inv)
        coef_ref[:width, width : 2 * width] = back
        coef_ref[:width, 2 * width :] = gain
        coef_ref[width:, :width] = back
        coef_ref[width:, width : 2 * width] = gain
        coef_ref[width:, 2 * width :] = jnp.zeros(square, F32)

    def blend_body(place_ref, x_ref, a_ref, b_ref, mine_ref, other_ref, coef_ref, w_ref, q_ref, out_ref, z_ref):
        settle(place_ref, mine_ref, other_ref, z_ref)
        total = jnp.zeros(square, F32)
        for n in range(0, rows, 2):
            qs = []
            stacks = [
                jnp.concatenate([x_ref[m], a_ref[m], b_ref[m], z_ref[m]], axis=0) for m in (n, n + 1)
            ]
            for m, both in zip((n, n + 1), wide_product(coef_ref[:, : 2 * width + part], stacks)):
                w_ref[m] = both[:width]
                q_ref[m] = both[width:]
                qs.append(both[width:])
            total += gram_step(qs, [qs])
        out_ref[...] = total

    def third_body(place_ref, mine_ref, other_ref, prior_ref, q_ref, gain_ref, w_ref, out_ref, z_ref):
        settle(place_ref, mine_ref, other_ref, z_ref)
        total = jnp.zeros((width, 2 * width), F32)
        for n in range(0, rows, 2):
            ws = []
            for m, w in zip((n, n + 1), wide_product(gain_ref[:, part:], [z_ref[n], z_ref[n + 1]])):
                w = w + prior_ref[m]
                w_ref[m] = w
                ws.append(w)
            total += gram_step(ws, [[q_ref[n], q_ref[n + 1]], ws])
        out_ref[...] = total

    def fourth_body(gram_ref, norm_ref, cross_ref, lower_ref, coef_ref):
        cross = gram_ref[:, :width]
        norm = norm_ref[...]
        taken = cross + SHIFT * (norm - identity())
        mixed = dot(taken, cross, tb=True)
        squared = gram_ref[:, width:] - mixed - mixed.T + dot(dot(taken, norm), taken, tb=True)
        upper, inverse = factor(squared)
        cross_ref[...] = taken + SHIFT * identity()
        lower_ref[...] = upper.T
        scale = math.sqrt(rows * length * peers)
        coef_ref[:, :width] = inverse * scale
        coef_ref[:, width:] = -dot(inverse, taken) * scale

    def last_body(w_ref, q_ref, coef_ref, a1_ref, l1_ref, a2_ref, l2_ref, out_ref, pack_ref):
        for n, ref in enumerate((a1_ref, l1_ref, a2_ref, l2_ref)):
            pack_ref[n] = ref[...]
        for n in range(0, rows, 2):
            stacks = [jnp.concatenate([w_ref[m], q_ref[m]], axis=0) for m in (n, n + 1)]
            for m, out in zip((n, n + 1), wide_product(coef_ref[...], stacks)):
                out_ref[m] = out

    swap = [(i, i ^ 1) for i in range(lanes)]
    cuts = [count * n // 3 for n in range(4)]
    groups = [list(range(cuts[n], cuts[n + 1])) for n in range(3)]

    def spread(sent):
        return [exchange(s, "res", entry["pairs"]) for s, entry in zip(sent, rounds)]

    def across(mine, *tokens):
        step = 2
        while step < lanes:
            got = lax.ppermute(mine, "vec", [(i, i ^ step) for i in range(lanes)])
            mine = mine + after(got, *tokens)
            step *= 2
        return mine

    def resend(mine, other):
        y, acc, *sent = call(
            resend_body,
            [chunk, chunk] + [packet] * count,
            [SMEM] * (3 + count) + [VMEM] * 4,
            name="resend",
        )(place, tile_rows, slot_counts, *asked, mine, other, diagonal, split)
        return y, acc, spread(sent)

    def own(acc, y):
        return call(own_body, [chunk], [SMEM] * 2 + [VMEM] * 3, name="own", aliases={4: 0})(
            tile_rows, tile_cols, y, split, acc
        )[0]

    asked = [exchange(tile_cols, "res", entry["pairs"]) for entry in rounds]
    x, split, acc_a, acc_b = call(
        prepare_body,
        [full, split_shape, chunk, chunk],
        [HBM] * 5,
        [
            pltpu.SMEM(tile_rows.shape, jnp.int32),
            pltpu.SMEM(tile_cols.shape, jnp.int32),
            pltpu.VMEM(diagonal.shape, F32),
            pltpu.VMEM((slots, length, length), F32),
            pltpu.SemaphoreType.DMA((8,)),
        ],
        name="prepare",
    )(tile_rows, tile_cols, start_block, diagonal, hess_tiles)
    sent = call(
        send_body, [packet] * (2 * count), [SMEM] * (3 + count) + [VMEM] * 2, name="send"
    )(place, tile_rows, slot_counts, *asked, x, split)
    got_a = spread(sent[:count])
    sent_b = list(sent[count:])
    for n in range(2):
        acc_a = join(acc_a, got_a, groups[n])
        acc_a, *gated = lax.optimization_barrier((acc_a, *[sent_b[p] for p in groups[n]]))
        for p, value in zip(groups[n], gated):
            sent_b[p] = value
    keep_a, give_a = join(acc_a, got_a, groups[2], last=True)
    for p in groups[2]:
        sent_b[p] = after(sent_b[p], keep_a)
    got_b = spread(sent_b)
    (gram,) = call(gram_body, [square], [VMEM], name="gram")(after(x, keep_a))

    core = lax.ppermute(give_a, "vec", swap)
    acc_b = join(after(acc_b, gram), got_b, groups[0])
    mine_a = keep_a + after(core, acc_b)
    acc_b = join(acc_b, got_b, groups[1])
    mine_a = across(mine_a, acc_b)
    other_a = lax.ppermute(mine_a, "vec", swap)
    keep_b, give_b = join(acc_b, got_b, groups[2], last=True)
    start_gram = start_sum(gram, "res")
    y_a, acc_a, got_a = resend(mine_a, after(other_a, keep_b, start_gram))

    core = lax.ppermute(give_b, "vec", swap)
    acc_a = join(acc_a, got_a, groups[0])
    mine_b = keep_b + after(core, acc_a)
    (start_inv,) = call(first_body, [square], [VMEM], name="first")(end_sum(start_gram, "res", mine_b))
    acc_a = own(after(acc_a, start_inv), y_a)
    acc_a = join(acc_a, got_a, groups[1])
    mine_b = across(mine_b, acc_a)
    other_b = lax.ppermute(mine_b, "vec", swap)
    keep_a, give_a = join(acc_a, got_a, groups[2], last=True)
    y_b, acc_b, got_b = resend(mine_b, after(other_b, keep_a))

    (gram,) = call(cross_body, [(width, 2 * width)], [VMEM] * 3, name="cross")(x, y_a, y_b)
    core = lax.ppermute(give_a, "vec", swap)
    acc_b = own(after(acc_b, gram), y_b)
    acc_b = join(acc_b, got_b, groups[0])
    mine_a = keep_a + after(core, acc_b)
    cross_gram = all_sum(gram, "res", mine_a)
    cross1, lower1, coef, gain = call(
        second_body, [square, square, (2 * width, 3 * width), square], [VMEM] * 2, name="second"
    )(cross_gram, start_inv)
    acc_b = join(after(acc_b, gain), got_b, groups[1])
    mine_a = across(mine_a, acc_b)
    other_a = lax.ppermute(mine_a, "vec", swap)
    keep_b, give_b = join(acc_b, got_b, groups[2], last=True)

    core = lax.ppermute(give_b, "vec", swap)
    mine_b = keep_b + core
    w_prior, q, norm = call(
        blend_body,
        [full, full, square],
        [SMEM] + [VMEM] * 6,
        [pltpu.VMEM(chunk, F32)],
        name="blend",
    )(place, x, y_a, y_b, mine_a, other_a, after(coef, mine_b))
    mine_b = across(mine_b, norm)
    other_b = lax.ppermute(mine_b, "vec", swap)
    w, gram = call(
        third_body,
        [full, (width, 2 * width)],
        [SMEM] + [VMEM] * 5,
        [pltpu.VMEM(chunk, F32)],
        name="third",
    )(place, mine_b, other_b, w_prior, q, gain)
    norm = all_sum(norm, "res")
    gram = all_sum(gram, "res")
    cross2, lower2, coef = call(
        fourth_body, [square, square, (width, 2 * width)], [VMEM] * 2, name="fourth"
    )(gram, norm)
    return call(last_body, [full, (4, width, width)], [VMEM] * 7, name="last")(
        w, q, coef, cross1, lower1, cross2, lower2
    )


def solution(mesh):
    in_specs = (
        P(("conf", "res"), None, None),
        P(("conf", "res"), None),
        P(("conf", "res"), "vec", None, None, None),
        P(("conf", "res"), "vec", None),
        P(("conf", "res"), "vec", None),
        P(("conf", "res"), "vec", None),
    )
    out_specs = (P(("conf", "res"), None, None), P("conf", None, None))
    return jax.shard_map(local, mesh=mesh, in_specs=in_specs, out_specs=out_specs, check_vma=False)
```

```python
import math

import jax
import jax.numpy as jnp
from jax import lax
from jax.experimental import pallas as pl
from jax.experimental.pallas import tpu as pltpu
from jax.sharding import PartitionSpec as P

OWN_SLOTS = 20
HOPS = 3
CAP = 8
SHIFT = 1.65
BF16 = jnp.bfloat16
F32 = jnp.float32

VMEM = pl.BlockSpec(memory_space=pltpu.VMEM)
SMEM = pl.BlockSpec(memory_space=pltpu.SMEM)
HBM = pl.BlockSpec(memory_space=pltpu.HBM)


def contract(a, b, ta=False, tb=False, precision=None):
    dims = (((0 if ta else 1,), (1 if tb else 0,)), ((), ()))
    return lax.dot_general(a, b, dims, precision=precision, preferred_element_type=F32)


def dot(a, b, ta=False, tb=False):
    return contract(a, b, ta, tb, lax.Precision.HIGHEST)


def pieces(x, count):
    out = []
    for _ in range(count):
        out.append(x.astype(BF16))
        x = x - out[-1].astype(F32)
    return out


def tile_product(x, tile_ref, slot, transposed):
    x1, x2 = pieces(x, 2)
    m1, m2 = tile_ref[slot, 0], tile_ref[slot, 1]
    axis = 1 if transposed else 0
    left = jnp.concatenate([x1, x2, x1], axis=1)
    return contract(left, jnp.concatenate([m1, m1, m2], axis=axis), tb=transposed)


def wide_product(coef, blocks):
    c1, c2, c3 = pieces(coef, 3)
    z1, z2, z3 = pieces(jnp.concatenate(blocks, axis=1), 3)
    left = jnp.concatenate([c1, c1, c1, c2, c2, c3], axis=1)
    out = contract(left, jnp.concatenate([z1, z2, z3, z1, z2, z1], axis=0))
    width = blocks[0].shape[1]
    return [out[:, n * width : (n + 1) * width] for n in range(len(blocks))]


def gram_step(left, right):
    a = jnp.concatenate(pieces(jnp.concatenate(left, axis=1), 2), axis=0)
    b = jnp.concatenate(
        [p for group in right for p in pieces(jnp.concatenate(group, axis=1), 2)], axis=0
    )
    out = contract(a, b, tb=True)
    size = left[0].shape[0]
    out = out[:size] + out[size:]
    return jnp.concatenate(
        [
            out[:, 2 * g * size : (2 * g + 1) * size] + out[:, (2 * g + 1) * size : (2 * g + 2) * size]
            for g in range(len(right))
        ],
        axis=1,
    )


def call(body, outs, in_specs, scratch=(), name=None, aliases=None, weight=0):
    shapes = [
        o if isinstance(o, jax.ShapeDtypeStruct) else jax.ShapeDtypeStruct(o, F32) for o in outs
    ]
    return pl.pallas_call(
        body,
        out_shape=shapes,
        in_specs=in_specs,
        out_specs=[VMEM] * len(outs),
        scratch_shapes=list(scratch),
        compiler_params=pltpu.CompilerParams(vmem_limit_bytes=40 << 20),
        input_output_aliases=aliases or {},
        cost_estimate=pl.CostEstimate(flops=weight, bytes_accessed=weight, transcendentals=0) if weight else None,
        name=name,
    )


def pinned(value):
    return pltpu.with_memory_space_constraint(value, pltpu.HBM)


def after(value, *tokens):
    return lax.optimization_barrier((value,) + tokens)[0]


def pairings(size):
    rounds = []
    for hop in range(1, HOPS + 1):
        for parity in range(2):
            pairs = [(i, i + hop) for i in range(size - hop) if (i // hop) % 2 == parity]
            if not pairs:
                continue
            used = {i for pair in pairs for i in pair}
            for entry in rounds:
                if not entry["used"] & used:
                    entry["used"] |= used
                    entry["pairs"] += pairs
                    entry["kinds"].append((hop, parity))
                    break
            else:
                rounds.append({"used": used, "pairs": pairs, "kinds": [(hop, parity)]})
    return rounds


def exchange(block, axis, pairs):
    return lax.ppermute(block, axis, [(a, b) for a, b in pairs] + [(b, a) for a, b in pairs])


def role_table(rounds, size):
    table = [[0] * size for _ in rounds]
    for p, entry in enumerate(rounds):
        for a, b in entry["pairs"]:
            table[p][a] = b - a
            table[p][b] = a - b
    return jnp.array(table, jnp.int32)


def sum_steps(size):
    return [1 << n for n in range(size.bit_length() - 1)]


def start_sum(block, axis):
    size = lax.axis_size(axis)
    if size & (size - 1):
        return block
    for step in sum_steps(size)[:-1]:
        block = block + lax.ppermute(block, axis, [(i, i ^ step) for i in range(size)])
    return block


def end_sum(block, axis, *tokens):
    size = lax.axis_size(axis)
    if size & (size - 1):
        return lax.psum(block, axis)
    for step in sum_steps(size)[-1:]:
        got = lax.ppermute(block, axis, [(i, i ^ step) for i in range(size)])
        block = block + (after(got, *tokens) if tokens else got)
    return block


def all_sum(block, axis, *tokens):
    return end_sum(start_sum(block, axis), axis, *tokens)


def factor(gram):
    size = gram.shape[0]
    tile = (8, 2 * size)
    row_id = lax.broadcasted_iota(jnp.int32, (size, size), 0)
    col_id = lax.broadcasted_iota(jnp.int32, (size, size), 1)
    work = jnp.concatenate([gram, (row_id == col_id).astype(F32)], axis=1)
    blocks = [work[8 * b : 8 * b + 8] for b in range(size // 8)]
    sub = lax.broadcasted_iota(jnp.int32, tile, 0)
    for j in range(0, size, 4):
        b, s = divmod(j, 8)
        later = range(b + s // 4, size // 8)
        line = [jnp.broadcast_to(blocks[b][s + k : s + k + 1], tile) for k in range(4)]
        cols = {
            o: [jnp.broadcast_to(blocks[o][:, j + k : j + k + 1], tile) for k in range(4)]
            for o in range(b, size // 8)
        }
        entry = {
            (k, l): jnp.broadcast_to(cols[b][l][s + k : s + k + 1], tile)
            for k in range(4)
            for l in range(k, 4)
        }
        scaled = []
        for k in range(4):
            inverse = 1.0 / entry[k, k]
            for l in range(k + 1, 4):
                ratio = entry[k, l] * inverse
                for p in range(l, 4):
                    entry[l, p] = entry[l, p] - ratio * entry[k, p]
                line[l] = line[l] - ratio * line[k]
                for o in later:
                    cols[o][l] = cols[o][l] - ratio * cols[o][k]
            scaled.append(inverse * line[k])
        for o in range(b, size // 8):
            new = blocks[o]
            if o in later:
                new = new - ((cols[o][0] * scaled[0] + cols[o][1] * scaled[1]) + (cols[o][2] * scaled[2] + cols[o][3] * scaled[3]))
            if o == b:
                new = jnp.where(sub > s + 3, new, blocks[o])
                for k in range(1, 4):
                    new = jnp.where(sub == s + k, line[k], new)
            blocks[o] = new
    work = jnp.concatenate(blocks, axis=0)
    pivots = jnp.sum(jnp.where(row_id == col_id, work[:, :size], 0.0), axis=1, keepdims=True)
    work = work / jnp.sqrt(pivots)
    upper = jnp.where(col_id >= row_id, work[:, :size], 0.0)
    inverse = jnp.where(col_id <= row_id, work[:, size:], 0.0)
    return upper, inverse


def local(start_block, diagonal, hess_tiles, tile_rows, tile_cols, slot_counts):
    peers = lax.axis_size("res")
    lanes = lax.axis_size("vec")
    rows, width, length = start_block.shape
    slots = hess_tiles.shape[2]
    half = rows // 2
    part = width // 2
    rounds = pairings(peers)
    count = len(rounds)
    full = (rows, width, length)
    halffull = (half, width, length)
    chunk = (rows, part, length)
    halfchunk = (half, part, length)
    packet = (CAP, part, length)
    square = (width, width)
    split_shape = jax.ShapeDtypeStruct((slots, 2, length, length), BF16)

    table = role_table(rounds, peers)
    place = jnp.concatenate(
        [lax.axis_index("vec").reshape(1), table[:, lax.axis_index("res")]]
    ).astype(jnp.int32)

    def own_sum(acc_refs, x_ref, split_ref, rows_ref, cols_ref):
        for s in range(OWN_SLOTS):
            i, j = rows_ref[0, 0, s], cols_ref[0, 0, s]
            direct = tile_product(x_ref[j], split_ref, s, True)
            mirror = tile_product(x_ref[i], split_ref, s, False)
            for n, acc_ref in enumerate(acc_refs):
                acc_ref[i] += direct[n * part : (n + 1) * part]
                acc_ref[j] += mirror[n * part : (n + 1) * part]

    def prepare_body(rows_hbm, cols_hbm, x_hbm, diag_hbm, tiles_hbm, *refs):
        x_ref, split_ref, a_ref, b_ref, rows_ref, cols_ref, diag_ref, raw_ref, sem = refs
        size = slots // 4
        copies = [
            pltpu.make_async_copy(src, dst, sem.at[n])
            for n, (src, dst) in enumerate(
                [(x_hbm, x_ref), (diag_hbm, diag_ref), (rows_hbm, rows_ref), (cols_hbm, cols_ref)]
            )
        ]
        tile_copies = [
            pltpu.make_async_copy(
                tiles_hbm.at[0, 0, pl.ds(n * size, size)], raw_ref.at[pl.ds(n * size, size)], sem.at[4 + n]
            )
            for n in range(4)
        ]
        for c in copies + tile_copies:
            c.start()
        for n in range(4):
            tile_copies[n].wait()
            for s in range(n * size, (n + 1) * size):
                split_ref[s, 0], split_ref[s, 1] = pieces(raw_ref[s], 2)
        for c in copies:
            c.wait()
        first = (lax.axis_index("vec") == 0).astype(F32)
        d = ((diag_ref[...] - SHIFT) * first)[:, None, :]
        a_ref[...] = x_ref[:, :part] * d
        b_ref[...] = x_ref[:, part:] * d
        own_sum([a_ref, b_ref], x_ref, split_ref, rows_ref, cols_ref)

    def own_body(rows_ref, cols_ref, x_ref, split_ref, prior_ref, acc_ref):
        own_sum([acc_ref], x_ref, split_ref, rows_ref, cols_ref)

    def pack(place_ref, rows_ref, counts_ref, asked_refs, x_ref, split_ref, outs):
        for p in range(count):
            role = place_ref[1 + p]

            def put(c, value, p=p):
                for n, ref in enumerate(outs[p]):
                    ref[c] = value[n * part : (n + 1) * part]

            @pl.when(role > 0)
            def _():
                base = OWN_SLOTS + (role - 1) * CAP
                for c in range(CAP):
                    term = tile_product(x_ref[rows_ref[0, 0, base + c]], split_ref, base + c, False)
                    put(c, jnp.where(c < counts_ref[0, 0, role - 1], term, 0.0))

            @pl.when(role < 0)
            def _():
                base = OWN_SLOTS + (-role - 1) * CAP
                for c in range(CAP):
                    put(c, x_ref[asked_refs[p][0, 0, base + c]])

    def send_body(place_ref, rows_ref, counts_ref, *refs):
        asked_refs, (x_ref, split_ref), outs = refs[:count], refs[count : count + 2], refs[count + 2 :]
        pack(
            place_ref, rows_ref, counts_ref, asked_refs, x_ref, split_ref,
            [(outs[p], outs[count + p]) for p in range(count)],
        )

    def settle(place_ref, mine_ref, other_ref, y_ref):
        core = place_ref[0] % 2
        y_ref[pl.ds(core * half, half)] = mine_ref[...]
        y_ref[pl.ds((1 - core) * half, half)] = other_ref[...]

    def resend_body(place_ref, rows_ref, counts_ref, *refs):
        asked_refs = refs[:count]
        mine_ref, other_ref, diag_ref, split_ref, y_ref, acc_ref = refs[count : count + 6]
        outs = refs[count + 6 :]
        settle(place_ref, mine_ref, other_ref, y_ref)
        pack(
            place_ref, rows_ref, counts_ref, asked_refs, y_ref, split_ref,
            [(outs[p],) for p in range(count)],
        )
        first = (place_ref[0] == 0).astype(F32)
        acc_ref[...] = y_ref[...] * ((diag_ref[...] - SHIFT) * first)[:, None, :]

    def join_rounds(members, place_ref, rows_ref, counts_ref, asked_refs, got_refs, split_ref, acc_ref):
        for n, p in enumerate(members):
            role = place_ref[1 + p]

            @pl.when(role > 0)
            def _():
                base = OWN_SLOTS + (role - 1) * CAP
                for c in range(CAP):
                    term = tile_product(got_refs[n][c], split_ref, base + c, True)
                    acc_ref[rows_ref[0, 0, base + c]] += jnp.where(
                        c < counts_ref[0, 0, role - 1], term, 0.0
                    )

            @pl.when(role < 0)
            def _():
                base = OWN_SLOTS + (-role - 1) * CAP
                for c in range(CAP):
                    acc_ref[asked_refs[n][0, 0, base + c]] += got_refs[n][c]

    def join(acc, got, members, last=False):
        size = len(members)

        def body(place_ref, rows_ref, counts_ref, *refs):
            asked_refs, got_refs = refs[:size], refs[size : 2 * size]
            split_ref, prior_ref = refs[2 * size : 2 * size + 2]
            outs = refs[2 * size + 2 :]
            if last:
                keep_ref, give_ref, acc_ref = outs
                acc_ref[...] = prior_ref[...]
            else:
                (acc_ref,) = outs
            join_rounds(
                members, place_ref, rows_ref, counts_ref, asked_refs, got_refs, split_ref, acc_ref
            )
            if last:
                core = place_ref[0] % 2
                keep_ref[...] = acc_ref[pl.ds(core * half, half)]
                give_ref[...] = acc_ref[pl.ds((1 - core) * half, half)]

        out = call(
            body,
            [halfchunk] * 2 if last else [chunk],
            [SMEM] * (3 + size) + [VMEM] * (size + 2),
            [pltpu.VMEM(chunk, F32)] if last else [],
            name="join",
            weight=10**10,
            aliases=None if last else {3 + 2 * size + 1: 0},
        )(
            place, tile_rows, slot_counts, *[asked[p] for p in members], *[got[p] for p in members], split, acc
        )
        return out if last else out[0]

    def gram_body(x_ref, out_ref):
        total = jnp.zeros(square, F32)
        for n in range(0, rows, 2):
            pair = [x_ref[n], x_ref[n + 1]]
            total += gram_step(pair, [pair])
        out_ref[...] = total

    def cross_body(x_ref, a_ref, b_ref, out_ref):
        total = jnp.zeros((width, 2 * width), F32)
        for n in range(0, rows, 2):
            y = [jnp.concatenate([a_ref[m], b_ref[m]], axis=0) for m in (n, n + 1)]
            total += gram_step(y, [[x_ref[n], x_ref[n + 1]], y])
        out_ref[...] = total

    def first_body(gram_ref, inverse_ref):
        _, inverse_ref[...] = factor(gram_ref[...])

    def identity():
        eye = lax.broadcasted_iota(jnp.int32, square, 0) == lax.broadcasted_iota(jnp.int32, square, 1)
        return eye.astype(F32)

    def second_body(gram_ref, inverse_ref, cross_ref, lower_ref, coef_ref, gain_ref):
        start_inv = inverse_ref[...]
        cross = dot(dot(start_inv, gram_ref[:, :width]), start_inv, tb=True)
        applied = dot(dot(start_inv, gram_ref[:, width:]), start_inv, tb=True)
        upper, inverse = factor(applied - dot(cross, cross, tb=True))
        lower = upper.T
        cross_ref[...] = cross + SHIFT * identity()
        lower_ref[...] = lower
        gain = dot(inverse, start_inv)
        back = -dot(dot(inverse, cross), start_inv)
        gain_ref[...] = gain
        coef_ref[:width, :width] = -dot(lower, start_inv)
        coef_ref[:width, width : 2 * width] = back
        coef_ref[:width, 2 * width :] = gain
        coef_ref[width:, :width] = back
        coef_ref[width:, width : 2 * width] = gain
        coef_ref[width:, 2 * width :] = jnp.zeros(square, F32)

    def blend(side, mine, other, coef):
        def body(place_ref, x_ref, a_ref, b_ref, mine_ref, other_ref, coef_ref, w_ref, q_ref, out_ref, z_ref):
            settle(place_ref, mine_ref, other_ref, z_ref)
            total = jnp.zeros(square, F32)
            for n in range(0, half, 2):
                qs = []
                stacks = [
                    jnp.concatenate([ref[side * half + m] for ref in (x_ref, a_ref, b_ref, z_ref)], axis=0)
                    for m in (n, n + 1)
                ]
                for m, both in zip((n, n + 1), wide_product(coef_ref[:, : 2 * width + part], stacks)):
                    w_ref[m] = both[:width]
                    q_ref[m] = both[width:]
                    qs.append(both[width:])
                total += gram_step(qs, [qs])
            out_ref[...] = total

        return call(
            body,
            [halffull, halffull, square],
            [SMEM] + [VMEM] * 6,
            [pltpu.VMEM(chunk, F32)],
            name="blend",
        )(place, x, y_a, y_b, mine, other, coef)

    def third_body(place_ref, mine_ref, other_ref, gain_ref, *refs):
        prior_refs, q_refs, norm_refs = refs[0:2], refs[2:4], refs[4:6]
        w_ref, out_ref, z_ref = refs[6:]
        settle(place_ref, mine_ref, other_ref, z_ref)
        total = jnp.zeros((width, 2 * width), F32)
        for n in range(0, rows, 2):
            side, m = divmod(n, half)
            ws = []
            for k, w in enumerate(wide_product(gain_ref[:, part:], [z_ref[n], z_ref[n + 1]])):
                w = w + prior_refs[side][m + k]
                w_ref[n + k] = w
                ws.append(w)
            total += gram_step(ws, [[q_refs[side][m], q_refs[side][m + 1]], ws])
        out_ref[:, : 2 * width] = total
        out_ref[:, 2 * width :] = norm_refs[0][...] + norm_refs[1][...]

    def fourth_body(gram_ref, cross_ref, lower_ref, coef_ref):
        cross = gram_ref[:, :width]
        norm = gram_ref[:, 2 * width :]
        taken = cross + SHIFT * (norm - identity())
        mixed = dot(taken, cross, tb=True)
        squared = gram_ref[:, width : 2 * width] - mixed - mixed.T + dot(dot(taken, norm), taken, tb=True)
        upper, inverse = factor(squared)
        cross_ref[...] = taken + SHIFT * identity()
        lower_ref[...] = upper.T
        scale = math.sqrt(rows * length * peers)
        coef_ref[:, :width] = inverse * scale
        coef_ref[:, width:] = -dot(inverse, taken) * scale

    def last_body(w_ref, low_ref, high_ref, coef_ref, a1_ref, l1_ref, a2_ref, l2_ref, out_ref, pack_ref):
        for n, ref in enumerate((a1_ref, l1_ref, a2_ref, l2_ref)):
            pack_ref[n] = ref[...]
        for n in range(0, rows, 2):
            side, at = divmod(n, half)
            q_ref = (low_ref, high_ref)[side]
            stacks = [jnp.concatenate([w_ref[n + k], q_ref[at + k]], axis=0) for k in range(2)]
            for m, out in zip((n, n + 1), wide_product(coef_ref[...], stacks)):
                out_ref[m] = out

    swap = [(i, i ^ 1) for i in range(lanes)]
    cuts = [count * n // 3 for n in range(4)]
    groups = [list(range(cuts[n], cuts[n + 1])) for n in range(3)]

    def spread(sent):
        return [exchange(s, "res", entry["pairs"]) for s, entry in zip(sent, rounds)]

    def across(mine, *tokens):
        step = 2
        while step < lanes:
            got = lax.ppermute(mine, "vec", [(i, i ^ step) for i in range(lanes)])
            mine = mine + after(got, *tokens)
            step *= 2
        return mine

    def resend(mine, other):
        y, acc, *sent = call(
            resend_body,
            [chunk, chunk] + [packet] * count,
            [SMEM] * (3 + count) + [VMEM] * 4,
            name="resend",
        )(place, tile_rows, slot_counts, *asked, mine, other, diagonal, split)
        return y, acc, spread(sent)

    def own(acc, y):
        return call(own_body, [chunk], [SMEM] * 2 + [VMEM] * 3, name="own", aliases={4: 0})(
            tile_rows, tile_cols, y, split, acc
        )[0]

    asked = [exchange(tile_cols, "res", entry["pairs"]) for entry in rounds]
    x, split, acc_a, acc_b = call(
        prepare_body,
        [full, split_shape, chunk, chunk],
        [HBM] * 5,
        [
            pltpu.SMEM(tile_rows.shape, jnp.int32),
            pltpu.SMEM(tile_cols.shape, jnp.int32),
            pltpu.VMEM(diagonal.shape, F32),
            pltpu.VMEM((slots, length, length), F32),
            pltpu.SemaphoreType.DMA((8,)),
        ],
        name="prepare",
    )(*[pinned(v) for v in (tile_rows, tile_cols, start_block, diagonal, hess_tiles)])
    sent = call(
        send_body, [packet] * (2 * count), [SMEM] * (3 + count) + [VMEM] * 2, name="send"
    )(place, tile_rows, slot_counts, *asked, x, split)
    got_a = spread(sent[:count])
    sent_b = list(sent[count:])
    for n in range(2):
        acc_a = join(acc_a, got_a, groups[n])
        acc_a, x, *gated = lax.optimization_barrier((acc_a, x, *[sent_b[p] for p in groups[n]]))
        for p, value in zip(groups[n], gated):
            sent_b[p] = value
        if n == 0:
            (gram,) = call(gram_body, [square], [VMEM], name="gram")(x)
            start_gram = start_sum(gram, "res")
    acc_a = after(acc_a, start_gram)
    keep_a, give_a = join(acc_a, got_a, groups[2], last=True)
    for p in groups[2]:
        sent_b[p] = after(sent_b[p], keep_a)
    got_b = spread(sent_b)

    core = lax.ppermute(give_a, "vec", swap)
    acc_b = join(acc_b, got_b, groups[0])
    mine_a = keep_a + after(core, acc_b)
    (start_inv,) = call(first_body, [square], [VMEM], name="first")(end_sum(start_gram, "res", mine_a))
    acc_b = join(after(acc_b, start_inv), got_b, groups[1])
    mine_a = across(mine_a, acc_b)
    other_a = lax.ppermute(mine_a, "vec", swap)
    keep_b, give_b = join(acc_b, got_b, groups[2], last=True)
    y_a, acc_a, got_a = resend(mine_a, after(other_a, keep_b))

    core = lax.ppermute(give_b, "vec", swap)
    acc_a = join(acc_a, got_a, groups[0])
    mine_b = keep_b + after(core, acc_a)
    acc_a = own(after(acc_a, mine_b), y_a)
    acc_a = join(acc_a, got_a, groups[1])
    mine_b = across(mine_b, acc_a)
    other_b = lax.ppermute(mine_b, "vec", swap)
    keep_a, give_a = join(acc_a, got_a, groups[2], last=True)
    y_b, acc_b, got_b = resend(mine_b, after(other_b, keep_a))

    (gram,) = call(cross_body, [(width, 2 * width)], [VMEM] * 3, name="cross")(x, y_a, y_b)
    core = lax.ppermute(give_a, "vec", swap)
    acc_b = own(after(acc_b, gram), y_b)
    acc_b = join(acc_b, got_b, groups[0])
    mine_a = keep_a + after(core, acc_b)
    cross_gram = start_sum(gram, "res")
    acc_b = join(after(acc_b, cross_gram, mine_a), got_b, groups[1])
    cross_gram = end_sum(cross_gram, "res", acc_b)
    acc_b = after(acc_b, cross_gram)
    mine_a = across(mine_a, acc_b)
    other_a = lax.ppermute(mine_a, "vec", swap)
    keep_b, give_b = join(acc_b, got_b, groups[2], last=True)

    core = lax.ppermute(give_b, "vec", swap)
    mine_b = keep_b + core
    cross1, lower1, coef, gain = call(
        second_body, [square, square, (2 * width, 3 * width), square], [VMEM] * 2, name="second"
    )(after(cross_gram, mine_b), start_inv)
    w_low, q_low, norm_low = blend(0, mine_a, other_a, coef)
    mine_b = across(mine_b, norm_low)
    other_b = lax.ppermute(mine_b, "vec", swap)
    w_high, q_high, norm_high = blend(1, mine_a, other_a, after(coef, mine_b))
    w, gram = call(
        third_body,
        [full, (width, 3 * width)],
        [SMEM] + [VMEM] * 9,
        [pltpu.VMEM(chunk, F32)],
        name="third",
    )(place, mine_b, after(other_b, norm_high), gain, w_low, w_high, q_low, q_high, norm_low, norm_high)
    gram = all_sum(gram, "res")
    cross2, lower2, coef = call(
        fourth_body, [square, square, (width, 2 * width)], [VMEM], name="fourth"
    )(gram)
    return call(last_body, [full, (4, width, width)], [VMEM] * 8, name="last")(
        w, q_low, q_high, coef, cross1, lower1, cross2, lower2
    )


def solution(mesh):
    in_specs = (
        P(("conf", "res"), None, None),
        P(("conf", "res"), None),
        P(("conf", "res"), "vec", None, None, None),
        P(("conf", "res"), "vec", None),
        P(("conf", "res"), "vec", None),
        P(("conf", "res"), "vec", None),
    )
    out_specs = (P(("conf", "res"), None, None), P("conf", None, None))
    return jax.shard_map(local, mesh=mesh, in_specs=in_specs, out_specs=out_specs, check_vma=False)
```

```python
import math

import jax
import jax.numpy as jnp
from jax import lax
from jax.experimental import pallas as pl
from jax.experimental.pallas import tpu as pltpu
from jax.sharding import PartitionSpec as P

OWN_SLOTS = 20
HOPS = 3
CAP = 8
SHIFT = 1.65
BF16 = jnp.bfloat16
F32 = jnp.float32

VMEM = pl.BlockSpec(memory_space=pltpu.VMEM)
SMEM = pl.BlockSpec(memory_space=pltpu.SMEM)
HBM = pl.BlockSpec(memory_space=pltpu.HBM)


def contract(a, b, ta=False, tb=False, precision=None):
    dims = (((0 if ta else 1,), (1 if tb else 0,)), ((), ()))
    return lax.dot_general(a, b, dims, precision=precision, preferred_element_type=F32)


def dot(a, b, ta=False, tb=False):
    return contract(a, b, ta, tb, lax.Precision.HIGHEST)


def pieces(x, count):
    out = []
    for _ in range(count):
        out.append(x.astype(BF16))
        x = x - out[-1].astype(F32)
    return out


def tile_product(x, tile_ref, slot, transposed):
    x1, x2 = pieces(x, 2)
    m1, m2 = tile_ref[slot, 0], tile_ref[slot, 1]
    axis = 1 if transposed else 0
    left = jnp.concatenate([x1, x2, x1], axis=1)
    return contract(left, jnp.concatenate([m1, m1, m2], axis=axis), tb=transposed)


def wide_product(coef, blocks, terms=6):
    pairs = [(0, 0), (0, 1), (1, 0), (1, 1)] if terms == 4 else [(0, 0), (0, 1), (0, 2), (1, 0), (1, 1), (2, 0)]
    c = pieces(coef, terms // 2)
    z = pieces(jnp.concatenate(blocks, axis=1), terms // 2)
    left = jnp.concatenate([c[m] for m, _ in pairs], axis=1)
    out = contract(left, jnp.concatenate([z[m] for _, m in pairs], axis=0))
    width = blocks[0].shape[1]
    return [out[:, n * width : (n + 1) * width] for n in range(len(blocks))]


def gram_step(left, right):
    a = jnp.concatenate(pieces(jnp.concatenate(left, axis=1), 2), axis=0)
    b = jnp.concatenate(
        [p for group in right for p in pieces(jnp.concatenate(group, axis=1), 2)], axis=0
    )
    out = contract(a, b, tb=True)
    size = left[0].shape[0]
    out = out[:size] + out[size:]
    return jnp.concatenate(
        [
            out[:, 2 * g * size : (2 * g + 1) * size] + out[:, (2 * g + 1) * size : (2 * g + 2) * size]
            for g in range(len(right))
        ],
        axis=1,
    )


def call(body, outs, in_specs, scratch=(), name=None, aliases=None, weight=0):
    shapes = [
        o if isinstance(o, jax.ShapeDtypeStruct) else jax.ShapeDtypeStruct(o, F32) for o in outs
    ]
    return pl.pallas_call(
        body,
        out_shape=shapes,
        in_specs=in_specs,
        out_specs=[VMEM] * len(outs),
        scratch_shapes=list(scratch),
        compiler_params=pltpu.CompilerParams(vmem_limit_bytes=40 << 20),
        input_output_aliases=aliases or {},
        cost_estimate=pl.CostEstimate(flops=weight, bytes_accessed=weight, transcendentals=0) if weight else None,
        name=name,
    )


def pinned(value):
    return pltpu.with_memory_space_constraint(value, pltpu.HBM)


def after(value, *tokens):
    return lax.optimization_barrier((value,) + tokens)[0]


def pairings(size):
    rounds = []
    for hop in range(1, HOPS + 1):
        for parity in range(2):
            pairs = [(i, i + hop) for i in range(size - hop) if (i // hop) % 2 == parity]
            if not pairs:
                continue
            used = {i for pair in pairs for i in pair}
            for entry in rounds:
                if not entry["used"] & used:
                    entry["used"] |= used
                    entry["pairs"] += pairs
                    entry["kinds"].append((hop, parity))
                    break
            else:
                rounds.append({"used": used, "pairs": pairs, "kinds": [(hop, parity)]})
    return rounds[::-1]


def exchange(block, axis, pairs):
    return lax.ppermute(block, axis, [(a, b) for a, b in pairs] + [(b, a) for a, b in pairs])


def role_table(rounds, size):
    table = [[0] * size for _ in rounds]
    for p, entry in enumerate(rounds):
        for a, b in entry["pairs"]:
            table[p][a] = b - a
            table[p][b] = a - b
    return jnp.array(table, jnp.int32)


def sum_steps(size):
    return [1 << n for n in range(size.bit_length() - 1)]


def start_sum(block, axis):
    size = lax.axis_size(axis)
    if size & (size - 1):
        return block
    for step in sum_steps(size)[:-1]:
        block = block + lax.ppermute(block, axis, [(i, i ^ step) for i in range(size)])
    return block


def end_sum(block, axis, *tokens):
    size = lax.axis_size(axis)
    if size & (size - 1):
        return lax.psum(block, axis)
    for step in sum_steps(size)[-1:]:
        got = lax.ppermute(block, axis, [(i, i ^ step) for i in range(size)])
        block = block + (after(got, *tokens) if tokens else got)
    return block


def all_sum(block, axis, *tokens):
    return end_sum(start_sum(block, axis), axis, *tokens)


def factor(gram):
    size = gram.shape[0]
    tile = (8, 2 * size)
    row_id = lax.broadcasted_iota(jnp.int32, (size, size), 0)
    col_id = lax.broadcasted_iota(jnp.int32, (size, size), 1)
    work = jnp.concatenate([gram, (row_id == col_id).astype(F32)], axis=1)
    blocks = [work[8 * b : 8 * b + 8] for b in range(size // 8)]
    sub = lax.broadcasted_iota(jnp.int32, tile, 0)
    for j in range(0, size, 4):
        b, s = divmod(j, 8)
        later = range(b + s // 4, size // 8)
        line = [jnp.broadcast_to(blocks[b][s + k : s + k + 1], tile) for k in range(4)]
        cols = {
            o: [jnp.broadcast_to(blocks[o][:, j + k : j + k + 1], tile) for k in range(4)]
            for o in range(b, size // 8)
        }
        entry = {
            (k, l): jnp.broadcast_to(cols[b][l][s + k : s + k + 1], tile)
            for k in range(4)
            for l in range(k, 4)
        }
        scaled = []
        for k in range(4):
            inverse = 1.0 / entry[k, k]
            for l in range(k + 1, 4):
                ratio = entry[k, l] * inverse
                for p in range(l, 4):
                    entry[l, p] = entry[l, p] - ratio * entry[k, p]
                line[l] = line[l] - ratio * line[k]
                for o in later:
                    cols[o][l] = cols[o][l] - ratio * cols[o][k]
            scaled.append(inverse * line[k])
        for o in range(b, size // 8):
            new = blocks[o]
            if o in later:
                new = new - ((cols[o][0] * scaled[0] + cols[o][1] * scaled[1]) + (cols[o][2] * scaled[2] + cols[o][3] * scaled[3]))
            if o == b:
                new = jnp.where(sub > s + 3, new, blocks[o])
                for k in range(1, 4):
                    new = jnp.where(sub == s + k, line[k], new)
            blocks[o] = new
    work = jnp.concatenate(blocks, axis=0)
    pivots = jnp.sum(jnp.where(row_id == col_id, work[:, :size], 0.0), axis=1, keepdims=True)
    work = work / jnp.sqrt(pivots)
    upper = jnp.where(col_id >= row_id, work[:, :size], 0.0)
    inverse = jnp.where(col_id <= row_id, work[:, size:], 0.0)
    return upper, inverse


def local(start_block, diagonal, hess_tiles, tile_rows, tile_cols, slot_counts):
    peers = lax.axis_size("res")
    lanes = lax.axis_size("vec")
    rows, width, length = start_block.shape
    slots = hess_tiles.shape[2]
    half = rows // 2
    part = width // 2
    rounds = pairings(peers)
    count = len(rounds)
    full = (rows, width, length)
    halffull = (half, width, length)
    chunk = (rows, part, length)
    halfchunk = (half, part, length)
    packet = (CAP, part, length)
    square = (width, width)
    split_shape = jax.ShapeDtypeStruct((slots, 2, length, length), BF16)

    table = role_table(rounds, peers)
    place = jnp.concatenate(
        [lax.axis_index("vec").reshape(1), table[:, lax.axis_index("res")]]
    ).astype(jnp.int32)

    def own_sum(acc_refs, x_ref, split_ref, rows_ref, cols_ref):
        for s in range(OWN_SLOTS):
            i, j = rows_ref[0, 0, s], cols_ref[0, 0, s]
            direct = tile_product(x_ref[j], split_ref, s, True)
            mirror = tile_product(x_ref[i], split_ref, s, False)
            for n, acc_ref in enumerate(acc_refs):
                acc_ref[i] += direct[n * part : (n + 1) * part]
                acc_ref[j] += mirror[n * part : (n + 1) * part]

    def prepare_body(x_hbm, diag_hbm, tiles_hbm, *refs):
        x_ref, split_ref, a_ref, b_ref, diag_ref, raw_ref, sem = refs
        size = slots // 4
        copies = [
            pltpu.make_async_copy(src, dst, sem.at[n])
            for n, (src, dst) in enumerate([(x_hbm, x_ref), (diag_hbm, diag_ref)])
        ]
        tile_copies = [
            pltpu.make_async_copy(
                tiles_hbm.at[0, 0, pl.ds(n * size, size)], raw_ref.at[pl.ds(n * size, size)], sem.at[2 + n]
            )
            for n in range(4)
        ]
        for c in copies + tile_copies:
            c.start()
        for n in range(4):
            tile_copies[n].wait()
            for s in range(n * size, (n + 1) * size):
                split_ref[s, 0], split_ref[s, 1] = pieces(raw_ref[s], 2)
        for c in copies:
            c.wait()
        first = (lax.axis_index("vec") == 0).astype(F32)
        d = ((diag_ref[...] - SHIFT) * first)[:, None, :]
        a_ref[...] = x_ref[:, :part] * d
        b_ref[...] = x_ref[:, part:] * d

    def own_body(rows_ref, cols_ref, x_ref, split_ref, *refs):
        own_sum(refs[len(refs) // 2 :], x_ref, split_ref, rows_ref, cols_ref)

    def pack(place_ref, rows_ref, counts_ref, asked_refs, x_ref, split_ref, outs):
        for p in range(count):
            role = place_ref[1 + p]

            def put(c, value, p=p):
                for n, ref in enumerate(outs[p]):
                    ref[c] = value[n * part : (n + 1) * part]

            @pl.when(role > 0)
            def _():
                base = OWN_SLOTS + (role - 1) * CAP
                for c in range(CAP):
                    term = tile_product(x_ref[rows_ref[0, 0, base + c]], split_ref, base + c, False)
                    put(c, jnp.where(c < counts_ref[0, 0, role - 1], term, 0.0))

            @pl.when(role < 0)
            def _():
                base = OWN_SLOTS + (-role - 1) * CAP
                for c in range(CAP):
                    put(c, x_ref[asked_refs[p][0, 0, base + c]])

    def send_body(place_ref, rows_ref, counts_ref, *refs):
        asked_refs, (x_ref, split_ref), outs = refs[:count], refs[count : count + 2], refs[count + 2 :]
        pack(
            place_ref, rows_ref, counts_ref, asked_refs, x_ref, split_ref,
            [(outs[p], outs[count + p]) for p in range(count)],
        )

    def settle(place_ref, mine_ref, other_ref, y_ref):
        core = place_ref[0] % 2
        y_ref[pl.ds(core * half, half)] = mine_ref[...]
        y_ref[pl.ds((1 - core) * half, half)] = other_ref[...]

    def resend_body(place_ref, rows_ref, counts_ref, *refs):
        asked_refs = refs[:count]
        mine_ref, other_ref, diag_ref, split_ref, y_ref, acc_ref = refs[count : count + 6]
        outs = refs[count + 6 :]
        settle(place_ref, mine_ref, other_ref, y_ref)
        pack(
            place_ref, rows_ref, counts_ref, asked_refs, y_ref, split_ref,
            [(outs[p],) for p in range(count)],
        )
        first = (place_ref[0] == 0).astype(F32)
        acc_ref[...] = y_ref[...] * ((diag_ref[...] - SHIFT) * first)[:, None, :]

    def join_rounds(members, place_ref, rows_ref, counts_ref, asked_refs, got_refs, split_ref, acc_ref):
        for n, p in enumerate(members):
            role = place_ref[1 + p]

            @pl.when(role > 0)
            def _():
                base = OWN_SLOTS + (role - 1) * CAP
                for c in range(CAP):
                    term = tile_product(got_refs[n][c], split_ref, base + c, True)
                    acc_ref[rows_ref[0, 0, base + c]] += jnp.where(
                        c < counts_ref[0, 0, role - 1], term, 0.0
                    )

            @pl.when(role < 0)
            def _():
                base = OWN_SLOTS + (-role - 1) * CAP
                for c in range(CAP):
                    acc_ref[asked_refs[n][0, 0, base + c]] += got_refs[n][c]

    def join(acc, got, members, last=False):
        size = len(members)

        def body(place_ref, rows_ref, counts_ref, *refs):
            asked_refs, got_refs = refs[:size], refs[size : 2 * size]
            split_ref, prior_ref = refs[2 * size : 2 * size + 2]
            outs = refs[2 * size + 2 :]
            if last:
                keep_ref, give_ref, acc_ref = outs
                acc_ref[...] = prior_ref[...]
            else:
                (acc_ref,) = outs
            join_rounds(
                members, place_ref, rows_ref, counts_ref, asked_refs, got_refs, split_ref, acc_ref
            )
            if last:
                core = place_ref[0] % 2
                keep_ref[...] = acc_ref[pl.ds(core * half, half)]
                give_ref[...] = acc_ref[pl.ds((1 - core) * half, half)]

        out = call(
            body,
            [halfchunk] * 2 if last else [chunk],
            [SMEM] * (3 + size) + [VMEM] * (size + 2),
            [pltpu.VMEM(chunk, F32)] if last else [],
            name="join",
            weight=10**10,
            aliases=None if last else {3 + 2 * size + 1: 0},
        )(
            place, tile_rows, slot_counts, *[asked[p] for p in members], *[got[p] for p in members], split, acc
        )
        return out if last else out[0]

    def gram_body(x_ref, out_ref):
        total = jnp.zeros(square, F32)
        for n in range(0, rows, 2):
            pair = [x_ref[n], x_ref[n + 1]]
            total += gram_step(pair, [pair])
        out_ref[...] = total

    def cross_body(x_ref, a_ref, b_ref, out_ref):
        total = jnp.zeros((width, 2 * width), F32)
        for n in range(0, rows, 2):
            y = [jnp.concatenate([a_ref[m], b_ref[m]], axis=0) for m in (n, n + 1)]
            total += gram_step(y, [[x_ref[n], x_ref[n + 1]], y])
        out_ref[...] = total

    def first_body(gram_ref, inverse_ref):
        _, inverse_ref[...] = factor(gram_ref[...])

    def identity():
        eye = lax.broadcasted_iota(jnp.int32, square, 0) == lax.broadcasted_iota(jnp.int32, square, 1)
        return eye.astype(F32)

    def lower_part():
        return lax.broadcasted_iota(jnp.int32, square, 0) >= lax.broadcasted_iota(jnp.int32, square, 1)

    def second_body(gram_ref, inverse_ref, cross_ref, lower_ref, coef_ref, gain_ref):
        start_inv = inverse_ref[...]
        cross = dot(dot(start_inv, gram_ref[:, :width]), start_inv, tb=True)
        applied = dot(dot(start_inv, gram_ref[:, width:]), start_inv, tb=True)
        upper, inverse = factor(applied - dot(cross, cross, tb=True))
        lower = upper.T
        cross_ref[...] = cross + SHIFT * identity()
        lower_ref[...] = lower
        gain = dot(inverse, start_inv)
        back = -dot(dot(inverse, cross), start_inv)
        gain_ref[...] = gain
        coef_ref[:width, :width] = -dot(lower, start_inv)
        coef_ref[:width, width : 2 * width] = back
        coef_ref[:width, 2 * width :] = gain
        coef_ref[width:, :width] = back
        coef_ref[width:, width : 2 * width] = gain
        coef_ref[width:, 2 * width :] = jnp.zeros(square, F32)

    def blend(side, mine, other, coef):
        def body(place_ref, x_ref, a_ref, b_ref, mine_ref, other_ref, coef_ref, w_ref, q_ref, out_ref, z_ref):
            settle(place_ref, mine_ref, other_ref, z_ref)
            total = jnp.zeros(square, F32)
            for n in range(0, half, 2):
                qs = []
                stacks = [
                    jnp.concatenate([ref[side * half + m] for ref in (x_ref, a_ref, b_ref, z_ref)], axis=0)
                    for m in (n, n + 1)
                ]
                for m, both in zip((n, n + 1), wide_product(coef_ref[:, : 2 * width + part], stacks)):
                    w_ref[m] = both[:width]
                    q_ref[m] = both[width:]
                    qs.append(both[width:])
                total += gram_step(qs, [qs])
            out_ref[...] = total

        return call(
            body,
            [halffull, halffull, square],
            [SMEM] + [VMEM] * 6,
            [pltpu.VMEM(chunk, F32)],
            name="blend",
        )(place, x, y_a, y_b, mine, other, coef)

    def third_body(place_ref, mine_ref, other_ref, gain_ref, *refs):
        prior_refs, q_refs, norm_refs = refs[0:2], refs[2:4], refs[4:6]
        w_ref, out_ref, z_ref = refs[6:]
        settle(place_ref, mine_ref, other_ref, z_ref)
        total = jnp.zeros((width, 2 * width), F32)
        for n in range(0, rows, 2):
            side, m = divmod(n, half)
            ws = []
            for k, w in enumerate(wide_product(gain_ref[:, part:], [z_ref[n], z_ref[n + 1]])):
                w = w + prior_refs[side][m + k]
                w_ref[n + k] = w
                ws.append(w)
            total += gram_step(ws, [[q_refs[side][m], q_refs[side][m + 1]], ws])
        norm = norm_refs[0][...] + norm_refs[1][...]
        out_ref[:width, :width] = total[:, :width]
        out_ref[:width, width:] = jnp.where(lower_part(), total[:, width:], norm)
        out_ref[width:, :] = jnp.zeros((8, 2 * width), F32)
        out_ref[width:, :width] = jnp.broadcast_to(
            jnp.sum(norm * identity(), axis=0, keepdims=True), (8, width)
        )

    def fourth_body(gram_ref, cross_ref, lower_ref, coef_ref):
        cross = gram_ref[:width, :width]
        packed = gram_ref[:width, width:]
        flipped = packed.T
        squares = jnp.where(lower_part(), packed, flipped)
        norm = jnp.where(lower_part(), flipped, packed)
        norm = jnp.where(identity() > 0, gram_ref[width : width + 1, :width], norm)
        taken = cross + SHIFT * (norm - identity())
        mixed = dot(taken, cross, tb=True)
        squared = squares - mixed - mixed.T + dot(dot(taken, norm), taken, tb=True)
        upper, inverse = factor(squared)
        cross_ref[...] = taken + SHIFT * identity()
        lower_ref[...] = upper.T
        scale = math.sqrt(rows * length * peers)
        coef_ref[:, :width] = inverse * scale
        coef_ref[:, width:] = -dot(inverse, taken) * scale

    def last_body(w_ref, low_ref, high_ref, coef_ref, a1_ref, l1_ref, a2_ref, l2_ref, out_ref, pack_ref):
        for n, ref in enumerate((a1_ref, l1_ref, a2_ref, l2_ref)):
            pack_ref[n] = ref[...]
        for n in range(0, rows, 2):
            side, at = divmod(n, half)
            q_ref = (low_ref, high_ref)[side]
            stacks = [jnp.concatenate([w_ref[n + k], q_ref[at + k]], axis=0) for k in range(2)]
            for m, out in zip((n, n + 1), wide_product(coef_ref[...], stacks, 4)):
                out_ref[m] = out

    swap = [(i, i ^ 1) for i in range(lanes)]
    cuts = [count * n // 3 for n in range(4)]
    groups = [list(range(cuts[n], cuts[n + 1])) for n in range(3)]

    def spread(sent):
        return [exchange(s, "res", entry["pairs"]) for s, entry in zip(sent, rounds)]

    def across(mine, *tokens):
        step = 2
        while step < lanes:
            got = lax.ppermute(mine, "vec", [(i, i ^ step) for i in range(lanes)])
            mine = mine + after(got, *tokens)
            step *= 2
        return mine

    def resend(mine, other):
        y, acc, *sent = call(
            resend_body,
            [chunk, chunk] + [packet] * count,
            [SMEM] * (3 + count) + [VMEM] * 4,
            name="resend",
        )(place, tile_rows, slot_counts, *asked, mine, other, diagonal, split)
        return y, acc, spread(sent)

    def own(y, *accs):
        return call(
            own_body,
            [chunk] * len(accs),
            [SMEM] * 2 + [VMEM] * (2 + len(accs)),
            name="own",
            aliases={4 + n: n for n in range(len(accs))},
        )(tile_rows, tile_cols, y, split, *accs)

    asked = [exchange(tile_cols, "res", entry["pairs"]) for entry in rounds]
    x, split, acc_a, acc_b = call(
        prepare_body,
        [full, split_shape, chunk, chunk],
        [HBM] * 3,
        [
            pltpu.VMEM(diagonal.shape, F32),
            pltpu.VMEM((slots, length, length), F32),
            pltpu.SemaphoreType.DMA((6,)),
        ],
        name="prepare",
    )(*[pinned(v) for v in (start_block, diagonal, hess_tiles)])
    sent = call(
        send_body, [packet] * (2 * count), [SMEM] * (3 + count) + [VMEM] * 2, name="send"
    )(place, tile_rows, slot_counts, *asked, x, split)
    got_a = spread(sent[:count])
    sent_b = list(sent[count:])
    acc_a, acc_b = own(x, after(acc_a, sent[0]), acc_b)
    for n in range(2):
        acc_a = join(acc_a, got_a, groups[n])
        acc_a, x, *gated = lax.optimization_barrier((acc_a, x, *[sent_b[p] for p in groups[n]]))
        for p, value in zip(groups[n], gated):
            sent_b[p] = value
        if n == 0:
            (gram,) = call(gram_body, [square], [VMEM], name="gram")(x)
            start_gram = start_sum(gram, "res")
    acc_a = after(acc_a, start_gram)
    keep_a, give_a = join(acc_a, got_a, groups[2], last=True)
    for p in groups[2]:
        sent_b[p] = after(sent_b[p], keep_a)
    got_b = spread(sent_b)

    core = lax.ppermute(give_a, "vec", swap)
    acc_b = join(acc_b, got_b, groups[0])
    mine_a = keep_a + after(core, acc_b)
    (start_inv,) = call(first_body, [square], [VMEM], name="first")(end_sum(start_gram, "res", mine_a))
    acc_b = join(after(acc_b, start_inv), got_b, groups[1])
    mine_a = across(mine_a, acc_b)
    other_a = lax.ppermute(mine_a, "vec", swap)
    keep_b, give_b = join(acc_b, got_b, groups[2], last=True)
    y_a, acc_a, got_a = resend(mine_a, after(other_a, keep_b))

    core = lax.ppermute(give_b, "vec", swap)
    acc_a = join(acc_a, got_a, groups[0])
    mine_b = keep_b + after(core, acc_a)
    (acc_a,) = own(y_a, after(acc_a, mine_b))
    acc_a = join(acc_a, got_a, groups[1])
    mine_b = across(mine_b, acc_a)
    other_b = lax.ppermute(mine_b, "vec", swap)
    keep_a, give_a = join(acc_a, got_a, groups[2], last=True)
    y_b, acc_b, got_b = resend(mine_b, after(other_b, keep_a))

    (gram,) = call(cross_body, [(width, 2 * width)], [VMEM] * 3, name="cross")(x, y_a, y_b)
    core = lax.ppermute(give_a, "vec", swap)
    (acc_b,) = own(y_b, after(acc_b, gram))
    acc_b = join(acc_b, got_b, groups[0])
    mine_a = keep_a + after(core, acc_b)
    cross_gram = start_sum(gram, "res")
    acc_b = join(after(acc_b, cross_gram, mine_a), got_b, groups[1])
    cross_gram = end_sum(cross_gram, "res", acc_b)
    acc_b = after(acc_b, cross_gram)
    mine_a = across(mine_a, acc_b)
    other_a = lax.ppermute(mine_a, "vec", swap)
    keep_b, give_b = join(acc_b, got_b, groups[2], last=True)

    core = lax.ppermute(give_b, "vec", swap)
    mine_b = keep_b + core
    cross1, lower1, coef, gain = call(
        second_body, [square, square, (2 * width, 3 * width), square], [VMEM] * 2, name="second"
    )(after(cross_gram, mine_b), start_inv)
    w_low, q_low, norm_low = blend(0, mine_a, other_a, coef)
    mine_b = across(mine_b, norm_low)
    other_b = lax.ppermute(mine_b, "vec", swap)
    w_high, q_high, norm_high = blend(1, mine_a, other_a, after(coef, mine_b))
    w, gram = call(
        third_body,
        [full, (width + 8, 2 * width)],
        [SMEM] + [VMEM] * 9,
        [pltpu.VMEM(chunk, F32)],
        name="third",
    )(place, mine_b, after(other_b, norm_high), gain, w_low, w_high, q_low, q_high, norm_low, norm_high)
    gram = all_sum(gram, "res")
    cross2, lower2, coef = call(
        fourth_body, [square, square, (width, 2 * width)], [VMEM], name="fourth"
    )(gram)
    return call(last_body, [full, (4, width, width)], [VMEM] * 8, name="last")(
        w, q_low, q_high, coef, cross1, lower1, cross2, lower2
    )


def solution(mesh):
    in_specs = (
        P(("conf", "res"), None, None),
        P(("conf", "res"), None),
        P(("conf", "res"), "vec", None, None, None),
        P(("conf", "res"), "vec", None),
        P(("conf", "res"), "vec", None),
        P(("conf", "res"), "vec", None),
    )
    out_specs = (P(("conf", "res"), None, None), P("conf", None, None))
    return jax.shard_map(local, mesh=mesh, in_specs=in_specs, out_specs=out_specs, check_vma=False)
```

```python
import math

import jax
import jax.numpy as jnp
from jax import lax
from jax.experimental import pallas as pl
from jax.experimental.pallas import tpu as pltpu
from jax.sharding import PartitionSpec as P

OWN_SLOTS = 20
HOPS = 3
CAP = 8
SHIFT = 1.65
BF16 = jnp.bfloat16
F32 = jnp.float32

VMEM = pl.BlockSpec(memory_space=pltpu.VMEM)
SMEM = pl.BlockSpec(memory_space=pltpu.SMEM)
HBM = pl.BlockSpec(memory_space=pltpu.HBM)


def contract(a, b, ta=False, tb=False, precision=None):
    dims = (((0 if ta else 1,), (1 if tb else 0,)), ((), ()))
    return lax.dot_general(a, b, dims, precision=precision, preferred_element_type=F32)


def dot(a, b, ta=False, tb=False):
    return contract(a, b, ta, tb, lax.Precision.HIGHEST)


def pieces(x, count):
    out = []
    for _ in range(count):
        out.append(x.astype(BF16))
        x = x - out[-1].astype(F32)
    return out


def tile_product(x, tile_ref, slot, transposed):
    x1, x2 = pieces(x, 2)
    m1, m2 = tile_ref[slot, 0], tile_ref[slot, 1]
    axis = 1 if transposed else 0
    left = jnp.concatenate([x1, x2, x1], axis=1)
    return contract(left, jnp.concatenate([m1, m1, m2], axis=axis), tb=transposed)


def wide_product(coef, blocks, terms=6):
    pairs = [(0, 0), (0, 1), (1, 0), (1, 1)] if terms == 4 else [(0, 0), (0, 1), (0, 2), (1, 0), (1, 1), (2, 0)]
    c = pieces(coef, terms // 2)
    z = pieces(jnp.concatenate(blocks, axis=1), terms // 2)
    left = jnp.concatenate([c[m] for m, _ in pairs], axis=1)
    out = contract(left, jnp.concatenate([z[m] for _, m in pairs], axis=0))
    width = blocks[0].shape[1]
    return [out[:, n * width : (n + 1) * width] for n in range(len(blocks))]


def gram_step(left, right):
    a = jnp.concatenate(pieces(jnp.concatenate(left, axis=1), 2), axis=0)
    b = jnp.concatenate(
        [p for group in right for p in pieces(jnp.concatenate(group, axis=1), 2)], axis=0
    )
    out = contract(a, b, tb=True)
    size = left[0].shape[0]
    out = out[:size] + out[size:]
    return jnp.concatenate(
        [
            out[:, 2 * g * size : (2 * g + 1) * size] + out[:, (2 * g + 1) * size : (2 * g + 2) * size]
            for g in range(len(right))
        ],
        axis=1,
    )


def call(body, outs, in_specs, scratch=(), name=None, aliases=None, weight=0):
    shapes = [
        o if isinstance(o, jax.ShapeDtypeStruct) else jax.ShapeDtypeStruct(o, F32) for o in outs
    ]
    return pl.pallas_call(
        body,
        out_shape=shapes,
        in_specs=in_specs,
        out_specs=[VMEM] * len(outs),
        scratch_shapes=list(scratch),
        compiler_params=pltpu.CompilerParams(vmem_limit_bytes=40 << 20),
        input_output_aliases=aliases or {},
        cost_estimate=pl.CostEstimate(flops=weight, bytes_accessed=weight, transcendentals=0) if weight else None,
        name=name,
    )


def pinned(value):
    return pltpu.with_memory_space_constraint(value, pltpu.HBM)


def after(value, *tokens):
    return lax.optimization_barrier((value,) + tokens)[0]


def pairings(size):
    rounds = []
    for hop in range(1, HOPS + 1):
        for parity in range(2):
            pairs = [(i, i + hop) for i in range(size - hop) if (i // hop) % 2 == parity]
            if not pairs:
                continue
            used = {i for pair in pairs for i in pair}
            for entry in rounds:
                if not entry["used"] & used:
                    entry["used"] |= used
                    entry["pairs"] += pairs
                    entry["kinds"].append((hop, parity))
                    break
            else:
                rounds.append({"used": used, "pairs": pairs, "kinds": [(hop, parity)]})
    return rounds


def exchange(block, axis, pairs):
    return lax.ppermute(block, axis, [(a, b) for a, b in pairs] + [(b, a) for a, b in pairs])


def role_table(rounds, size):
    table = [[0] * size for _ in rounds]
    for p, entry in enumerate(rounds):
        for a, b in entry["pairs"]:
            table[p][a] = b - a
            table[p][b] = a - b
    return jnp.array(table, jnp.int32)


def sum_steps(size):
    return [1 << n for n in range(size.bit_length() - 1)]


def start_sum(block, axis):
    size = lax.axis_size(axis)
    if size & (size - 1):
        return block
    for step in sum_steps(size)[:-1]:
        block = block + lax.ppermute(block, axis, [(i, i ^ step) for i in range(size)])
    return block


def end_sum(block, axis, *tokens):
    size = lax.axis_size(axis)
    if size & (size - 1):
        return lax.psum(block, axis)
    for step in sum_steps(size)[-1:]:
        got = lax.ppermute(block, axis, [(i, i ^ step) for i in range(size)])
        block = block + (after(got, *tokens) if tokens else got)
    return block


def all_sum(block, axis, *tokens):
    return end_sum(start_sum(block, axis), axis, *tokens)


def factor(gram):
    size = gram.shape[0]
    tile = (8, 2 * size)
    row_id = lax.broadcasted_iota(jnp.int32, (size, size), 0)
    col_id = lax.broadcasted_iota(jnp.int32, (size, size), 1)
    work = jnp.concatenate([gram, (row_id == col_id).astype(F32)], axis=1)
    blocks = [work[8 * b : 8 * b + 8] for b in range(size // 8)]
    sub = lax.broadcasted_iota(jnp.int32, tile, 0)
    for j in range(0, size, 4):
        b, s = divmod(j, 8)
        later = range(b + s // 4, size // 8)
        line = [jnp.broadcast_to(blocks[b][s + k : s + k + 1], tile) for k in range(4)]
        cols = {
            o: [jnp.broadcast_to(blocks[o][:, j + k : j + k + 1], tile) for k in range(4)]
            for o in range(b, size // 8)
        }
        entry = {
            (k, l): jnp.broadcast_to(cols[b][l][s + k : s + k + 1], tile)
            for k in range(4)
            for l in range(k, 4)
        }
        scaled = []
        for k in range(4):
            inverse = 1.0 / entry[k, k]
            for l in range(k + 1, 4):
                ratio = entry[k, l] * inverse
                for p in range(l, 4):
                    entry[l, p] = entry[l, p] - ratio * entry[k, p]
                line[l] = line[l] - ratio * line[k]
                for o in later:
                    cols[o][l] = cols[o][l] - ratio * cols[o][k]
            scaled.append(inverse * line[k])
        for o in range(b, size // 8):
            new = blocks[o]
            if o in later:
                new = new - ((cols[o][0] * scaled[0] + cols[o][1] * scaled[1]) + (cols[o][2] * scaled[2] + cols[o][3] * scaled[3]))
            if o == b:
                new = jnp.where(sub > s + 3, new, blocks[o])
                for k in range(1, 4):
                    new = jnp.where(sub == s + k, line[k], new)
            blocks[o] = new
    work = jnp.concatenate(blocks, axis=0)
    pivots = jnp.sum(jnp.where(row_id == col_id, work[:, :size], 0.0), axis=1, keepdims=True)
    work = work / jnp.sqrt(pivots)
    upper = jnp.where(col_id >= row_id, work[:, :size], 0.0)
    inverse = jnp.where(col_id <= row_id, work[:, size:], 0.0)
    return upper, inverse


def local(start_block, diagonal, hess_tiles, tile_rows, tile_cols, slot_counts):
    peers = lax.axis_size("res")
    lanes = lax.axis_size("vec")
    rows, width, length = start_block.shape
    slots = hess_tiles.shape[2]
    half = rows // 2
    part = width // 2
    rounds = pairings(peers)
    count = len(rounds)
    full = (rows, width, length)
    halffull = (half, width, length)
    chunk = (rows, part, length)
    halfchunk = (half, part, length)
    packet = (CAP, part, length)
    square = (width, width)
    split_shape = jax.ShapeDtypeStruct((slots, 2, length, length), BF16)

    table = role_table(rounds, peers)
    place = jnp.concatenate(
        [lax.axis_index("vec").reshape(1), table[:, lax.axis_index("res")]]
    ).astype(jnp.int32)

    def own_sum(acc_refs, x_ref, split_ref, rows_ref, cols_ref):
        for s in range(OWN_SLOTS):
            i, j = rows_ref[0, 0, s], cols_ref[0, 0, s]
            direct = tile_product(x_ref[j], split_ref, s, True)
            mirror = tile_product(x_ref[i], split_ref, s, False)
            for n, acc_ref in enumerate(acc_refs):
                acc_ref[i] += direct[n * part : (n + 1) * part]
                acc_ref[j] += mirror[n * part : (n + 1) * part]

    def prepare_body(x_hbm, diag_hbm, tiles_hbm, *refs):
        x_ref, split_ref, a_ref, b_ref, diag_ref, raw_ref, sem = refs
        size = slots // 4
        copies = [
            pltpu.make_async_copy(src, dst, sem.at[n])
            for n, (src, dst) in enumerate([(x_hbm, x_ref), (diag_hbm, diag_ref)])
        ]
        tile_copies = [
            pltpu.make_async_copy(
                tiles_hbm.at[0, 0, pl.ds(n * size, size)], raw_ref.at[pl.ds(n * size, size)], sem.at[2 + n]
            )
            for n in range(4)
        ]
        for c in copies + tile_copies:
            c.start()
        for n in range(4):
            tile_copies[n].wait()
            for s in range(n * size, (n + 1) * size):
                split_ref[s, 0], split_ref[s, 1] = pieces(raw_ref[s], 2)
        for c in copies:
            c.wait()
        first = (lax.axis_index("vec") == 0).astype(F32)
        d = ((diag_ref[...] - SHIFT) * first)[:, None, :]
        a_ref[...] = x_ref[:, :part] * d
        b_ref[...] = x_ref[:, part:] * d

    def own_body(rows_ref, cols_ref, x_ref, split_ref, *refs):
        own_sum(refs[len(refs) // 2 :], x_ref, split_ref, rows_ref, cols_ref)

    def pack(place_ref, rows_ref, counts_ref, asked_refs, x_ref, split_ref, outs):
        for p in range(count):
            role = place_ref[1 + p]

            def put(c, value, p=p):
                for n, ref in enumerate(outs[p]):
                    ref[c] = value[n * part : (n + 1) * part]

            @pl.when(role > 0)
            def _():
                base = OWN_SLOTS + (role - 1) * CAP
                for c in range(CAP):
                    term = tile_product(x_ref[rows_ref[0, 0, base + c]], split_ref, base + c, False)
                    put(c, jnp.where(c < counts_ref[0, 0, role - 1], term, 0.0))

            @pl.when(role < 0)
            def _():
                base = OWN_SLOTS + (-role - 1) * CAP
                for c in range(CAP):
                    put(c, x_ref[asked_refs[p][0, 0, base + c]])

    def send_body(place_ref, rows_ref, counts_ref, *refs):
        asked_refs, (x_ref, split_ref), outs = refs[:count], refs[count : count + 2], refs[count + 2 :]
        pack(
            place_ref, rows_ref, counts_ref, asked_refs, x_ref, split_ref,
            [(outs[p], outs[count + p]) for p in range(count)],
        )

    def settle(place_ref, mine_ref, other_ref, y_ref):
        core = place_ref[0] % 2
        y_ref[pl.ds(core * half, half)] = mine_ref[...]
        y_ref[pl.ds((1 - core) * half, half)] = other_ref[...]

    def resend_body(place_ref, rows_ref, counts_ref, *refs):
        asked_refs = refs[:count]
        mine_ref, other_ref, diag_ref, split_ref, y_ref, acc_ref = refs[count : count + 6]
        outs = refs[count + 6 :]
        settle(place_ref, mine_ref, other_ref, y_ref)
        pack(
            place_ref, rows_ref, counts_ref, asked_refs, y_ref, split_ref,
            [(outs[p],) for p in range(count)],
        )
        first = (place_ref[0] == 0).astype(F32)
        acc_ref[...] = y_ref[...] * ((diag_ref[...] - SHIFT) * first)[:, None, :]

    def join_rounds(members, place_ref, rows_ref, counts_ref, asked_refs, got_refs, split_ref, acc_ref):
        for n, p in enumerate(members):
            role = place_ref[1 + p]

            @pl.when(role > 0)
            def _():
                base = OWN_SLOTS + (role - 1) * CAP
                for c in range(CAP):
                    term = tile_product(got_refs[n][c], split_ref, base + c, True)
                    acc_ref[rows_ref[0, 0, base + c]] += jnp.where(
                        c < counts_ref[0, 0, role - 1], term, 0.0
                    )

            @pl.when(role < 0)
            def _():
                base = OWN_SLOTS + (-role - 1) * CAP
                for c in range(CAP):
                    acc_ref[asked_refs[n][0, 0, base + c]] += got_refs[n][c]

    def join(acc, got, members, last=False):
        size = len(members)

        def body(place_ref, rows_ref, counts_ref, *refs):
            asked_refs, got_refs = refs[:size], refs[size : 2 * size]
            split_ref, prior_ref = refs[2 * size : 2 * size + 2]
            outs = refs[2 * size + 2 :]
            if last:
                keep_ref, give_ref, acc_ref = outs
                acc_ref[...] = prior_ref[...]
            else:
                (acc_ref,) = outs
            join_rounds(
                members, place_ref, rows_ref, counts_ref, asked_refs, got_refs, split_ref, acc_ref
            )
            if last:
                core = place_ref[0] % 2
                keep_ref[...] = acc_ref[pl.ds(core * half, half)]
                give_ref[...] = acc_ref[pl.ds((1 - core) * half, half)]

        out = call(
            body,
            [halfchunk] * 2 if last else [chunk],
            [SMEM] * (3 + size) + [VMEM] * (size + 2),
            [pltpu.VMEM(chunk, F32)] if last else [],
            name="join",
            weight=10**10,
            aliases=None if last else {3 + 2 * size + 1: 0},
        )(
            place, tile_rows, slot_counts, *[asked[p] for p in members], *[got[p] for p in members], split, acc
        )
        return out if last else out[0]

    def gram_body(x_ref, out_ref):
        total = jnp.zeros(square, F32)
        for n in range(0, rows, 2):
            pair = [x_ref[n], x_ref[n + 1]]
            total += gram_step(pair, [pair])
        out_ref[...] = total

    def cross_body(x_ref, a_ref, b_ref, out_ref):
        total = jnp.zeros((width, 2 * width), F32)
        for n in range(0, rows, 2):
            y = [jnp.concatenate([a_ref[m], b_ref[m]], axis=0) for m in (n, n + 1)]
            total += gram_step(y, [[x_ref[n], x_ref[n + 1]], y])
        out_ref[...] = total

    def first_body(gram_ref, inverse_ref):
        _, inverse_ref[...] = factor(gram_ref[...])

    def identity():
        eye = lax.broadcasted_iota(jnp.int32, square, 0) == lax.broadcasted_iota(jnp.int32, square, 1)
        return eye.astype(F32)

    def lower_part():
        return lax.broadcasted_iota(jnp.int32, square, 0) >= lax.broadcasted_iota(jnp.int32, square, 1)

    def second_body(gram_ref, inverse_ref, cross_ref, lower_ref, coef_ref, gain_ref):
        start_inv = inverse_ref[...]
        cross = dot(dot(start_inv, gram_ref[:, :width]), start_inv, tb=True)
        applied = dot(dot(start_inv, gram_ref[:, width:]), start_inv, tb=True)
        upper, inverse = factor(applied - dot(cross, cross, tb=True))
        lower = upper.T
        cross_ref[...] = cross + SHIFT * identity()
        lower_ref[...] = lower
        gain = dot(inverse, start_inv)
        back = -dot(dot(inverse, cross), start_inv)
        gain_ref[...] = gain
        coef_ref[:width, :width] = -dot(lower, start_inv)
        coef_ref[:width, width : 2 * width] = back
        coef_ref[:width, 2 * width :] = gain
        coef_ref[width:, :width] = back
        coef_ref[width:, width : 2 * width] = gain
        coef_ref[width:, 2 * width :] = jnp.zeros(square, F32)

    def blend(side, mine, other, coef):
        def body(place_ref, x_ref, a_ref, b_ref, mine_ref, other_ref, coef_ref, w_ref, q_ref, out_ref, z_ref):
            settle(place_ref, mine_ref, other_ref, z_ref)
            total = jnp.zeros(square, F32)
            for n in range(0, half, 2):
                qs = []
                stacks = [
                    jnp.concatenate([ref[side * half + m] for ref in (x_ref, a_ref, b_ref, z_ref)], axis=0)
                    for m in (n, n + 1)
                ]
                for m, both in zip((n, n + 1), wide_product(coef_ref[:, : 2 * width + part], stacks)):
                    w_ref[m] = both[:width]
                    q_ref[m] = both[width:]
                    qs.append(both[width:])
                total += gram_step(qs, [qs])
            out_ref[...] = total

        return call(
            body,
            [halffull, halffull, square],
            [SMEM] + [VMEM] * 6,
            [pltpu.VMEM(chunk, F32)],
            name="blend",
        )(place, x, y_a, y_b, mine, other, coef)

    def third_body(place_ref, mine_ref, other_ref, gain_ref, *refs):
        prior_refs, q_refs, norm_refs = refs[0:2], refs[2:4], refs[4:6]
        w_ref, out_ref, z_ref = refs[6:]
        settle(place_ref, mine_ref, other_ref, z_ref)
        total = jnp.zeros((width, 2 * width), F32)
        for n in range(0, rows, 2):
            side, m = divmod(n, half)
            ws = []
            for k, w in enumerate(wide_product(gain_ref[:, part:], [z_ref[n], z_ref[n + 1]])):
                w = w + prior_refs[side][m + k]
                w_ref[n + k] = w
                ws.append(w)
            total += gram_step(ws, [[q_refs[side][m], q_refs[side][m + 1]], ws])
        norm = norm_refs[0][...] + norm_refs[1][...]
        out_ref[:width, :width] = total[:, :width]
        out_ref[:width, width:] = jnp.where(lower_part(), total[:, width:], norm)
        out_ref[width:, :] = jnp.zeros((8, 2 * width), F32)
        out_ref[width:, :width] = jnp.broadcast_to(
            jnp.sum(norm * identity(), axis=0, keepdims=True), (8, width)
        )

    def fourth_body(gram_ref, cross_ref, lower_ref, coef_ref):
        cross = gram_ref[:width, :width]
        packed = gram_ref[:width, width:]
        flipped = packed.T
        squares = jnp.where(lower_part(), packed, flipped)
        norm = jnp.where(lower_part(), flipped, packed)
        norm = jnp.where(identity() > 0, gram_ref[width : width + 1, :width], norm)
        taken = cross + SHIFT * (norm - identity())
        mixed = dot(taken, cross, tb=True)
        squared = squares - mixed - mixed.T + dot(dot(taken, norm), taken, tb=True)
        upper, inverse = factor(squared)
        cross_ref[...] = taken + SHIFT * identity()
        lower_ref[...] = upper.T
        scale = math.sqrt(rows * length * peers)
        coef_ref[:, :width] = inverse * scale
        coef_ref[:, width:] = -dot(inverse, taken) * scale

    def last_body(w_ref, low_ref, high_ref, coef_ref, a1_ref, l1_ref, a2_ref, l2_ref, out_ref, pack_ref):
        for n, ref in enumerate((a1_ref, l1_ref, a2_ref, l2_ref)):
            pack_ref[n] = ref[...]
        for n in range(0, rows, 2):
            side, at = divmod(n, half)
            q_ref = (low_ref, high_ref)[side]
            stacks = [jnp.concatenate([w_ref[n + k], q_ref[at + k]], axis=0) for k in range(2)]
            for m, out in zip((n, n + 1), wide_product(coef_ref[...], stacks, 4)):
                out_ref[m] = out

    swap = [(i, i ^ 1) for i in range(lanes)]
    cuts = [count * n // 3 for n in range(4)]
    groups = [list(range(cuts[n], cuts[n + 1])) for n in range(3)]

    def spread(sent):
        return [exchange(s, "res", entry["pairs"]) for s, entry in zip(sent, rounds)]

    def across(mine, *tokens):
        step = 2
        while step < lanes:
            got = lax.ppermute(mine, "vec", [(i, i ^ step) for i in range(lanes)])
            mine = mine + after(got, *tokens)
            step *= 2
        return mine

    def resend(mine, other):
        y, acc, *sent = call(
            resend_body,
            [chunk, chunk] + [packet] * count,
            [SMEM] * (3 + count) + [VMEM] * 4,
            name="resend",
        )(place, tile_rows, slot_counts, *asked, mine, other, diagonal, split)
        return y, acc, spread(sent)

    def own(y, *accs):
        return call(
            own_body,
            [chunk] * len(accs),
            [SMEM] * 2 + [VMEM] * (2 + len(accs)),
            name="own",
            aliases={4 + n: n for n in range(len(accs))},
        )(tile_rows, tile_cols, y, split, *accs)

    asked = [exchange(tile_cols, "res", entry["pairs"]) for entry in rounds]
    x, split, acc_a, acc_b = call(
        prepare_body,
        [full, split_shape, chunk, chunk],
        [HBM] * 3,
        [
            pltpu.VMEM(diagonal.shape, F32),
            pltpu.VMEM((slots, length, length), F32),
            pltpu.SemaphoreType.DMA((6,)),
        ],
        name="prepare",
    )(*[pinned(v) for v in (start_block, diagonal, hess_tiles)])
    sent = call(
        send_body, [packet] * (2 * count), [SMEM] * (3 + count) + [VMEM] * 2, name="send"
    )(place, tile_rows, slot_counts, *asked, x, split)
    got_a = spread(sent[:count])
    sent_b = list(sent[count:])
    acc_a, acc_b = own(x, after(acc_a, sent[0]), acc_b)
    for n in range(2):
        acc_a = join(acc_a, got_a, groups[n])
        acc_a, x, *gated = lax.optimization_barrier((acc_a, x, *[sent_b[p] for p in groups[n]]))
        for p, value in zip(groups[n], gated):
            sent_b[p] = value
        if n == 0:
            (gram,) = call(gram_body, [square], [VMEM], name="gram")(x)
            start_gram = start_sum(gram, "res")
    acc_a = after(acc_a, start_gram)
    keep_a, give_a = join(acc_a, got_a, groups[2], last=True)
    for p in groups[2]:
        sent_b[p] = after(sent_b[p], keep_a)
    got_b = spread(sent_b)

    core = lax.ppermute(give_a, "vec", swap)
    acc_b = join(acc_b, got_b, groups[0])
    mine_a = keep_a + after(core, acc_b)
    (start_inv,) = call(first_body, [square], [VMEM], name="first")(end_sum(start_gram, "res", mine_a))
    acc_b = join(after(acc_b, start_inv), got_b, groups[1])
    mine_a = across(mine_a, acc_b)
    other_a = lax.ppermute(mine_a, "vec", swap)
    keep_b, give_b = join(acc_b, got_b, groups[2], last=True)
    y_a, acc_a, got_a = resend(mine_a, after(other_a, keep_b))

    core = lax.ppermute(give_b, "vec", swap)
    mine_b = keep_b + after(core, y_a)
    acc_a = join(after(acc_a, mine_b), got_a, groups[2])
    (acc_a,) = own(y_a, acc_a)
    acc_a = join(acc_a, got_a, groups[1])
    mine_b = across(mine_b, acc_a)
    other_b = lax.ppermute(mine_b, "vec", swap)
    keep_a, give_a = join(acc_a, got_a, groups[0], last=True)
    y_b, acc_b, got_b = resend(mine_b, after(other_b, keep_a))

    core = lax.ppermute(give_a, "vec", swap)
    mine_a = keep_a + after(core, y_b)
    acc_b = join(after(acc_b, mine_a), got_b, groups[2])
    (acc_b,) = own(y_b, acc_b)
    acc_b = join(acc_b, got_b, groups[1])
    (gram,) = call(cross_body, [(width, 2 * width)], [VMEM] * 3, name="cross")(x, y_a, after(y_b, acc_b))
    cross_gram = start_sum(gram, "res")
    mine_a = across(mine_a, gram)
    other_a = lax.ppermute(mine_a, "vec", swap)
    keep_b, give_b = join(after(acc_b, cross_gram), got_b, groups[0], last=True)

    core = lax.ppermute(give_b, "vec", swap)
    cross_gram = end_sum(cross_gram, "res")
    mine_b = keep_b + after(core, cross_gram)
    cross1, lower1, coef, gain = call(
        second_body, [square, square, (2 * width, 3 * width), square], [VMEM] * 2, name="second"
    )(after(cross_gram, mine_b), start_inv)
    w_low, q_low, norm_low = blend(0, mine_a, other_a, coef)
    mine_b = across(mine_b, norm_low)
    other_b = lax.ppermute(mine_b, "vec", swap)
    w_high, q_high, norm_high = blend(1, mine_a, other_a, after(coef, mine_b))
    w, gram = call(
        third_body,
        [full, (width + 8, 2 * width)],
        [SMEM] + [VMEM] * 9,
        [pltpu.VMEM(chunk, F32)],
        name="third",
    )(place, mine_b, after(other_b, norm_high), gain, w_low, w_high, q_low, q_high, norm_low, norm_high)
    gram = all_sum(gram, "res")
    cross2, lower2, coef = call(
        fourth_body, [square, square, (width, 2 * width)], [VMEM], name="fourth"
    )(gram)
    return call(last_body, [full, (4, width, width)], [VMEM] * 8, name="last")(
        w, q_low, q_high, coef, cross1, lower1, cross2, lower2
    )


def solution(mesh):
    in_specs = (
        P(("conf", "res"), None, None),
        P(("conf", "res"), None),
        P(("conf", "res"), "vec", None, None, None),
        P(("conf", "res"), "vec", None),
        P(("conf", "res"), "vec", None),
        P(("conf", "res"), "vec", None),
    )
    out_specs = (P(("conf", "res"), None, None), P("conf", None, None))
    return jax.shard_map(local, mesh=mesh, in_specs=in_specs, out_specs=out_specs, check_vma=False)
```

```python
import math

import jax
import jax.numpy as jnp
from jax import lax
from jax.experimental import pallas as pl
from jax.experimental.pallas import tpu as pltpu
from jax.sharding import PartitionSpec as P

OWN_SLOTS = 20
HOPS = 3
CAP = 8
SHIFT = 1.65
BF16 = jnp.bfloat16
F32 = jnp.float32

VMEM = pl.BlockSpec(memory_space=pltpu.VMEM)
SMEM = pl.BlockSpec(memory_space=pltpu.SMEM)
HBM = pl.BlockSpec(memory_space=pltpu.HBM)


def contract(a, b, ta=False, tb=False, precision=None):
    dims = (((0 if ta else 1,), (1 if tb else 0,)), ((), ()))
    return lax.dot_general(a, b, dims, precision=precision, preferred_element_type=F32)


def dot(a, b, ta=False, tb=False):
    return contract(a, b, ta, tb, lax.Precision.HIGHEST)


def pieces(x, count):
    out = []
    for _ in range(count):
        out.append(x.astype(BF16))
        x = x - out[-1].astype(F32)
    return out


def tile_product(x, tile_ref, slot, transposed):
    x1, x2 = pieces(x, 2)
    m1, m2 = tile_ref[slot, 0], tile_ref[slot, 1]
    axis = 1 if transposed else 0
    left = jnp.concatenate([x1, x2, x1], axis=1)
    return contract(left, jnp.concatenate([m1, m1, m2], axis=axis), tb=transposed)


def wide_product(coef, blocks, terms=6):
    pairs = [(0, 0), (0, 1), (1, 0), (1, 1)] if terms == 4 else [(0, 0), (0, 1), (0, 2), (1, 0), (1, 1), (2, 0)]
    c = pieces(coef, terms // 2)
    z = pieces(jnp.concatenate(blocks, axis=1), terms // 2)
    left = jnp.concatenate([c[m] for m, _ in pairs], axis=1)
    out = contract(left, jnp.concatenate([z[m] for _, m in pairs], axis=0))
    width = blocks[0].shape[1]
    return [out[:, n * width : (n + 1) * width] for n in range(len(blocks))]


def gram_step(left, right):
    a = jnp.concatenate(pieces(jnp.concatenate(left, axis=1), 2), axis=0)
    b = jnp.concatenate(
        [p for group in right for p in pieces(jnp.concatenate(group, axis=1), 2)], axis=0
    )
    out = contract(a, b, tb=True)
    size = left[0].shape[0]
    out = out[:size] + out[size:]
    return jnp.concatenate(
        [
            out[:, 2 * g * size : (2 * g + 1) * size] + out[:, (2 * g + 1) * size : (2 * g + 2) * size]
            for g in range(len(right))
        ],
        axis=1,
    )


def call(body, outs, in_specs, scratch=(), name=None, aliases=None, weight=0):
    shapes = [
        o if isinstance(o, jax.ShapeDtypeStruct) else jax.ShapeDtypeStruct(o, F32) for o in outs
    ]
    return pl.pallas_call(
        body,
        out_shape=shapes,
        in_specs=in_specs,
        out_specs=[VMEM] * len(outs),
        scratch_shapes=list(scratch),
        compiler_params=pltpu.CompilerParams(vmem_limit_bytes=40 << 20),
        input_output_aliases=aliases or {},
        cost_estimate=pl.CostEstimate(flops=weight, bytes_accessed=weight, transcendentals=0) if weight else None,
        name=name,
    )


def pinned(value):
    return pltpu.with_memory_space_constraint(value, pltpu.HBM)


def after(value, *tokens):
    return lax.optimization_barrier((value,) + tokens)[0]


def pairings(size):
    rounds = []
    for hop in range(1, HOPS + 1):
        for parity in range(2):
            pairs = [(i, i + hop) for i in range(size - hop) if (i // hop) % 2 == parity]
            if not pairs:
                continue
            used = {i for pair in pairs for i in pair}
            for entry in rounds:
                if not entry["used"] & used:
                    entry["used"] |= used
                    entry["pairs"] += pairs
                    entry["kinds"].append((hop, parity))
                    break
            else:
                rounds.append({"used": used, "pairs": pairs, "kinds": [(hop, parity)]})
    return rounds


def exchange(block, axis, pairs):
    return lax.ppermute(block, axis, [(a, b) for a, b in pairs] + [(b, a) for a, b in pairs])


def role_table(rounds, size):
    table = [[0] * size for _ in rounds]
    for p, entry in enumerate(rounds):
        for a, b in entry["pairs"]:
            table[p][a] = b - a
            table[p][b] = a - b
    return jnp.array(table, jnp.int32)


def sum_steps(size):
    return [1 << n for n in range(size.bit_length() - 1)]


def start_sum(block, axis):
    size = lax.axis_size(axis)
    if size & (size - 1):
        return block
    for step in sum_steps(size)[:-1]:
        block = block + lax.ppermute(block, axis, [(i, i ^ step) for i in range(size)])
    return block


def end_sum(block, axis, *tokens):
    size = lax.axis_size(axis)
    if size & (size - 1):
        return lax.psum(block, axis)
    for step in sum_steps(size)[-1:]:
        got = lax.ppermute(block, axis, [(i, i ^ step) for i in range(size)])
        block = block + (after(got, *tokens) if tokens else got)
    return block


def all_sum(block, axis, *tokens):
    return end_sum(start_sum(block, axis), axis, *tokens)


def factor(gram):
    size = gram.shape[0]
    tile = (8, 2 * size)
    row_id = lax.broadcasted_iota(jnp.int32, (size, size), 0)
    col_id = lax.broadcasted_iota(jnp.int32, (size, size), 1)
    work = jnp.concatenate([gram, (row_id == col_id).astype(F32)], axis=1)
    blocks = [work[8 * b : 8 * b + 8] for b in range(size // 8)]
    sub = lax.broadcasted_iota(jnp.int32, tile, 0)
    for j in range(0, size, 4):
        b, s = divmod(j, 8)
        later = range(b + s // 4, size // 8)
        line = [jnp.broadcast_to(blocks[b][s + k : s + k + 1], tile) for k in range(4)]
        cols = {
            o: [jnp.broadcast_to(blocks[o][:, j + k : j + k + 1], tile) for k in range(4)]
            for o in range(b, size // 8)
        }
        entry = {
            (k, l): jnp.broadcast_to(cols[b][l][s + k : s + k + 1], tile)
            for k in range(4)
            for l in range(k, 4)
        }
        scaled = []
        for k in range(4):
            inverse = 1.0 / entry[k, k]
            for l in range(k + 1, 4):
                ratio = entry[k, l] * inverse
                for p in range(l, 4):
                    entry[l, p] = entry[l, p] - ratio * entry[k, p]
                line[l] = line[l] - ratio * line[k]
                for o in later:
                    cols[o][l] = cols[o][l] - ratio * cols[o][k]
            scaled.append(inverse * line[k])
        for o in range(b, size // 8):
            new = blocks[o]
            if o in later:
                new = new - ((cols[o][0] * scaled[0] + cols[o][1] * scaled[1]) + (cols[o][2] * scaled[2] + cols[o][3] * scaled[3]))
            if o == b:
                new = jnp.where(sub > s + 3, new, blocks[o])
                for k in range(1, 4):
                    new = jnp.where(sub == s + k, line[k], new)
            blocks[o] = new
    work = jnp.concatenate(blocks, axis=0)
    pivots = jnp.sum(jnp.where(row_id == col_id, work[:, :size], 0.0), axis=1, keepdims=True)
    work = work / jnp.sqrt(pivots)
    upper = jnp.where(col_id >= row_id, work[:, :size], 0.0)
    inverse = jnp.where(col_id <= row_id, work[:, size:], 0.0)
    return upper, inverse


def local(start_block, diagonal, hess_tiles, tile_rows, tile_cols, slot_counts):
    peers = lax.axis_size("res")
    lanes = lax.axis_size("vec")
    rows, width, length = start_block.shape
    slots = hess_tiles.shape[2]
    half = rows // 2
    part = width // 2
    rounds = pairings(peers)
    count = len(rounds)
    full = (rows, width, length)
    halffull = (half, width, length)
    chunk = (rows, part, length)
    halfchunk = (half, part, length)
    packet = (CAP, part, length)
    square = (width, width)
    split_shape = jax.ShapeDtypeStruct((slots, 2, length, length), BF16)

    table = role_table(rounds, peers)
    place = jnp.concatenate(
        [lax.axis_index("vec").reshape(1), table[:, lax.axis_index("res")]]
    ).astype(jnp.int32)

    def own_sum(acc_refs, x_ref, split_ref, rows_ref, cols_ref):
        for s in range(OWN_SLOTS):
            i, j = rows_ref[0, 0, s], cols_ref[0, 0, s]
            direct = tile_product(x_ref[j], split_ref, s, True)
            mirror = tile_product(x_ref[i], split_ref, s, False)
            for n, acc_ref in enumerate(acc_refs):
                acc_ref[i] += direct[n * part : (n + 1) * part]
                acc_ref[j] += mirror[n * part : (n + 1) * part]

    def prepare_body(x_hbm, diag_hbm, tiles_hbm, *refs):
        x_ref, split_ref, a_ref, b_ref, diag_ref, raw_ref, sem = refs
        size = slots // 4
        copies = [
            pltpu.make_async_copy(src, dst, sem.at[n])
            for n, (src, dst) in enumerate([(x_hbm, x_ref), (diag_hbm, diag_ref)])
        ]
        tile_copies = [
            pltpu.make_async_copy(
                tiles_hbm.at[0, 0, pl.ds(n * size, size)], raw_ref.at[pl.ds(n * size, size)], sem.at[2 + n]
            )
            for n in range(4)
        ]
        for c in copies + tile_copies:
            c.start()
        for n in range(4):
            tile_copies[n].wait()
            for s in range(n * size, (n + 1) * size):
                split_ref[s, 0], split_ref[s, 1] = pieces(raw_ref[s], 2)
        for c in copies:
            c.wait()
        first = (lax.axis_index("vec") == 0).astype(F32)
        d = ((diag_ref[...] - SHIFT) * first)[:, None, :]
        a_ref[...] = x_ref[:, :part] * d
        b_ref[...] = x_ref[:, part:] * d

    def own_body(rows_ref, cols_ref, x_ref, split_ref, *refs):
        own_sum(refs[len(refs) // 2 :], x_ref, split_ref, rows_ref, cols_ref)

    def pack(place_ref, rows_ref, counts_ref, asked_refs, x_ref, split_ref, outs):
        for p in range(count):
            role = place_ref[1 + p]

            def put(c, value, p=p):
                for n, ref in enumerate(outs[p]):
                    ref[c] = value[n * part : (n + 1) * part]

            @pl.when(role > 0)
            def _():
                base = OWN_SLOTS + (role - 1) * CAP
                for c in range(CAP):
                    term = tile_product(x_ref[rows_ref[0, 0, base + c]], split_ref, base + c, False)
                    put(c, jnp.where(c < counts_ref[0, 0, role - 1], term, 0.0))

            @pl.when(role < 0)
            def _():
                base = OWN_SLOTS + (-role - 1) * CAP
                for c in range(CAP):
                    put(c, x_ref[asked_refs[p][0, 0, base + c]])

    def send_body(place_ref, rows_ref, counts_ref, *refs):
        asked_refs, (x_ref, split_ref), outs = refs[:count], refs[count : count + 2], refs[count + 2 :]
        pack(
            place_ref, rows_ref, counts_ref, asked_refs, x_ref, split_ref,
            [(outs[p], outs[count + p]) for p in range(count)],
        )

    def settle(place_ref, mine_ref, other_ref, y_ref):
        core = place_ref[0] % 2
        y_ref[pl.ds(core * half, half)] = mine_ref[...]
        y_ref[pl.ds((1 - core) * half, half)] = other_ref[...]

    def resend_body(place_ref, rows_ref, counts_ref, *refs):
        asked_refs = refs[:count]
        mine_ref, other_ref, diag_ref, split_ref, y_ref, acc_ref = refs[count : count + 6]
        outs = refs[count + 6 :]
        settle(place_ref, mine_ref, other_ref, y_ref)
        pack(
            place_ref, rows_ref, counts_ref, asked_refs, y_ref, split_ref,
            [(outs[p],) for p in range(count)],
        )
        first = (place_ref[0] == 0).astype(F32)
        acc_ref[...] = y_ref[...] * ((diag_ref[...] - SHIFT) * first)[:, None, :]

    def join_rounds(members, place_ref, rows_ref, counts_ref, asked_refs, got_refs, split_ref, acc_ref):
        for n, p in enumerate(members):
            role = place_ref[1 + p]

            @pl.when(role > 0)
            def _():
                base = OWN_SLOTS + (role - 1) * CAP
                for c in range(CAP):
                    term = tile_product(got_refs[n][c], split_ref, base + c, True)
                    acc_ref[rows_ref[0, 0, base + c]] += jnp.where(
                        c < counts_ref[0, 0, role - 1], term, 0.0
                    )

            @pl.when(role < 0)
            def _():
                base = OWN_SLOTS + (-role - 1) * CAP
                for c in range(CAP):
                    acc_ref[asked_refs[n][0, 0, base + c]] += got_refs[n][c]

    def join(acc, got, members, last=False):
        size = len(members)

        def body(place_ref, rows_ref, counts_ref, *refs):
            asked_refs, got_refs = refs[:size], refs[size : 2 * size]
            split_ref, prior_ref = refs[2 * size : 2 * size + 2]
            outs = refs[2 * size + 2 :]
            if last:
                keep_ref, give_ref, acc_ref = outs
                acc_ref[...] = prior_ref[...]
            else:
                (acc_ref,) = outs
            join_rounds(
                members, place_ref, rows_ref, counts_ref, asked_refs, got_refs, split_ref, acc_ref
            )
            if last:
                core = place_ref[0] % 2
                keep_ref[...] = acc_ref[pl.ds(core * half, half)]
                give_ref[...] = acc_ref[pl.ds((1 - core) * half, half)]

        out = call(
            body,
            [halfchunk] * 2 if last else [chunk],
            [SMEM] * (3 + size) + [VMEM] * (size + 2),
            [pltpu.VMEM(chunk, F32)] if last else [],
            name="join",
            weight=10**10,
            aliases=None if last else {3 + 2 * size + 1: 0},
        )(
            place, tile_rows, slot_counts, *[asked[p] for p in members], *[got[p] for p in members], split, acc
        )
        return out if last else out[0]

    def gram_body(x_ref, out_ref):
        total = jnp.zeros(square, F32)
        for n in range(0, rows, 2):
            pair = [x_ref[n], x_ref[n + 1]]
            total += gram_step(pair, [pair])
        out_ref[...] = total

    def cross_body(x_ref, a_ref, b_ref, out_ref):
        total = jnp.zeros((width, 2 * width), F32)
        for n in range(0, rows, 2):
            y = [jnp.concatenate([a_ref[m], b_ref[m]], axis=0) for m in (n, n + 1)]
            total += gram_step(y, [[x_ref[n], x_ref[n + 1]], y])
        out_ref[...] = total

    def first_body(gram_ref, inverse_ref):
        _, inverse_ref[...] = factor(gram_ref[...])

    def identity():
        eye = lax.broadcasted_iota(jnp.int32, square, 0) == lax.broadcasted_iota(jnp.int32, square, 1)
        return eye.astype(F32)

    def lower_part():
        return lax.broadcasted_iota(jnp.int32, square, 0) >= lax.broadcasted_iota(jnp.int32, square, 1)

    def second_body(gram_ref, inverse_ref, cross_ref, lower_ref, coef_ref, gain_ref):
        start_inv = inverse_ref[...]
        cross = dot(dot(start_inv, gram_ref[:, :width]), start_inv, tb=True)
        applied = dot(dot(start_inv, gram_ref[:, width:]), start_inv, tb=True)
        upper, inverse = factor(applied - dot(cross, cross, tb=True))
        lower = upper.T
        cross_ref[...] = cross + SHIFT * identity()
        lower_ref[...] = lower
        gain = dot(inverse, start_inv)
        back = -dot(dot(inverse, cross), start_inv)
        gain_ref[...] = gain
        coef_ref[:width, :width] = -dot(lower, start_inv)
        coef_ref[:width, width : 2 * width] = back
        coef_ref[:width, 2 * width :] = gain
        coef_ref[width:, :width] = back
        coef_ref[width:, width : 2 * width] = gain
        coef_ref[width:, 2 * width :] = jnp.zeros(square, F32)

    def blend(side, mine, other, coef):
        def body(place_ref, x_ref, a_ref, b_ref, mine_ref, other_ref, coef_ref, w_ref, q_ref, out_ref, z_ref):
            settle(place_ref, mine_ref, other_ref, z_ref)
            for n in range(0, half, 2):
                stacks = [
                    jnp.concatenate([ref[side * half + m] for ref in (x_ref, a_ref, b_ref, z_ref)], axis=0)
                    for m in (n, n + 1)
                ]
                for m, both in zip((n, n + 1), wide_product(coef_ref[:, : 2 * width + part], stacks)):
                    w_ref[m] = both[:width]
                    q_ref[m] = both[width:]
            total = jnp.zeros(square, F32)
            for n in range(0, half, 2):
                qs = [q_ref[n], q_ref[n + 1]]
                total += gram_step(qs, [qs])
            out_ref[...] = total

        return call(
            body,
            [halffull, halffull, square],
            [SMEM] + [VMEM] * 6,
            [pltpu.VMEM(chunk, F32)],
            name="blend",
        )(place, x, y_a, y_b, mine, other, coef)

    def third_body(place_ref, mine_ref, other_ref, gain_ref, *refs):
        prior_refs, q_refs, norm_refs = refs[0:2], refs[2:4], refs[4:6]
        w_ref, out_ref, z_ref = refs[6:]
        settle(place_ref, mine_ref, other_ref, z_ref)
        for n in range(0, rows, 2):
            side, m = divmod(n, half)
            for k, w in enumerate(wide_product(gain_ref[:, part:], [z_ref[n], z_ref[n + 1]])):
                w_ref[n + k] = w + prior_refs[side][m + k]
        total = jnp.zeros((width, 2 * width), F32)
        for n in range(0, rows, 2):
            side, m = divmod(n, half)
            ws = [w_ref[n], w_ref[n + 1]]
            total += gram_step(ws, [[q_refs[side][m], q_refs[side][m + 1]], ws])
        norm = norm_refs[0][...] + norm_refs[1][...]
        out_ref[:width, :width] = total[:, :width]
        out_ref[:width, width:] = jnp.where(lower_part(), total[:, width:], norm)
        out_ref[width:, :] = jnp.zeros((8, 2 * width), F32)
        out_ref[width:, :width] = jnp.broadcast_to(
            jnp.sum(norm * identity(), axis=0, keepdims=True), (8, width)
        )

    def fourth_body(gram_ref, cross_ref, lower_ref, coef_ref):
        cross = gram_ref[:width, :width]
        packed = gram_ref[:width, width:]
        flipped = packed.T
        squares = jnp.where(lower_part(), packed, flipped)
        norm = jnp.where(lower_part(), flipped, packed)
        norm = jnp.where(identity() > 0, gram_ref[width : width + 1, :width], norm)
        taken = cross + SHIFT * (norm - identity())
        mixed = dot(taken, cross, tb=True)
        squared = squares - mixed - mixed.T + dot(dot(taken, norm), taken, tb=True)
        upper, inverse = factor(squared)
        cross_ref[...] = taken + SHIFT * identity()
        lower_ref[...] = upper.T
        scale = math.sqrt(rows * length * peers)
        coef_ref[:, :width] = inverse * scale
        coef_ref[:, width:] = -dot(inverse, taken) * scale

    def last_body(w_ref, low_ref, high_ref, coef_ref, a1_ref, l1_ref, a2_ref, l2_ref, out_ref, pack_ref):
        for n, ref in enumerate((a1_ref, l1_ref, a2_ref, l2_ref)):
            pack_ref[n] = ref[...]
        for n in range(0, rows, 2):
            side, at = divmod(n, half)
            q_ref = (low_ref, high_ref)[side]
            stacks = [jnp.concatenate([w_ref[n + k], q_ref[at + k]], axis=0) for k in range(2)]
            for m, out in zip((n, n + 1), wide_product(coef_ref[...], stacks, 4)):
                out_ref[m] = out

    swap = [(i, i ^ 1) for i in range(lanes)]
    cuts = [count * n // 3 for n in range(4)]
    groups = [list(range(cuts[n], cuts[n + 1])) for n in range(3)]

    def spread(sent):
        return [exchange(s, "res", entry["pairs"]) for s, entry in zip(sent, rounds)]

    def across(mine, *tokens):
        step = 2
        while step < lanes:
            got = lax.ppermute(mine, "vec", [(i, i ^ step) for i in range(lanes)])
            mine = mine + after(got, *tokens)
            step *= 2
        return mine

    def resend(mine, other):
        y, acc, *sent = call(
            resend_body,
            [chunk, chunk] + [packet] * count,
            [SMEM] * (3 + count) + [VMEM] * 4,
            name="resend",
        )(place, tile_rows, slot_counts, *asked, mine, other, diagonal, split)
        return y, acc, spread(sent)

    def own(y, *accs):
        return call(
            own_body,
            [chunk] * len(accs),
            [SMEM] * 2 + [VMEM] * (2 + len(accs)),
            name="own",
            aliases={4 + n: n for n in range(len(accs))},
        )(tile_rows, tile_cols, y, split, *accs)

    asked = [exchange(tile_cols, "res", entry["pairs"]) for entry in rounds]
    x, split, acc_a, acc_b = call(
        prepare_body,
        [full, split_shape, chunk, chunk],
        [HBM] * 3,
        [
            pltpu.VMEM(diagonal.shape, F32),
            pltpu.VMEM((slots, length, length), F32),
            pltpu.SemaphoreType.DMA((6,)),
        ],
        name="prepare",
    )(*[pinned(v) for v in (start_block, diagonal, hess_tiles)])
    sent = call(
        send_body, [packet] * (2 * count), [SMEM] * (3 + count) + [VMEM] * 2, name="send"
    )(place, tile_rows, slot_counts, *asked, x, split)
    got_a = spread(sent[:count])
    sent_b = list(sent[count:])
    acc_a, acc_b = own(x, after(acc_a, sent[0]), acc_b)
    for n in range(2):
        acc_a = join(acc_a, got_a, groups[n])
        acc_a, x, *gated = lax.optimization_barrier((acc_a, x, *[sent_b[p] for p in groups[n]]))
        for p, value in zip(groups[n], gated):
            sent_b[p] = value
        if n == 0:
            (gram,) = call(gram_body, [square], [VMEM], name="gram")(x)
            start_gram = start_sum(gram, "res")
    acc_a = after(acc_a, start_gram)
    keep_a, give_a = join(acc_a, got_a, groups[2], last=True)
    for p in groups[2]:
        sent_b[p] = after(sent_b[p], keep_a)
    got_b = spread(sent_b)

    core = lax.ppermute(give_a, "vec", swap)
    acc_b = join(acc_b, got_b, groups[0])
    mine_a = keep_a + after(core, acc_b)
    (start_inv,) = call(first_body, [square], [VMEM], name="first")(end_sum(start_gram, "res", mine_a))
    acc_b = join(after(acc_b, start_inv), got_b, groups[1])
    mine_a = across(mine_a, acc_b)
    other_a = lax.ppermute(mine_a, "vec", swap)
    keep_b, give_b = join(acc_b, got_b, groups[2], last=True)
    y_a, acc_a, got_a = resend(mine_a, after(other_a, keep_b))

    core = lax.ppermute(give_b, "vec", swap)
    mine_b = keep_b + after(core, y_a)
    acc_a = join(after(acc_a, mine_b), got_a, groups[2])
    (acc_a,) = own(y_a, acc_a)
    acc_a = join(acc_a, got_a, groups[1])
    mine_b = across(mine_b, acc_a)
    other_b = lax.ppermute(mine_b, "vec", swap)
    keep_a, give_a = join(acc_a, got_a, groups[0], last=True)
    y_b, acc_b, got_b = resend(mine_b, after(other_b, keep_a))

    (gram,) = call(cross_body, [(width, 2 * width)], [VMEM] * 3, name="cross")(x, y_a, y_b)
    core = lax.ppermute(give_a, "vec", swap)
    (acc_b,) = own(y_b, after(acc_b, gram))
    acc_b = join(acc_b, got_b, groups[0])
    mine_a = keep_a + after(core, acc_b)
    cross_gram = start_sum(gram, "res")
    acc_b = join(after(acc_b, cross_gram, mine_a), got_b, groups[1])
    cross_gram = end_sum(cross_gram, "res", acc_b)
    acc_b = after(acc_b, cross_gram)
    mine_a = across(mine_a, acc_b)
    other_a = lax.ppermute(mine_a, "vec", swap)
    keep_b, give_b = join(acc_b, got_b, groups[2], last=True)

    core = lax.ppermute(give_b, "vec", swap)
    mine_b = keep_b + core
    cross1, lower1, coef, gain = call(
        second_body, [square, square, (2 * width, 3 * width), square], [VMEM] * 2, name="second"
    )(after(cross_gram, mine_b), start_inv)
    w_low, q_low, norm_low = blend(0, mine_a, other_a, coef)
    w_high, q_high, norm_high = blend(1, mine_a, other_a, coef)
    mine_b = across(mine_b, norm_low, norm_high)
    other_b = lax.ppermute(mine_b, "vec", swap)
    w, gram = call(
        third_body,
        [full, (width + 8, 2 * width)],
        [SMEM] + [VMEM] * 9,
        [pltpu.VMEM(chunk, F32)],
        name="third",
    )(place, mine_b, other_b, gain, w_low, w_high, q_low, q_high, norm_low, norm_high)
    gram = all_sum(gram, "res")
    cross2, lower2, coef = call(
        fourth_body, [square, square, (width, 2 * width)], [VMEM], name="fourth"
    )(gram)
    return call(last_body, [full, (4, width, width)], [VMEM] * 8, name="last")(
        w, q_low, q_high, coef, cross1, lower1, cross2, lower2
    )


def solution(mesh):
    in_specs = (
        P(("conf", "res"), None, None),
        P(("conf", "res"), None),
        P(("conf", "res"), "vec", None, None, None),
        P(("conf", "res"), "vec", None),
        P(("conf", "res"), "vec", None),
        P(("conf", "res"), "vec", None),
    )
    out_specs = (P(("conf", "res"), None, None), P("conf", None, None))
    return jax.shard_map(local, mesh=mesh, in_specs=in_specs, out_specs=out_specs, check_vma=False)
```

```python
import math

import jax
import jax.numpy as jnp
from jax import lax
from jax.experimental import pallas as pl
from jax.experimental.pallas import tpu as pltpu
from jax.sharding import PartitionSpec as P

OWN_SLOTS = 20
HOPS = 3
CAP = 8
SHIFT = 1.65
BF16 = jnp.bfloat16
F32 = jnp.float32

VMEM = pl.BlockSpec(memory_space=pltpu.VMEM)
SMEM = pl.BlockSpec(memory_space=pltpu.SMEM)
HBM = pl.BlockSpec(memory_space=pltpu.HBM)


def contract(a, b, ta=False, tb=False, precision=None):
    dims = (((0 if ta else 1,), (1 if tb else 0,)), ((), ()))
    return lax.dot_general(a, b, dims, precision=precision, preferred_element_type=F32)


def dot(a, b, ta=False, tb=False):
    return contract(a, b, ta, tb, lax.Precision.HIGHEST)


def pieces(x, count):
    out = []
    for _ in range(count):
        out.append(x.astype(BF16))
        x = x - out[-1].astype(F32)
    return out


def tile_product(x, tile_ref, slot, transposed):
    x1, x2 = pieces(x, 2)
    m1, m2 = tile_ref[slot, 0], tile_ref[slot, 1]
    axis = 1 if transposed else 0
    left = jnp.concatenate([x1, x2, x1], axis=1)
    return contract(left, jnp.concatenate([m1, m1, m2], axis=axis), tb=transposed)


def wide_product(coef, blocks, terms=6):
    pairs = [(0, 0), (0, 1), (1, 0), (1, 1)] if terms == 4 else [(0, 0), (0, 1), (0, 2), (1, 0), (1, 1), (2, 0)]
    c = pieces(coef, terms // 2)
    z = pieces(jnp.concatenate(blocks, axis=1), terms // 2)
    left = jnp.concatenate([c[m] for m, _ in pairs], axis=1)
    out = contract(left, jnp.concatenate([z[m] for _, m in pairs], axis=0))
    width = blocks[0].shape[1]
    return [out[:, n * width : (n + 1) * width] for n in range(len(blocks))]


def gram_step(left, right):
    a = jnp.concatenate(pieces(jnp.concatenate(left, axis=1), 2), axis=0)
    b = jnp.concatenate(
        [p for group in right for p in pieces(jnp.concatenate(group, axis=1), 2)], axis=0
    )
    out = contract(a, b, tb=True)
    size = left[0].shape[0]
    out = out[:size] + out[size:]
    return jnp.concatenate(
        [
            out[:, 2 * g * size : (2 * g + 1) * size] + out[:, (2 * g + 1) * size : (2 * g + 2) * size]
            for g in range(len(right))
        ],
        axis=1,
    )


def call(body, outs, in_specs, scratch=(), name=None, aliases=None, weight=0):
    shapes = [
        o if isinstance(o, jax.ShapeDtypeStruct) else jax.ShapeDtypeStruct(o, F32) for o in outs
    ]
    return pl.pallas_call(
        body,
        out_shape=shapes,
        in_specs=in_specs,
        out_specs=[VMEM] * len(outs),
        scratch_shapes=list(scratch),
        compiler_params=pltpu.CompilerParams(vmem_limit_bytes=40 << 20),
        input_output_aliases=aliases or {},
        cost_estimate=pl.CostEstimate(flops=weight, bytes_accessed=weight, transcendentals=0) if weight else None,
        name=name,
    )


def pinned(value):
    return pltpu.with_memory_space_constraint(value, pltpu.HBM)


def after(value, *tokens):
    return lax.optimization_barrier((value,) + tokens)[0]


def pairings(size):
    rounds = []
    for hop in range(1, HOPS + 1):
        for parity in range(2):
            pairs = [(i, i + hop) for i in range(size - hop) if (i // hop) % 2 == parity]
            if not pairs:
                continue
            used = {i for pair in pairs for i in pair}
            for entry in rounds:
                if not entry["used"] & used:
                    entry["used"] |= used
                    entry["pairs"] += pairs
                    entry["kinds"].append((hop, parity))
                    break
            else:
                rounds.append({"used": used, "pairs": pairs, "kinds": [(hop, parity)]})
    return rounds


def exchange(block, axis, pairs):
    return lax.ppermute(block, axis, [(a, b) for a, b in pairs] + [(b, a) for a, b in pairs])


def role_table(rounds, size):
    table = [[0] * size for _ in rounds]
    for p, entry in enumerate(rounds):
        for a, b in entry["pairs"]:
            table[p][a] = b - a
            table[p][b] = a - b
    return jnp.array(table, jnp.int32)


def sum_steps(size):
    return [1 << n for n in range(size.bit_length() - 1)]


def start_sum(block, axis):
    size = lax.axis_size(axis)
    if size & (size - 1):
        return block
    for step in sum_steps(size)[:-1]:
        block = block + lax.ppermute(block, axis, [(i, i ^ step) for i in range(size)])
    return block


def end_sum(block, axis, *tokens):
    size = lax.axis_size(axis)
    if size & (size - 1):
        return lax.psum(block, axis)
    for step in sum_steps(size)[-1:]:
        got = lax.ppermute(block, axis, [(i, i ^ step) for i in range(size)])
        block = block + (after(got, *tokens) if tokens else got)
    return block


def all_sum(block, axis, *tokens):
    return end_sum(start_sum(block, axis), axis, *tokens)


def factor(gram):
    size = gram.shape[0]
    tile = (8, 2 * size)
    row_id = lax.broadcasted_iota(jnp.int32, (size, size), 0)
    col_id = lax.broadcasted_iota(jnp.int32, (size, size), 1)
    work = jnp.concatenate([gram, (row_id == col_id).astype(F32)], axis=1)
    blocks = [work[8 * b : 8 * b + 8] for b in range(size // 8)]
    sub = lax.broadcasted_iota(jnp.int32, tile, 0)
    for j in range(0, size, 4):
        b, s = divmod(j, 8)
        later = range(b + s // 4, size // 8)
        line = [jnp.broadcast_to(blocks[b][s + k : s + k + 1], tile) for k in range(4)]
        cols = {
            o: [jnp.broadcast_to(blocks[o][:, j + k : j + k + 1], tile) for k in range(4)]
            for o in range(b, size // 8)
        }
        entry = {
            (k, l): jnp.broadcast_to(cols[b][l][s + k : s + k + 1], tile)
            for k in range(4)
            for l in range(k, 4)
        }
        scaled = []
        for k in range(4):
            inverse = 1.0 / entry[k, k]
            for l in range(k + 1, 4):
                ratio = entry[k, l] * inverse
                for p in range(l, 4):
                    entry[l, p] = entry[l, p] - ratio * entry[k, p]
                line[l] = line[l] - ratio * line[k]
                for o in later:
                    cols[o][l] = cols[o][l] - ratio * cols[o][k]
            scaled.append(inverse * line[k])
        for o in range(b, size // 8):
            new = blocks[o]
            if o in later:
                new = new - ((cols[o][0] * scaled[0] + cols[o][1] * scaled[1]) + (cols[o][2] * scaled[2] + cols[o][3] * scaled[3]))
            if o == b:
                new = jnp.where(sub > s + 3, new, blocks[o])
                for k in range(1, 4):
                    new = jnp.where(sub == s + k, line[k], new)
            blocks[o] = new
    work = jnp.concatenate(blocks, axis=0)
    pivots = jnp.sum(jnp.where(row_id == col_id, work[:, :size], 0.0), axis=1, keepdims=True)
    work = work / jnp.sqrt(pivots)
    upper = jnp.where(col_id >= row_id, work[:, :size], 0.0)
    inverse = jnp.where(col_id <= row_id, work[:, size:], 0.0)
    return upper, inverse


def local(start_block, diagonal, hess_tiles, tile_rows, tile_cols, slot_counts):
    peers = lax.axis_size("res")
    lanes = lax.axis_size("vec")
    rows, width, length = start_block.shape
    slots = hess_tiles.shape[2]
    half = rows // 2
    part = width // 2
    rounds = pairings(peers)
    count = len(rounds)
    full = (rows, width, length)
    halffull = (half, width, length)
    chunk = (rows, part, length)
    halfchunk = (half, part, length)
    packet = (CAP, part, length)
    square = (width, width)
    split_shape = jax.ShapeDtypeStruct((slots, 2, length, length), BF16)

    table = role_table(rounds, peers)
    place = jnp.concatenate(
        [lax.axis_index("vec").reshape(1), table[:, lax.axis_index("res")]]
    ).astype(jnp.int32)

    def own_sum(acc_refs, x_ref, split_ref, rows_ref, cols_ref):
        batch = 4
        for first in range(0, OWN_SLOTS, batch):
            members = range(first, first + batch)
            ends = [(rows_ref[0, 0, s], cols_ref[0, 0, s]) for s in members]
            terms = [
                (
                    tile_product(x_ref[j], split_ref, s, True),
                    tile_product(x_ref[i], split_ref, s, False),
                )
                for s, (i, j) in zip(members, ends)
            ]
            for (i, j), (direct, mirror) in zip(ends, terms):
                for n, acc_ref in enumerate(acc_refs):
                    acc_ref[i] += direct[n * part : (n + 1) * part]
                    acc_ref[j] += mirror[n * part : (n + 1) * part]

    def prepare_body(x_hbm, diag_hbm, tiles_hbm, *refs):
        x_ref, split_ref, a_ref, b_ref, diag_ref, raw_ref, sem = refs
        size = slots // 4
        copies = [
            pltpu.make_async_copy(src, dst, sem.at[n])
            for n, (src, dst) in enumerate([(x_hbm, x_ref), (diag_hbm, diag_ref)])
        ]
        tile_copies = [
            pltpu.make_async_copy(
                tiles_hbm.at[0, 0, pl.ds(n * size, size)], raw_ref.at[pl.ds(n * size, size)], sem.at[2 + n]
            )
            for n in range(4)
        ]
        for c in copies + tile_copies:
            c.start()
        for n in range(4):
            tile_copies[n].wait()
            for s in range(n * size, (n + 1) * size):
                split_ref[s, 0], split_ref[s, 1] = pieces(raw_ref[s], 2)
        for c in copies:
            c.wait()
        first = (lax.axis_index("vec") == 0).astype(F32)
        d = ((diag_ref[...] - SHIFT) * first)[:, None, :]
        a_ref[...] = x_ref[:, :part] * d
        b_ref[...] = x_ref[:, part:] * d

    def own_body(rows_ref, cols_ref, x_ref, split_ref, *refs):
        own_sum(refs[len(refs) // 2 :], x_ref, split_ref, rows_ref, cols_ref)

    def pack(place_ref, rows_ref, counts_ref, asked_refs, x_ref, split_ref, outs):
        for p in range(count):
            role = place_ref[1 + p]

            def put(c, value, p=p):
                for n, ref in enumerate(outs[p]):
                    ref[c] = value[n * part : (n + 1) * part]

            @pl.when(role > 0)
            def _():
                base = OWN_SLOTS + (role - 1) * CAP
                terms = [
                    tile_product(x_ref[rows_ref[0, 0, base + c]], split_ref, base + c, False)
                    for c in range(CAP)
                ]
                for c, term in enumerate(terms):
                    put(c, jnp.where(c < counts_ref[0, 0, role - 1], term, 0.0))

            @pl.when(role < 0)
            def _():
                base = OWN_SLOTS + (-role - 1) * CAP
                for c in range(CAP):
                    put(c, x_ref[asked_refs[p][0, 0, base + c]])

    def send_body(place_ref, rows_ref, counts_ref, *refs):
        asked_refs, (x_ref, split_ref), outs = refs[:count], refs[count : count + 2], refs[count + 2 :]
        pack(
            place_ref, rows_ref, counts_ref, asked_refs, x_ref, split_ref,
            [(outs[p], outs[count + p]) for p in range(count)],
        )

    def settle(place_ref, mine_ref, other_ref, y_ref):
        core = place_ref[0] % 2
        y_ref[pl.ds(core * half, half)] = mine_ref[...]
        y_ref[pl.ds((1 - core) * half, half)] = other_ref[...]

    def resend_body(place_ref, rows_ref, counts_ref, *refs):
        asked_refs = refs[:count]
        mine_ref, other_ref, diag_ref, split_ref, y_ref, acc_ref = refs[count : count + 6]
        outs = refs[count + 6 :]
        settle(place_ref, mine_ref, other_ref, y_ref)
        pack(
            place_ref, rows_ref, counts_ref, asked_refs, y_ref, split_ref,
            [(outs[p],) for p in range(count)],
        )
        first = (place_ref[0] == 0).astype(F32)
        acc_ref[...] = y_ref[...] * ((diag_ref[...] - SHIFT) * first)[:, None, :]

    def join_rounds(members, place_ref, rows_ref, counts_ref, asked_refs, got_refs, split_ref, acc_ref):
        for n, p in enumerate(members):
            role = place_ref[1 + p]

            @pl.when(role > 0)
            def _():
                base = OWN_SLOTS + (role - 1) * CAP
                terms = [
                    tile_product(got_refs[n][c], split_ref, base + c, True) for c in range(CAP)
                ]
                for c, term in enumerate(terms):
                    acc_ref[rows_ref[0, 0, base + c]] += jnp.where(
                        c < counts_ref[0, 0, role - 1], term, 0.0
                    )

            @pl.when(role < 0)
            def _():
                base = OWN_SLOTS + (-role - 1) * CAP
                for c in range(CAP):
                    acc_ref[asked_refs[n][0, 0, base + c]] += got_refs[n][c]

    def join(acc, got, members, last=False):
        size = len(members)

        def body(place_ref, rows_ref, counts_ref, *refs):
            asked_refs, got_refs = refs[:size], refs[size : 2 * size]
            split_ref, prior_ref = refs[2 * size : 2 * size + 2]
            outs = refs[2 * size + 2 :]
            if last:
                keep_ref, give_ref, acc_ref = outs
                acc_ref[...] = prior_ref[...]
            else:
                (acc_ref,) = outs
            join_rounds(
                members, place_ref, rows_ref, counts_ref, asked_refs, got_refs, split_ref, acc_ref
            )
            if last:
                core = place_ref[0] % 2
                keep_ref[...] = acc_ref[pl.ds(core * half, half)]
                give_ref[...] = acc_ref[pl.ds((1 - core) * half, half)]

        out = call(
            body,
            [halfchunk] * 2 if last else [chunk],
            [SMEM] * (3 + size) + [VMEM] * (size + 2),
            [pltpu.VMEM(chunk, F32)] if last else [],
            name="join",
            weight=10**10,
            aliases=None if last else {3 + 2 * size + 1: 0},
        )(
            place, tile_rows, slot_counts, *[asked[p] for p in members], *[got[p] for p in members], split, acc
        )
        return out if last else out[0]

    def gram_body(x_ref, out_ref):
        total = jnp.zeros(square, F32)
        for n in range(0, rows, 2):
            pair = [x_ref[n], x_ref[n + 1]]
            total += gram_step(pair, [pair])
        out_ref[...] = total

    def cross_body(x_ref, a_ref, b_ref, out_ref):
        total = jnp.zeros((width, 2 * width), F32)
        for n in range(0, rows, 2):
            y = [jnp.concatenate([a_ref[m], b_ref[m]], axis=0) for m in (n, n + 1)]
            total += gram_step(y, [[x_ref[n], x_ref[n + 1]], y])
        out_ref[...] = total

    def first_body(gram_ref, inverse_ref):
        _, inverse_ref[...] = factor(gram_ref[...])

    def identity():
        eye = lax.broadcasted_iota(jnp.int32, square, 0) == lax.broadcasted_iota(jnp.int32, square, 1)
        return eye.astype(F32)

    def lower_part():
        return lax.broadcasted_iota(jnp.int32, square, 0) >= lax.broadcasted_iota(jnp.int32, square, 1)

    def second_body(gram_ref, inverse_ref, cross_ref, lower_ref, coef_ref, gain_ref):
        start_inv = inverse_ref[...]
        cross = dot(dot(start_inv, gram_ref[:, :width]), start_inv, tb=True)
        applied = dot(dot(start_inv, gram_ref[:, width:]), start_inv, tb=True)
        upper, inverse = factor(applied - dot(cross, cross, tb=True))
        lower = upper.T
        cross_ref[...] = cross + SHIFT * identity()
        lower_ref[...] = lower
        gain = dot(inverse, start_inv)
        back = -dot(dot(inverse, cross), start_inv)
        gain_ref[...] = gain
        coef_ref[:width, :width] = -dot(lower, start_inv)
        coef_ref[:width, width : 2 * width] = back
        coef_ref[:width, 2 * width :] = gain
        coef_ref[width:, :width] = back
        coef_ref[width:, width : 2 * width] = gain
        coef_ref[width:, 2 * width :] = jnp.zeros(square, F32)

    def blend(side, mine, other, coef):
        def body(place_ref, x_ref, a_ref, b_ref, mine_ref, other_ref, coef_ref, w_ref, q_ref, out_ref, z_ref):
            settle(place_ref, mine_ref, other_ref, z_ref)
            for n in range(0, half, 2):
                stacks = [
                    jnp.concatenate([ref[side * half + m] for ref in (x_ref, a_ref, b_ref, z_ref)], axis=0)
                    for m in (n, n + 1)
                ]
                for m, both in zip((n, n + 1), wide_product(coef_ref[:, : 2 * width + part], stacks)):
                    w_ref[m] = both[:width]
                    q_ref[m] = both[width:]
            total = jnp.zeros(square, F32)
            for n in range(0, half, 2):
                qs = [q_ref[n], q_ref[n + 1]]
                total += gram_step(qs, [qs])
            out_ref[...] = total

        return call(
            body,
            [halffull, halffull, square],
            [SMEM] + [VMEM] * 6,
            [pltpu.VMEM(chunk, F32)],
            name="blend",
        )(place, x, y_a, y_b, mine, other, coef)

    def third_body(place_ref, mine_ref, other_ref, gain_ref, *refs):
        prior_refs, q_refs, norm_refs = refs[0:2], refs[2:4], refs[4:6]
        w_ref, out_ref, z_ref = refs[6:]
        settle(place_ref, mine_ref, other_ref, z_ref)
        for n in range(0, rows, 2):
            side, m = divmod(n, half)
            for k, w in enumerate(wide_product(gain_ref[:, part:], [z_ref[n], z_ref[n + 1]])):
                w_ref[n + k] = w + prior_refs[side][m + k]
        total = jnp.zeros((width, 2 * width), F32)
        for n in range(0, rows, 2):
            side, m = divmod(n, half)
            ws = [w_ref[n], w_ref[n + 1]]
            total += gram_step(ws, [[q_refs[side][m], q_refs[side][m + 1]], ws])
        norm = norm_refs[0][...] + norm_refs[1][...]
        out_ref[:width, :width] = total[:, :width]
        out_ref[:width, width:] = jnp.where(lower_part(), total[:, width:], norm)
        out_ref[width:, :] = jnp.zeros((8, 2 * width), F32)
        out_ref[width:, :width] = jnp.broadcast_to(
            jnp.sum(norm * identity(), axis=0, keepdims=True), (8, width)
        )

    def fourth_body(gram_ref, cross_ref, lower_ref, coef_ref):
        cross = gram_ref[:width, :width]
        packed = gram_ref[:width, width:]
        flipped = packed.T
        squares = jnp.where(lower_part(), packed, flipped)
        norm = jnp.where(lower_part(), flipped, packed)
        norm = jnp.where(identity() > 0, gram_ref[width : width + 1, :width], norm)
        taken = cross + SHIFT * (norm - identity())
        mixed = dot(taken, cross, tb=True)
        squared = squares - mixed - mixed.T + dot(dot(taken, norm), taken, tb=True)
        upper, inverse = factor(squared)
        cross_ref[...] = taken + SHIFT * identity()
        lower_ref[...] = upper.T
        scale = math.sqrt(rows * length * peers)
        coef_ref[:, :width] = inverse * scale
        coef_ref[:, width:] = -dot(inverse, taken) * scale

    def last_body(w_ref, low_ref, high_ref, coef_ref, a1_ref, l1_ref, a2_ref, l2_ref, out_ref, pack_ref):
        for n, ref in enumerate((a1_ref, l1_ref, a2_ref, l2_ref)):
            pack_ref[n] = ref[...]
        for n in range(0, rows, 2):
            side, at = divmod(n, half)
            q_ref = (low_ref, high_ref)[side]
            stacks = [jnp.concatenate([w_ref[n + k], q_ref[at + k]], axis=0) for k in range(2)]
            for m, out in zip((n, n + 1), wide_product(coef_ref[...], stacks, 4)):
                out_ref[m] = out

    swap = [(i, i ^ 1) for i in range(lanes)]
    cuts = [count * n // 3 for n in range(4)]
    groups = [list(range(cuts[n], cuts[n + 1])) for n in range(3)]

    def spread(sent):
        return [exchange(s, "res", entry["pairs"]) for s, entry in zip(sent, rounds)]

    def across(mine, *tokens):
        step = 2
        while step < lanes:
            got = lax.ppermute(mine, "vec", [(i, i ^ step) for i in range(lanes)])
            mine = mine + after(got, *tokens)
            step *= 2
        return mine

    def resend(mine, other):
        y, acc, *sent = call(
            resend_body,
            [chunk, chunk] + [packet] * count,
            [SMEM] * (3 + count) + [VMEM] * 4,
            name="resend",
        )(place, tile_rows, slot_counts, *asked, mine, other, diagonal, split)
        return y, acc, spread(sent)

    def own(y, *accs):
        return call(
            own_body,
            [chunk] * len(accs),
            [SMEM] * 2 + [VMEM] * (2 + len(accs)),
            name="own",
            aliases={4 + n: n for n in range(len(accs))},
        )(tile_rows, tile_cols, y, split, *accs)

    asked = [exchange(tile_cols, "res", entry["pairs"]) for entry in rounds]
    x, split, acc_a, acc_b = call(
        prepare_body,
        [full, split_shape, chunk, chunk],
        [HBM] * 3,
        [
            pltpu.VMEM(diagonal.shape, F32),
            pltpu.VMEM((slots, length, length), F32),
            pltpu.SemaphoreType.DMA((6,)),
        ],
        name="prepare",
    )(*[pinned(v) for v in (start_block, diagonal, hess_tiles)])
    sent = call(
        send_body, [packet] * (2 * count), [SMEM] * (3 + count) + [VMEM] * 2, name="send"
    )(place, tile_rows, slot_counts, *asked, x, split)
    got_a = spread(sent[:count])
    sent_b = list(sent[count:])
    acc_a, acc_b = own(x, after(acc_a, sent[0]), acc_b)
    for n in range(2):
        acc_a = join(acc_a, got_a, groups[n])
        acc_a, x, *gated = lax.optimization_barrier((acc_a, x, *[sent_b[p] for p in groups[n]]))
        for p, value in zip(groups[n], gated):
            sent_b[p] = value
        if n == 0:
            (gram,) = call(gram_body, [square], [VMEM], name="gram")(x)
            start_gram = start_sum(gram, "res")
    acc_a = after(acc_a, start_gram)
    keep_a, give_a = join(acc_a, got_a, groups[2], last=True)
    for p in groups[2]:
        sent_b[p] = after(sent_b[p], keep_a)
    got_b = spread(sent_b)

    core = lax.ppermute(give_a, "vec", swap)
    acc_b = join(acc_b, got_b, groups[0])
    mine_a = keep_a + after(core, acc_b)
    (start_inv,) = call(first_body, [square], [VMEM], name="first")(end_sum(start_gram, "res", mine_a))
    acc_b = join(after(acc_b, start_inv), got_b, groups[1])
    mine_a = across(mine_a, acc_b)
    other_a = lax.ppermute(mine_a, "vec", swap)
    keep_b, give_b = join(acc_b, got_b, groups[2], last=True)
    y_a, acc_a, got_a = resend(mine_a, after(other_a, keep_b))

    core = lax.ppermute(give_b, "vec", swap)
    mine_b = keep_b + after(core, y_a)
    (acc_a,) = own(y_a, after(acc_a, mine_b))
    acc_a = join(acc_a, got_a, groups[2])
    acc_a = join(acc_a, got_a, groups[1])
    mine_b = across(mine_b, acc_a)
    other_b = lax.ppermute(mine_b, "vec", swap)
    keep_a, give_a = join(acc_a, got_a, groups[0], last=True)
    y_b, acc_b, got_b = resend(mine_b, after(other_b, keep_a))

    core = lax.ppermute(give_a, "vec", swap)
    mine_a = keep_a + after(core, y_b)
    (gram,) = call(cross_body, [(width, 2 * width)], [VMEM] * 3, name="cross")(x, y_a, after(y_b, mine_a))
    (acc_b,) = own(y_b, after(acc_b, gram))
    cross_gram = start_sum(gram, "res")
    acc_b = join(after(acc_b, cross_gram), got_b, groups[2])
    acc_b = join(acc_b, got_b, groups[1])
    cross_gram = end_sum(cross_gram, "res", acc_b)
    acc_b = after(acc_b, cross_gram)
    mine_a = across(mine_a, acc_b)
    other_a = lax.ppermute(mine_a, "vec", swap)
    keep_b, give_b = join(acc_b, got_b, groups[0], last=True)

    core = lax.ppermute(give_b, "vec", swap)
    mine_b = keep_b + core
    cross1, lower1, coef, gain = call(
        second_body, [square, square, (2 * width, 3 * width), square], [VMEM] * 2, name="second"
    )(after(cross_gram, mine_b), start_inv)
    w_low, q_low, norm_low = blend(0, mine_a, other_a, coef)
    w_high, q_high, norm_high = blend(1, mine_a, other_a, coef)
    mine_b = across(mine_b, norm_low, norm_high)
    other_b = lax.ppermute(mine_b, "vec", swap)
    w, gram = call(
        third_body,
        [full, (width + 8, 2 * width)],
        [SMEM] + [VMEM] * 9,
        [pltpu.VMEM(chunk, F32)],
        name="third",
    )(place, mine_b, other_b, gain, w_low, w_high, q_low, q_high, norm_low, norm_high)
    gram = all_sum(gram, "res")
    cross2, lower2, coef = call(
        fourth_body, [square, square, (width, 2 * width)], [VMEM], name="fourth"
    )(gram)
    return call(last_body, [full, (4, width, width)], [VMEM] * 8, name="last")(
        w, q_low, q_high, coef, cross1, lower1, cross2, lower2
    )


def solution(mesh):
    in_specs = (
        P(("conf", "res"), None, None),
        P(("conf", "res"), None),
        P(("conf", "res"), "vec", None, None, None),
        P(("conf", "res"), "vec", None),
        P(("conf", "res"), "vec", None),
        P(("conf", "res"), "vec", None),
    )
    out_specs = (P(("conf", "res"), None, None), P("conf", None, None))
    return jax.shard_map(local, mesh=mesh, in_specs=in_specs, out_specs=out_specs, check_vma=False)
```

```python
import math

import jax
import jax.numpy as jnp
from jax import lax
from jax.experimental import pallas as pl
from jax.experimental.pallas import tpu as pltpu
from jax.sharding import PartitionSpec as P

OWN_SLOTS = 20
HOPS = 3
CAP = 8
SHIFT = 1.65
BF16 = jnp.bfloat16
F32 = jnp.float32

VMEM = pl.BlockSpec(memory_space=pltpu.VMEM)
SMEM = pl.BlockSpec(memory_space=pltpu.SMEM)
HBM = pl.BlockSpec(memory_space=pltpu.HBM)


def contract(a, b, ta=False, tb=False, precision=None):
    dims = (((0 if ta else 1,), (1 if tb else 0,)), ((), ()))
    return lax.dot_general(a, b, dims, precision=precision, preferred_element_type=F32)


def dot(a, b, ta=False, tb=False):
    return contract(a, b, ta, tb, lax.Precision.HIGHEST)


def pieces(x, count):
    out = []
    for _ in range(count):
        out.append(x.astype(BF16))
        x = x - out[-1].astype(F32)
    return out


def tile_product(x, tile_ref, slot, transposed):
    x1, x2 = pieces(x, 2)
    m1, m2 = tile_ref[slot, 0], tile_ref[slot, 1]
    axis = 1 if transposed else 0
    left = jnp.concatenate([x1, x2, x1], axis=1)
    return contract(left, jnp.concatenate([m1, m1, m2], axis=axis), tb=transposed)


def wide_product(coef, blocks, terms=6):
    pairs = [(0, 0), (0, 1), (1, 0), (1, 1)] if terms == 4 else [(0, 0), (0, 1), (0, 2), (1, 0), (1, 1), (2, 0)]
    c = pieces(coef, terms // 2)
    z = pieces(jnp.concatenate(blocks, axis=1), terms // 2)
    left = jnp.concatenate([c[m] for m, _ in pairs], axis=1)
    out = contract(left, jnp.concatenate([z[m] for _, m in pairs], axis=0))
    width = blocks[0].shape[1]
    return [out[:, n * width : (n + 1) * width] for n in range(len(blocks))]


def gram_step(left, right):
    a = jnp.concatenate(pieces(jnp.concatenate(left, axis=1), 2), axis=0)
    b = jnp.concatenate(
        [p for group in right for p in pieces(jnp.concatenate(group, axis=1), 2)], axis=0
    )
    out = contract(a, b, tb=True)
    size = left[0].shape[0]
    out = out[:size] + out[size:]
    return jnp.concatenate(
        [
            out[:, 2 * g * size : (2 * g + 1) * size] + out[:, (2 * g + 1) * size : (2 * g + 2) * size]
            for g in range(len(right))
        ],
        axis=1,
    )


def call(body, outs, in_specs, scratch=(), name=None, aliases=None, weight=0):
    shapes = [
        o if isinstance(o, jax.ShapeDtypeStruct) else jax.ShapeDtypeStruct(o, F32) for o in outs
    ]
    return pl.pallas_call(
        body,
        out_shape=shapes,
        in_specs=in_specs,
        out_specs=[VMEM] * len(outs),
        scratch_shapes=list(scratch),
        compiler_params=pltpu.CompilerParams(vmem_limit_bytes=40 << 20),
        input_output_aliases=aliases or {},
        cost_estimate=pl.CostEstimate(flops=weight, bytes_accessed=weight, transcendentals=0) if weight else None,
        name=name,
    )


def pinned(value):
    return pltpu.with_memory_space_constraint(value, pltpu.HBM)


def after(value, *tokens):
    return lax.optimization_barrier((value,) + tokens)[0]


def pairings(size):
    rounds = []
    for hop in range(1, HOPS + 1):
        for parity in range(2):
            pairs = [(i, i + hop) for i in range(size - hop) if (i // hop) % 2 == parity]
            if not pairs:
                continue
            used = {i for pair in pairs for i in pair}
            for entry in rounds:
                if not entry["used"] & used:
                    entry["used"] |= used
                    entry["pairs"] += pairs
                    entry["kinds"].append((hop, parity))
                    break
            else:
                rounds.append({"used": used, "pairs": pairs, "kinds": [(hop, parity)]})
    return rounds


def exchange(block, axis, pairs):
    return lax.ppermute(block, axis, [(a, b) for a, b in pairs] + [(b, a) for a, b in pairs])


def role_table(rounds, size):
    table = [[0] * size for _ in rounds]
    for p, entry in enumerate(rounds):
        for a, b in entry["pairs"]:
            table[p][a] = b - a
            table[p][b] = a - b
    return jnp.array(table, jnp.int32)


def sum_steps(size):
    return [1 << n for n in range(size.bit_length() - 1)]


def start_sum(block, axis):
    size = lax.axis_size(axis)
    if size & (size - 1):
        return block
    for step in sum_steps(size)[:-1]:
        block = block + lax.ppermute(block, axis, [(i, i ^ step) for i in range(size)])
    return block


def end_sum(block, axis, *tokens):
    size = lax.axis_size(axis)
    if size & (size - 1):
        return lax.psum(block, axis)
    for step in sum_steps(size)[-1:]:
        got = lax.ppermute(block, axis, [(i, i ^ step) for i in range(size)])
        block = block + (after(got, *tokens) if tokens else got)
    return block


def all_sum(block, axis, *tokens):
    return end_sum(start_sum(block, axis), axis, *tokens)


def factor(gram):
    size = gram.shape[0]
    tile = (8, 2 * size)
    row_id = lax.broadcasted_iota(jnp.int32, (size, size), 0)
    col_id = lax.broadcasted_iota(jnp.int32, (size, size), 1)
    work = jnp.concatenate([gram, (row_id == col_id).astype(F32)], axis=1)
    blocks = [work[8 * b : 8 * b + 8] for b in range(size // 8)]
    sub = lax.broadcasted_iota(jnp.int32, tile, 0)
    for j in range(0, size, 4):
        b, s = divmod(j, 8)
        later = range(b + s // 4, size // 8)
        line = [jnp.broadcast_to(blocks[b][s + k : s + k + 1], tile) for k in range(4)]
        cols = {
            o: [jnp.broadcast_to(blocks[o][:, j + k : j + k + 1], tile) for k in range(4)]
            for o in range(b, size // 8)
        }
        entry = {
            (k, l): jnp.broadcast_to(cols[b][l][s + k : s + k + 1], tile)
            for k in range(4)
            for l in range(k, 4)
        }
        scaled = []
        for k in range(4):
            inverse = 1.0 / entry[k, k]
            for l in range(k + 1, 4):
                ratio = entry[k, l] * inverse
                for p in range(l, 4):
                    entry[l, p] = entry[l, p] - ratio * entry[k, p]
                line[l] = line[l] - ratio * line[k]
                for o in later:
                    cols[o][l] = cols[o][l] - ratio * cols[o][k]
            scaled.append(inverse * line[k])
        for o in range(b, size // 8):
            new = blocks[o]
            if o in later:
                new = new - ((cols[o][0] * scaled[0] + cols[o][1] * scaled[1]) + (cols[o][2] * scaled[2] + cols[o][3] * scaled[3]))
            if o == b:
                new = jnp.where(sub > s + 3, new, blocks[o])
                for k in range(1, 4):
                    new = jnp.where(sub == s + k, line[k], new)
            blocks[o] = new
    work = jnp.concatenate(blocks, axis=0)
    pivots = jnp.sum(jnp.where(row_id == col_id, work[:, :size], 0.0), axis=1, keepdims=True)
    work = work / jnp.sqrt(pivots)
    upper = jnp.where(col_id >= row_id, work[:, :size], 0.0)
    inverse = jnp.where(col_id <= row_id, work[:, size:], 0.0)
    return upper, inverse


def local(start_block, diagonal, hess_tiles, tile_rows, tile_cols, slot_counts):
    peers = lax.axis_size("res")
    lanes = lax.axis_size("vec")
    rows, width, length = start_block.shape
    slots = hess_tiles.shape[2]
    half = rows // 2
    part = width // 2
    rounds = pairings(peers)
    count = len(rounds)
    full = (rows, width, length)
    halffull = (half, width, length)
    chunk = (rows, part, length)
    halfchunk = (half, part, length)
    packet = (CAP, part, length)
    square = (width, width)
    split_shape = jax.ShapeDtypeStruct((slots, 2, length, length), BF16)

    table = role_table(rounds, peers)
    place = jnp.concatenate(
        [lax.axis_index("vec").reshape(1), table[:, lax.axis_index("res")]]
    ).astype(jnp.int32)

    def own_sum(acc_refs, x_ref, split_ref, rows_ref, cols_ref):
        batch = 4
        for first in range(0, OWN_SLOTS, batch):
            members = range(first, first + batch)
            ends = [(rows_ref[0, 0, s], cols_ref[0, 0, s]) for s in members]
            terms = [
                (
                    tile_product(x_ref[j], split_ref, s, True),
                    tile_product(x_ref[i], split_ref, s, False),
                )
                for s, (i, j) in zip(members, ends)
            ]
            for (i, j), (direct, mirror) in zip(ends, terms):
                for n, acc_ref in enumerate(acc_refs):
                    acc_ref[i] += direct[n * part : (n + 1) * part]
                    acc_ref[j] += mirror[n * part : (n + 1) * part]

    def prepare_body(x_hbm, diag_hbm, tiles_hbm, *refs):
        x_ref, split_ref, a_ref, b_ref, diag_ref, raw_ref, sem = refs
        size = slots // 4
        copies = [
            pltpu.make_async_copy(src, dst, sem.at[n])
            for n, (src, dst) in enumerate([(x_hbm, x_ref), (diag_hbm, diag_ref)])
        ]
        tile_copies = [
            pltpu.make_async_copy(
                tiles_hbm.at[0, 0, pl.ds(n * size, size)], raw_ref.at[pl.ds(n * size, size)], sem.at[2 + n]
            )
            for n in range(4)
        ]
        for c in copies + tile_copies:
            c.start()
        for n in range(4):
            tile_copies[n].wait()
            for s in range(n * size, (n + 1) * size):
                split_ref[s, 0], split_ref[s, 1] = pieces(raw_ref[s], 2)
        for c in copies:
            c.wait()
        first = (lax.axis_index("vec") == 0).astype(F32)
        d = ((diag_ref[...] - SHIFT) * first)[:, None, :]
        a_ref[...] = x_ref[:, :part] * d
        b_ref[...] = x_ref[:, part:] * d

    def own_body(rows_ref, cols_ref, x_ref, split_ref, *refs):
        own_sum(refs[len(refs) // 2 :], x_ref, split_ref, rows_ref, cols_ref)

    def pack(place_ref, rows_ref, counts_ref, asked_refs, x_ref, split_ref, outs):
        for p in range(count):
            role = place_ref[1 + p]

            def put(c, value, p=p):
                for n, ref in enumerate(outs[p]):
                    ref[c] = value[n * part : (n + 1) * part]

            @pl.when(role > 0)
            def _():
                base = OWN_SLOTS + (role - 1) * CAP
                terms = [
                    tile_product(x_ref[rows_ref[0, 0, base + c]], split_ref, base + c, False)
                    for c in range(CAP)
                ]
                for c, term in enumerate(terms):
                    put(c, jnp.where(c < counts_ref[0, 0, role - 1], term, 0.0))

            @pl.when(role < 0)
            def _():
                base = OWN_SLOTS + (-role - 1) * CAP
                for c in range(CAP):
                    put(c, x_ref[asked_refs[p][0, 0, base + c]])

    def send_body(place_ref, rows_ref, counts_ref, *refs):
        asked_refs, (x_ref, split_ref), outs = refs[:count], refs[count : count + 2], refs[count + 2 :]
        pack(
            place_ref, rows_ref, counts_ref, asked_refs, x_ref, split_ref,
            [(outs[p], outs[count + p]) for p in range(count)],
        )

    def settle(place_ref, mine_ref, other_ref, y_ref):
        core = place_ref[0] % 2
        y_ref[pl.ds(core * half, half)] = mine_ref[...]
        y_ref[pl.ds((1 - core) * half, half)] = other_ref[...]

    def resend_body(place_ref, rows_ref, counts_ref, *refs):
        asked_refs = refs[:count]
        mine_ref, other_ref, diag_ref, split_ref, y_ref, acc_ref = refs[count : count + 6]
        outs = refs[count + 6 :]
        settle(place_ref, mine_ref, other_ref, y_ref)
        pack(
            place_ref, rows_ref, counts_ref, asked_refs, y_ref, split_ref,
            [(outs[p],) for p in range(count)],
        )
        first = (place_ref[0] == 0).astype(F32)
        acc_ref[...] = y_ref[...] * ((diag_ref[...] - SHIFT) * first)[:, None, :]

    def join_rounds(members, place_ref, rows_ref, counts_ref, asked_refs, got_refs, split_ref, acc_ref):
        for n, p in enumerate(members):
            role = place_ref[1 + p]

            @pl.when(role > 0)
            def _():
                base = OWN_SLOTS + (role - 1) * CAP
                terms = [
                    tile_product(got_refs[n][c], split_ref, base + c, True) for c in range(CAP)
                ]
                for c, term in enumerate(terms):
                    acc_ref[rows_ref[0, 0, base + c]] += jnp.where(
                        c < counts_ref[0, 0, role - 1], term, 0.0
                    )

            @pl.when(role < 0)
            def _():
                base = OWN_SLOTS + (-role - 1) * CAP
                for c in range(CAP):
                    acc_ref[asked_refs[n][0, 0, base + c]] += got_refs[n][c]

    def join(acc, got, members, last=False):
        size = len(members)

        def body(place_ref, rows_ref, counts_ref, *refs):
            asked_refs, got_refs = refs[:size], refs[size : 2 * size]
            split_ref, prior_ref = refs[2 * size : 2 * size + 2]
            outs = refs[2 * size + 2 :]
            if last:
                keep_ref, give_ref, acc_ref = outs
                acc_ref[...] = prior_ref[...]
            else:
                (acc_ref,) = outs
            join_rounds(
                members, place_ref, rows_ref, counts_ref, asked_refs, got_refs, split_ref, acc_ref
            )
            if last:
                core = place_ref[0] % 2
                keep_ref[...] = acc_ref[pl.ds(core * half, half)]
                give_ref[...] = acc_ref[pl.ds((1 - core) * half, half)]

        out = call(
            body,
            [halfchunk] * 2 if last else [chunk],
            [SMEM] * (3 + size) + [VMEM] * (size + 2),
            [pltpu.VMEM(chunk, F32)] if last else [],
            name="join",
            weight=10**10,
            aliases=None if last else {3 + 2 * size + 1: 0},
        )(
            place, tile_rows, slot_counts, *[asked[p] for p in members], *[got[p] for p in members], split, acc
        )
        return out if last else out[0]

    def gram_body(x_ref, out_ref):
        total = jnp.zeros(square, F32)
        for n in range(0, rows, 2):
            pair = [x_ref[n], x_ref[n + 1]]
            total += gram_step(pair, [pair])
        out_ref[...] = total

    def cross_body(x_ref, a_ref, b_ref, out_ref):
        total = jnp.zeros((width, 2 * width), F32)
        for n in range(0, rows, 2):
            y = [jnp.concatenate([a_ref[m], b_ref[m]], axis=0) for m in (n, n + 1)]
            total += gram_step(y, [[x_ref[n], x_ref[n + 1]], y])
        out_ref[...] = total

    def first_body(gram_ref, inverse_ref):
        _, inverse_ref[...] = factor(gram_ref[...])

    def identity():
        eye = lax.broadcasted_iota(jnp.int32, square, 0) == lax.broadcasted_iota(jnp.int32, square, 1)
        return eye.astype(F32)

    def lower_part():
        return lax.broadcasted_iota(jnp.int32, square, 0) >= lax.broadcasted_iota(jnp.int32, square, 1)

    def second_body(gram_ref, inverse_ref, cross_ref, lower_ref, coef_ref, gain_ref):
        start_inv = inverse_ref[...]
        cross = dot(dot(start_inv, gram_ref[:, :width]), start_inv, tb=True)
        applied = dot(dot(start_inv, gram_ref[:, width:]), start_inv, tb=True)
        upper, inverse = factor(applied - dot(cross, cross, tb=True))
        lower = upper.T
        cross_ref[...] = cross + SHIFT * identity()
        lower_ref[...] = lower
        gain = dot(inverse, start_inv)
        back = -dot(dot(inverse, cross), start_inv)
        gain_ref[...] = gain
        coef_ref[:width, :width] = -dot(lower, start_inv)
        coef_ref[:width, width : 2 * width] = back
        coef_ref[:width, 2 * width :] = gain
        coef_ref[width:, :width] = back
        coef_ref[width:, width : 2 * width] = gain
        coef_ref[width:, 2 * width :] = jnp.zeros(square, F32)

    def blend(side, mine, other, coef):
        def body(place_ref, x_ref, a_ref, b_ref, mine_ref, other_ref, coef_ref, w_ref, q_ref, out_ref, z_ref):
            settle(place_ref, mine_ref, other_ref, z_ref)
            for n in range(0, half, 2):
                stacks = [
                    jnp.concatenate([ref[side * half + m] for ref in (x_ref, a_ref, b_ref, z_ref)], axis=0)
                    for m in (n, n + 1)
                ]
                for m, both in zip((n, n + 1), wide_product(coef_ref[:, : 2 * width + part], stacks)):
                    w_ref[m] = both[:width]
                    q_ref[m] = both[width:]
            total = jnp.zeros(square, F32)
            for n in range(0, half, 2):
                qs = [q_ref[n], q_ref[n + 1]]
                total += gram_step(qs, [qs])
            out_ref[...] = total

        return call(
            body,
            [halffull, halffull, square],
            [SMEM] + [VMEM] * 6,
            [pltpu.VMEM(chunk, F32)],
            name="blend",
        )(place, x, y_a, y_b, mine, other, coef)

    def third_body(place_ref, mine_ref, other_ref, gain_ref, *refs):
        prior_refs, q_refs, norm_refs = refs[0:2], refs[2:4], refs[4:6]
        w_ref, out_ref, z_ref = refs[6:]
        settle(place_ref, mine_ref, other_ref, z_ref)
        for n in range(0, rows, 2):
            side, m = divmod(n, half)
            for k, w in enumerate(wide_product(gain_ref[:, part:], [z_ref[n], z_ref[n + 1]])):
                w_ref[n + k] = w + prior_refs[side][m + k]
        total = jnp.zeros((width, 2 * width), F32)
        for n in range(0, rows, 2):
            side, m = divmod(n, half)
            ws = [w_ref[n], w_ref[n + 1]]
            total += gram_step(ws, [[q_refs[side][m], q_refs[side][m + 1]], ws])
        norm = norm_refs[0][...] + norm_refs[1][...]
        out_ref[:width, :width] = total[:, :width]
        out_ref[:width, width:] = jnp.where(lower_part(), total[:, width:], norm)
        out_ref[width:, :] = jnp.zeros((8, 2 * width), F32)
        out_ref[width:, :width] = jnp.broadcast_to(
            jnp.sum(norm * identity(), axis=0, keepdims=True), (8, width)
        )

    def fourth_body(gram_ref, cross_ref, lower_ref, coef_ref):
        cross = gram_ref[:width, :width]
        packed = gram_ref[:width, width:]
        flipped = packed.T
        squares = jnp.where(lower_part(), packed, flipped)
        norm = jnp.where(lower_part(), flipped, packed)
        norm = jnp.where(identity() > 0, gram_ref[width : width + 1, :width], norm)
        taken = cross + SHIFT * (norm - identity())
        mixed = dot(taken, cross, tb=True)
        squared = squares - mixed - mixed.T + dot(dot(taken, norm), taken, tb=True)
        upper, inverse = factor(squared)
        cross_ref[...] = taken + SHIFT * identity()
        lower_ref[...] = upper.T
        scale = math.sqrt(rows * length * peers)
        coef_ref[:, :width] = inverse * scale
        coef_ref[:, width:] = -dot(inverse, taken) * scale

    def last_body(w_ref, low_ref, high_ref, coef_ref, a1_ref, l1_ref, a2_ref, l2_ref, out_ref, pack_ref):
        for n, ref in enumerate((a1_ref, l1_ref, a2_ref, l2_ref)):
            pack_ref[n] = ref[...]
        for n in range(0, rows, 2):
            side, at = divmod(n, half)
            q_ref = (low_ref, high_ref)[side]
            stacks = [jnp.concatenate([w_ref[n + k], q_ref[at + k]], axis=0) for k in range(2)]
            for m, out in zip((n, n + 1), wide_product(coef_ref[...], stacks, 4)):
                out_ref[m] = out

    swap = [(i, i ^ 1) for i in range(lanes)]
    cuts = [count * n // 3 for n in range(4)]
    groups = [list(range(cuts[n], cuts[n + 1])) for n in range(3)]

    def spread(sent):
        return [exchange(s, "res", entry["pairs"]) for s, entry in zip(sent, rounds)]

    def across(mine, *tokens):
        step = 2
        while step < lanes:
            got = lax.ppermute(mine, "vec", [(i, i ^ step) for i in range(lanes)])
            mine = mine + after(got, *tokens)
            step *= 2
        return mine

    def resend(mine, other):
        y, acc, *sent = call(
            resend_body,
            [chunk, chunk] + [packet] * count,
            [SMEM] * (3 + count) + [VMEM] * 4,
            name="resend",
        )(place, tile_rows, slot_counts, *asked, mine, other, diagonal, split)
        return y, acc, spread(sent)

    def own(y, *accs):
        return call(
            own_body,
            [chunk] * len(accs),
            [SMEM] * 2 + [VMEM] * (2 + len(accs)),
            name="own",
            aliases={4 + n: n for n in range(len(accs))},
        )(tile_rows, tile_cols, y, split, *accs)

    asked = [exchange(tile_cols, "res", entry["pairs"]) for entry in rounds]
    x, split, acc_a, acc_b = call(
        prepare_body,
        [full, split_shape, chunk, chunk],
        [HBM] * 3,
        [
            pltpu.VMEM(diagonal.shape, F32),
            pltpu.VMEM((slots, length, length), F32),
            pltpu.SemaphoreType.DMA((6,)),
        ],
        name="prepare",
    )(*[pinned(v) for v in (start_block, diagonal, hess_tiles)])
    sent = call(
        send_body, [packet] * (2 * count), [SMEM] * (3 + count) + [VMEM] * 2, name="send"
    )(place, tile_rows, slot_counts, *asked, x, split)
    got_a = spread(sent[:count])
    sent_b = list(sent[count:])
    acc_a, acc_b = own(x, after(acc_a, sent[0]), acc_b)
    for n in range(2):
        acc_a = join(acc_a, got_a, groups[n])
        turn = groups[0] if n == 1 else []
        acc_a, x, *gated = lax.optimization_barrier((acc_a, x, *[sent_b[p] for p in turn]))
        for p, value in zip(turn, gated):
            sent_b[p] = value
        if n == 0:
            (gram,) = call(gram_body, [square], [VMEM], name="gram")(x)
            start_gram = start_sum(gram, "res")
    acc_a = after(acc_a, start_gram)
    keep_a, give_a = join(acc_a, got_a, groups[2], last=True)
    for p in groups[1] + groups[2]:
        sent_b[p] = after(sent_b[p], keep_a)
    got_b = spread(sent_b)

    core = lax.ppermute(give_a, "vec", swap)
    acc_b = join(acc_b, got_b, groups[0])
    mine_a = keep_a + after(core, acc_b)
    (start_inv,) = call(first_body, [square], [VMEM], name="first")(end_sum(start_gram, "res", mine_a))
    acc_b = join(after(acc_b, start_inv), got_b, groups[1])
    mine_a = across(mine_a, acc_b)
    other_a = lax.ppermute(mine_a, "vec", swap)
    keep_b, give_b = join(acc_b, got_b, groups[2], last=True)
    y_a, acc_a, got_a = resend(mine_a, after(other_a, keep_b))

    core = lax.ppermute(give_b, "vec", swap)
    mine_b = keep_b + after(core, y_a)
    (acc_a,) = own(y_a, after(acc_a, mine_b))
    acc_a = join(acc_a, got_a, groups[2])
    acc_a = join(acc_a, got_a, groups[1])
    mine_b = across(mine_b, acc_a)
    other_b = lax.ppermute(mine_b, "vec", swap)
    keep_a, give_a = join(acc_a, got_a, groups[0], last=True)
    y_b, acc_b, got_b = resend(mine_b, after(other_b, keep_a))

    core = lax.ppermute(give_a, "vec", swap)
    mine_a = keep_a + after(core, y_b)
    (gram,) = call(cross_body, [(width, 2 * width)], [VMEM] * 3, name="cross")(x, y_a, after(y_b, mine_a))
    cross_gram = start_sum(gram, "res")
    acc_b = join(after(acc_b, cross_gram), got_b, groups[2])
    (acc_b,) = own(y_b, acc_b)
    acc_b = join(acc_b, got_b, groups[1])
    cross_gram = end_sum(cross_gram, "res", acc_b)
    acc_b = after(acc_b, cross_gram)
    mine_a = across(mine_a, acc_b)
    other_a = lax.ppermute(mine_a, "vec", swap)
    keep_b, give_b = join(acc_b, got_b, groups[0], last=True)

    core = lax.ppermute(give_b, "vec", swap)
    mine_b = keep_b + core
    cross1, lower1, coef, gain = call(
        second_body, [square, square, (2 * width, 3 * width), square], [VMEM] * 2, name="second"
    )(after(cross_gram, mine_b), start_inv)
    w_low, q_low, norm_low = blend(0, mine_a, other_a, coef)
    w_high, q_high, norm_high = blend(1, mine_a, other_a, coef)
    mine_b = across(mine_b, norm_low, norm_high)
    other_b = lax.ppermute(mine_b, "vec", swap)
    w, gram = call(
        third_body,
        [full, (width + 8, 2 * width)],
        [SMEM] + [VMEM] * 9,
        [pltpu.VMEM(chunk, F32)],
        name="third",
    )(place, mine_b, other_b, gain, w_low, w_high, q_low, q_high, norm_low, norm_high)
    gram = all_sum(gram, "res")
    cross2, lower2, coef = call(
        fourth_body, [square, square, (width, 2 * width)], [VMEM], name="fourth"
    )(gram)
    return call(last_body, [full, (4, width, width)], [VMEM] * 8, name="last")(
        w, q_low, q_high, coef, cross1, lower1, cross2, lower2
    )


def solution(mesh):
    in_specs = (
        P(("conf", "res"), None, None),
        P(("conf", "res"), None),
        P(("conf", "res"), "vec", None, None, None),
        P(("conf", "res"), "vec", None),
        P(("conf", "res"), "vec", None),
        P(("conf", "res"), "vec", None),
    )
    out_specs = (P(("conf", "res"), None, None), P("conf", None, None))
    return jax.shard_map(local, mesh=mesh, in_specs=in_specs, out_specs=out_specs, check_vma=False)
```

```python
import math

import jax
import jax.numpy as jnp
from jax import lax
from jax.experimental import pallas as pl
from jax.experimental.pallas import tpu as pltpu
from jax.sharding import PartitionSpec as P

OWN_SLOTS = 20
HOPS = 3
CAP = 8
SHIFT = 1.65
BF16 = jnp.bfloat16
F32 = jnp.float32

VMEM = pl.BlockSpec(memory_space=pltpu.VMEM)
SMEM = pl.BlockSpec(memory_space=pltpu.SMEM)
HBM = pl.BlockSpec(memory_space=pltpu.HBM)


def contract(a, b, ta=False, tb=False, precision=None):
    dims = (((0 if ta else 1,), (1 if tb else 0,)), ((), ()))
    return lax.dot_general(a, b, dims, precision=precision, preferred_element_type=F32)


def dot(a, b, ta=False, tb=False):
    return contract(a, b, ta, tb, lax.Precision.HIGHEST)


def pieces(x, count):
    out = []
    for _ in range(count):
        out.append(x.astype(BF16))
        x = x - out[-1].astype(F32)
    return out


def tile_product(x, tile_ref, slot, transposed):
    x1, x2 = pieces(x, 2)
    m1, m2 = tile_ref[slot, 0], tile_ref[slot, 1]
    axis = 1 if transposed else 0
    left = jnp.concatenate([x1, x2, x1], axis=1)
    return contract(left, jnp.concatenate([m1, m1, m2], axis=axis), tb=transposed)


def wide_product(coef, blocks, terms=6):
    pairs = [(0, 0), (0, 1), (1, 0), (1, 1)] if terms == 4 else [(0, 0), (0, 1), (0, 2), (1, 0), (1, 1), (2, 0)]
    c = pieces(coef, terms // 2)
    z = pieces(jnp.concatenate(blocks, axis=1), terms // 2)
    left = jnp.concatenate([c[m] for m, _ in pairs], axis=1)
    out = contract(left, jnp.concatenate([z[m] for _, m in pairs], axis=0))
    width = blocks[0].shape[1]
    return [out[:, n * width : (n + 1) * width] for n in range(len(blocks))]


def gram_step(left, right):
    a = jnp.concatenate(pieces(jnp.concatenate(left, axis=1), 2), axis=0)
    b = jnp.concatenate(
        [p for group in right for p in pieces(jnp.concatenate(group, axis=1), 2)], axis=0
    )
    out = contract(a, b, tb=True)
    size = left[0].shape[0]
    out = out[:size] + out[size:]
    return jnp.concatenate(
        [
            out[:, 2 * g * size : (2 * g + 1) * size] + out[:, (2 * g + 1) * size : (2 * g + 2) * size]
            for g in range(len(right))
        ],
        axis=1,
    )


def call(body, outs, in_specs, scratch=(), name=None, aliases=None, weight=0):
    shapes = [
        o if isinstance(o, jax.ShapeDtypeStruct) else jax.ShapeDtypeStruct(o, F32) for o in outs
    ]
    return pl.pallas_call(
        body,
        out_shape=shapes,
        in_specs=in_specs,
        out_specs=[VMEM] * len(outs),
        scratch_shapes=list(scratch),
        compiler_params=pltpu.CompilerParams(vmem_limit_bytes=40 << 20),
        input_output_aliases=aliases or {},
        cost_estimate=pl.CostEstimate(flops=weight, bytes_accessed=weight, transcendentals=0) if weight else None,
        name=name,
    )


def pinned(value):
    return pltpu.with_memory_space_constraint(value, pltpu.HBM)


def after(value, *tokens):
    return lax.optimization_barrier((value,) + tokens)[0]


def pairings(size):
    rounds = []
    for hop in range(1, HOPS + 1):
        for parity in range(2):
            pairs = [(i, i + hop) for i in range(size - hop) if (i // hop) % 2 == parity]
            if not pairs:
                continue
            used = {i for pair in pairs for i in pair}
            for entry in rounds:
                if not entry["used"] & used:
                    entry["used"] |= used
                    entry["pairs"] += pairs
                    entry["kinds"].append((hop, parity))
                    break
            else:
                rounds.append({"used": used, "pairs": pairs, "kinds": [(hop, parity)]})
    return rounds


def exchange(block, axis, pairs):
    return lax.ppermute(block, axis, [(a, b) for a, b in pairs] + [(b, a) for a, b in pairs])


def role_table(rounds, size):
    table = [[0] * size for _ in rounds]
    for p, entry in enumerate(rounds):
        for a, b in entry["pairs"]:
            table[p][a] = b - a
            table[p][b] = a - b
    return jnp.array(table, jnp.int32)


def sum_steps(size):
    return [1 << n for n in range(size.bit_length() - 1)]


def start_sum(block, axis):
    size = lax.axis_size(axis)
    if size & (size - 1):
        return block
    for step in sum_steps(size)[:-1]:
        block = block + lax.ppermute(block, axis, [(i, i ^ step) for i in range(size)])
    return block


def end_sum(block, axis, *tokens):
    size = lax.axis_size(axis)
    if size & (size - 1):
        return lax.psum(block, axis)
    for step in sum_steps(size)[-1:]:
        got = lax.ppermute(block, axis, [(i, i ^ step) for i in range(size)])
        block = block + (after(got, *tokens) if tokens else got)
    return block


def all_sum(block, axis, *tokens):
    return end_sum(start_sum(block, axis), axis, *tokens)


def factor(gram):
    size = gram.shape[0]
    tile = (8, 2 * size)
    row_id = lax.broadcasted_iota(jnp.int32, (size, size), 0)
    col_id = lax.broadcasted_iota(jnp.int32, (size, size), 1)
    work = jnp.concatenate([gram, (row_id == col_id).astype(F32)], axis=1)
    blocks = [work[8 * b : 8 * b + 8] for b in range(size // 8)]
    sub = lax.broadcasted_iota(jnp.int32, tile, 0)
    for j in range(0, size, 4):
        b, s = divmod(j, 8)
        later = range(b + s // 4, size // 8)
        line = [jnp.broadcast_to(blocks[b][s + k : s + k + 1], tile) for k in range(4)]
        cols = {
            o: [jnp.broadcast_to(blocks[o][:, j + k : j + k + 1], tile) for k in range(4)]
            for o in range(b, size // 8)
        }
        entry = {
            (k, l): jnp.broadcast_to(cols[b][l][s + k : s + k + 1], tile)
            for k in range(4)
            for l in range(k, 4)
        }
        scaled = []
        for k in range(4):
            inverse = 1.0 / entry[k, k]
            for l in range(k + 1, 4):
                ratio = entry[k, l] * inverse
                for p in range(l, 4):
                    entry[l, p] = entry[l, p] - ratio * entry[k, p]
                line[l] = line[l] - ratio * line[k]
                for o in later:
                    cols[o][l] = cols[o][l] - ratio * cols[o][k]
            scaled.append(inverse * line[k])
        for o in range(b, size // 8):
            new = blocks[o]
            if o in later:
                new = new - ((cols[o][0] * scaled[0] + cols[o][1] * scaled[1]) + (cols[o][2] * scaled[2] + cols[o][3] * scaled[3]))
            if o == b:
                new = jnp.where(sub > s + 3, new, blocks[o])
                for k in range(1, 4):
                    new = jnp.where(sub == s + k, line[k], new)
            blocks[o] = new
    work = jnp.concatenate(blocks, axis=0)
    pivots = jnp.sum(jnp.where(row_id == col_id, work[:, :size], 0.0), axis=1, keepdims=True)
    work = work / jnp.sqrt(pivots)
    upper = jnp.where(col_id >= row_id, work[:, :size], 0.0)
    inverse = jnp.where(col_id <= row_id, work[:, size:], 0.0)
    return upper, inverse


def local(start_block, diagonal, hess_tiles, tile_rows, tile_cols, slot_counts):
    peers = lax.axis_size("res")
    lanes = lax.axis_size("vec")
    rows, width, length = start_block.shape
    slots = hess_tiles.shape[2]
    half = rows // 2
    part = width // 2
    rounds = pairings(peers)
    count = len(rounds)
    full = (rows, width, length)
    halffull = (half, width, length)
    chunk = (rows, part, length)
    halfchunk = (half, part, length)
    packet = (CAP, part, length)
    square = (width, width)
    split_shape = jax.ShapeDtypeStruct((slots, 2, length, length), BF16)

    table = role_table(rounds, peers)
    place = jnp.concatenate(
        [lax.axis_index("vec").reshape(1), table[:, lax.axis_index("res")]]
    ).astype(jnp.int32)

    def own_sum(acc_refs, x_ref, split_ref, rows_ref, cols_ref):
        batch = 4
        for first in range(0, OWN_SLOTS, batch):
            members = range(first, first + batch)
            ends = [(rows_ref[0, 0, s], cols_ref[0, 0, s]) for s in members]
            terms = [
                (
                    tile_product(x_ref[j], split_ref, s, True),
                    tile_product(x_ref[i], split_ref, s, False),
                )
                for s, (i, j) in zip(members, ends)
            ]
            for (i, j), (direct, mirror) in zip(ends, terms):
                for n, acc_ref in enumerate(acc_refs):
                    acc_ref[i] += direct[n * part : (n + 1) * part]
                    acc_ref[j] += mirror[n * part : (n + 1) * part]

    def prepare_body(x_hbm, diag_hbm, tiles_hbm, *refs):
        x_ref, split_ref, a_ref, b_ref, diag_ref, raw_ref, sem = refs
        size = slots // 4
        copies = [
            pltpu.make_async_copy(src, dst, sem.at[n])
            for n, (src, dst) in enumerate([(x_hbm, x_ref), (diag_hbm, diag_ref)])
        ]
        tile_copies = [
            pltpu.make_async_copy(
                tiles_hbm.at[0, 0, pl.ds(n * size, size)], raw_ref.at[pl.ds(n * size, size)], sem.at[2 + n]
            )
            for n in range(4)
        ]
        for c in copies + tile_copies:
            c.start()
        for n in range(4):
            tile_copies[n].wait()
            for s in range(n * size, (n + 1) * size):
                split_ref[s, 0], split_ref[s, 1] = pieces(raw_ref[s], 2)
        for c in copies:
            c.wait()
        first = (lax.axis_index("vec") == 0).astype(F32)
        d = ((diag_ref[...] - SHIFT) * first)[:, None, :]
        a_ref[...] = x_ref[:, :part] * d
        b_ref[...] = x_ref[:, part:] * d

    def own_body(rows_ref, cols_ref, x_ref, split_ref, *refs):
        own_sum(refs[len(refs) // 2 :], x_ref, split_ref, rows_ref, cols_ref)

    def pack(place_ref, rows_ref, counts_ref, asked_refs, x_ref, split_ref, outs):
        for p in range(count):
            role = place_ref[1 + p]

            def put(c, value, p=p):
                for n, ref in enumerate(outs[p]):
                    ref[c] = value[n * part : (n + 1) * part]

            @pl.when(role > 0)
            def _():
                base = OWN_SLOTS + (role - 1) * CAP
                terms = [
                    tile_product(x_ref[rows_ref[0, 0, base + c]], split_ref, base + c, False)
                    for c in range(CAP)
                ]
                for c, term in enumerate(terms):
                    put(c, jnp.where(c < counts_ref[0, 0, role - 1], term, 0.0))

            @pl.when(role < 0)
            def _():
                base = OWN_SLOTS + (-role - 1) * CAP
                for c in range(CAP):
                    put(c, x_ref[asked_refs[p][0, 0, base + c]])

    def send_body(place_ref, rows_ref, counts_ref, *refs):
        asked_refs, (x_ref, split_ref), outs = refs[:count], refs[count : count + 2], refs[count + 2 :]
        pack(
            place_ref, rows_ref, counts_ref, asked_refs, x_ref, split_ref,
            [(outs[p], outs[count + p]) for p in range(count)],
        )

    def settle(place_ref, mine_ref, other_ref, y_ref):
        core = place_ref[0] % 2
        y_ref[pl.ds(core * half, half)] = mine_ref[...]
        y_ref[pl.ds((1 - core) * half, half)] = other_ref[...]

    def resend_body(place_ref, rows_ref, counts_ref, *refs):
        asked_refs = refs[:count]
        mine_ref, other_ref, diag_ref, split_ref, y_ref, acc_ref = refs[count : count + 6]
        outs = refs[count + 6 :]
        settle(place_ref, mine_ref, other_ref, y_ref)
        pack(
            place_ref, rows_ref, counts_ref, asked_refs, y_ref, split_ref,
            [(outs[p],) for p in range(count)],
        )
        first = (place_ref[0] == 0).astype(F32)
        acc_ref[...] = y_ref[...] * ((diag_ref[...] - SHIFT) * first)[:, None, :]

    def join_rounds(members, place_ref, rows_ref, counts_ref, asked_refs, got_refs, split_ref, acc_ref):
        for n, p in enumerate(members):
            role = place_ref[1 + p]

            @pl.when(role > 0)
            def _():
                base = OWN_SLOTS + (role - 1) * CAP
                terms = [
                    tile_product(got_refs[n][c], split_ref, base + c, True) for c in range(CAP)
                ]
                for c, term in enumerate(terms):
                    acc_ref[rows_ref[0, 0, base + c]] += jnp.where(
                        c < counts_ref[0, 0, role - 1], term, 0.0
                    )

            @pl.when(role < 0)
            def _():
                base = OWN_SLOTS + (-role - 1) * CAP
                for c in range(CAP):
                    acc_ref[asked_refs[n][0, 0, base + c]] += got_refs[n][c]

    def join(acc, got, members, last=False):
        size = len(members)

        def body(place_ref, rows_ref, counts_ref, *refs):
            asked_refs, got_refs = refs[:size], refs[size : 2 * size]
            split_ref, prior_ref = refs[2 * size : 2 * size + 2]
            outs = refs[2 * size + 2 :]
            if last:
                keep_ref, give_ref, acc_ref = outs
                acc_ref[...] = prior_ref[...]
            else:
                (acc_ref,) = outs
            join_rounds(
                members, place_ref, rows_ref, counts_ref, asked_refs, got_refs, split_ref, acc_ref
            )
            if last:
                core = place_ref[0] % 2
                keep_ref[...] = acc_ref[pl.ds(core * half, half)]
                give_ref[...] = acc_ref[pl.ds((1 - core) * half, half)]

        out = call(
            body,
            [halfchunk] * 2 if last else [chunk],
            [SMEM] * (3 + size) + [VMEM] * (size + 2),
            [pltpu.VMEM(chunk, F32)] if last else [],
            name="join",
            weight=10**10,
            aliases=None if last else {3 + 2 * size + 1: 0},
        )(
            place, tile_rows, slot_counts, *[asked[p] for p in members], *[got[p] for p in members], split, acc
        )
        return out if last else out[0]

    def gram_body(x_ref, out_ref):
        total = jnp.zeros(square, F32)
        for n in range(0, rows, 2):
            pair = [x_ref[n], x_ref[n + 1]]
            total += gram_step(pair, [pair])
        out_ref[...] = total

    def cross_body(x_ref, a_ref, b_ref, out_ref):
        total = jnp.zeros((width, 2 * width), F32)
        for n in range(0, rows, 2):
            y = [jnp.concatenate([a_ref[m], b_ref[m]], axis=0) for m in (n, n + 1)]
            total += gram_step(y, [[x_ref[n], x_ref[n + 1]], y])
        out_ref[...] = total

    def first_body(gram_ref, inverse_ref):
        _, inverse_ref[...] = factor(gram_ref[...])

    def identity():
        eye = lax.broadcasted_iota(jnp.int32, square, 0) == lax.broadcasted_iota(jnp.int32, square, 1)
        return eye.astype(F32)

    def lower_part():
        return lax.broadcasted_iota(jnp.int32, square, 0) >= lax.broadcasted_iota(jnp.int32, square, 1)

    def second_body(gram_ref, inverse_ref, cross_ref, lower_ref, coef_ref, gain_ref):
        start_inv = inverse_ref[...]
        cross = dot(dot(start_inv, gram_ref[:, :width]), start_inv, tb=True)
        applied = dot(dot(start_inv, gram_ref[:, width:]), start_inv, tb=True)
        upper, inverse = factor(applied - dot(cross, cross, tb=True))
        lower = upper.T
        cross_ref[...] = cross + SHIFT * identity()
        lower_ref[...] = lower
        gain = dot(inverse, start_inv)
        back = -dot(dot(inverse, cross), start_inv)
        gain_ref[...] = gain
        coef_ref[:width, :width] = -dot(lower, start_inv)
        coef_ref[:width, width : 2 * width] = back
        coef_ref[:width, 2 * width :] = gain
        coef_ref[width:, :width] = back
        coef_ref[width:, width : 2 * width] = gain
        coef_ref[width:, 2 * width :] = jnp.zeros(square, F32)

    def blend(side, mine, other, coef):
        def body(place_ref, x_ref, a_ref, b_ref, mine_ref, other_ref, coef_ref, w_ref, q_ref, out_ref, z_ref):
            settle(place_ref, mine_ref, other_ref, z_ref)
            for n in range(0, half, 2):
                stacks = [
                    jnp.concatenate([ref[side * half + m] for ref in (x_ref, a_ref, b_ref, z_ref)], axis=0)
                    for m in (n, n + 1)
                ]
                for m, both in zip((n, n + 1), wide_product(coef_ref[:, : 2 * width + part], stacks)):
                    w_ref[m] = both[:width]
                    q_ref[m] = both[width:]
            total = jnp.zeros(square, F32)
            for n in range(0, half, 2):
                qs = [q_ref[n], q_ref[n + 1]]
                total += gram_step(qs, [qs])
            out_ref[...] = total

        return call(
            body,
            [halffull, halffull, square],
            [SMEM] + [VMEM] * 6,
            [pltpu.VMEM(chunk, F32)],
            name="blend",
        )(place, x, y_a, y_b, mine, other, coef)

    def third_body(place_ref, mine_ref, other_ref, gain_ref, *refs):
        prior_refs, q_refs, norm_refs = refs[0:2], refs[2:4], refs[4:6]
        w_ref, out_ref, z_ref = refs[6:]
        settle(place_ref, mine_ref, other_ref, z_ref)
        for n in range(0, rows, 2):
            side, m = divmod(n, half)
            for k, w in enumerate(wide_product(gain_ref[:, part:], [z_ref[n], z_ref[n + 1]])):
                w_ref[n + k] = w + prior_refs[side][m + k]
        total = jnp.zeros((width, 2 * width), F32)
        for n in range(0, rows, 2):
            side, m = divmod(n, half)
            ws = [w_ref[n], w_ref[n + 1]]
            total += gram_step(ws, [[q_refs[side][m], q_refs[side][m + 1]], ws])
        norm = norm_refs[0][...] + norm_refs[1][...]
        out_ref[:width, :width] = total[:, :width]
        out_ref[:width, width:] = jnp.where(lower_part(), total[:, width:], norm)
        out_ref[width:, :] = jnp.zeros((8, 2 * width), F32)
        out_ref[width:, :width] = jnp.broadcast_to(
            jnp.sum(norm * identity(), axis=0, keepdims=True), (8, width)
        )

    def fourth_body(gram_ref, cross_ref, lower_ref, coef_ref):
        cross = gram_ref[:width, :width]
        packed = gram_ref[:width, width:]
        flipped = packed.T
        squares = jnp.where(lower_part(), packed, flipped)
        norm = jnp.where(lower_part(), flipped, packed)
        norm = jnp.where(identity() > 0, gram_ref[width : width + 1, :width], norm)
        taken = cross + SHIFT * (norm - identity())
        mixed = dot(taken, cross, tb=True)
        squared = squares - mixed - mixed.T + dot(dot(taken, norm), taken, tb=True)
        upper, inverse = factor(squared)
        cross_ref[...] = taken + SHIFT * identity()
        lower_ref[...] = upper.T
        scale = math.sqrt(rows * length * peers)
        coef_ref[:, :width] = inverse * scale
        coef_ref[:, width:] = -dot(inverse, taken) * scale

    def last_body(w_ref, low_ref, high_ref, coef_ref, a1_ref, l1_ref, a2_ref, l2_ref, out_ref, pack_ref):
        for n, ref in enumerate((a1_ref, l1_ref, a2_ref, l2_ref)):
            pack_ref[n] = ref[...]
        for n in range(0, rows, 2):
            side, at = divmod(n, half)
            q_ref = (low_ref, high_ref)[side]
            stacks = [jnp.concatenate([w_ref[n + k], q_ref[at + k]], axis=0) for k in range(2)]
            for m, out in zip((n, n + 1), wide_product(coef_ref[...], stacks, 4)):
                out_ref[m] = out

    swap = [(i, i ^ 1) for i in range(lanes)]
    cuts = [count * n // 3 for n in range(4)]
    groups = [list(range(cuts[n], cuts[n + 1])) for n in range(3)]

    def spread(sent):
        return [exchange(s, "res", entry["pairs"]) for s, entry in zip(sent, rounds)]

    def across(mine, *tokens):
        step = 2
        while step < lanes:
            got = lax.ppermute(mine, "vec", [(i, i ^ step) for i in range(lanes)])
            mine = mine + after(got, *tokens)
            step *= 2
        return mine

    def resend(mine, other):
        y, acc, *sent = call(
            resend_body,
            [chunk, chunk] + [packet] * count,
            [SMEM] * (3 + count) + [VMEM] * 4,
            name="resend",
        )(place, tile_rows, slot_counts, *asked, mine, other, diagonal, split)
        return y, acc, spread(sent)

    def own(y, *accs):
        return call(
            own_body,
            [chunk] * len(accs),
            [SMEM] * 2 + [VMEM] * (2 + len(accs)),
            name="own",
            aliases={4 + n: n for n in range(len(accs))},
        )(tile_rows, tile_cols, y, split, *accs)

    asked = [exchange(tile_cols, "res", entry["pairs"]) for entry in rounds]
    x, split, acc_a, acc_b = call(
        prepare_body,
        [full, split_shape, chunk, chunk],
        [HBM] * 3,
        [
            pltpu.VMEM(diagonal.shape, F32),
            pltpu.VMEM((slots, length, length), F32),
            pltpu.SemaphoreType.DMA((6,)),
        ],
        name="prepare",
    )(*[pinned(v) for v in (start_block, diagonal, hess_tiles)])
    sent = call(
        send_body, [packet] * (2 * count), [SMEM] * (3 + count) + [VMEM] * 2, name="send"
    )(place, tile_rows, slot_counts, *asked, x, split)
    got_a = spread(sent[:count])
    sent_b = list(sent[count:])
    acc_a, acc_b = own(x, after(acc_a, sent[0]), acc_b)
    for n in range(2):
        acc_a = join(acc_a, got_a, groups[n])
        turn = groups[0] if n == 1 else []
        acc_a, x, *gated = lax.optimization_barrier((acc_a, x, *[sent_b[p] for p in turn]))
        for p, value in zip(turn, gated):
            sent_b[p] = value
        if n == 0:
            (gram,) = call(gram_body, [square], [VMEM], name="gram")(x)
            start_gram = start_sum(gram, "res")
    acc_a = after(acc_a, start_gram)
    keep_a, give_a = join(acc_a, got_a, groups[2], last=True)
    for p in groups[1] + groups[2]:
        sent_b[p] = after(sent_b[p], keep_a)
    got_b = spread(sent_b)

    core = lax.ppermute(give_a, "vec", swap)
    acc_b = join(acc_b, got_b, groups[0])
    mine_a = keep_a + after(core, acc_b)
    (start_inv,) = call(first_body, [square], [VMEM], name="first")(end_sum(start_gram, "res", mine_a))
    acc_b = join(after(acc_b, start_inv), got_b, groups[1])
    mine_a = across(mine_a, acc_b)
    other_a = lax.ppermute(mine_a, "vec", swap)
    keep_b, give_b = join(acc_b, got_b, groups[2], last=True)
    y_a, acc_a, got_a = resend(mine_a, after(other_a, keep_b))

    core = lax.ppermute(give_b, "vec", swap)
    mine_b = keep_b + after(core, y_a)
    (acc_a,) = own(y_a, after(acc_a, mine_b))
    mine_b = across(mine_b, acc_a)
    other_b = lax.ppermute(mine_b, "vec", swap)
    acc_a = join(after(acc_a, mine_b), got_a, groups[2])
    y_b, acc_b, got_b = resend(mine_b, after(other_b, acc_a))
    acc_a = join(after(acc_a, y_b), got_a, groups[1])
    keep_a, give_a = join(acc_a, got_a, groups[0], last=True)

    core = lax.ppermute(give_a, "vec", swap)
    acc_b = join(acc_b, got_b, groups[0])
    mine_a = keep_a + after(core, acc_b)
    (gram,) = call(cross_body, [(width, 2 * width)], [VMEM] * 3, name="cross")(x, y_a, after(y_b, mine_a))
    cross_gram = start_sum(gram, "res")
    (acc_b,) = own(y_b, after(acc_b, gram))
    acc_b = after(acc_b, cross_gram)
    acc_b = join(acc_b, got_b, groups[1])
    cross_gram = end_sum(cross_gram, "res", acc_b)
    acc_b = after(acc_b, cross_gram)
    mine_a = across(mine_a, acc_b)
    other_a = lax.ppermute(mine_a, "vec", swap)
    keep_b, give_b = join(acc_b, got_b, groups[2], last=True)

    core = lax.ppermute(give_b, "vec", swap)
    mine_b = keep_b + core
    cross1, lower1, coef, gain = call(
        second_body, [square, square, (2 * width, 3 * width), square], [VMEM] * 2, name="second"
    )(after(cross_gram, mine_b), start_inv)
    w_low, q_low, norm_low = blend(0, mine_a, other_a, coef)
    w_high, q_high, norm_high = blend(1, mine_a, other_a, coef)
    mine_b = across(mine_b, norm_low, norm_high)
    other_b = lax.ppermute(mine_b, "vec", swap)
    w, gram = call(
        third_body,
        [full, (width + 8, 2 * width)],
        [SMEM] + [VMEM] * 9,
        [pltpu.VMEM(chunk, F32)],
        name="third",
    )(place, mine_b, other_b, gain, w_low, w_high, q_low, q_high, norm_low, norm_high)
    gram = all_sum(gram, "res")
    cross2, lower2, coef = call(
        fourth_body, [square, square, (width, 2 * width)], [VMEM], name="fourth"
    )(gram)
    return call(last_body, [full, (4, width, width)], [VMEM] * 8, name="last")(
        w, q_low, q_high, coef, cross1, lower1, cross2, lower2
    )


def solution(mesh):
    in_specs = (
        P(("conf", "res"), None, None),
        P(("conf", "res"), None),
        P(("conf", "res"), "vec", None, None, None),
        P(("conf", "res"), "vec", None),
        P(("conf", "res"), "vec", None),
        P(("conf", "res"), "vec", None),
    )
    out_specs = (P(("conf", "res"), None, None), P("conf", None, None))
    return jax.shard_map(local, mesh=mesh, in_specs=in_specs, out_specs=out_specs, check_vma=False)
```

```python
import math

import jax
import jax.numpy as jnp
from jax import lax
from jax.experimental import pallas as pl
from jax.experimental.pallas import tpu as pltpu
from jax.sharding import PartitionSpec as P

OWN_SLOTS = 20
HOPS = 3
CAP = 8
SHIFT = 1.65
BF16 = jnp.bfloat16
F32 = jnp.float32

VMEM = pl.BlockSpec(memory_space=pltpu.VMEM)
SMEM = pl.BlockSpec(memory_space=pltpu.SMEM)
HBM = pl.BlockSpec(memory_space=pltpu.HBM)


def contract(a, b, ta=False, tb=False, precision=None):
    dims = (((0 if ta else 1,), (1 if tb else 0,)), ((), ()))
    return lax.dot_general(a, b, dims, precision=precision, preferred_element_type=F32)


def dot(a, b, ta=False, tb=False):
    return contract(a, b, ta, tb, lax.Precision.HIGHEST)


def pieces(x, count):
    out = []
    for _ in range(count):
        out.append(x.astype(BF16))
        x = x - out[-1].astype(F32)
    return out


def tile_product(x, tile_ref, slot, transposed):
    x1, x2 = pieces(x, 2)
    m1, m2 = tile_ref[slot, 0], tile_ref[slot, 1]
    axis = 1 if transposed else 0
    left = jnp.concatenate([x1, x2, x1], axis=1)
    return contract(left, jnp.concatenate([m1, m1, m2], axis=axis), tb=transposed)


def wide_product(coef, blocks, terms=6):
    pairs = [(0, 0), (0, 1), (1, 0), (1, 1)] if terms == 4 else [(0, 0), (0, 1), (0, 2), (1, 0), (1, 1), (2, 0)]
    c = pieces(coef, terms // 2)
    z = pieces(jnp.concatenate(blocks, axis=1), terms // 2)
    left = jnp.concatenate([c[m] for m, _ in pairs], axis=1)
    out = contract(left, jnp.concatenate([z[m] for _, m in pairs], axis=0))
    width = blocks[0].shape[1]
    return [out[:, n * width : (n + 1) * width] for n in range(len(blocks))]


def gram_step(left, right):
    a = jnp.concatenate(pieces(jnp.concatenate(left, axis=1), 2), axis=0)
    b = jnp.concatenate(
        [p for group in right for p in pieces(jnp.concatenate(group, axis=1), 2)], axis=0
    )
    out = contract(a, b, tb=True)
    size = left[0].shape[0]
    out = out[:size] + out[size:]
    return jnp.concatenate(
        [
            out[:, 2 * g * size : (2 * g + 1) * size] + out[:, (2 * g + 1) * size : (2 * g + 2) * size]
            for g in range(len(right))
        ],
        axis=1,
    )


def call(body, outs, in_specs, scratch=(), name=None, aliases=None, weight=0):
    shapes = [
        o if isinstance(o, jax.ShapeDtypeStruct) else jax.ShapeDtypeStruct(o, F32) for o in outs
    ]
    return pl.pallas_call(
        body,
        out_shape=shapes,
        in_specs=in_specs,
        out_specs=[VMEM] * len(outs),
        scratch_shapes=list(scratch),
        compiler_params=pltpu.CompilerParams(vmem_limit_bytes=40 << 20),
        input_output_aliases=aliases or {},
        cost_estimate=pl.CostEstimate(flops=weight, bytes_accessed=weight, transcendentals=0) if weight else None,
        name=name,
    )


def pinned(value):
    return pltpu.with_memory_space_constraint(value, pltpu.HBM)


def after(value, *tokens):
    return lax.optimization_barrier((value,) + tokens)[0]


def pairings(size):
    rounds = []
    for hop in range(1, HOPS + 1):
        for parity in range(2):
            pairs = [(i, i + hop) for i in range(size - hop) if (i // hop) % 2 == parity]
            if not pairs:
                continue
            used = {i for pair in pairs for i in pair}
            for entry in rounds:
                if not entry["used"] & used:
                    entry["used"] |= used
                    entry["pairs"] += pairs
                    entry["kinds"].append((hop, parity))
                    break
            else:
                rounds.append({"used": used, "pairs": pairs, "kinds": [(hop, parity)]})
    return rounds


def exchange(block, axis, pairs):
    return lax.ppermute(block, axis, [(a, b) for a, b in pairs] + [(b, a) for a, b in pairs])


def role_table(rounds, size):
    table = [[0] * size for _ in rounds]
    for p, entry in enumerate(rounds):
        for a, b in entry["pairs"]:
            table[p][a] = b - a
            table[p][b] = a - b
    return jnp.array(table, jnp.int32)


def sum_steps(size):
    return [1 << n for n in range(size.bit_length() - 1)]


def start_sum(block, axis):
    size = lax.axis_size(axis)
    if size & (size - 1):
        return block
    for step in sum_steps(size)[:-1]:
        block = block + lax.ppermute(block, axis, [(i, i ^ step) for i in range(size)])
    return block


def end_sum(block, axis, *tokens):
    size = lax.axis_size(axis)
    if size & (size - 1):
        return lax.psum(block, axis)
    for step in sum_steps(size)[-1:]:
        got = lax.ppermute(block, axis, [(i, i ^ step) for i in range(size)])
        block = block + (after(got, *tokens) if tokens else got)
    return block


def all_sum(block, axis, *tokens):
    return end_sum(start_sum(block, axis), axis, *tokens)


def factor(gram):
    size = gram.shape[0]
    tile = (8, 2 * size)
    row_id = lax.broadcasted_iota(jnp.int32, (size, size), 0)
    col_id = lax.broadcasted_iota(jnp.int32, (size, size), 1)
    work = jnp.concatenate([gram, (row_id == col_id).astype(F32)], axis=1)
    blocks = [work[8 * b : 8 * b + 8] for b in range(size // 8)]
    sub = lax.broadcasted_iota(jnp.int32, tile, 0)
    for j in range(0, size, 4):
        b, s = divmod(j, 8)
        later = range(b + s // 4, size // 8)
        line = [jnp.broadcast_to(blocks[b][s + k : s + k + 1], tile) for k in range(4)]
        cols = {
            o: [jnp.broadcast_to(blocks[o][:, j + k : j + k + 1], tile) for k in range(4)]
            for o in range(b, size // 8)
        }
        entry = {
            (k, l): jnp.broadcast_to(cols[b][l][s + k : s + k + 1], tile)
            for k in range(4)
            for l in range(k, 4)
        }
        scaled = []
        for k in range(4):
            inverse = 1.0 / entry[k, k]
            for l in range(k + 1, 4):
                ratio = entry[k, l] * inverse
                for p in range(l, 4):
                    entry[l, p] = entry[l, p] - ratio * entry[k, p]
                line[l] = line[l] - ratio * line[k]
                for o in later:
                    cols[o][l] = cols[o][l] - ratio * cols[o][k]
            scaled.append(inverse * line[k])
        for o in range(b, size // 8):
            new = blocks[o]
            if o in later:
                new = new - ((cols[o][0] * scaled[0] + cols[o][1] * scaled[1]) + (cols[o][2] * scaled[2] + cols[o][3] * scaled[3]))
            if o == b:
                new = jnp.where(sub > s + 3, new, blocks[o])
                for k in range(1, 4):
                    new = jnp.where(sub == s + k, line[k], new)
            blocks[o] = new
    work = jnp.concatenate(blocks, axis=0)
    pivots = jnp.sum(jnp.where(row_id == col_id, work[:, :size], 0.0), axis=1, keepdims=True)
    work = work / jnp.sqrt(pivots)
    upper = jnp.where(col_id >= row_id, work[:, :size], 0.0)
    inverse = jnp.where(col_id <= row_id, work[:, size:], 0.0)
    return upper, inverse


def local(start_block, diagonal, hess_tiles, tile_rows, tile_cols, slot_counts):
    peers = lax.axis_size("res")
    lanes = lax.axis_size("vec")
    rows, width, length = start_block.shape
    slots = hess_tiles.shape[2]
    half = rows // 2
    part = width // 2
    rounds = pairings(peers)
    count = len(rounds)
    full = (rows, width, length)
    halffull = (half, width, length)
    chunk = (rows, part, length)
    halfchunk = (half, part, length)
    packet = (CAP, part, length)
    square = (width, width)
    split_shape = jax.ShapeDtypeStruct((slots, 2, length, length), BF16)

    table = role_table(rounds, peers)
    place = jnp.concatenate(
        [lax.axis_index("vec").reshape(1), table[:, lax.axis_index("res")]]
    ).astype(jnp.int32)

    def own_sum(acc_refs, x_ref, split_ref, rows_ref, cols_ref):
        batch = 4
        for first in range(0, OWN_SLOTS, batch):
            members = range(first, first + batch)
            ends = [(rows_ref[0, 0, s], cols_ref[0, 0, s]) for s in members]
            terms = [
                (
                    tile_product(x_ref[j], split_ref, s, True),
                    tile_product(x_ref[i], split_ref, s, False),
                )
                for s, (i, j) in zip(members, ends)
            ]
            for (i, j), (direct, mirror) in zip(ends, terms):
                for n, acc_ref in enumerate(acc_refs):
                    acc_ref[i] += direct[n * part : (n + 1) * part]
                    acc_ref[j] += mirror[n * part : (n + 1) * part]

    def prepare_body(x_hbm, diag_hbm, tiles_hbm, *refs):
        x_ref, split_ref, a_ref, b_ref, diag_ref, raw_ref, sem = refs
        size = slots // 4
        copies = [
            pltpu.make_async_copy(src, dst, sem.at[n])
            for n, (src, dst) in enumerate([(x_hbm, x_ref), (diag_hbm, diag_ref)])
        ]
        tile_copies = [
            pltpu.make_async_copy(
                tiles_hbm.at[0, 0, pl.ds(n * size, size)], raw_ref.at[pl.ds(n * size, size)], sem.at[2 + n]
            )
            for n in range(4)
        ]
        for c in copies + tile_copies:
            c.start()
        for n in range(4):
            tile_copies[n].wait()
            for s in range(n * size, (n + 1) * size):
                split_ref[s, 0], split_ref[s, 1] = pieces(raw_ref[s], 2)
        for c in copies:
            c.wait()
        first = (lax.axis_index("vec") == 0).astype(F32)
        d = ((diag_ref[...] - SHIFT) * first)[:, None, :]
        a_ref[...] = x_ref[:, :part] * d
        b_ref[...] = x_ref[:, part:] * d

    def own_body(rows_ref, cols_ref, x_ref, split_ref, *refs):
        own_sum(refs[len(refs) // 2 :], x_ref, split_ref, rows_ref, cols_ref)

    def pack(place_ref, rows_ref, counts_ref, asked_refs, x_ref, split_ref, outs):
        for p in range(count):
            role = place_ref[1 + p]

            def put(c, value, p=p):
                for n, ref in enumerate(outs[p]):
                    ref[c] = value[n * part : (n + 1) * part]

            @pl.when(role > 0)
            def _():
                base = OWN_SLOTS + (role - 1) * CAP
                terms = [
                    tile_product(x_ref[rows_ref[0, 0, base + c]], split_ref, base + c, False)
                    for c in range(CAP)
                ]
                for c, term in enumerate(terms):
                    put(c, jnp.where(c < counts_ref[0, 0, role - 1], term, 0.0))

            @pl.when(role < 0)
            def _():
                base = OWN_SLOTS + (-role - 1) * CAP
                for c in range(CAP):
                    put(c, x_ref[asked_refs[p][0, 0, base + c]])

    def send_body(place_ref, rows_ref, counts_ref, *refs):
        asked_refs, (x_ref, split_ref), outs = refs[:count], refs[count : count + 2], refs[count + 2 :]
        pack(
            place_ref, rows_ref, counts_ref, asked_refs, x_ref, split_ref,
            [(outs[p], outs[count + p]) for p in range(count)],
        )

    def settle(place_ref, mine_ref, other_ref, y_ref):
        core = place_ref[0] % 2
        y_ref[pl.ds(core * half, half)] = mine_ref[...]
        y_ref[pl.ds((1 - core) * half, half)] = other_ref[...]

    def resend_body(place_ref, rows_ref, counts_ref, *refs):
        asked_refs = refs[:count]
        mine_ref, other_ref, diag_ref, split_ref, y_ref, acc_ref = refs[count : count + 6]
        outs = refs[count + 6 :]
        settle(place_ref, mine_ref, other_ref, y_ref)
        pack(
            place_ref, rows_ref, counts_ref, asked_refs, y_ref, split_ref,
            [(outs[p],) for p in range(count)],
        )
        first = (place_ref[0] == 0).astype(F32)
        acc_ref[...] = y_ref[...] * ((diag_ref[...] - SHIFT) * first)[:, None, :]

    def join_rounds(members, place_ref, rows_ref, counts_ref, asked_refs, got_refs, split_ref, acc_ref):
        for n, p in enumerate(members):
            role = place_ref[1 + p]

            @pl.when(role > 0)
            def _():
                base = OWN_SLOTS + (role - 1) * CAP
                terms = [
                    tile_product(got_refs[n][c], split_ref, base + c, True) for c in range(CAP)
                ]
                for c, term in enumerate(terms):
                    acc_ref[rows_ref[0, 0, base + c]] += jnp.where(
                        c < counts_ref[0, 0, role - 1], term, 0.0
                    )

            @pl.when(role < 0)
            def _():
                base = OWN_SLOTS + (-role - 1) * CAP
                for c in range(CAP):
                    acc_ref[asked_refs[n][0, 0, base + c]] += got_refs[n][c]

    def join(acc, got, members, last=False):
        size = len(members)

        def body(place_ref, rows_ref, counts_ref, *refs):
            asked_refs, got_refs = refs[:size], refs[size : 2 * size]
            split_ref, prior_ref = refs[2 * size : 2 * size + 2]
            outs = refs[2 * size + 2 :]
            if last:
                keep_ref, give_ref, acc_ref = outs
                acc_ref[...] = prior_ref[...]
            else:
                (acc_ref,) = outs
            join_rounds(
                members, place_ref, rows_ref, counts_ref, asked_refs, got_refs, split_ref, acc_ref
            )
            if last:
                core = place_ref[0] % 2
                keep_ref[...] = acc_ref[pl.ds(core * half, half)]
                give_ref[...] = acc_ref[pl.ds((1 - core) * half, half)]

        out = call(
            body,
            [halfchunk] * 2 if last else [chunk],
            [SMEM] * (3 + size) + [VMEM] * (size + 2),
            [pltpu.VMEM(chunk, F32)] if last else [],
            name="join",
            weight=10**10,
            aliases=None if last else {3 + 2 * size + 1: 0},
        )(
            place, tile_rows, slot_counts, *[asked[p] for p in members], *[got[p] for p in members], split, acc
        )
        return out if last else out[0]

    def gram_body(x_ref, out_ref):
        total = jnp.zeros(square, F32)
        for n in range(0, rows, 2):
            pair = [x_ref[n], x_ref[n + 1]]
            total += gram_step(pair, [pair])
        out_ref[...] = total

    def cross_body(x_ref, a_ref, b_ref, out_ref):
        total = jnp.zeros((width, 2 * width), F32)
        for n in range(0, rows, 2):
            y = [jnp.concatenate([a_ref[m], b_ref[m]], axis=0) for m in (n, n + 1)]
            total += gram_step(y, [[x_ref[n], x_ref[n + 1]], y])
        out_ref[...] = total

    def first_body(gram_ref, inverse_ref):
        _, inverse_ref[...] = factor(gram_ref[...])

    def identity():
        eye = lax.broadcasted_iota(jnp.int32, square, 0) == lax.broadcasted_iota(jnp.int32, square, 1)
        return eye.astype(F32)

    def lower_part():
        return lax.broadcasted_iota(jnp.int32, square, 0) >= lax.broadcasted_iota(jnp.int32, square, 1)

    def second_body(gram_ref, inverse_ref, cross_ref, lower_ref, coef_ref, gain_ref):
        start_inv = inverse_ref[...]
        cross = dot(dot(start_inv, gram_ref[:, :width]), start_inv, tb=True)
        applied = dot(dot(start_inv, gram_ref[:, width:]), start_inv, tb=True)
        upper, inverse = factor(applied - dot(cross, cross, tb=True))
        lower = upper.T
        cross_ref[...] = cross + SHIFT * identity()
        lower_ref[...] = lower
        gain = dot(inverse, start_inv)
        back = -dot(dot(inverse, cross), start_inv)
        gain_ref[...] = gain
        coef_ref[:width, :width] = -dot(lower, start_inv)
        coef_ref[:width, width : 2 * width] = back
        coef_ref[:width, 2 * width :] = gain
        coef_ref[width:, :width] = back
        coef_ref[width:, width : 2 * width] = gain
        coef_ref[width:, 2 * width :] = jnp.zeros(square, F32)

    def blend(side, mine, other, coef):
        def body(place_ref, x_ref, a_ref, b_ref, mine_ref, other_ref, coef_ref, w_ref, q_ref, out_ref, z_ref):
            settle(place_ref, mine_ref, other_ref, z_ref)
            for n in range(0, half, 2):
                stacks = [
                    jnp.concatenate([ref[side * half + m] for ref in (x_ref, a_ref, b_ref, z_ref)], axis=0)
                    for m in (n, n + 1)
                ]
                for m, both in zip((n, n + 1), wide_product(coef_ref[:, : 2 * width + part], stacks)):
                    w_ref[m] = both[:width]
                    q_ref[m] = both[width:]
            total = jnp.zeros(square, F32)
            for n in range(0, half, 2):
                qs = [q_ref[n], q_ref[n + 1]]
                total += gram_step(qs, [qs])
            out_ref[...] = total

        return call(
            body,
            [halffull, halffull, square],
            [SMEM] + [VMEM] * 6,
            [pltpu.VMEM(chunk, F32)],
            name="blend",
        )(place, x, y_a, y_b, mine, other, coef)

    def third_body(place_ref, mine_ref, other_ref, gain_ref, *refs):
        prior_refs, q_refs, norm_refs = refs[0:2], refs[2:4], refs[4:6]
        w_ref, out_ref, z_ref = refs[6:]
        settle(place_ref, mine_ref, other_ref, z_ref)
        for n in range(0, rows, 2):
            side, m = divmod(n, half)
            for k, w in enumerate(wide_product(gain_ref[:, part:], [z_ref[n], z_ref[n + 1]])):
                w_ref[n + k] = w + prior_refs[side][m + k]
        total = jnp.zeros((width, 2 * width), F32)
        for n in range(0, rows, 2):
            side, m = divmod(n, half)
            ws = [w_ref[n], w_ref[n + 1]]
            total += gram_step(ws, [[q_refs[side][m], q_refs[side][m + 1]], ws])
        norm = norm_refs[0][...] + norm_refs[1][...]
        out_ref[:width, :width] = total[:, :width]
        out_ref[:width, width:] = jnp.where(lower_part(), total[:, width:], norm)
        out_ref[width:, :] = jnp.zeros((8, 2 * width), F32)
        out_ref[width:, :width] = jnp.broadcast_to(
            jnp.sum(norm * identity(), axis=0, keepdims=True), (8, width)
        )

    def fourth_body(gram_ref, cross_ref, lower_ref, coef_ref):
        cross = gram_ref[:width, :width]
        packed = gram_ref[:width, width:]
        flipped = packed.T
        squares = jnp.where(lower_part(), packed, flipped)
        norm = jnp.where(lower_part(), flipped, packed)
        norm = jnp.where(identity() > 0, gram_ref[width : width + 1, :width], norm)
        taken = cross + SHIFT * (norm - identity())
        mixed = dot(taken, cross, tb=True)
        squared = squares - mixed - mixed.T + dot(dot(taken, norm), taken, tb=True)
        upper, inverse = factor(squared)
        cross_ref[...] = taken + SHIFT * identity()
        lower_ref[...] = upper.T
        scale = math.sqrt(rows * length * peers)
        coef_ref[:, :width] = inverse * scale
        coef_ref[:, width:] = -dot(inverse, taken) * scale

    def last_body(w_ref, low_ref, high_ref, coef_ref, a1_ref, l1_ref, a2_ref, l2_ref, out_ref, pack_ref):
        for n, ref in enumerate((a1_ref, l1_ref, a2_ref, l2_ref)):
            pack_ref[n] = ref[...]
        for n in range(0, rows, 2):
            side, at = divmod(n, half)
            q_ref = (low_ref, high_ref)[side]
            stacks = [jnp.concatenate([w_ref[n + k], q_ref[at + k]], axis=0) for k in range(2)]
            for m, out in zip((n, n + 1), wide_product(coef_ref[...], stacks, 4)):
                out_ref[m] = out

    swap = [(i, i ^ 1) for i in range(lanes)]
    cuts = [count * n // 3 for n in range(4)]
    groups = [list(range(cuts[n], cuts[n + 1])) for n in range(3)]

    def spread(sent):
        return [exchange(s, "res", entry["pairs"]) for s, entry in zip(sent, rounds)]

    def across(mine, *tokens):
        step = 2
        while step < lanes:
            got = lax.ppermute(mine, "vec", [(i, i ^ step) for i in range(lanes)])
            mine = mine + after(got, *tokens)
            step *= 2
        return mine

    def resend(mine, other):
        y, acc, *sent = call(
            resend_body,
            [chunk, chunk] + [packet] * count,
            [SMEM] * (3 + count) + [VMEM] * 4,
            name="resend",
        )(place, tile_rows, slot_counts, *asked, mine, other, diagonal, split)
        return y, acc, spread(sent)

    def own(y, *accs):
        return call(
            own_body,
            [chunk] * len(accs),
            [SMEM] * 2 + [VMEM] * (2 + len(accs)),
            name="own",
            aliases={4 + n: n for n in range(len(accs))},
        )(tile_rows, tile_cols, y, split, *accs)

    asked = [exchange(tile_cols, "res", entry["pairs"]) for entry in rounds]
    x, split, acc_a, acc_b = call(
        prepare_body,
        [full, split_shape, chunk, chunk],
        [HBM] * 3,
        [
            pltpu.VMEM(diagonal.shape, F32),
            pltpu.VMEM((slots, length, length), F32),
            pltpu.SemaphoreType.DMA((6,)),
        ],
        name="prepare",
    )(*[pinned(v) for v in (start_block, diagonal, hess_tiles)])
    sent = call(
        send_body, [packet] * (2 * count), [SMEM] * (3 + count) + [VMEM] * 2, name="send"
    )(place, tile_rows, slot_counts, *asked, x, split)
    got_a = spread(sent[:count])
    sent_b = list(sent[count:])
    acc_a, acc_b = own(x, after(acc_a, sent[0]), acc_b)
    for n in range(2):
        acc_a = join(acc_a, got_a, groups[n])
        turn = groups[0] if n == 1 else []
        acc_a, x, *gated = lax.optimization_barrier((acc_a, x, *[sent_b[p] for p in turn]))
        for p, value in zip(turn, gated):
            sent_b[p] = value
        if n == 0:
            (gram,) = call(gram_body, [square], [VMEM], name="gram")(x)
            start_gram = start_sum(gram, "res")
    acc_a = after(acc_a, start_gram)
    keep_a, give_a = join(acc_a, got_a, groups[2], last=True)
    for p in groups[1] + groups[2]:
        sent_b[p] = after(sent_b[p], keep_a)
    got_b = spread(sent_b)

    core = lax.ppermute(give_a, "vec", swap)
    acc_b = join(acc_b, got_b, groups[0])
    mine_a = keep_a + after(core, acc_b)
    (start_inv,) = call(first_body, [square], [VMEM], name="first")(end_sum(start_gram, "res", mine_a))
    acc_b = join(after(acc_b, start_inv), got_b, groups[1])
    mine_a = across(mine_a, acc_b)
    other_a = lax.ppermute(mine_a, "vec", swap)
    keep_b, give_b = join(acc_b, got_b, groups[2], last=True)
    y_a, acc_a, got_a = resend(mine_a, after(other_a, keep_b))

    core = lax.ppermute(give_b, "vec", swap)
    mine_b = keep_b + after(core, y_a)
    (acc_a,) = own(y_a, after(acc_a, mine_b))
    mine_b = across(mine_b, acc_a)
    other_b = lax.ppermute(mine_b, "vec", swap)
    acc_a = join(after(acc_a, mine_b), got_a, groups[2])
    y_b, acc_b, got_b = resend(mine_b, after(other_b, acc_a))
    acc_a = join(after(acc_a, y_b), got_a, groups[1])
    keep_a, give_a = join(acc_a, got_a, groups[0], last=True)

    core = lax.ppermute(give_a, "vec", swap)
    acc_b = join(acc_b, got_b, groups[0])
    mine_a = keep_a + after(core, acc_b)
    (gram,) = call(cross_body, [(width, 2 * width)], [VMEM] * 3, name="cross")(x, y_a, after(y_b, mine_a))
    (acc_b,) = own(y_b, after(acc_b, gram))
    acc_b = join(acc_b, got_b, groups[1])
    cross_gram = start_sum(gram, "res")
    keep_b, give_b = join(after(acc_b, cross_gram), got_b, groups[2], last=True)

    core = lax.ppermute(give_b, "vec", swap)
    mine_a = across(mine_a, cross_gram)
    other_a = lax.ppermute(mine_a, "vec", swap)
    cross_gram = end_sum(cross_gram, "res")
    mine_b = keep_b + after(core, mine_a, cross_gram)
    cross1, lower1, coef, gain = call(
        second_body, [square, square, (2 * width, 3 * width), square], [VMEM] * 2, name="second"
    )(after(cross_gram, mine_b), start_inv)
    w_low, q_low, norm_low = blend(0, mine_a, other_a, coef)
    w_high, q_high, norm_high = blend(1, mine_a, other_a, coef)
    mine_b = across(mine_b, norm_low, norm_high)
    other_b = lax.ppermute(mine_b, "vec", swap)
    w, gram = call(
        third_body,
        [full, (width + 8, 2 * width)],
        [SMEM] + [VMEM] * 9,
        [pltpu.VMEM(chunk, F32)],
        name="third",
    )(place, mine_b, other_b, gain, w_low, w_high, q_low, q_high, norm_low, norm_high)
    gram = all_sum(gram, "res")
    cross2, lower2, coef = call(
        fourth_body, [square, square, (width, 2 * width)], [VMEM], name="fourth"
    )(gram)
    return call(last_body, [full, (4, width, width)], [VMEM] * 8, name="last")(
        w, q_low, q_high, coef, cross1, lower1, cross2, lower2
    )


def solution(mesh):
    in_specs = (
        P(("conf", "res"), None, None),
        P(("conf", "res"), None),
        P(("conf", "res"), "vec", None, None, None),
        P(("conf", "res"), "vec", None),
        P(("conf", "res"), "vec", None),
        P(("conf", "res"), "vec", None),
    )
    out_specs = (P(("conf", "res"), None, None), P("conf", None, None))
    return jax.shard_map(local, mesh=mesh, in_specs=in_specs, out_specs=out_specs, check_vma=False)
```

```python
import math

import jax
import jax.numpy as jnp
from jax import lax
from jax.experimental import pallas as pl
from jax.experimental.pallas import tpu as pltpu
from jax.sharding import PartitionSpec as P

OWN_SLOTS = 20
HOPS = 3
CAP = 8
SHIFT = 1.65
BF16 = jnp.bfloat16
F32 = jnp.float32

VMEM = pl.BlockSpec(memory_space=pltpu.VMEM)
SMEM = pl.BlockSpec(memory_space=pltpu.SMEM)
HBM = pl.BlockSpec(memory_space=pltpu.HBM)


def contract(a, b, ta=False, tb=False, precision=None):
    dims = (((0 if ta else 1,), (1 if tb else 0,)), ((), ()))
    return lax.dot_general(a, b, dims, precision=precision, preferred_element_type=F32)


def dot(a, b, ta=False, tb=False):
    return contract(a, b, ta, tb, lax.Precision.HIGHEST)


def pieces(x, count):
    out = []
    for _ in range(count):
        out.append(x.astype(BF16))
        x = x - out[-1].astype(F32)
    return out


def tile_product(x, tile_ref, slot, transposed):
    x1, x2 = pieces(x, 2)
    m1, m2 = tile_ref[slot, 0], tile_ref[slot, 1]
    axis = 1 if transposed else 0
    left = jnp.concatenate([x1, x2, x1], axis=1)
    return contract(left, jnp.concatenate([m1, m1, m2], axis=axis), tb=transposed)


def wide_product(coef, blocks, terms=6):
    pairs = [(0, 0), (0, 1), (1, 0), (1, 1)] if terms == 4 else [(0, 0), (0, 1), (0, 2), (1, 0), (1, 1), (2, 0)]
    c = pieces(coef, terms // 2)
    z = pieces(jnp.concatenate(blocks, axis=1), terms // 2)
    left = jnp.concatenate([c[m] for m, _ in pairs], axis=1)
    out = contract(left, jnp.concatenate([z[m] for _, m in pairs], axis=0))
    width = blocks[0].shape[1]
    return [out[:, n * width : (n + 1) * width] for n in range(len(blocks))]


def gram_step(left, right):
    a = jnp.concatenate(pieces(jnp.concatenate(left, axis=1), 2), axis=0)
    b = jnp.concatenate(
        [p for group in right for p in pieces(jnp.concatenate(group, axis=1), 2)], axis=0
    )
    out = contract(a, b, tb=True)
    size = left[0].shape[0]
    out = out[:size] + out[size:]
    return jnp.concatenate(
        [
            out[:, 2 * g * size : (2 * g + 1) * size] + out[:, (2 * g + 1) * size : (2 * g + 2) * size]
            for g in range(len(right))
        ],
        axis=1,
    )


def call(body, outs, in_specs, scratch=(), name=None, aliases=None, weight=0):
    shapes = [
        o if isinstance(o, jax.ShapeDtypeStruct) else jax.ShapeDtypeStruct(o, F32) for o in outs
    ]
    return pl.pallas_call(
        body,
        out_shape=shapes,
        in_specs=in_specs,
        out_specs=[VMEM] * len(outs),
        scratch_shapes=list(scratch),
        compiler_params=pltpu.CompilerParams(vmem_limit_bytes=40 << 20),
        input_output_aliases=aliases or {},
        cost_estimate=pl.CostEstimate(flops=weight, bytes_accessed=weight, transcendentals=0) if weight else None,
        name=name,
    )


def pinned(value):
    return pltpu.with_memory_space_constraint(value, pltpu.HBM)


def after(value, *tokens):
    return lax.optimization_barrier((value,) + tokens)[0]


def pairings(size):
    rounds = []
    for hop in range(1, HOPS + 1):
        for parity in range(2):
            pairs = [(i, i + hop) for i in range(size - hop) if (i // hop) % 2 == parity]
            if not pairs:
                continue
            used = {i for pair in pairs for i in pair}
            for entry in rounds:
                if not entry["used"] & used:
                    entry["used"] |= used
                    entry["pairs"] += pairs
                    entry["kinds"].append((hop, parity))
                    break
            else:
                rounds.append({"used": used, "pairs": pairs, "kinds": [(hop, parity)]})
    return rounds


def exchange(block, axis, pairs):
    return lax.ppermute(block, axis, [(a, b) for a, b in pairs] + [(b, a) for a, b in pairs])


def role_table(rounds, size):
    table = [[0] * size for _ in rounds]
    for p, entry in enumerate(rounds):
        for a, b in entry["pairs"]:
            table[p][a] = b - a
            table[p][b] = a - b
    return jnp.array(table, jnp.int32)


def sum_steps(size):
    return [1 << n for n in range(size.bit_length() - 1)]


def start_sum(block, axis):
    size = lax.axis_size(axis)
    if size & (size - 1):
        return block
    for step in sum_steps(size)[:-1]:
        block = block + lax.ppermute(block, axis, [(i, i ^ step) for i in range(size)])
    return block


def end_sum(block, axis, *tokens):
    size = lax.axis_size(axis)
    if size & (size - 1):
        return lax.psum(block, axis)
    for step in sum_steps(size)[-1:]:
        got = lax.ppermute(block, axis, [(i, i ^ step) for i in range(size)])
        block = block + (after(got, *tokens) if tokens else got)
    return block


def all_sum(block, axis, *tokens):
    return end_sum(start_sum(block, axis), axis, *tokens)


def factor(gram):
    size = gram.shape[0]
    tile = (8, 2 * size)
    row_id = lax.broadcasted_iota(jnp.int32, (size, size), 0)
    col_id = lax.broadcasted_iota(jnp.int32, (size, size), 1)
    work = jnp.concatenate([gram, (row_id == col_id).astype(F32)], axis=1)
    blocks = [work[8 * b : 8 * b + 8] for b in range(size // 8)]
    sub = lax.broadcasted_iota(jnp.int32, tile, 0)
    for j in range(0, size, 4):
        b, s = divmod(j, 8)
        later = range(b + s // 4, size // 8)
        line = [jnp.broadcast_to(blocks[b][s + k : s + k + 1], tile) for k in range(4)]
        cols = {
            o: [jnp.broadcast_to(blocks[o][:, j + k : j + k + 1], tile) for k in range(4)]
            for o in range(b, size // 8)
        }
        entry = {
            (k, l): jnp.broadcast_to(cols[b][l][s + k : s + k + 1], tile)
            for k in range(4)
            for l in range(k, 4)
        }
        scaled = []
        for k in range(4):
            inverse = 1.0 / entry[k, k]
            for l in range(k + 1, 4):
                ratio = entry[k, l] * inverse
                for p in range(l, 4):
                    entry[l, p] = entry[l, p] - ratio * entry[k, p]
                line[l] = line[l] - ratio * line[k]
                for o in later:
                    cols[o][l] = cols[o][l] - ratio * cols[o][k]
            scaled.append(inverse * line[k])
        for o in range(b, size // 8):
            new = blocks[o]
            if o in later:
                new = new - ((cols[o][0] * scaled[0] + cols[o][1] * scaled[1]) + (cols[o][2] * scaled[2] + cols[o][3] * scaled[3]))
            if o == b:
                new = jnp.where(sub > s + 3, new, blocks[o])
                for k in range(1, 4):
                    new = jnp.where(sub == s + k, line[k], new)
            blocks[o] = new
    work = jnp.concatenate(blocks, axis=0)
    pivots = jnp.sum(jnp.where(row_id == col_id, work[:, :size], 0.0), axis=1, keepdims=True)
    work = work / jnp.sqrt(pivots)
    upper = jnp.where(col_id >= row_id, work[:, :size], 0.0)
    inverse = jnp.where(col_id <= row_id, work[:, size:], 0.0)
    return upper, inverse


def local(start_block, diagonal, hess_tiles, tile_rows, tile_cols, slot_counts):
    peers = lax.axis_size("res")
    lanes = lax.axis_size("vec")
    rows, width, length = start_block.shape
    slots = hess_tiles.shape[2]
    half = rows // 2
    part = width // 2
    rounds = pairings(peers)
    count = len(rounds)
    full = (rows, width, length)
    halffull = (half, width, length)
    chunk = (rows, part, length)
    halfchunk = (half, part, length)
    packet = (CAP, part, length)
    square = (width, width)
    split_shape = jax.ShapeDtypeStruct((slots, 2, length, length), BF16)

    table = role_table(rounds, peers)
    place = jnp.concatenate(
        [lax.axis_index("vec").reshape(1), table[:, lax.axis_index("res")]]
    ).astype(jnp.int32)

    def own_sum(acc_refs, x_ref, split_ref, rows_ref, cols_ref):
        batch = 4
        for first in range(0, OWN_SLOTS, batch):
            members = range(first, first + batch)
            ends = [(rows_ref[0, 0, s], cols_ref[0, 0, s]) for s in members]
            terms = [
                (
                    tile_product(x_ref[j], split_ref, s, True),
                    tile_product(x_ref[i], split_ref, s, False),
                )
                for s, (i, j) in zip(members, ends)
            ]
            for (i, j), (direct, mirror) in zip(ends, terms):
                for n, acc_ref in enumerate(acc_refs):
                    acc_ref[i] += direct[n * part : (n + 1) * part]
                    acc_ref[j] += mirror[n * part : (n + 1) * part]

    def prepare_body(x_hbm, diag_hbm, tiles_hbm, *refs):
        x_ref, split_ref, a_ref, b_ref, diag_ref, raw_ref, sem = refs
        size = slots // 4
        copies = [
            pltpu.make_async_copy(src, dst, sem.at[n])
            for n, (src, dst) in enumerate([(x_hbm, x_ref), (diag_hbm, diag_ref)])
        ]
        tile_copies = [
            pltpu.make_async_copy(
                tiles_hbm.at[0, 0, pl.ds(n * size, size)], raw_ref.at[pl.ds(n * size, size)], sem.at[2 + n]
            )
            for n in range(4)
        ]
        for c in copies + tile_copies:
            c.start()
        for n in range(4):
            tile_copies[n].wait()
            for s in range(n * size, (n + 1) * size):
                split_ref[s, 0], split_ref[s, 1] = pieces(raw_ref[s], 2)
        for c in copies:
            c.wait()
        first = (lax.axis_index("vec") == 0).astype(F32)
        d = ((diag_ref[...] - SHIFT) * first)[:, None, :]
        a_ref[...] = x_ref[:, :part] * d
        b_ref[...] = x_ref[:, part:] * d

    def own_body(rows_ref, cols_ref, x_ref, split_ref, *refs):
        own_sum(refs[len(refs) // 2 :], x_ref, split_ref, rows_ref, cols_ref)

    def pack(place_ref, rows_ref, counts_ref, asked_refs, x_ref, split_ref, outs):
        for p in range(count):
            role = place_ref[1 + p]

            def put(c, value, p=p):
                for n, ref in enumerate(outs[p]):
                    ref[c] = value[n * part : (n + 1) * part]

            @pl.when(role > 0)
            def _():
                base = OWN_SLOTS + (role - 1) * CAP
                terms = [
                    tile_product(x_ref[rows_ref[0, 0, base + c]], split_ref, base + c, False)
                    for c in range(CAP)
                ]
                for c, term in enumerate(terms):
                    put(c, jnp.where(c < counts_ref[0, 0, role - 1], term, 0.0))

            @pl.when(role < 0)
            def _():
                base = OWN_SLOTS + (-role - 1) * CAP
                for c in range(CAP):
                    put(c, x_ref[asked_refs[p][0, 0, base + c]])

    def send_body(place_ref, rows_ref, counts_ref, *refs):
        asked_refs, (x_ref, split_ref), outs = refs[:count], refs[count : count + 2], refs[count + 2 :]
        pack(
            place_ref, rows_ref, counts_ref, asked_refs, x_ref, split_ref,
            [(outs[p], outs[count + p]) for p in range(count)],
        )

    def settle(place_ref, mine_ref, other_ref, y_ref):
        core = place_ref[0] % 2
        y_ref[pl.ds(core * half, half)] = mine_ref[...]
        y_ref[pl.ds((1 - core) * half, half)] = other_ref[...]

    def resend_body(place_ref, rows_ref, counts_ref, *refs):
        asked_refs = refs[:count]
        mine_ref, other_ref, diag_ref, split_ref, y_ref, acc_ref = refs[count : count + 6]
        outs = refs[count + 6 :]
        settle(place_ref, mine_ref, other_ref, y_ref)
        pack(
            place_ref, rows_ref, counts_ref, asked_refs, y_ref, split_ref,
            [(outs[p],) for p in range(count)],
        )
        first = (place_ref[0] == 0).astype(F32)
        acc_ref[...] = y_ref[...] * ((diag_ref[...] - SHIFT) * first)[:, None, :]

    def join_rounds(members, place_ref, rows_ref, counts_ref, asked_refs, got_refs, split_ref, acc_ref):
        for n, p in enumerate(members):
            role = place_ref[1 + p]

            @pl.when(role > 0)
            def _():
                base = OWN_SLOTS + (role - 1) * CAP
                terms = [
                    tile_product(got_refs[n][c], split_ref, base + c, True) for c in range(CAP)
                ]
                for c, term in enumerate(terms):
                    acc_ref[rows_ref[0, 0, base + c]] += jnp.where(
                        c < counts_ref[0, 0, role - 1], term, 0.0
                    )

            @pl.when(role < 0)
            def _():
                base = OWN_SLOTS + (-role - 1) * CAP
                for c in range(CAP):
                    acc_ref[asked_refs[n][0, 0, base + c]] += got_refs[n][c]

    def join(acc, got, members, last=False):
        size = len(members)

        def body(place_ref, rows_ref, counts_ref, *refs):
            asked_refs, got_refs = refs[:size], refs[size : 2 * size]
            split_ref, prior_ref = refs[2 * size : 2 * size + 2]
            outs = refs[2 * size + 2 :]
            if last:
                keep_ref, give_ref, acc_ref = outs
                acc_ref[...] = prior_ref[...]
            else:
                (acc_ref,) = outs
            join_rounds(
                members, place_ref, rows_ref, counts_ref, asked_refs, got_refs, split_ref, acc_ref
            )
            if last:
                core = place_ref[0] % 2
                keep_ref[...] = acc_ref[pl.ds(core * half, half)]
                give_ref[...] = acc_ref[pl.ds((1 - core) * half, half)]

        out = call(
            body,
            [halfchunk] * 2 if last else [chunk],
            [SMEM] * (3 + size) + [VMEM] * (size + 2),
            [pltpu.VMEM(chunk, F32)] if last else [],
            name="join",
            weight=10**10,
            aliases=None if last else {3 + 2 * size + 1: 0},
        )(
            place, tile_rows, slot_counts, *[asked[p] for p in members], *[got[p] for p in members], split, acc
        )
        return out if last else out[0]

    def gram_body(x_ref, out_ref):
        total = jnp.zeros(square, F32)
        for n in range(0, rows, 2):
            pair = [x_ref[n], x_ref[n + 1]]
            total += gram_step(pair, [pair])
        out_ref[...] = total

    def cross_body(x_ref, a_ref, b_ref, out_ref):
        total = jnp.zeros((width, 2 * width), F32)
        for n in range(0, rows, 2):
            y = [jnp.concatenate([a_ref[m], b_ref[m]], axis=0) for m in (n, n + 1)]
            total += gram_step(y, [[x_ref[n], x_ref[n + 1]], y])
        out_ref[...] = total

    def first_body(gram_ref, inverse_ref):
        _, inverse_ref[...] = factor(gram_ref[...])

    def identity():
        eye = lax.broadcasted_iota(jnp.int32, square, 0) == lax.broadcasted_iota(jnp.int32, square, 1)
        return eye.astype(F32)

    def lower_part():
        return lax.broadcasted_iota(jnp.int32, square, 0) >= lax.broadcasted_iota(jnp.int32, square, 1)

    def second_body(gram_ref, inverse_ref, cross_ref, lower_ref, coef_ref, gain_ref):
        start_inv = inverse_ref[...]
        cross = dot(dot(start_inv, gram_ref[:, :width]), start_inv, tb=True)
        applied = dot(dot(start_inv, gram_ref[:, width:]), start_inv, tb=True)
        upper, inverse = factor(applied - dot(cross, cross, tb=True))
        lower = upper.T
        cross_ref[...] = cross + SHIFT * identity()
        lower_ref[...] = lower
        gain = dot(inverse, start_inv)
        back = -dot(dot(inverse, cross), start_inv)
        gain_ref[...] = gain
        coef_ref[:width, :width] = -dot(lower, start_inv)
        coef_ref[:width, width : 2 * width] = back
        coef_ref[:width, 2 * width :] = gain
        coef_ref[width:, :width] = back
        coef_ref[width:, width : 2 * width] = gain
        coef_ref[width:, 2 * width :] = jnp.zeros(square, F32)

    def blend(side, mine, other, coef):
        def body(place_ref, x_ref, a_ref, b_ref, mine_ref, other_ref, coef_ref, w_ref, q_ref, out_ref, z_ref):
            settle(place_ref, mine_ref, other_ref, z_ref)
            for n in range(0, half, 2):
                stacks = [
                    jnp.concatenate([ref[side * half + m] for ref in (x_ref, a_ref, b_ref, z_ref)], axis=0)
                    for m in (n, n + 1)
                ]
                for m, both in zip((n, n + 1), wide_product(coef_ref[:, : 2 * width + part], stacks)):
                    w_ref[m] = both[:width]
                    q_ref[m] = both[width:]
            total = jnp.zeros(square, F32)
            for n in range(0, half, 2):
                qs = [q_ref[n], q_ref[n + 1]]
                total += gram_step(qs, [qs])
            out_ref[...] = total

        return call(
            body,
            [halffull, halffull, square],
            [SMEM] + [VMEM] * 6,
            [pltpu.VMEM(chunk, F32)],
            name="blend",
        )(place, x, y_a, y_b, mine, other, coef)

    def third_body(place_ref, mine_ref, other_ref, gain_ref, *refs):
        prior_refs, q_refs, norm_refs = refs[0:2], refs[2:4], refs[4:6]
        w_ref, out_ref, z_ref = refs[6:]
        settle(place_ref, mine_ref, other_ref, z_ref)
        for n in range(0, rows, 2):
            side, m = divmod(n, half)
            for k, w in enumerate(wide_product(gain_ref[:, part:], [z_ref[n], z_ref[n + 1]])):
                w_ref[n + k] = w + prior_refs[side][m + k]
        total = jnp.zeros((width, 2 * width), F32)
        for n in range(0, rows, 2):
            side, m = divmod(n, half)
            ws = [w_ref[n], w_ref[n + 1]]
            total += gram_step(ws, [[q_refs[side][m], q_refs[side][m + 1]], ws])
        norm = norm_refs[0][...] + norm_refs[1][...]
        out_ref[:width, :width] = total[:, :width]
        out_ref[:width, width:] = jnp.where(lower_part(), total[:, width:], norm)
        out_ref[width:, :] = jnp.zeros((8, 2 * width), F32)
        out_ref[width:, :width] = jnp.broadcast_to(
            jnp.sum(norm * identity(), axis=0, keepdims=True), (8, width)
        )

    def fourth_body(gram_ref, cross_ref, lower_ref, coef_ref):
        cross = gram_ref[:width, :width]
        packed = gram_ref[:width, width:]
        flipped = packed.T
        squares = jnp.where(lower_part(), packed, flipped)
        norm = jnp.where(lower_part(), flipped, packed)
        norm = jnp.where(identity() > 0, gram_ref[width : width + 1, :width], norm)
        taken = cross + SHIFT * (norm - identity())
        mixed = dot(taken, cross, tb=True)
        squared = squares - mixed - mixed.T + dot(dot(taken, norm), taken, tb=True)
        upper, inverse = factor(squared)
        cross_ref[...] = taken + SHIFT * identity()
        lower_ref[...] = upper.T
        scale = math.sqrt(rows * length * peers)
        coef_ref[:, :width] = inverse * scale
        coef_ref[:, width:] = -dot(inverse, taken) * scale

    def last_body(w_ref, low_ref, high_ref, coef_ref, a1_ref, l1_ref, a2_ref, l2_ref, out_ref, pack_ref):
        for n, ref in enumerate((a1_ref, l1_ref, a2_ref, l2_ref)):
            pack_ref[n] = ref[...]
        for n in range(0, rows, 2):
            side, at = divmod(n, half)
            q_ref = (low_ref, high_ref)[side]
            stacks = [jnp.concatenate([w_ref[n + k], q_ref[at + k]], axis=0) for k in range(2)]
            for m, out in zip((n, n + 1), wide_product(coef_ref[...], stacks, 4)):
                out_ref[m] = out

    swap = [(i, i ^ 1) for i in range(lanes)]
    cuts = [count * n // 3 for n in range(4)]
    groups = [list(range(cuts[n], cuts[n + 1])) for n in range(3)]

    def spread(sent):
        return [exchange(s, "res", entry["pairs"]) for s, entry in zip(sent, rounds)]

    def across(mine, *tokens):
        step = 2
        while step < lanes:
            got = lax.ppermute(mine, "vec", [(i, i ^ step) for i in range(lanes)])
            mine = mine + after(got, *tokens)
            step *= 2
        return mine

    def resend(mine, other):
        y, acc, *sent = call(
            resend_body,
            [chunk, chunk] + [packet] * count,
            [SMEM] * (3 + count) + [VMEM] * 4,
            name="resend",
        )(place, tile_rows, slot_counts, *asked, mine, other, diagonal, split)
        return y, acc, spread(sent)

    def own(y, *accs):
        return call(
            own_body,
            [chunk] * len(accs),
            [SMEM] * 2 + [VMEM] * (2 + len(accs)),
            name="own",
            aliases={4 + n: n for n in range(len(accs))},
        )(tile_rows, tile_cols, y, split, *accs)

    asked = [exchange(tile_cols, "res", entry["pairs"]) for entry in rounds]
    x, split, acc_a, acc_b = call(
        prepare_body,
        [full, split_shape, chunk, chunk],
        [HBM] * 3,
        [
            pltpu.VMEM(diagonal.shape, F32),
            pltpu.VMEM((slots, length, length), F32),
            pltpu.SemaphoreType.DMA((6,)),
        ],
        name="prepare",
    )(*[pinned(v) for v in (start_block, diagonal, hess_tiles)])
    sent = call(
        send_body, [packet] * (2 * count), [SMEM] * (3 + count) + [VMEM] * 2, name="send"
    )(place, tile_rows, slot_counts, *asked, x, split)
    got_a = spread(sent[:count])
    sent_b = list(sent[count:])
    acc_a, acc_b = own(x, after(acc_a, sent[0]), acc_b)
    for n in range(2):
        acc_a = join(acc_a, got_a, groups[n])
        turn = groups[0] if n == 1 else []
        acc_a, x, *gated = lax.optimization_barrier((acc_a, x, *[sent_b[p] for p in turn]))
        for p, value in zip(turn, gated):
            sent_b[p] = value
        if n == 0:
            (gram,) = call(gram_body, [square], [VMEM], name="gram")(x)
            start_gram = start_sum(gram, "res")
    acc_a = after(acc_a, start_gram)
    keep_a, give_a = join(acc_a, got_a, groups[2], last=True)
    for p in groups[1] + groups[2]:
        sent_b[p] = after(sent_b[p], keep_a)
    got_b = spread(sent_b)

    core = lax.ppermute(give_a, "vec", swap)
    acc_b = join(acc_b, got_b, groups[0])
    mine_a = keep_a + after(core, acc_b)
    (start_inv,) = call(first_body, [square], [VMEM], name="first")(end_sum(start_gram, "res", mine_a))
    acc_b = join(after(acc_b, start_inv), got_b, groups[1])
    mine_a = across(mine_a, acc_b)
    other_a = lax.ppermute(mine_a, "vec", swap)
    keep_b, give_b = join(acc_b, got_b, groups[2], last=True)
    y_a, acc_a, got_a = resend(mine_a, after(other_a, keep_b))

    core = lax.ppermute(give_b, "vec", swap)
    mine_b = keep_b + after(core, y_a)
    (acc_a,) = own(y_a, after(acc_a, mine_b))
    mine_b = across(mine_b, acc_a)
    other_b = lax.ppermute(mine_b, "vec", swap)
    acc_a = join(after(acc_a, mine_b), got_a, groups[2])
    y_b, acc_b, got_b = resend(mine_b, after(other_b, acc_a))
    acc_a = join(after(acc_a, y_b), got_a, groups[1])
    keep_a, give_a = join(acc_a, got_a, groups[0], last=True)

    core = lax.ppermute(give_a, "vec", swap)
    (gram,) = call(cross_body, [(width, 2 * width)], [VMEM] * 3, name="cross")(x, y_a, after(y_b, keep_a))
    (acc_b,) = own(y_b, after(acc_b, gram))
    cross_gram = start_sum(gram, "res")
    acc_b = join(acc_b, got_b, groups[0])
    mine_a = keep_a + after(core, acc_b)
    acc_b = join(after(acc_b, mine_a, cross_gram), got_b, groups[1])
    cross_gram = end_sum(cross_gram, "res", acc_b)
    keep_b, give_b = join(after(acc_b, cross_gram), got_b, groups[2], last=True)

    mine_a = across(mine_a, keep_b)
    other_a = lax.ppermute(mine_a, "vec", swap)
    core = lax.ppermute(give_b, "vec", swap)
    mine_b = keep_b + after(core, mine_a)
    cross1, lower1, coef, gain = call(
        second_body, [square, square, (2 * width, 3 * width), square], [VMEM] * 2, name="second"
    )(after(cross_gram, mine_b), start_inv)
    w_low, q_low, norm_low = blend(0, mine_a, other_a, coef)
    w_high, q_high, norm_high = blend(1, mine_a, other_a, coef)
    mine_b = across(mine_b, norm_low, norm_high)
    other_b = lax.ppermute(mine_b, "vec", swap)
    w, gram = call(
        third_body,
        [full, (width + 8, 2 * width)],
        [SMEM] + [VMEM] * 9,
        [pltpu.VMEM(chunk, F32)],
        name="third",
    )(place, mine_b, other_b, gain, w_low, w_high, q_low, q_high, norm_low, norm_high)
    gram = all_sum(gram, "res")
    cross2, lower2, coef = call(
        fourth_body, [square, square, (width, 2 * width)], [VMEM], name="fourth"
    )(gram)
    return call(last_body, [full, (4, width, width)], [VMEM] * 8, name="last")(
        w, q_low, q_high, coef, cross1, lower1, cross2, lower2
    )


def solution(mesh):
    in_specs = (
        P(("conf", "res"), None, None),
        P(("conf", "res"), None),
        P(("conf", "res"), "vec", None, None, None),
        P(("conf", "res"), "vec", None),
        P(("conf", "res"), "vec", None),
        P(("conf", "res"), "vec", None),
    )
    out_specs = (P(("conf", "res"), None, None), P("conf", None, None))
    return jax.shard_map(local, mesh=mesh, in_specs=in_specs, out_specs=out_specs, check_vma=False)
```

```python
import math

import jax
import jax.numpy as jnp
from jax import lax
from jax.experimental import pallas as pl
from jax.experimental.pallas import tpu as pltpu
from jax.sharding import PartitionSpec as P

OWN_SLOTS = 20
HOPS = 3
CAP = 8
SHIFT = 1.65
BF16 = jnp.bfloat16
F32 = jnp.float32

VMEM = pl.BlockSpec(memory_space=pltpu.VMEM)
SMEM = pl.BlockSpec(memory_space=pltpu.SMEM)
HBM = pl.BlockSpec(memory_space=pltpu.HBM)


def contract(a, b, ta=False, tb=False, precision=None):
    dims = (((0 if ta else 1,), (1 if tb else 0,)), ((), ()))
    return lax.dot_general(a, b, dims, precision=precision, preferred_element_type=F32)


def dot(a, b, ta=False, tb=False):
    return contract(a, b, ta, tb, lax.Precision.HIGHEST)


def pieces(x, count):
    out = []
    for _ in range(count):
        out.append(x.astype(BF16))
        x = x - out[-1].astype(F32)
    return out


def tile_product(x, tile_ref, slot, transposed):
    x1, x2 = pieces(x, 2)
    m1, m2 = tile_ref[slot, 0], tile_ref[slot, 1]
    axis = 1 if transposed else 0
    left = jnp.concatenate([x1, x2, x1], axis=1)
    return contract(left, jnp.concatenate([m1, m1, m2], axis=axis), tb=transposed)


def wide_product(coef, blocks, terms=6):
    pairs = [(0, 0), (0, 1), (1, 0), (1, 1)] if terms == 4 else [(0, 0), (0, 1), (0, 2), (1, 0), (1, 1), (2, 0)]
    c = pieces(coef, terms // 2)
    z = pieces(jnp.concatenate(blocks, axis=1), terms // 2)
    left = jnp.concatenate([c[m] for m, _ in pairs], axis=1)
    out = contract(left, jnp.concatenate([z[m] for _, m in pairs], axis=0))
    width = blocks[0].shape[1]
    return [out[:, n * width : (n + 1) * width] for n in range(len(blocks))]


def gram_step(left, right):
    a = jnp.concatenate(pieces(jnp.concatenate(left, axis=1), 2), axis=0)
    b = jnp.concatenate(
        [p for group in right for p in pieces(jnp.concatenate(group, axis=1), 2)], axis=0
    )
    out = contract(a, b, tb=True)
    size = left[0].shape[0]
    out = out[:size] + out[size:]
    return jnp.concatenate(
        [
            out[:, 2 * g * size : (2 * g + 1) * size] + out[:, (2 * g + 1) * size : (2 * g + 2) * size]
            for g in range(len(right))
        ],
        axis=1,
    )


def call(body, outs, in_specs, scratch=(), name=None, aliases=None, weight=0):
    shapes = [
        o if isinstance(o, jax.ShapeDtypeStruct) else jax.ShapeDtypeStruct(o, F32) for o in outs
    ]
    return pl.pallas_call(
        body,
        out_shape=shapes,
        in_specs=in_specs,
        out_specs=[VMEM] * len(outs),
        scratch_shapes=list(scratch),
        compiler_params=pltpu.CompilerParams(vmem_limit_bytes=40 << 20),
        input_output_aliases=aliases or {},
        cost_estimate=pl.CostEstimate(flops=weight, bytes_accessed=weight, transcendentals=0) if weight else None,
        name=name,
    )


def pinned(value):
    return pltpu.with_memory_space_constraint(value, pltpu.HBM)


def after(value, *tokens):
    return lax.optimization_barrier((value,) + tokens)[0]


def pairings(size):
    rounds = []
    for hop in range(1, HOPS + 1):
        for parity in range(2):
            pairs = [(i, i + hop) for i in range(size - hop) if (i // hop) % 2 == parity]
            if not pairs:
                continue
            used = {i for pair in pairs for i in pair}
            for entry in rounds:
                if not entry["used"] & used:
                    entry["used"] |= used
                    entry["pairs"] += pairs
                    entry["kinds"].append((hop, parity))
                    break
            else:
                rounds.append({"used": used, "pairs": pairs, "kinds": [(hop, parity)]})
    return rounds


def exchange(block, axis, pairs):
    return lax.ppermute(block, axis, [(a, b) for a, b in pairs] + [(b, a) for a, b in pairs])


def role_table(rounds, size):
    table = [[0] * size for _ in rounds]
    for p, entry in enumerate(rounds):
        for a, b in entry["pairs"]:
            table[p][a] = b - a
            table[p][b] = a - b
    return jnp.array(table, jnp.int32)


def sum_steps(size):
    return [1 << n for n in range(size.bit_length() - 1)]


def start_sum(block, axis):
    size = lax.axis_size(axis)
    if size & (size - 1):
        return block
    for step in sum_steps(size)[:-1]:
        block = block + lax.ppermute(block, axis, [(i, i ^ step) for i in range(size)])
    return block


def end_sum(block, axis, *tokens):
    size = lax.axis_size(axis)
    if size & (size - 1):
        return lax.psum(block, axis)
    for step in sum_steps(size)[-1:]:
        got = lax.ppermute(block, axis, [(i, i ^ step) for i in range(size)])
        block = block + (after(got, *tokens) if tokens else got)
    return block


def all_sum(block, axis):
    size = lax.axis_size(axis)
    if size & (size - 1):
        return lax.psum(block, axis)
    step = 1
    while step < size:
        masks = [step] if 2 * step >= size else [step, 2 * step, 3 * step]
        got = [lax.ppermute(block, axis, [(i, i ^ m) for i in range(size)]) for m in masks]
        if len(got) == 1:
            block = block + got[0]
            step *= 2
        else:
            block = (block + got[0]) + (got[1] + got[2])
            step *= 4
    return block


def factor(gram):
    size = gram.shape[0]
    tile = (8, 2 * size)
    row_id = lax.broadcasted_iota(jnp.int32, (size, size), 0)
    col_id = lax.broadcasted_iota(jnp.int32, (size, size), 1)
    work = jnp.concatenate([gram, (row_id == col_id).astype(F32)], axis=1)
    blocks = [work[8 * b : 8 * b + 8] for b in range(size // 8)]
    sub = lax.broadcasted_iota(jnp.int32, tile, 0)
    for j in range(0, size, 4):
        b, s = divmod(j, 8)
        later = range(b + s // 4, size // 8)
        line = [jnp.broadcast_to(blocks[b][s + k : s + k + 1], tile) for k in range(4)]
        cols = {
            o: [jnp.broadcast_to(blocks[o][:, j + k : j + k + 1], tile) for k in range(4)]
            for o in range(b, size // 8)
        }
        entry = {
            (k, l): jnp.broadcast_to(cols[b][l][s + k : s + k + 1], tile)
            for k in range(4)
            for l in range(k, 4)
        }
        scaled = []
        for k in range(4):
            inverse = 1.0 / entry[k, k]
            for l in range(k + 1, 4):
                ratio = entry[k, l] * inverse
                for p in range(l, 4):
                    entry[l, p] = entry[l, p] - ratio * entry[k, p]
                line[l] = line[l] - ratio * line[k]
                for o in later:
                    cols[o][l] = cols[o][l] - ratio * cols[o][k]
            scaled.append(inverse * line[k])
        for o in range(b, size // 8):
            new = blocks[o]
            if o in later:
                new = new - ((cols[o][0] * scaled[0] + cols[o][1] * scaled[1]) + (cols[o][2] * scaled[2] + cols[o][3] * scaled[3]))
            if o == b:
                new = jnp.where(sub > s + 3, new, blocks[o])
                for k in range(1, 4):
                    new = jnp.where(sub == s + k, line[k], new)
            blocks[o] = new
    work = jnp.concatenate(blocks, axis=0)
    pivots = jnp.sum(jnp.where(row_id == col_id, work[:, :size], 0.0), axis=1, keepdims=True)
    work = work / jnp.sqrt(pivots)
    upper = jnp.where(col_id >= row_id, work[:, :size], 0.0)
    inverse = jnp.where(col_id <= row_id, work[:, size:], 0.0)
    return upper, inverse


def local(start_block, diagonal, hess_tiles, tile_rows, tile_cols, slot_counts):
    peers = lax.axis_size("res")
    lanes = lax.axis_size("vec")
    rows, width, length = start_block.shape
    slots = hess_tiles.shape[2]
    half = rows // 2
    part = width // 2
    rounds = pairings(peers)
    count = len(rounds)
    full = (rows, width, length)
    halffull = (half, width, length)
    chunk = (rows, part, length)
    halfchunk = (half, part, length)
    packet = (CAP, part, length)
    square = (width, width)
    split_shape = jax.ShapeDtypeStruct((slots, 2, length, length), BF16)

    table = role_table(rounds, peers)
    place = jnp.concatenate(
        [lax.axis_index("vec").reshape(1), table[:, lax.axis_index("res")]]
    ).astype(jnp.int32)

    def own_sum(acc_refs, x_ref, split_ref, rows_ref, cols_ref):
        batch = 4
        for first in range(0, OWN_SLOTS, batch):
            members = range(first, first + batch)
            ends = [(rows_ref[0, 0, s], cols_ref[0, 0, s]) for s in members]
            terms = [
                (
                    tile_product(x_ref[j], split_ref, s, True),
                    tile_product(x_ref[i], split_ref, s, False),
                )
                for s, (i, j) in zip(members, ends)
            ]
            for (i, j), (direct, mirror) in zip(ends, terms):
                for n, acc_ref in enumerate(acc_refs):
                    acc_ref[i] += direct[n * part : (n + 1) * part]
                    acc_ref[j] += mirror[n * part : (n + 1) * part]

    def prepare_body(x_hbm, diag_hbm, tiles_hbm, *refs):
        x_ref, split_ref, a_ref, b_ref, diag_ref, raw_ref, sem = refs
        size = slots // 4
        copies = [
            pltpu.make_async_copy(src, dst, sem.at[n])
            for n, (src, dst) in enumerate([(x_hbm, x_ref), (diag_hbm, diag_ref)])
        ]
        tile_copies = [
            pltpu.make_async_copy(
                tiles_hbm.at[0, 0, pl.ds(n * size, size)], raw_ref.at[pl.ds(n * size, size)], sem.at[2 + n]
            )
            for n in range(4)
        ]
        for c in copies + tile_copies:
            c.start()
        for n in range(4):
            tile_copies[n].wait()
            for s in range(n * size, (n + 1) * size):
                split_ref[s, 0], split_ref[s, 1] = pieces(raw_ref[s], 2)
        for c in copies:
            c.wait()
        first = (lax.axis_index("vec") == 0).astype(F32)
        d = ((diag_ref[...] - SHIFT) * first)[:, None, :]
        a_ref[...] = x_ref[:, :part] * d
        b_ref[...] = x_ref[:, part:] * d

    def own_body(rows_ref, cols_ref, x_ref, split_ref, *refs):
        own_sum(refs[len(refs) // 2 :], x_ref, split_ref, rows_ref, cols_ref)

    def pack(place_ref, rows_ref, counts_ref, asked_refs, x_ref, split_ref, outs):
        for p in range(count):
            role = place_ref[1 + p]

            def put(c, value, p=p):
                for n, ref in enumerate(outs[p]):
                    ref[c] = value[n * part : (n + 1) * part]

            @pl.when(role > 0)
            def _():
                base = OWN_SLOTS + (role - 1) * CAP
                terms = [
                    tile_product(x_ref[rows_ref[0, 0, base + c]], split_ref, base + c, False)
                    for c in range(CAP)
                ]
                for c, term in enumerate(terms):
                    put(c, jnp.where(c < counts_ref[0, 0, role - 1], term, 0.0))

            @pl.when(role < 0)
            def _():
                base = OWN_SLOTS + (-role - 1) * CAP
                for c in range(CAP):
                    put(c, x_ref[asked_refs[p][0, 0, base + c]])

    def send_body(place_ref, rows_ref, counts_ref, *refs):
        asked_refs, (x_ref, split_ref), outs = refs[:count], refs[count : count + 2], refs[count + 2 :]
        pack(
            place_ref, rows_ref, counts_ref, asked_refs, x_ref, split_ref,
            [(outs[p], outs[count + p]) for p in range(count)],
        )

    def settle(place_ref, mine_ref, other_ref, y_ref):
        core = place_ref[0] % 2
        y_ref[pl.ds(core * half, half)] = mine_ref[...]
        y_ref[pl.ds((1 - core) * half, half)] = other_ref[...]

    def resend_body(place_ref, rows_ref, counts_ref, *refs):
        asked_refs = refs[:count]
        mine_ref, other_ref, diag_ref, split_ref, y_ref, acc_ref = refs[count : count + 6]
        outs = refs[count + 6 :]
        settle(place_ref, mine_ref, other_ref, y_ref)
        pack(
            place_ref, rows_ref, counts_ref, asked_refs, y_ref, split_ref,
            [(outs[p],) for p in range(count)],
        )
        first = (place_ref[0] == 0).astype(F32)
        acc_ref[...] = y_ref[...] * ((diag_ref[...] - SHIFT) * first)[:, None, :]

    def join_rounds(members, place_ref, rows_ref, counts_ref, asked_refs, got_refs, split_ref, acc_ref):
        for n, p in enumerate(members):
            role = place_ref[1 + p]

            @pl.when(role > 0)
            def _():
                base = OWN_SLOTS + (role - 1) * CAP
                terms = [
                    tile_product(got_refs[n][c], split_ref, base + c, True) for c in range(CAP)
                ]
                for c, term in enumerate(terms):
                    acc_ref[rows_ref[0, 0, base + c]] += jnp.where(
                        c < counts_ref[0, 0, role - 1], term, 0.0
                    )

            @pl.when(role < 0)
            def _():
                base = OWN_SLOTS + (-role - 1) * CAP
                for c in range(CAP):
                    acc_ref[asked_refs[n][0, 0, base + c]] += got_refs[n][c]

    def join(acc, got, members, last=False):
        size = len(members)

        def body(place_ref, rows_ref, counts_ref, *refs):
            asked_refs, got_refs = refs[:size], refs[size : 2 * size]
            split_ref, prior_ref = refs[2 * size : 2 * size + 2]
            outs = refs[2 * size + 2 :]
            if last:
                keep_ref, give_ref, acc_ref = outs
                acc_ref[...] = prior_ref[...]
            else:
                (acc_ref,) = outs
            join_rounds(
                members, place_ref, rows_ref, counts_ref, asked_refs, got_refs, split_ref, acc_ref
            )
            if last:
                core = place_ref[0] % 2
                keep_ref[...] = acc_ref[pl.ds(core * half, half)]
                give_ref[...] = acc_ref[pl.ds((1 - core) * half, half)]

        out = call(
            body,
            [halfchunk] * 2 if last else [chunk],
            [SMEM] * (3 + size) + [VMEM] * (size + 2),
            [pltpu.VMEM(chunk, F32)] if last else [],
            name="join",
            weight=10**10,
            aliases=None if last else {3 + 2 * size + 1: 0},
        )(
            place, tile_rows, slot_counts, *[asked[p] for p in members], *[got[p] for p in members], split, acc
        )
        return out if last else out[0]

    def gram_body(x_ref, out_ref):
        total = jnp.zeros(square, F32)
        for n in range(0, rows, 2):
            pair = [x_ref[n], x_ref[n + 1]]
            total += gram_step(pair, [pair])
        out_ref[...] = total

    def cross_body(x_ref, a_ref, b_ref, out_ref):
        total = jnp.zeros((width, 2 * width), F32)
        for n in range(0, rows, 2):
            y = [jnp.concatenate([a_ref[m], b_ref[m]], axis=0) for m in (n, n + 1)]
            total += gram_step(y, [[x_ref[n], x_ref[n + 1]], y])
        out_ref[...] = total

    def first_body(gram_ref, inverse_ref):
        _, inverse_ref[...] = factor(gram_ref[...])

    def identity():
        eye = lax.broadcasted_iota(jnp.int32, square, 0) == lax.broadcasted_iota(jnp.int32, square, 1)
        return eye.astype(F32)

    def lower_part():
        return lax.broadcasted_iota(jnp.int32, square, 0) >= lax.broadcasted_iota(jnp.int32, square, 1)

    def second_body(gram_ref, inverse_ref, cross_ref, lower_ref, coef_ref, gain_ref):
        start_inv = inverse_ref[...]
        cross = dot(dot(start_inv, gram_ref[:, :width]), start_inv, tb=True)
        applied = dot(dot(start_inv, gram_ref[:, width:]), start_inv, tb=True)
        upper, inverse = factor(applied - dot(cross, cross, tb=True))
        lower = upper.T
        cross_ref[...] = cross + SHIFT * identity()
        lower_ref[...] = lower
        gain = dot(inverse, start_inv)
        back = -dot(dot(inverse, cross), start_inv)
        gain_ref[...] = gain
        coef_ref[:width, :width] = -dot(lower, start_inv)
        coef_ref[:width, width : 2 * width] = back
        coef_ref[:width, 2 * width :] = gain
        coef_ref[width:, :width] = back
        coef_ref[width:, width : 2 * width] = gain
        coef_ref[width:, 2 * width :] = jnp.zeros(square, F32)

    def blend(side, mine, other, coef):
        def body(place_ref, x_ref, a_ref, b_ref, mine_ref, other_ref, coef_ref, w_ref, q_ref, out_ref, z_ref):
            settle(place_ref, mine_ref, other_ref, z_ref)
            for n in range(0, half, 2):
                stacks = [
                    jnp.concatenate([ref[side * half + m] for ref in (x_ref, a_ref, b_ref, z_ref)], axis=0)
                    for m in (n, n + 1)
                ]
                for m, both in zip((n, n + 1), wide_product(coef_ref[:, : 2 * width + part], stacks)):
                    w_ref[m] = both[:width]
                    q_ref[m] = both[width:]
            total = jnp.zeros(square, F32)
            for n in range(0, half, 2):
                qs = [q_ref[n], q_ref[n + 1]]
                total += gram_step(qs, [qs])
            out_ref[...] = total

        return call(
            body,
            [halffull, halffull, square],
            [SMEM] + [VMEM] * 6,
            [pltpu.VMEM(chunk, F32)],
            name="blend",
        )(place, x, y_a, y_b, mine, other, coef)

    def third_body(place_ref, mine_ref, other_ref, gain_ref, *refs):
        prior_refs, q_refs, norm_refs = refs[0:2], refs[2:4], refs[4:6]
        w_ref, out_ref, z_ref = refs[6:]
        settle(place_ref, mine_ref, other_ref, z_ref)
        for n in range(0, rows, 2):
            side, m = divmod(n, half)
            for k, w in enumerate(wide_product(gain_ref[:, part:], [z_ref[n], z_ref[n + 1]])):
                w_ref[n + k] = w + prior_refs[side][m + k]
        total = jnp.zeros((width, 2 * width), F32)
        for n in range(0, rows, 2):
            side, m = divmod(n, half)
            ws = [w_ref[n], w_ref[n + 1]]
            total += gram_step(ws, [[q_refs[side][m], q_refs[side][m + 1]], ws])
        norm = norm_refs[0][...] + norm_refs[1][...]
        out_ref[:width, :width] = total[:, :width]
        out_ref[:width, width:] = jnp.where(lower_part(), total[:, width:], norm)
        out_ref[width:, :] = jnp.zeros((8, 2 * width), F32)
        out_ref[width:, :width] = jnp.broadcast_to(
            jnp.sum(norm * identity(), axis=0, keepdims=True), (8, width)
        )

    def fourth_body(gram_ref, cross_ref, lower_ref, coef_ref):
        cross = gram_ref[:width, :width]
        packed = gram_ref[:width, width:]
        flipped = packed.T
        squares = jnp.where(lower_part(), packed, flipped)
        norm = jnp.where(lower_part(), flipped, packed)
        norm = jnp.where(identity() > 0, gram_ref[width : width + 1, :width], norm)
        taken = cross + SHIFT * (norm - identity())
        mixed = dot(taken, cross, tb=True)
        squared = squares - mixed - mixed.T + dot(dot(taken, norm), taken, tb=True)
        upper, inverse = factor(squared)
        cross_ref[...] = taken + SHIFT * identity()
        lower_ref[...] = upper.T
        scale = math.sqrt(rows * length * peers)
        coef_ref[:, :width] = inverse * scale
        coef_ref[:, width:] = -dot(inverse, taken) * scale

    def last_body(w_ref, low_ref, high_ref, coef_ref, a1_ref, l1_ref, a2_ref, l2_ref, out_ref, pack_ref):
        for n, ref in enumerate((a1_ref, l1_ref, a2_ref, l2_ref)):
            pack_ref[n] = ref[...]
        for n in range(0, rows, 2):
            side, at = divmod(n, half)
            q_ref = (low_ref, high_ref)[side]
            stacks = [jnp.concatenate([w_ref[n + k], q_ref[at + k]], axis=0) for k in range(2)]
            for m, out in zip((n, n + 1), wide_product(coef_ref[...], stacks, 4)):
                out_ref[m] = out

    swap = [(i, i ^ 1) for i in range(lanes)]
    cuts = [count * n // 3 for n in range(4)]
    groups = [list(range(cuts[n], cuts[n + 1])) for n in range(3)]

    def spread(sent):
        return [exchange(s, "res", entry["pairs"]) for s, entry in zip(sent, rounds)]

    def across(mine, *tokens):
        step = 2
        while step < lanes:
            got = lax.ppermute(mine, "vec", [(i, i ^ step) for i in range(lanes)])
            mine = mine + after(got, *tokens)
            step *= 2
        return mine

    def resend(mine, other):
        y, acc, *sent = call(
            resend_body,
            [chunk, chunk] + [packet] * count,
            [SMEM] * (3 + count) + [VMEM] * 4,
            name="resend",
        )(place, tile_rows, slot_counts, *asked, mine, other, diagonal, split)
        return y, acc, spread(sent)

    def own(y, *accs):
        return call(
            own_body,
            [chunk] * len(accs),
            [SMEM] * 2 + [VMEM] * (2 + len(accs)),
            name="own",
            aliases={4 + n: n for n in range(len(accs))},
        )(tile_rows, tile_cols, y, split, *accs)

    asked = [exchange(tile_cols, "res", entry["pairs"]) for entry in rounds]
    x, split, acc_a, acc_b = call(
        prepare_body,
        [full, split_shape, chunk, chunk],
        [HBM] * 3,
        [
            pltpu.VMEM(diagonal.shape, F32),
            pltpu.VMEM((slots, length, length), F32),
            pltpu.SemaphoreType.DMA((6,)),
        ],
        name="prepare",
    )(*[pinned(v) for v in (start_block, diagonal, hess_tiles)])
    sent = call(
        send_body, [packet] * (2 * count), [SMEM] * (3 + count) + [VMEM] * 2, name="send"
    )(place, tile_rows, slot_counts, *asked, x, split)
    got_a = spread(sent[:count])
    sent_b = list(sent[count:])
    acc_a, acc_b = own(x, after(acc_a, sent[0]), acc_b)
    for n in range(2):
        acc_a = join(acc_a, got_a, groups[n])
        turn = groups[0] if n == 1 else []
        acc_a, x, *gated = lax.optimization_barrier((acc_a, x, *[sent_b[p] for p in turn]))
        for p, value in zip(turn, gated):
            sent_b[p] = value
        if n == 0:
            (gram,) = call(gram_body, [square], [VMEM], name="gram")(x)
            start_gram = start_sum(gram, "res")
    acc_a = after(acc_a, start_gram)
    keep_a, give_a = join(acc_a, got_a, groups[2], last=True)
    for p in groups[1] + groups[2]:
        sent_b[p] = after(sent_b[p], keep_a)
    got_b = spread(sent_b)

    core = lax.ppermute(give_a, "vec", swap)
    acc_b = join(acc_b, got_b, groups[0])
    mine_a = keep_a + after(core, acc_b)
    (start_inv,) = call(first_body, [square], [VMEM], name="first")(end_sum(start_gram, "res", mine_a))
    acc_b = join(after(acc_b, start_inv), got_b, groups[1])
    mine_a = across(mine_a, acc_b)
    other_a = lax.ppermute(mine_a, "vec", swap)
    keep_b, give_b = join(acc_b, got_b, groups[2], last=True)
    y_a, acc_a, got_a = resend(mine_a, after(other_a, keep_b))

    core = lax.ppermute(give_b, "vec", swap)
    mine_b = keep_b + after(core, y_a)
    (acc_a,) = own(y_a, after(acc_a, mine_b))
    mine_b = across(mine_b, acc_a)
    other_b = lax.ppermute(mine_b, "vec", swap)
    acc_a = join(after(acc_a, mine_b), got_a, groups[2])
    y_b, acc_b, got_b = resend(mine_b, after(other_b, acc_a))
    acc_a = join(after(acc_a, y_b), got_a, groups[1])
    keep_a, give_a = join(acc_a, got_a, groups[0], last=True)

    core = lax.ppermute(give_a, "vec", swap)
    (acc_b,) = own(after(y_b, keep_a), acc_b)
    acc_b = join(acc_b, got_b, groups[0])
    mine_a = keep_a + after(core, acc_b)
    (gram,) = call(cross_body, [(width, 2 * width)], [VMEM] * 3, name="cross")(x, y_a, after(y_b, mine_a))
    acc_b = join(after(acc_b, gram), got_b, groups[1])
    cross_gram = start_sum(gram, "res")
    keep_b, give_b = join(after(acc_b, cross_gram), got_b, groups[2], last=True)

    core = lax.ppermute(give_b, "vec", swap)
    mine_a = across(mine_a, cross_gram)
    other_a = lax.ppermute(mine_a, "vec", swap)
    mine_b = keep_b + after(core, mine_a)
    cross_gram = end_sum(cross_gram, "res", mine_b)
    cross1, lower1, coef, gain = call(
        second_body, [square, square, (2 * width, 3 * width), square], [VMEM] * 2, name="second"
    )(after(cross_gram, mine_b), start_inv)
    w_low, q_low, norm_low = blend(0, mine_a, other_a, coef)
    w_high, q_high, norm_high = blend(1, mine_a, other_a, coef)
    mine_b = across(mine_b, norm_low, norm_high)
    other_b = lax.ppermute(mine_b, "vec", swap)
    w, gram = call(
        third_body,
        [full, (width + 8, 2 * width)],
        [SMEM] + [VMEM] * 9,
        [pltpu.VMEM(chunk, F32)],
        name="third",
    )(place, mine_b, other_b, gain, w_low, w_high, q_low, q_high, norm_low, norm_high)
    gram = all_sum(gram, "res")
    cross2, lower2, coef = call(
        fourth_body, [square, square, (width, 2 * width)], [VMEM], name="fourth"
    )(gram)
    return call(last_body, [full, (4, width, width)], [VMEM] * 8, name="last")(
        w, q_low, q_high, coef, cross1, lower1, cross2, lower2
    )


def solution(mesh):
    in_specs = (
        P(("conf", "res"), None, None),
        P(("conf", "res"), None),
        P(("conf", "res"), "vec", None, None, None),
        P(("conf", "res"), "vec", None),
        P(("conf", "res"), "vec", None),
        P(("conf", "res"), "vec", None),
    )
    out_specs = (P(("conf", "res"), None, None), P("conf", None, None))
    return jax.shard_map(local, mesh=mesh, in_specs=in_specs, out_specs=out_specs, check_vma=False)
```

```python
import math

import jax
import jax.numpy as jnp
from jax import lax
from jax.experimental import pallas as pl
from jax.experimental.pallas import tpu as pltpu
from jax.sharding import PartitionSpec as P

OWN_SLOTS = 20
HOPS = 3
CAP = 8
SHIFT = 1.65
BF16 = jnp.bfloat16
F32 = jnp.float32

VMEM = pl.BlockSpec(memory_space=pltpu.VMEM)
SMEM = pl.BlockSpec(memory_space=pltpu.SMEM)
HBM = pl.BlockSpec(memory_space=pltpu.HBM)


def contract(a, b, ta=False, tb=False, precision=None):
    dims = (((0 if ta else 1,), (1 if tb else 0,)), ((), ()))
    return lax.dot_general(a, b, dims, precision=precision, preferred_element_type=F32)


def dot(a, b, ta=False, tb=False):
    return contract(a, b, ta, tb, lax.Precision.HIGHEST)


def pieces(x, count):
    out = []
    for _ in range(count):
        out.append(x.astype(BF16))
        x = x - out[-1].astype(F32)
    return out


def tile_product(x, tile_ref, slot, transposed):
    x1, x2 = pieces(x, 2)
    m1, m2 = tile_ref[slot, 0], tile_ref[slot, 1]
    axis = 1 if transposed else 0
    left = jnp.concatenate([x1, x2, x1], axis=1)
    return contract(left, jnp.concatenate([m1, m1, m2], axis=axis), tb=transposed)


def wide_product(coef, blocks, terms=6):
    pairs = [(0, 0), (0, 1), (1, 0), (1, 1)] if terms == 4 else [(0, 0), (0, 1), (0, 2), (1, 0), (1, 1), (2, 0)]
    c = pieces(coef, terms // 2)
    z = pieces(jnp.concatenate(blocks, axis=1), terms // 2)
    left = jnp.concatenate([c[m] for m, _ in pairs], axis=1)
    out = contract(left, jnp.concatenate([z[m] for _, m in pairs], axis=0))
    width = blocks[0].shape[1]
    return [out[:, n * width : (n + 1) * width] for n in range(len(blocks))]


def gram_step(left, right):
    a = jnp.concatenate(pieces(jnp.concatenate(left, axis=1), 2), axis=0)
    b = jnp.concatenate(
        [p for group in right for p in pieces(jnp.concatenate(group, axis=1), 2)], axis=0
    )
    out = contract(a, b, tb=True)
    size = left[0].shape[0]
    out = out[:size] + out[size:]
    return jnp.concatenate(
        [
            out[:, 2 * g * size : (2 * g + 1) * size] + out[:, (2 * g + 1) * size : (2 * g + 2) * size]
            for g in range(len(right))
        ],
        axis=1,
    )


def call(body, outs, in_specs, scratch=(), name=None, aliases=None, weight=0):
    shapes = [
        o if isinstance(o, jax.ShapeDtypeStruct) else jax.ShapeDtypeStruct(o, F32) for o in outs
    ]
    return pl.pallas_call(
        body,
        out_shape=shapes,
        in_specs=in_specs,
        out_specs=[VMEM] * len(outs),
        scratch_shapes=list(scratch),
        compiler_params=pltpu.CompilerParams(vmem_limit_bytes=40 << 20),
        input_output_aliases=aliases or {},
        cost_estimate=pl.CostEstimate(flops=weight, bytes_accessed=weight, transcendentals=0) if weight else None,
        name=name,
    )


def pinned(value):
    return pltpu.with_memory_space_constraint(value, pltpu.HBM)


def after(value, *tokens):
    return lax.optimization_barrier((value,) + tokens)[0]


def pairings(size):
    rounds = []
    for hop in range(1, HOPS + 1):
        for parity in range(2):
            pairs = [(i, i + hop) for i in range(size - hop) if (i // hop) % 2 == parity]
            if not pairs:
                continue
            used = {i for pair in pairs for i in pair}
            for entry in rounds:
                if not entry["used"] & used:
                    entry["used"] |= used
                    entry["pairs"] += pairs
                    entry["kinds"].append((hop, parity))
                    break
            else:
                rounds.append({"used": used, "pairs": pairs, "kinds": [(hop, parity)]})
    return rounds


def exchange(block, axis, pairs):
    return lax.ppermute(block, axis, [(a, b) for a, b in pairs] + [(b, a) for a, b in pairs])


def role_table(rounds, size):
    table = [[0] * size for _ in rounds]
    for p, entry in enumerate(rounds):
        for a, b in entry["pairs"]:
            table[p][a] = b - a
            table[p][b] = a - b
    return jnp.array(table, jnp.int32)


def sum_steps(size):
    return [1 << n for n in range(size.bit_length() - 1)]


def start_sum(block, axis):
    size = lax.axis_size(axis)
    if size & (size - 1):
        return block
    for step in sum_steps(size)[:-1]:
        block = block + lax.ppermute(block, axis, [(i, i ^ step) for i in range(size)])
    return block


def end_sum(block, axis, *tokens):
    size = lax.axis_size(axis)
    if size & (size - 1):
        return lax.psum(block, axis)
    for step in sum_steps(size)[-1:]:
        got = lax.ppermute(block, axis, [(i, i ^ step) for i in range(size)])
        block = block + (after(got, *tokens) if tokens else got)
    return block


def all_sum(block, axis):
    size = lax.axis_size(axis)
    if size & (size - 1):
        return lax.psum(block, axis)
    step = 1
    while step < size:
        masks = [step] if 2 * step >= size else [step, 2 * step, 3 * step]
        got = [lax.ppermute(block, axis, [(i, i ^ m) for i in range(size)]) for m in masks]
        if len(got) == 1:
            block = block + got[0]
            step *= 2
        else:
            block = (block + got[0]) + (got[1] + got[2])
            step *= 4
    return block


def factor(gram):
    size = gram.shape[0]
    tile = (8, 2 * size)
    row_id = lax.broadcasted_iota(jnp.int32, (size, size), 0)
    col_id = lax.broadcasted_iota(jnp.int32, (size, size), 1)
    work = jnp.concatenate([gram, (row_id == col_id).astype(F32)], axis=1)
    blocks = [work[8 * b : 8 * b + 8] for b in range(size // 8)]
    sub = lax.broadcasted_iota(jnp.int32, tile, 0)
    for j in range(0, size, 4):
        b, s = divmod(j, 8)
        later = range(b + s // 4, size // 8)
        line = [jnp.broadcast_to(blocks[b][s + k : s + k + 1], tile) for k in range(4)]
        cols = {
            o: [jnp.broadcast_to(blocks[o][:, j + k : j + k + 1], tile) for k in range(4)]
            for o in range(b, size // 8)
        }
        entry = {
            (k, l): jnp.broadcast_to(cols[b][l][s + k : s + k + 1], tile)
            for k in range(4)
            for l in range(k, 4)
        }
        scaled = []
        for k in range(4):
            inverse = 1.0 / entry[k, k]
            for l in range(k + 1, 4):
                ratio = entry[k, l] * inverse
                for p in range(l, 4):
                    entry[l, p] = entry[l, p] - ratio * entry[k, p]
                line[l] = line[l] - ratio * line[k]
                for o in later:
                    cols[o][l] = cols[o][l] - ratio * cols[o][k]
            scaled.append(inverse * line[k])
        for o in range(b, size // 8):
            new = blocks[o]
            if o in later:
                new = new - ((cols[o][0] * scaled[0] + cols[o][1] * scaled[1]) + (cols[o][2] * scaled[2] + cols[o][3] * scaled[3]))
            if o == b:
                new = jnp.where(sub > s + 3, new, blocks[o])
                for k in range(1, 4):
                    new = jnp.where(sub == s + k, line[k], new)
            blocks[o] = new
    work = jnp.concatenate(blocks, axis=0)
    pivots = jnp.sum(jnp.where(row_id == col_id, work[:, :size], 0.0), axis=1, keepdims=True)
    work = work / jnp.sqrt(pivots)
    upper = jnp.where(col_id >= row_id, work[:, :size], 0.0)
    inverse = jnp.where(col_id <= row_id, work[:, size:], 0.0)
    return upper, inverse


def local(start_block, diagonal, hess_tiles, tile_rows, tile_cols, slot_counts):
    peers = lax.axis_size("res")
    lanes = lax.axis_size("vec")
    rows, width, length = start_block.shape
    slots = hess_tiles.shape[2]
    half = rows // 2
    part = width // 2
    rounds = pairings(peers)
    count = len(rounds)
    full = (rows, width, length)
    halffull = (half, width, length)
    chunk = (rows, part, length)
    halfchunk = (half, part, length)
    packet = (CAP, part, length)
    square = (width, width)
    split_shape = jax.ShapeDtypeStruct((slots, 2, length, length), BF16)

    table = role_table(rounds, peers)
    place = jnp.concatenate(
        [lax.axis_index("vec").reshape(1), table[:, lax.axis_index("res")]]
    ).astype(jnp.int32)

    def own_sum(acc_refs, x_ref, split_ref, rows_ref, cols_ref):
        batch = 4
        for first in range(0, OWN_SLOTS, batch):
            members = range(first, first + batch)
            ends = [(rows_ref[0, 0, s], cols_ref[0, 0, s]) for s in members]
            terms = [
                (
                    tile_product(x_ref[j], split_ref, s, True),
                    tile_product(x_ref[i], split_ref, s, False),
                )
                for s, (i, j) in zip(members, ends)
            ]
            for (i, j), (direct, mirror) in zip(ends, terms):
                for n, acc_ref in enumerate(acc_refs):
                    acc_ref[i] += direct[n * part : (n + 1) * part]
                    acc_ref[j] += mirror[n * part : (n + 1) * part]

    def prepare_body(x_hbm, diag_hbm, tiles_hbm, *refs):
        x_ref, split_ref, a_ref, b_ref, diag_ref, raw_ref, sem = refs
        size = slots // 4
        copies = [
            pltpu.make_async_copy(src, dst, sem.at[n])
            for n, (src, dst) in enumerate([(x_hbm, x_ref), (diag_hbm, diag_ref)])
        ]
        tile_copies = [
            pltpu.make_async_copy(
                tiles_hbm.at[0, 0, pl.ds(n * size, size)], raw_ref.at[pl.ds(n * size, size)], sem.at[2 + n]
            )
            for n in range(4)
        ]
        for c in copies + tile_copies:
            c.start()
        for n in range(4):
            tile_copies[n].wait()
            for s in range(n * size, (n + 1) * size):
                split_ref[s, 0], split_ref[s, 1] = pieces(raw_ref[s], 2)
        for c in copies:
            c.wait()
        first = (lax.axis_index("vec") == 0).astype(F32)
        d = ((diag_ref[...] - SHIFT) * first)[:, None, :]
        a_ref[...] = x_ref[:, :part] * d
        b_ref[...] = x_ref[:, part:] * d

    def own_body(rows_ref, cols_ref, x_ref, split_ref, *refs):
        own_sum(refs[len(refs) // 2 :], x_ref, split_ref, rows_ref, cols_ref)

    def pack(place_ref, rows_ref, counts_ref, asked_refs, x_ref, split_ref, outs):
        for p in range(count):
            role = place_ref[1 + p]

            def put(c, value, p=p):
                for n, ref in enumerate(outs[p]):
                    ref[c] = value[n * part : (n + 1) * part]

            @pl.when(role > 0)
            def _():
                base = OWN_SLOTS + (role - 1) * CAP
                terms = [
                    tile_product(x_ref[rows_ref[0, 0, base + c]], split_ref, base + c, False)
                    for c in range(CAP)
                ]
                for c, term in enumerate(terms):
                    put(c, jnp.where(c < counts_ref[0, 0, role - 1], term, 0.0))

            @pl.when(role < 0)
            def _():
                base = OWN_SLOTS + (-role - 1) * CAP
                for c in range(CAP):
                    put(c, x_ref[asked_refs[p][0, 0, base + c]])

    def send_body(place_ref, rows_ref, counts_ref, *refs):
        asked_refs, (x_ref, split_ref), outs = refs[:count], refs[count : count + 2], refs[count + 2 :]
        pack(
            place_ref, rows_ref, counts_ref, asked_refs, x_ref, split_ref,
            [(outs[p], outs[count + p]) for p in range(count)],
        )

    def settle(place_ref, mine_ref, other_ref, y_ref):
        core = place_ref[0] % 2
        y_ref[pl.ds(core * half, half)] = mine_ref[...]
        y_ref[pl.ds((1 - core) * half, half)] = other_ref[...]

    def resend_body(place_ref, rows_ref, counts_ref, *refs):
        asked_refs = refs[:count]
        mine_ref, other_ref, diag_ref, split_ref, y_ref, acc_ref = refs[count : count + 6]
        outs = refs[count + 6 :]
        settle(place_ref, mine_ref, other_ref, y_ref)
        pack(
            place_ref, rows_ref, counts_ref, asked_refs, y_ref, split_ref,
            [(outs[p],) for p in range(count)],
        )
        first = (place_ref[0] == 0).astype(F32)
        acc_ref[...] = y_ref[...] * ((diag_ref[...] - SHIFT) * first)[:, None, :]

    def join_rounds(members, place_ref, rows_ref, counts_ref, asked_refs, got_refs, split_ref, acc_ref):
        for n, p in enumerate(members):
            role = place_ref[1 + p]

            @pl.when(role > 0)
            def _():
                base = OWN_SLOTS + (role - 1) * CAP
                terms = [
                    tile_product(got_refs[n][c], split_ref, base + c, True) for c in range(CAP)
                ]
                for c, term in enumerate(terms):
                    acc_ref[rows_ref[0, 0, base + c]] += jnp.where(
                        c < counts_ref[0, 0, role - 1], term, 0.0
                    )

            @pl.when(role < 0)
            def _():
                base = OWN_SLOTS + (-role - 1) * CAP
                for c in range(CAP):
                    acc_ref[asked_refs[n][0, 0, base + c]] += got_refs[n][c]

    def join(acc, got, members, last=False):
        size = len(members)

        def body(place_ref, rows_ref, counts_ref, *refs):
            asked_refs, got_refs = refs[:size], refs[size : 2 * size]
            split_ref, prior_ref = refs[2 * size : 2 * size + 2]
            outs = refs[2 * size + 2 :]
            if last:
                keep_ref, give_ref, acc_ref = outs
                acc_ref[...] = prior_ref[...]
            else:
                (acc_ref,) = outs
            join_rounds(
                members, place_ref, rows_ref, counts_ref, asked_refs, got_refs, split_ref, acc_ref
            )
            if last:
                core = place_ref[0] % 2
                keep_ref[...] = acc_ref[pl.ds(core * half, half)]
                give_ref[...] = acc_ref[pl.ds((1 - core) * half, half)]

        out = call(
            body,
            [halfchunk] * 2 if last else [chunk],
            [SMEM] * (3 + size) + [VMEM] * (size + 2),
            [pltpu.VMEM(chunk, F32)] if last else [],
            name="join",
            weight=10**10,
            aliases=None if last else {3 + 2 * size + 1: 0},
        )(
            place, tile_rows, slot_counts, *[asked[p] for p in members], *[got[p] for p in members], split, acc
        )
        return out if last else out[0]

    def gram_body(x_ref, out_ref):
        total = jnp.zeros(square, F32)
        for n in range(0, rows, 2):
            pair = [x_ref[n], x_ref[n + 1]]
            total += gram_step(pair, [pair])
        out_ref[...] = total

    def cross_body(x_ref, a_ref, b_ref, out_ref):
        total = jnp.zeros((width, 2 * width), F32)
        for n in range(0, rows, 2):
            y = [jnp.concatenate([a_ref[m], b_ref[m]], axis=0) for m in (n, n + 1)]
            total += gram_step(y, [[x_ref[n], x_ref[n + 1]], y])
        out_ref[...] = total

    def first_body(gram_ref, inverse_ref):
        _, inverse_ref[...] = factor(gram_ref[...])

    def identity():
        eye = lax.broadcasted_iota(jnp.int32, square, 0) == lax.broadcasted_iota(jnp.int32, square, 1)
        return eye.astype(F32)

    def lower_part():
        return lax.broadcasted_iota(jnp.int32, square, 0) >= lax.broadcasted_iota(jnp.int32, square, 1)

    def second_body(gram_ref, inverse_ref, cross_ref, lower_ref, coef_ref, gain_ref):
        start_inv = inverse_ref[...]
        cross = dot(dot(start_inv, gram_ref[:, :width]), start_inv, tb=True)
        applied = dot(dot(start_inv, gram_ref[:, width:]), start_inv, tb=True)
        upper, inverse = factor(applied - dot(cross, cross, tb=True))
        lower = upper.T
        cross_ref[...] = cross + SHIFT * identity()
        lower_ref[...] = lower
        gain = dot(inverse, start_inv)
        back = -dot(dot(inverse, cross), start_inv)
        gain_ref[...] = gain
        coef_ref[:width, :width] = -dot(lower, start_inv)
        coef_ref[:width, width : 2 * width] = back
        coef_ref[:width, 2 * width :] = gain
        coef_ref[width:, :width] = back
        coef_ref[width:, width : 2 * width] = gain
        coef_ref[width:, 2 * width :] = jnp.zeros(square, F32)

    def blend(side, mine, other, coef):
        def body(place_ref, x_ref, a_ref, b_ref, mine_ref, other_ref, coef_ref, w_ref, q_ref, out_ref, z_ref):
            settle(place_ref, mine_ref, other_ref, z_ref)
            for n in range(0, half, 2):
                stacks = [
                    jnp.concatenate([ref[side * half + m] for ref in (x_ref, a_ref, b_ref, z_ref)], axis=0)
                    for m in (n, n + 1)
                ]
                for m, both in zip((n, n + 1), wide_product(coef_ref[:, : 2 * width + part], stacks)):
                    w_ref[m] = both[:width]
                    q_ref[m] = both[width:]
            total = jnp.zeros(square, F32)
            for n in range(0, half, 2):
                qs = [q_ref[n], q_ref[n + 1]]
                total += gram_step(qs, [qs])
            out_ref[...] = total

        return call(
            body,
            [halffull, halffull, square],
            [SMEM] + [VMEM] * 6,
            [pltpu.VMEM(chunk, F32)],
            name="blend",
        )(place, x, y_a, y_b, mine, other, coef)

    def third_body(place_ref, mine_ref, other_ref, gain_ref, *refs):
        prior_refs, q_refs, norm_refs = refs[0:2], refs[2:4], refs[4:6]
        w_ref, out_ref, z_ref = refs[6:]
        settle(place_ref, mine_ref, other_ref, z_ref)
        for n in range(0, rows, 2):
            side, m = divmod(n, half)
            for k, w in enumerate(wide_product(gain_ref[:, part:], [z_ref[n], z_ref[n + 1]])):
                w_ref[n + k] = w + prior_refs[side][m + k]
        total = jnp.zeros((width, 2 * width), F32)
        for n in range(0, rows, 2):
            side, m = divmod(n, half)
            ws = [w_ref[n], w_ref[n + 1]]
            total += gram_step(ws, [[q_refs[side][m], q_refs[side][m + 1]], ws])
        norm = norm_refs[0][...] + norm_refs[1][...]
        out_ref[:width, :width] = total[:, :width]
        out_ref[:width, width:] = jnp.where(lower_part(), total[:, width:], norm)
        out_ref[width:, :] = jnp.zeros((8, 2 * width), F32)
        out_ref[width:, :width] = jnp.broadcast_to(
            jnp.sum(norm * identity(), axis=0, keepdims=True), (8, width)
        )

    def fourth_body(gram_ref, cross_ref, lower_ref, coef_ref):
        cross = gram_ref[:width, :width]
        packed = gram_ref[:width, width:]
        flipped = packed.T
        squares = jnp.where(lower_part(), packed, flipped)
        norm = jnp.where(lower_part(), flipped, packed)
        norm = jnp.where(identity() > 0, gram_ref[width : width + 1, :width], norm)
        taken = cross + SHIFT * (norm - identity())
        mixed = dot(taken, cross, tb=True)
        squared = squares - mixed - mixed.T + dot(dot(taken, norm), taken, tb=True)
        upper, inverse = factor(squared)
        cross_ref[...] = taken + SHIFT * identity()
        lower_ref[...] = upper.T
        scale = math.sqrt(rows * length * peers)
        coef_ref[:, :width] = inverse * scale
        coef_ref[:, width:] = -dot(inverse, taken) * scale

    def last_body(w_ref, low_ref, high_ref, coef_ref, a1_ref, l1_ref, a2_ref, l2_ref, out_ref, pack_ref):
        for n, ref in enumerate((a1_ref, l1_ref, a2_ref, l2_ref)):
            pack_ref[n] = ref[...]
        for n in range(0, rows, 2):
            side, at = divmod(n, half)
            q_ref = (low_ref, high_ref)[side]
            stacks = [jnp.concatenate([w_ref[n + k], q_ref[at + k]], axis=0) for k in range(2)]
            for m, out in zip((n, n + 1), wide_product(coef_ref[...], stacks, 4)):
                out_ref[m] = out

    swap = [(i, i ^ 1) for i in range(lanes)]
    cuts = [count * n // 3 for n in range(4)]
    groups = [list(range(cuts[n], cuts[n + 1])) for n in range(3)]

    def spread(sent):
        return [exchange(s, "res", entry["pairs"]) for s, entry in zip(sent, rounds)]

    def across(mine, *tokens):
        step = 2
        while step < lanes:
            got = lax.ppermute(mine, "vec", [(i, i ^ step) for i in range(lanes)])
            mine = mine + after(got, *tokens)
            step *= 2
        return mine

    def resend(mine, other):
        y, acc, *sent = call(
            resend_body,
            [chunk, chunk] + [packet] * count,
            [SMEM] * (3 + count) + [VMEM] * 4,
            name="resend",
        )(place, tile_rows, slot_counts, *asked, mine, other, diagonal, split)
        return y, acc, spread(sent)

    def own(y, *accs):
        return call(
            own_body,
            [chunk] * len(accs),
            [SMEM] * 2 + [VMEM] * (2 + len(accs)),
            name="own",
            aliases={4 + n: n for n in range(len(accs))},
        )(tile_rows, tile_cols, y, split, *accs)

    asked = [exchange(tile_cols, "res", entry["pairs"]) for entry in rounds]
    x, split, acc_a, acc_b = call(
        prepare_body,
        [full, split_shape, chunk, chunk],
        [HBM] * 3,
        [
            pltpu.VMEM(diagonal.shape, F32),
            pltpu.VMEM((slots, length, length), F32),
            pltpu.SemaphoreType.DMA((6,)),
        ],
        name="prepare",
    )(*[pinned(v) for v in (start_block, diagonal, hess_tiles)])
    sent = call(
        send_body, [packet] * (2 * count), [SMEM] * (3 + count) + [VMEM] * 2, name="send"
    )(place, tile_rows, slot_counts, *asked, x, split)
    got_a = spread(sent[:count])
    sent_b = list(sent[count:])
    acc_a, acc_b = own(x, after(acc_a, sent[0]), acc_b)
    for n in range(2):
        acc_a = join(acc_a, got_a, groups[n])
        turn = groups[0] if n == 1 else []
        acc_a, x, *gated = lax.optimization_barrier((acc_a, x, *[sent_b[p] for p in turn]))
        for p, value in zip(turn, gated):
            sent_b[p] = value
        if n == 0:
            (gram,) = call(gram_body, [square], [VMEM], name="gram")(x)
            start_gram = start_sum(gram, "res")
    acc_a = after(acc_a, start_gram)
    keep_a, give_a = join(acc_a, got_a, groups[2], last=True)
    for p in groups[1] + groups[2]:
        sent_b[p] = after(sent_b[p], keep_a)
    got_b = spread(sent_b)

    core = lax.ppermute(give_a, "vec", swap)
    acc_b = join(acc_b, got_b, groups[0])
    mine_a = keep_a + after(core, acc_b)
    (start_inv,) = call(first_body, [square], [VMEM], name="first")(end_sum(start_gram, "res", mine_a))
    acc_b = join(after(acc_b, start_inv), got_b, groups[1])
    mine_a = across(mine_a, acc_b)
    other_a = lax.ppermute(mine_a, "vec", swap)
    keep_b, give_b = join(acc_b, got_b, groups[2], last=True)
    y_a, acc_a, got_a = resend(mine_a, after(other_a, keep_b))

    core = lax.ppermute(give_b, "vec", swap)
    mine_b = keep_b + after(core, y_a)
    (acc_a,) = own(y_a, after(acc_a, mine_b))
    mine_b = across(mine_b, acc_a)
    other_b = lax.ppermute(mine_b, "vec", swap)
    acc_a = join(after(acc_a, mine_b), got_a, groups[2])
    y_b, acc_b, got_b = resend(mine_b, after(other_b, acc_a))
    acc_a = join(after(acc_a, y_b), got_a, groups[1])
    keep_a, give_a = join(acc_a, got_a, groups[0], last=True)

    core = lax.ppermute(give_a, "vec", swap)
    (acc_b,) = own(after(y_b, keep_a), acc_b)
    acc_b = join(acc_b, got_b, groups[0])
    mine_a = keep_a + after(core, acc_b)
    (gram,) = call(cross_body, [(width, 2 * width)], [VMEM] * 3, name="cross")(x, y_a, after(y_b, mine_a))
    acc_b = join(after(acc_b, gram), got_b, groups[1])
    cross_gram = start_sum(gram, "res")
    keep_b, give_b = join(after(acc_b, cross_gram), got_b, groups[2], last=True)

    core = lax.ppermute(give_b, "vec", swap)
    mine_a = across(mine_a, cross_gram)
    other_a = lax.ppermute(mine_a, "vec", swap)
    cross_gram = end_sum(cross_gram, "res")
    mine_b = keep_b + after(core, mine_a, cross_gram)
    cross1, lower1, coef, gain = call(
        second_body, [square, square, (2 * width, 3 * width), square], [VMEM] * 2, name="second"
    )(after(cross_gram, mine_b), start_inv)
    w_low, q_low, norm_low = blend(0, mine_a, other_a, coef)
    w_high, q_high, norm_high = blend(1, mine_a, other_a, coef)
    mine_b = across(mine_b, norm_low, norm_high)
    other_b = lax.ppermute(mine_b, "vec", swap)
    w, gram = call(
        third_body,
        [full, (width + 8, 2 * width)],
        [SMEM] + [VMEM] * 9,
        [pltpu.VMEM(chunk, F32)],
        name="third",
    )(place, mine_b, other_b, gain, w_low, w_high, q_low, q_high, norm_low, norm_high)
    gram = all_sum(gram, "res")
    cross2, lower2, coef = call(
        fourth_body, [square, square, (width, 2 * width)], [VMEM], name="fourth"
    )(gram)
    return call(last_body, [full, (4, width, width)], [VMEM] * 8, name="last")(
        w, q_low, q_high, coef, cross1, lower1, cross2, lower2
    )


def solution(mesh):
    in_specs = (
        P(("conf", "res"), None, None),
        P(("conf", "res"), None),
        P(("conf", "res"), "vec", None, None, None),
        P(("conf", "res"), "vec", None),
        P(("conf", "res"), "vec", None),
        P(("conf", "res"), "vec", None),
    )
    out_specs = (P(("conf", "res"), None, None), P("conf", None, None))
    return jax.shard_map(local, mesh=mesh, in_specs=in_specs, out_specs=out_specs, check_vma=False)
```

```python
import math

import jax
import jax.numpy as jnp
from jax import lax
from jax.experimental import pallas as pl
from jax.experimental.pallas import tpu as pltpu
from jax.sharding import PartitionSpec as P

OWN_SLOTS = 20
HOPS = 3
CAP = 8
SHIFT = 1.65
BF16 = jnp.bfloat16
F32 = jnp.float32

VMEM = pl.BlockSpec(memory_space=pltpu.VMEM)
SMEM = pl.BlockSpec(memory_space=pltpu.SMEM)
HBM = pl.BlockSpec(memory_space=pltpu.HBM)


def contract(a, b, ta=False, tb=False, precision=None):
    dims = (((0 if ta else 1,), (1 if tb else 0,)), ((), ()))
    return lax.dot_general(a, b, dims, precision=precision, preferred_element_type=F32)


def dot(a, b, ta=False, tb=False):
    return contract(a, b, ta, tb, lax.Precision.HIGHEST)


def pieces(x, count):
    out = []
    for _ in range(count):
        out.append(x.astype(BF16))
        x = x - out[-1].astype(F32)
    return out


def tile_product(x, tile_ref, slot, transposed):
    x1, x2 = pieces(x, 2)
    m1, m2 = tile_ref[slot, 0], tile_ref[slot, 1]
    axis = 1 if transposed else 0
    left = jnp.concatenate([x1, x2, x1], axis=1)
    return contract(left, jnp.concatenate([m1, m1, m2], axis=axis), tb=transposed)


def wide_product(coef, blocks, terms=6):
    pairs = [(0, 0), (0, 1), (1, 0), (1, 1)] if terms == 4 else [(0, 0), (0, 1), (0, 2), (1, 0), (1, 1), (2, 0)]
    c = pieces(coef, terms // 2)
    z = pieces(jnp.concatenate(blocks, axis=1), terms // 2)
    left = jnp.concatenate([c[m] for m, _ in pairs], axis=1)
    out = contract(left, jnp.concatenate([z[m] for _, m in pairs], axis=0))
    width = blocks[0].shape[1]
    return [out[:, n * width : (n + 1) * width] for n in range(len(blocks))]


def gram_step(left, right):
    a = jnp.concatenate(pieces(jnp.concatenate(left, axis=1), 2), axis=0)
    b = jnp.concatenate(
        [p for group in right for p in pieces(jnp.concatenate(group, axis=1), 2)], axis=0
    )
    out = contract(a, b, tb=True)
    size = left[0].shape[0]
    out = out[:size] + out[size:]
    return jnp.concatenate(
        [
            out[:, 2 * g * size : (2 * g + 1) * size] + out[:, (2 * g + 1) * size : (2 * g + 2) * size]
            for g in range(len(right))
        ],
        axis=1,
    )


def call(body, outs, in_specs, scratch=(), name=None, aliases=None, weight=0):
    shapes = [
        o if isinstance(o, jax.ShapeDtypeStruct) else jax.ShapeDtypeStruct(o, F32) for o in outs
    ]
    return pl.pallas_call(
        body,
        out_shape=shapes,
        in_specs=in_specs,
        out_specs=[VMEM] * len(outs),
        scratch_shapes=list(scratch),
        compiler_params=pltpu.CompilerParams(vmem_limit_bytes=40 << 20),
        input_output_aliases=aliases or {},
        cost_estimate=pl.CostEstimate(flops=weight, bytes_accessed=weight, transcendentals=0) if weight else None,
        name=name,
    )


def pinned(value):
    return pltpu.with_memory_space_constraint(value, pltpu.HBM)


def after(value, *tokens):
    return lax.optimization_barrier((value,) + tokens)[0]


def pairings(size):
    rounds = []
    for hop in range(1, HOPS + 1):
        for parity in range(2):
            pairs = [(i, i + hop) for i in range(size - hop) if (i // hop) % 2 == parity]
            if not pairs:
                continue
            used = {i for pair in pairs for i in pair}
            for entry in rounds:
                if not entry["used"] & used:
                    entry["used"] |= used
                    entry["pairs"] += pairs
                    entry["kinds"].append((hop, parity))
                    break
            else:
                rounds.append({"used": used, "pairs": pairs, "kinds": [(hop, parity)]})
    return rounds


def exchange(block, axis, pairs):
    return lax.ppermute(block, axis, [(a, b) for a, b in pairs] + [(b, a) for a, b in pairs])


def role_table(rounds, size):
    table = [[0] * size for _ in rounds]
    for p, entry in enumerate(rounds):
        for a, b in entry["pairs"]:
            table[p][a] = b - a
            table[p][b] = a - b
    return jnp.array(table, jnp.int32)


def sum_steps(size):
    return [1 << n for n in range(size.bit_length() - 1)]


def start_sum(block, axis):
    size = lax.axis_size(axis)
    if size & (size - 1):
        return block
    for step in sum_steps(size)[:-1]:
        block = block + lax.ppermute(block, axis, [(i, i ^ step) for i in range(size)])
    return block


def end_sum(block, axis, *tokens):
    size = lax.axis_size(axis)
    if size & (size - 1):
        return lax.psum(block, axis)
    for step in sum_steps(size)[-1:]:
        got = lax.ppermute(block, axis, [(i, i ^ step) for i in range(size)])
        block = block + (after(got, *tokens) if tokens else got)
    return block


def all_sum(block, axis):
    size = lax.axis_size(axis)
    if size & (size - 1):
        return lax.psum(block, axis)
    step = 1
    while step < size:
        masks = [step] if 2 * step >= size else [step, 2 * step, 3 * step]
        got = [lax.ppermute(block, axis, [(i, i ^ m) for i in range(size)]) for m in masks]
        if len(got) == 1:
            block = block + got[0]
            step *= 2
        else:
            block = (block + got[0]) + (got[1] + got[2])
            step *= 4
    return block


def factor(gram):
    size = gram.shape[0]
    tile = (8, 2 * size)
    row_id = lax.broadcasted_iota(jnp.int32, (size, size), 0)
    col_id = lax.broadcasted_iota(jnp.int32, (size, size), 1)
    work = jnp.concatenate([gram, (row_id == col_id).astype(F32)], axis=1)
    blocks = [work[8 * b : 8 * b + 8] for b in range(size // 8)]
    sub = lax.broadcasted_iota(jnp.int32, tile, 0)

    def column(block, j):
        return jnp.broadcast_to(block[:, j : j + 1], tile)

    for b in range(size // 8):
        line = [jnp.broadcast_to(blocks[b][k : k + 1], tile) for k in range(8)]
        cols = [column(blocks[b], 8 * b + k) for k in range(8)]
        entry = {
            (k, l): jnp.broadcast_to(cols[l][k : k + 1], tile) for k in range(8) for l in range(k, 8)
        }
        ratio = {}
        solved = []
        for k in range(8):
            inverse = 1.0 / entry[k, k]
            for l in range(k + 1, 8):
                ratio[k, l] = entry[k, l] * inverse
                for p in range(l, 8):
                    entry[l, p] = entry[l, p] - ratio[k, l] * entry[k, p]
                line[l] = line[l] - ratio[k, l] * line[k]
            solved.append(inverse * line[k])
        for l in reversed(range(1, 8)):
            for k in range(l):
                solved[k] = solved[k] - ratio[k, l] * solved[l]
        for o in range(b + 1, size // 8):
            terms = [column(blocks[o], 8 * b + k) * solved[k] for k in range(8)]
            while len(terms) > 1:
                terms = [terms[n] + terms[n + 1] for n in range(0, len(terms), 2)]
            blocks[o] = blocks[o] - terms[0]
        new = line[0]
        for k in range(1, 8):
            new = jnp.where(sub == k, line[k], new)
        blocks[b] = new
    work = jnp.concatenate(blocks, axis=0)
    pivots = jnp.sum(jnp.where(row_id == col_id, work[:, :size], 0.0), axis=1, keepdims=True)
    work = work / jnp.sqrt(pivots)
    upper = jnp.where(col_id >= row_id, work[:, :size], 0.0)
    inverse = jnp.where(col_id <= row_id, work[:, size:], 0.0)
    return upper, inverse


def local(start_block, diagonal, hess_tiles, tile_rows, tile_cols, slot_counts):
    peers = lax.axis_size("res")
    lanes = lax.axis_size("vec")
    rows, width, length = start_block.shape
    slots = hess_tiles.shape[2]
    half = rows // 2
    part = width // 2
    rounds = pairings(peers)
    count = len(rounds)
    full = (rows, width, length)
    halffull = (half, width, length)
    chunk = (rows, part, length)
    halfchunk = (half, part, length)
    packet = (CAP, part, length)
    square = (width, width)
    split_shape = jax.ShapeDtypeStruct((slots, 2, length, length), BF16)

    table = role_table(rounds, peers)
    place = jnp.concatenate(
        [lax.axis_index("vec").reshape(1), table[:, lax.axis_index("res")]]
    ).astype(jnp.int32)

    def own_sum(acc_refs, x_ref, split_ref, rows_ref, cols_ref):
        batch = 4
        for first in range(0, OWN_SLOTS, batch):
            members = range(first, first + batch)
            ends = [(rows_ref[0, 0, s], cols_ref[0, 0, s]) for s in members]
            terms = [
                (
                    tile_product(x_ref[j], split_ref, s, True),
                    tile_product(x_ref[i], split_ref, s, False),
                )
                for s, (i, j) in zip(members, ends)
            ]
            for (i, j), (direct, mirror) in zip(ends, terms):
                for n, acc_ref in enumerate(acc_refs):
                    acc_ref[i] += direct[n * part : (n + 1) * part]
                    acc_ref[j] += mirror[n * part : (n + 1) * part]

    def prepare_body(x_hbm, diag_hbm, tiles_hbm, *refs):
        x_ref, split_ref, a_ref, b_ref, diag_ref, raw_ref, sem = refs
        size = slots // 4
        copies = [
            pltpu.make_async_copy(src, dst, sem.at[n])
            for n, (src, dst) in enumerate([(x_hbm, x_ref), (diag_hbm, diag_ref)])
        ]
        tile_copies = [
            pltpu.make_async_copy(
                tiles_hbm.at[0, 0, pl.ds(n * size, size)], raw_ref.at[pl.ds(n * size, size)], sem.at[2 + n]
            )
            for n in range(4)
        ]
        for c in copies + tile_copies:
            c.start()
        for n in range(4):
            tile_copies[n].wait()
            for s in range(n * size, (n + 1) * size):
                split_ref[s, 0], split_ref[s, 1] = pieces(raw_ref[s], 2)
        for c in copies:
            c.wait()
        first = (lax.axis_index("vec") == 0).astype(F32)
        d = ((diag_ref[...] - SHIFT) * first)[:, None, :]
        a_ref[...] = x_ref[:, :part] * d
        b_ref[...] = x_ref[:, part:] * d

    def own_body(rows_ref, cols_ref, x_ref, split_ref, *refs):
        own_sum(refs[len(refs) // 2 :], x_ref, split_ref, rows_ref, cols_ref)

    def pack(place_ref, rows_ref, counts_ref, asked_refs, x_ref, split_ref, outs):
        for p in range(count):
            role = place_ref[1 + p]

            def put(c, value, p=p):
                for n, ref in enumerate(outs[p]):
                    ref[c] = value[n * part : (n + 1) * part]

            @pl.when(role > 0)
            def _():
                base = OWN_SLOTS + (role - 1) * CAP
                terms = [
                    tile_product(x_ref[rows_ref[0, 0, base + c]], split_ref, base + c, False)
                    for c in range(CAP)
                ]
                for c, term in enumerate(terms):
                    put(c, jnp.where(c < counts_ref[0, 0, role - 1], term, 0.0))

            @pl.when(role < 0)
            def _():
                base = OWN_SLOTS + (-role - 1) * CAP
                for c in range(CAP):
                    put(c, x_ref[asked_refs[p][0, 0, base + c]])

    def send_body(place_ref, rows_ref, counts_ref, *refs):
        asked_refs, (x_ref, split_ref), outs = refs[:count], refs[count : count + 2], refs[count + 2 :]
        pack(
            place_ref, rows_ref, counts_ref, asked_refs, x_ref, split_ref,
            [(outs[p], outs[count + p]) for p in range(count)],
        )

    def settle(place_ref, mine_ref, other_ref, y_ref):
        core = place_ref[0] % 2
        y_ref[pl.ds(core * half, half)] = mine_ref[...]
        y_ref[pl.ds((1 - core) * half, half)] = other_ref[...]

    def resend_body(place_ref, rows_ref, counts_ref, *refs):
        asked_refs = refs[:count]
        mine_ref, other_ref, diag_ref, split_ref, y_ref, acc_ref = refs[count : count + 6]
        outs = refs[count + 6 :]
        settle(place_ref, mine_ref, other_ref, y_ref)
        pack(
            place_ref, rows_ref, counts_ref, asked_refs, y_ref, split_ref,
            [(outs[p],) for p in range(count)],
        )
        first = (place_ref[0] == 0).astype(F32)
        acc_ref[...] = y_ref[...] * ((diag_ref[...] - SHIFT) * first)[:, None, :]

    def join_rounds(members, place_ref, rows_ref, counts_ref, asked_refs, got_refs, split_ref, acc_ref):
        for n, p in enumerate(members):
            role = place_ref[1 + p]

            @pl.when(role > 0)
            def _():
                base = OWN_SLOTS + (role - 1) * CAP
                terms = [
                    tile_product(got_refs[n][c], split_ref, base + c, True) for c in range(CAP)
                ]
                for c, term in enumerate(terms):
                    acc_ref[rows_ref[0, 0, base + c]] += jnp.where(
                        c < counts_ref[0, 0, role - 1], term, 0.0
                    )

            @pl.when(role < 0)
            def _():
                base = OWN_SLOTS + (-role - 1) * CAP
                for c in range(CAP):
                    acc_ref[asked_refs[n][0, 0, base + c]] += got_refs[n][c]

    def join(acc, got, members, last=False):
        size = len(members)

        def body(place_ref, rows_ref, counts_ref, *refs):
            asked_refs, got_refs = refs[:size], refs[size : 2 * size]
            split_ref, prior_ref = refs[2 * size : 2 * size + 2]
            outs = refs[2 * size + 2 :]
            if last:
                keep_ref, give_ref, acc_ref = outs
                acc_ref[...] = prior_ref[...]
            else:
                (acc_ref,) = outs
            join_rounds(
                members, place_ref, rows_ref, counts_ref, asked_refs, got_refs, split_ref, acc_ref
            )
            if last:
                core = place_ref[0] % 2
                keep_ref[...] = acc_ref[pl.ds(core * half, half)]
                give_ref[...] = acc_ref[pl.ds((1 - core) * half, half)]

        out = call(
            body,
            [halfchunk] * 2 if last else [chunk],
            [SMEM] * (3 + size) + [VMEM] * (size + 2),
            [pltpu.VMEM(chunk, F32)] if last else [],
            name="join",
            weight=10**10,
            aliases=None if last else {3 + 2 * size + 1: 0},
        )(
            place, tile_rows, slot_counts, *[asked[p] for p in members], *[got[p] for p in members], split, acc
        )
        return out if last else out[0]

    def gram_body(x_ref, out_ref):
        total = jnp.zeros(square, F32)
        for n in range(0, rows, 2):
            pair = [x_ref[n], x_ref[n + 1]]
            total += gram_step(pair, [pair])
        out_ref[...] = total

    def cross_body(x_ref, a_ref, b_ref, out_ref):
        total = jnp.zeros((width, 2 * width), F32)
        for n in range(0, rows, 2):
            y = [jnp.concatenate([a_ref[m], b_ref[m]], axis=0) for m in (n, n + 1)]
            total += gram_step(y, [[x_ref[n], x_ref[n + 1]], y])
        out_ref[...] = total

    def first_body(gram_ref, inverse_ref):
        _, inverse_ref[...] = factor(gram_ref[...])

    def identity():
        eye = lax.broadcasted_iota(jnp.int32, square, 0) == lax.broadcasted_iota(jnp.int32, square, 1)
        return eye.astype(F32)

    def lower_part():
        return lax.broadcasted_iota(jnp.int32, square, 0) >= lax.broadcasted_iota(jnp.int32, square, 1)

    def second_body(gram_ref, inverse_ref, cross_ref, lower_ref, coef_ref, gain_ref):
        start_inv = inverse_ref[...]
        cross = dot(dot(start_inv, gram_ref[:, :width]), start_inv, tb=True)
        applied = dot(dot(start_inv, gram_ref[:, width:]), start_inv, tb=True)
        upper, inverse = factor(applied - dot(cross, cross, tb=True))
        lower = upper.T
        cross_ref[...] = cross + SHIFT * identity()
        lower_ref[...] = lower
        gain = dot(inverse, start_inv)
        back = -dot(dot(inverse, cross), start_inv)
        gain_ref[...] = gain
        coef_ref[:width, :width] = -dot(lower, start_inv)
        coef_ref[:width, width : 2 * width] = back
        coef_ref[:width, 2 * width :] = gain
        coef_ref[width:, :width] = back
        coef_ref[width:, width : 2 * width] = gain
        coef_ref[width:, 2 * width :] = jnp.zeros(square, F32)

    def blend(side, mine, other, coef):
        def body(place_ref, x_ref, a_ref, b_ref, mine_ref, other_ref, coef_ref, w_ref, q_ref, out_ref, z_ref):
            settle(place_ref, mine_ref, other_ref, z_ref)
            for n in range(0, half, 2):
                stacks = [
                    jnp.concatenate([ref[side * half + m] for ref in (x_ref, a_ref, b_ref, z_ref)], axis=0)
                    for m in (n, n + 1)
                ]
                for m, both in zip((n, n + 1), wide_product(coef_ref[:, : 2 * width + part], stacks)):
                    w_ref[m] = both[:width]
                    q_ref[m] = both[width:]
            total = jnp.zeros(square, F32)
            for n in range(0, half, 2):
                qs = [q_ref[n], q_ref[n + 1]]
                total += gram_step(qs, [qs])
            out_ref[...] = total

        return call(
            body,
            [halffull, halffull, square],
            [SMEM] + [VMEM] * 6,
            [pltpu.VMEM(chunk, F32)],
            name="blend",
        )(place, x, y_a, y_b, mine, other, coef)

    def third_body(place_ref, mine_ref, other_ref, gain_ref, *refs):
        prior_refs, q_refs, norm_refs = refs[0:2], refs[2:4], refs[4:6]
        w_ref, out_ref, z_ref = refs[6:]
        settle(place_ref, mine_ref, other_ref, z_ref)
        for n in range(0, rows, 2):
            side, m = divmod(n, half)
            for k, w in enumerate(wide_product(gain_ref[:, part:], [z_ref[n], z_ref[n + 1]])):
                w_ref[n + k] = w + prior_refs[side][m + k]
        total = jnp.zeros((width, 2 * width), F32)
        for n in range(0, rows, 2):
            side, m = divmod(n, half)
            ws = [w_ref[n], w_ref[n + 1]]
            total += gram_step(ws, [[q_refs[side][m], q_refs[side][m + 1]], ws])
        norm = norm_refs[0][...] + norm_refs[1][...]
        out_ref[:width, :width] = total[:, :width]
        out_ref[:width, width:] = jnp.where(lower_part(), total[:, width:], norm)
        out_ref[width:, :] = jnp.zeros((8, 2 * width), F32)
        out_ref[width:, :width] = jnp.broadcast_to(
            jnp.sum(norm * identity(), axis=0, keepdims=True), (8, width)
        )

    def fourth_body(gram_ref, cross_ref, lower_ref, coef_ref):
        cross = gram_ref[:width, :width]
        packed = gram_ref[:width, width:]
        flipped = packed.T
        squares = jnp.where(lower_part(), packed, flipped)
        norm = jnp.where(lower_part(), flipped, packed)
        norm = jnp.where(identity() > 0, gram_ref[width : width + 1, :width], norm)
        taken = cross + SHIFT * (norm - identity())
        mixed = dot(taken, cross, tb=True)
        squared = squares - mixed - mixed.T + dot(dot(taken, norm), taken, tb=True)
        upper, inverse = factor(squared)
        cross_ref[...] = taken + SHIFT * identity()
        lower_ref[...] = upper.T
        scale = math.sqrt(rows * length * peers)
        coef_ref[:, :width] = inverse * scale
        coef_ref[:, width:] = -dot(inverse, taken) * scale

    def last_body(w_ref, low_ref, high_ref, coef_ref, a1_ref, l1_ref, a2_ref, l2_ref, out_ref, pack_ref):
        for n, ref in enumerate((a1_ref, l1_ref, a2_ref, l2_ref)):
            pack_ref[n] = ref[...]
        for n in range(0, rows, 2):
            side, at = divmod(n, half)
            q_ref = (low_ref, high_ref)[side]
            stacks = [jnp.concatenate([w_ref[n + k], q_ref[at + k]], axis=0) for k in range(2)]
            for m, out in zip((n, n + 1), wide_product(coef_ref[...], stacks, 4)):
                out_ref[m] = out

    swap = [(i, i ^ 1) for i in range(lanes)]
    cuts = [count * n // 3 for n in range(4)]
    groups = [list(range(cuts[n], cuts[n + 1])) for n in range(3)]

    def spread(sent):
        return [exchange(s, "res", entry["pairs"]) for s, entry in zip(sent, rounds)]

    def across(mine, *tokens):
        step = 2
        while step < lanes:
            got = lax.ppermute(mine, "vec", [(i, i ^ step) for i in range(lanes)])
            mine = mine + after(got, *tokens)
            step *= 2
        return mine

    def resend(mine, other):
        y, acc, *sent = call(
            resend_body,
            [chunk, chunk] + [packet] * count,
            [SMEM] * (3 + count) + [VMEM] * 4,
            name="resend",
        )(place, tile_rows, slot_counts, *asked, mine, other, diagonal, split)
        return y, acc, spread(sent)

    def own(y, *accs):
        return call(
            own_body,
            [chunk] * len(accs),
            [SMEM] * 2 + [VMEM] * (2 + len(accs)),
            name="own",
            aliases={4 + n: n for n in range(len(accs))},
        )(tile_rows, tile_cols, y, split, *accs)

    asked = [exchange(tile_cols, "res", entry["pairs"]) for entry in rounds]
    x, split, acc_a, acc_b = call(
        prepare_body,
        [full, split_shape, chunk, chunk],
        [HBM] * 3,
        [
            pltpu.VMEM(diagonal.shape, F32),
            pltpu.VMEM((slots, length, length), F32),
            pltpu.SemaphoreType.DMA((6,)),
        ],
        name="prepare",
    )(*[pinned(v) for v in (start_block, diagonal, hess_tiles)])
    sent = call(
        send_body, [packet] * (2 * count), [SMEM] * (3 + count) + [VMEM] * 2, name="send"
    )(place, tile_rows, slot_counts, *asked, x, split)
    got_a = spread(sent[:count])
    sent_b = list(sent[count:])
    acc_a, acc_b = own(x, after(acc_a, sent[0]), acc_b)
    for n in range(2):
        acc_a = join(acc_a, got_a, groups[n])
        turn = groups[0] if n == 1 else []
        acc_a, x, *gated = lax.optimization_barrier((acc_a, x, *[sent_b[p] for p in turn]))
        for p, value in zip(turn, gated):
            sent_b[p] = value
        if n == 0:
            (gram,) = call(gram_body, [square], [VMEM], name="gram")(x)
            start_gram = start_sum(gram, "res")
    acc_a = after(acc_a, start_gram)
    keep_a, give_a = join(acc_a, got_a, groups[2], last=True)
    for p in groups[1] + groups[2]:
        sent_b[p] = after(sent_b[p], keep_a)
    got_b = spread(sent_b)

    core = lax.ppermute(give_a, "vec", swap)
    acc_b = join(acc_b, got_b, groups[0])
    mine_a = keep_a + after(core, acc_b)
    (start_inv,) = call(first_body, [square], [VMEM], name="first")(end_sum(start_gram, "res", mine_a))
    acc_b = join(after(acc_b, start_inv), got_b, groups[1])
    mine_a = across(mine_a, acc_b)
    other_a = lax.ppermute(mine_a, "vec", swap)
    keep_b, give_b = join(acc_b, got_b, groups[2], last=True)
    y_a, acc_a, got_a = resend(mine_a, after(other_a, keep_b))

    core = lax.ppermute(give_b, "vec", swap)
    mine_b = keep_b + after(core, y_a)
    (acc_a,) = own(y_a, after(acc_a, mine_b))
    mine_b = across(mine_b, acc_a)
    other_b = lax.ppermute(mine_b, "vec", swap)
    acc_a = join(after(acc_a, mine_b), got_a, groups[2])
    y_b, acc_b, got_b = resend(mine_b, after(other_b, acc_a))
    acc_a = join(after(acc_a, y_b), got_a, groups[1])
    keep_a, give_a = join(acc_a, got_a, groups[0], last=True)

    core = lax.ppermute(give_a, "vec", swap)
    (acc_b,) = own(after(y_b, keep_a), acc_b)
    acc_b = join(acc_b, got_b, groups[0])
    mine_a = keep_a + after(core, acc_b)
    (gram,) = call(cross_body, [(width, 2 * width)], [VMEM] * 3, name="cross")(x, y_a, after(y_b, mine_a))
    acc_b = join(after(acc_b, gram), got_b, groups[1])
    cross_gram = start_sum(gram, "res")
    keep_b, give_b = join(after(acc_b, cross_gram), got_b, groups[2], last=True)

    core = lax.ppermute(give_b, "vec", swap)
    mine_a = across(mine_a, cross_gram)
    other_a = lax.ppermute(mine_a, "vec", swap)
    cross_gram = end_sum(cross_gram, "res")
    mine_b = keep_b + after(core, mine_a, cross_gram)
    cross1, lower1, coef, gain = call(
        second_body, [square, square, (2 * width, 3 * width), square], [VMEM] * 2, name="second"
    )(after(cross_gram, mine_b), start_inv)
    w_low, q_low, norm_low = blend(0, mine_a, other_a, coef)
    w_high, q_high, norm_high = blend(1, mine_a, other_a, coef)
    mine_b = across(mine_b, norm_low, norm_high)
    other_b = lax.ppermute(mine_b, "vec", swap)
    w, gram = call(
        third_body,
        [full, (width + 8, 2 * width)],
        [SMEM] + [VMEM] * 9,
        [pltpu.VMEM(chunk, F32)],
        name="third",
    )(place, mine_b, other_b, gain, w_low, w_high, q_low, q_high, norm_low, norm_high)
    gram = all_sum(gram, "res")
    cross2, lower2, coef = call(
        fourth_body, [square, square, (width, 2 * width)], [VMEM], name="fourth"
    )(gram)
    return call(last_body, [full, (4, width, width)], [VMEM] * 8, name="last")(
        w, q_low, q_high, coef, cross1, lower1, cross2, lower2
    )


def solution(mesh):
    in_specs = (
        P(("conf", "res"), None, None),
        P(("conf", "res"), None),
        P(("conf", "res"), "vec", None, None, None),
        P(("conf", "res"), "vec", None),
        P(("conf", "res"), "vec", None),
        P(("conf", "res"), "vec", None),
    )
    out_specs = (P(("conf", "res"), None, None), P("conf", None, None))
    return jax.shard_map(local, mesh=mesh, in_specs=in_specs, out_specs=out_specs, check_vma=False)
```

```python
import math

import jax
import jax.numpy as jnp
from jax import lax
from jax.experimental import pallas as pl
from jax.experimental.pallas import tpu as pltpu
from jax.sharding import PartitionSpec as P

OWN_SLOTS = 20
HOPS = 3
CAP = 8
SHIFT = 1.65
BF16 = jnp.bfloat16
F32 = jnp.float32

VMEM = pl.BlockSpec(memory_space=pltpu.VMEM)
SMEM = pl.BlockSpec(memory_space=pltpu.SMEM)
HBM = pl.BlockSpec(memory_space=pltpu.HBM)


def contract(a, b, ta=False, tb=False, precision=None):
    dims = (((0 if ta else 1,), (1 if tb else 0,)), ((), ()))
    return lax.dot_general(a, b, dims, precision=precision, preferred_element_type=F32)


def dot(a, b, ta=False, tb=False):
    return contract(a, b, ta, tb, lax.Precision.HIGHEST)


def pieces(x, count):
    out = []
    for _ in range(count):
        out.append(x.astype(BF16))
        x = x - out[-1].astype(F32)
    return out


def tile_product(x, tile_ref, slot, transposed):
    x1, x2 = pieces(x, 2)
    m1, m2 = tile_ref[slot, 0], tile_ref[slot, 1]
    axis = 1 if transposed else 0
    left = jnp.concatenate([x1, x2, x1], axis=1)
    return contract(left, jnp.concatenate([m1, m1, m2], axis=axis), tb=transposed)


def wide_product(coef, blocks, terms=6):
    pairs = [(0, 0), (0, 1), (1, 0), (1, 1)] if terms == 4 else [(0, 0), (0, 1), (0, 2), (1, 0), (1, 1), (2, 0)]
    c = pieces(coef, terms // 2)
    z = pieces(jnp.concatenate(blocks, axis=1), terms // 2)
    left = jnp.concatenate([c[m] for m, _ in pairs], axis=1)
    out = contract(left, jnp.concatenate([z[m] for _, m in pairs], axis=0))
    width = blocks[0].shape[1]
    return [out[:, n * width : (n + 1) * width] for n in range(len(blocks))]


def gram_step(left, right):
    a = jnp.concatenate(pieces(jnp.concatenate(left, axis=1), 2), axis=0)
    b = jnp.concatenate(
        [p for group in right for p in pieces(jnp.concatenate(group, axis=1), 2)], axis=0
    )
    out = contract(a, b, tb=True)
    size = left[0].shape[0]
    out = out[:size] + out[size:]
    return jnp.concatenate(
        [
            out[:, 2 * g * size : (2 * g + 1) * size] + out[:, (2 * g + 1) * size : (2 * g + 2) * size]
            for g in range(len(right))
        ],
        axis=1,
    )


def call(body, outs, in_specs, scratch=(), name=None, aliases=None, weight=0):
    shapes = [
        o if isinstance(o, jax.ShapeDtypeStruct) else jax.ShapeDtypeStruct(o, F32) for o in outs
    ]
    return pl.pallas_call(
        body,
        out_shape=shapes,
        in_specs=in_specs,
        out_specs=[VMEM] * len(outs),
        scratch_shapes=list(scratch),
        compiler_params=pltpu.CompilerParams(vmem_limit_bytes=40 << 20),
        input_output_aliases=aliases or {},
        cost_estimate=pl.CostEstimate(flops=weight, bytes_accessed=weight, transcendentals=0) if weight else None,
        name=name,
    )


def pinned(value):
    return pltpu.with_memory_space_constraint(value, pltpu.HBM)


def after(value, *tokens):
    return lax.optimization_barrier((value,) + tokens)[0]


def pairings(size):
    rounds = []
    for hop in range(1, HOPS + 1):
        for parity in range(2):
            pairs = [(i, i + hop) for i in range(size - hop) if (i // hop) % 2 == parity]
            if not pairs:
                continue
            used = {i for pair in pairs for i in pair}
            for entry in rounds:
                if not entry["used"] & used:
                    entry["used"] |= used
                    entry["pairs"] += pairs
                    entry["kinds"].append((hop, parity))
                    break
            else:
                rounds.append({"used": used, "pairs": pairs, "kinds": [(hop, parity)]})
    return rounds


def exchange(block, axis, pairs):
    return lax.ppermute(block, axis, [(a, b) for a, b in pairs] + [(b, a) for a, b in pairs])


def role_table(rounds, size):
    table = [[0] * size for _ in rounds]
    for p, entry in enumerate(rounds):
        for a, b in entry["pairs"]:
            table[p][a] = b - a
            table[p][b] = a - b
    return jnp.array(table, jnp.int32)


def sum_steps(size):
    return [1 << n for n in range(size.bit_length() - 1)]


def start_sum(block, axis):
    size = lax.axis_size(axis)
    if size & (size - 1):
        return block
    for step in sum_steps(size)[:-1]:
        block = block + lax.ppermute(block, axis, [(i, i ^ step) for i in range(size)])
    return block


def end_sum(block, axis, *tokens):
    size = lax.axis_size(axis)
    if size & (size - 1):
        return lax.psum(block, axis)
    for step in sum_steps(size)[-1:]:
        got = lax.ppermute(block, axis, [(i, i ^ step) for i in range(size)])
        block = block + (after(got, *tokens) if tokens else got)
    return block


def all_sum(block, axis):
    size = lax.axis_size(axis)
    if size & (size - 1):
        return lax.psum(block, axis)
    step = 1
    while step < size:
        masks = [step] if 2 * step >= size else [step, 2 * step, 3 * step]
        got = [lax.ppermute(block, axis, [(i, i ^ m) for i in range(size)]) for m in masks]
        if len(got) == 1:
            block = block + got[0]
            step *= 2
        else:
            block = (block + got[0]) + (got[1] + got[2])
            step *= 4
    return block


def factor(gram):
    size = gram.shape[0]
    tile = (8, 2 * size)
    row_id = lax.broadcasted_iota(jnp.int32, (size, size), 0)
    col_id = lax.broadcasted_iota(jnp.int32, (size, size), 1)
    work = jnp.concatenate([gram, (row_id == col_id).astype(F32)], axis=1)
    blocks = [work[8 * b : 8 * b + 8] for b in range(size // 8)]
    sub = lax.broadcasted_iota(jnp.int32, tile, 0)

    def column(block, j):
        return jnp.broadcast_to(block[:, j : j + 1], tile)

    for b in range(size // 8):
        line = [jnp.broadcast_to(blocks[b][k : k + 1], tile) for k in range(8)]
        cols = [column(blocks[b], 8 * b + k) for k in range(8)]
        entry = {
            (k, l): jnp.broadcast_to(cols[l][k : k + 1], tile) for k in range(8) for l in range(k, 8)
        }
        ratio = {}
        solved = []
        for k in range(8):
            inverse = 1.0 / entry[k, k]
            for l in range(k + 1, 8):
                ratio[k, l] = entry[k, l] * inverse
                for p in range(l, 8):
                    entry[l, p] = entry[l, p] - ratio[k, l] * entry[k, p]
                line[l] = line[l] - ratio[k, l] * line[k]
            solved.append(inverse * line[k])
        for l in reversed(range(1, 8)):
            for k in range(l):
                solved[k] = solved[k] - ratio[k, l] * solved[l]
        for o in range(b + 1, size // 8):
            terms = [column(blocks[o], 8 * b + k) * solved[k] for k in range(8)]
            while len(terms) > 1:
                terms = [terms[n] + terms[n + 1] for n in range(0, len(terms), 2)]
            blocks[o] = blocks[o] - terms[0]
        new = line[0]
        for k in range(1, 8):
            new = jnp.where(sub == k, line[k], new)
        blocks[b] = new
    work = jnp.concatenate(blocks, axis=0)
    pivots = jnp.sum(jnp.where(row_id == col_id, work[:, :size], 0.0), axis=1, keepdims=True)
    work = work / jnp.sqrt(pivots)
    upper = jnp.where(col_id >= row_id, work[:, :size], 0.0)
    inverse = jnp.where(col_id <= row_id, work[:, size:], 0.0)
    return upper, inverse


def local(start_block, diagonal, hess_tiles, tile_rows, tile_cols, slot_counts):
    peers = lax.axis_size("res")
    lanes = lax.axis_size("vec")
    rows, width, length = start_block.shape
    slots = hess_tiles.shape[2]
    half = rows // 2
    part = width // 2
    rounds = pairings(peers)
    count = len(rounds)
    full = (rows, width, length)
    halffull = (half, width, length)
    chunk = (rows, part, length)
    halfchunk = (half, part, length)
    packet = (CAP, part, length)
    square = (width, width)
    split_shape = jax.ShapeDtypeStruct((slots, 2, length, length), BF16)

    table = role_table(rounds, peers)
    place = jnp.concatenate(
        [lax.axis_index("vec").reshape(1), table[:, lax.axis_index("res")]]
    ).astype(jnp.int32)

    def own_sum(acc_refs, x_ref, split_ref, rows_ref, cols_ref):
        batch = 4
        for first in range(0, OWN_SLOTS, batch):
            members = range(first, first + batch)
            ends = [(rows_ref[0, 0, s], cols_ref[0, 0, s]) for s in members]
            terms = [
                (
                    tile_product(x_ref[j], split_ref, s, True),
                    tile_product(x_ref[i], split_ref, s, False),
                )
                for s, (i, j) in zip(members, ends)
            ]
            for (i, j), (direct, mirror) in zip(ends, terms):
                for n, acc_ref in enumerate(acc_refs):
                    acc_ref[i] += direct[n * part : (n + 1) * part]
                    acc_ref[j] += mirror[n * part : (n + 1) * part]

    def prepare_body(x_hbm, diag_hbm, tiles_hbm, *refs):
        x_ref, split_ref, a_ref, b_ref, diag_ref, raw_ref, sem = refs
        size = slots // 4
        copies = [
            pltpu.make_async_copy(src, dst, sem.at[n])
            for n, (src, dst) in enumerate([(x_hbm, x_ref), (diag_hbm, diag_ref)])
        ]
        tile_copies = [
            pltpu.make_async_copy(
                tiles_hbm.at[0, 0, pl.ds(n * size, size)], raw_ref.at[pl.ds(n * size, size)], sem.at[2 + n]
            )
            for n in range(4)
        ]
        for c in copies + tile_copies:
            c.start()
        for n in range(4):
            tile_copies[n].wait()
            for s in range(n * size, (n + 1) * size):
                split_ref[s, 0], split_ref[s, 1] = pieces(raw_ref[s], 2)
        for c in copies:
            c.wait()
        first = (lax.axis_index("vec") == 0).astype(F32)
        d = ((diag_ref[...] - SHIFT) * first)[:, None, :]
        a_ref[...] = x_ref[:, :part] * d
        b_ref[...] = x_ref[:, part:] * d

    def own_body(rows_ref, cols_ref, x_ref, split_ref, *refs):
        own_sum(refs[len(refs) // 2 :], x_ref, split_ref, rows_ref, cols_ref)

    def pack(place_ref, rows_ref, counts_ref, asked_refs, x_ref, split_ref, outs):
        for p in range(count):
            role = place_ref[1 + p]

            def put(c, value, p=p):
                for n, ref in enumerate(outs[p]):
                    ref[c] = value[n * part : (n + 1) * part]

            @pl.when(role > 0)
            def _():
                base = OWN_SLOTS + (role - 1) * CAP
                terms = [
                    tile_product(x_ref[rows_ref[0, 0, base + c]], split_ref, base + c, False)
                    for c in range(CAP)
                ]
                for c, term in enumerate(terms):
                    put(c, jnp.where(c < counts_ref[0, 0, role - 1], term, 0.0))

            @pl.when(role < 0)
            def _():
                base = OWN_SLOTS + (-role - 1) * CAP
                for c in range(CAP):
                    put(c, x_ref[asked_refs[p][0, 0, base + c]])

    def send_body(place_ref, rows_ref, counts_ref, *refs):
        asked_refs, (x_ref, split_ref), outs = refs[:count], refs[count : count + 2], refs[count + 2 :]
        pack(
            place_ref, rows_ref, counts_ref, asked_refs, x_ref, split_ref,
            [(outs[p], outs[count + p]) for p in range(count)],
        )

    def settle(place_ref, mine_ref, other_ref, y_ref):
        core = place_ref[0] % 2
        y_ref[pl.ds(core * half, half)] = mine_ref[...]
        y_ref[pl.ds((1 - core) * half, half)] = other_ref[...]

    def resend_body(place_ref, rows_ref, counts_ref, *refs):
        asked_refs = refs[:count]
        mine_ref, other_ref, diag_ref, split_ref, y_ref, acc_ref = refs[count : count + 6]
        outs = refs[count + 6 :]
        settle(place_ref, mine_ref, other_ref, y_ref)
        pack(
            place_ref, rows_ref, counts_ref, asked_refs, y_ref, split_ref,
            [(outs[p],) for p in range(count)],
        )
        first = (place_ref[0] == 0).astype(F32)
        acc_ref[...] = y_ref[...] * (diag_ref[...] * first)[:, None, :]

    def join_rounds(members, place_ref, rows_ref, counts_ref, asked_refs, got_refs, split_ref, acc_ref):
        for n, p in enumerate(members):
            role = place_ref[1 + p]

            @pl.when(role > 0)
            def _():
                base = OWN_SLOTS + (role - 1) * CAP
                terms = [
                    tile_product(got_refs[n][c], split_ref, base + c, True) for c in range(CAP)
                ]
                for c, term in enumerate(terms):
                    acc_ref[rows_ref[0, 0, base + c]] += jnp.where(
                        c < counts_ref[0, 0, role - 1], term, 0.0
                    )

            @pl.when(role < 0)
            def _():
                base = OWN_SLOTS + (-role - 1) * CAP
                for c in range(CAP):
                    acc_ref[asked_refs[n][0, 0, base + c]] += got_refs[n][c]

    def join(acc, got, members, last=False):
        size = len(members)

        def body(place_ref, rows_ref, counts_ref, *refs):
            asked_refs, got_refs = refs[:size], refs[size : 2 * size]
            split_ref, prior_ref = refs[2 * size : 2 * size + 2]
            outs = refs[2 * size + 2 :]
            if last:
                keep_ref, give_ref, acc_ref = outs
                acc_ref[...] = prior_ref[...]
            else:
                (acc_ref,) = outs
            join_rounds(
                members, place_ref, rows_ref, counts_ref, asked_refs, got_refs, split_ref, acc_ref
            )
            if last:
                core = place_ref[0] % 2
                keep_ref[...] = acc_ref[pl.ds(core * half, half)]
                give_ref[...] = acc_ref[pl.ds((1 - core) * half, half)]

        out = call(
            body,
            [halfchunk] * 2 if last else [chunk],
            [SMEM] * (3 + size) + [VMEM] * (size + 2),
            [pltpu.VMEM(chunk, F32)] if last else [],
            name="join",
            weight=10**10,
            aliases=None if last else {3 + 2 * size + 1: 0},
        )(
            place, tile_rows, slot_counts, *[asked[p] for p in members], *[got[p] for p in members], split, acc
        )
        return out if last else out[0]

    def gram_body(x_ref, out_ref):
        total = jnp.zeros(square, F32)
        for n in range(0, rows, 2):
            pair = [x_ref[n], x_ref[n + 1]]
            total += gram_step(pair, [pair])
        out_ref[...] = total

    def cross_body(x_ref, a_ref, b_ref, out_ref):
        total = jnp.zeros((width, 2 * width), F32)
        for n in range(0, rows, 2):
            y = [jnp.concatenate([a_ref[m], b_ref[m]], axis=0) for m in (n, n + 1)]
            total += gram_step(y, [[x_ref[n], x_ref[n + 1]], y])
        out_ref[...] = total

    def first_body(gram_ref, inverse_ref):
        _, inverse_ref[...] = factor(gram_ref[...])

    def identity():
        eye = lax.broadcasted_iota(jnp.int32, square, 0) == lax.broadcasted_iota(jnp.int32, square, 1)
        return eye.astype(F32)

    def lower_part():
        return lax.broadcasted_iota(jnp.int32, square, 0) >= lax.broadcasted_iota(jnp.int32, square, 1)

    def second_body(gram_ref, inverse_ref, shift_ref, cross_ref, lower_ref, coef_ref, gain_ref):
        start_inv = inverse_ref[...]
        cross = dot(dot(start_inv, gram_ref[:, :width]), start_inv, tb=True)
        applied = dot(dot(start_inv, gram_ref[:, width:]), start_inv, tb=True)
        upper, inverse = factor(applied - dot(cross, cross, tb=True))
        lower = upper.T
        cross_ref[...] = cross + shift_ref[:1, :width] * identity()
        lower_ref[...] = lower
        gain = dot(inverse, start_inv)
        back = -dot(dot(inverse, cross), start_inv)
        gain_ref[...] = gain
        coef_ref[:width, :width] = -dot(lower, start_inv)
        coef_ref[:width, width : 2 * width] = back
        coef_ref[:width, 2 * width :] = gain
        coef_ref[width:, :width] = back
        coef_ref[width:, width : 2 * width] = gain
        coef_ref[width:, 2 * width :] = jnp.zeros(square, F32)

    def blend(side, mine, other, coef):
        def body(place_ref, x_ref, a_ref, b_ref, mine_ref, other_ref, coef_ref, w_ref, q_ref, out_ref, z_ref):
            settle(place_ref, mine_ref, other_ref, z_ref)
            for n in range(0, half, 2):
                stacks = [
                    jnp.concatenate([ref[side * half + m] for ref in (x_ref, a_ref, b_ref, z_ref)], axis=0)
                    for m in (n, n + 1)
                ]
                for m, both in zip((n, n + 1), wide_product(coef_ref[:, : 2 * width + part], stacks)):
                    w_ref[m] = both[:width]
                    q_ref[m] = both[width:]
            total = jnp.zeros(square, F32)
            for n in range(0, half, 2):
                qs = [q_ref[n], q_ref[n + 1]]
                total += gram_step(qs, [qs])
            out_ref[...] = total

        return call(
            body,
            [halffull, halffull, square],
            [SMEM] + [VMEM] * 6,
            [pltpu.VMEM(chunk, F32)],
            name="blend",
        )(place, x, y_a, y_b, mine, other, coef)

    def third_body(place_ref, mine_ref, other_ref, gain_ref, *refs):
        prior_refs, q_refs, norm_refs = refs[0:2], refs[2:4], refs[4:6]
        w_ref, out_ref, z_ref = refs[6:]
        settle(place_ref, mine_ref, other_ref, z_ref)
        for n in range(0, rows, 2):
            side, m = divmod(n, half)
            for k, w in enumerate(wide_product(gain_ref[:, part:], [z_ref[n], z_ref[n + 1]])):
                w_ref[n + k] = w + prior_refs[side][m + k]
        total = jnp.zeros((width, 2 * width), F32)
        for n in range(0, rows, 2):
            side, m = divmod(n, half)
            ws = [w_ref[n], w_ref[n + 1]]
            total += gram_step(ws, [[q_refs[side][m], q_refs[side][m + 1]], ws])
        norm = norm_refs[0][...] + norm_refs[1][...]
        out_ref[:width, :width] = total[:, :width]
        out_ref[:width, width:] = jnp.where(lower_part(), total[:, width:], norm)
        out_ref[width:, :] = jnp.zeros((8, 2 * width), F32)
        out_ref[width:, :width] = jnp.broadcast_to(
            jnp.sum(norm * identity(), axis=0, keepdims=True), (8, width)
        )

    def fourth_body(gram_ref, shift_ref, cross_ref, lower_ref, coef_ref):
        cross = gram_ref[:width, :width]
        packed = gram_ref[:width, width:]
        flipped = packed.T
        squares = jnp.where(lower_part(), packed, flipped)
        norm = jnp.where(lower_part(), flipped, packed)
        norm = jnp.where(identity() > 0, gram_ref[width : width + 1, :width], norm)
        taken = cross + shift_ref[:1, :width] * (norm - identity())
        mixed = dot(taken, cross, tb=True)
        squared = squares - mixed - mixed.T + dot(dot(taken, norm), taken, tb=True)
        upper, inverse = factor(squared)
        cross_ref[...] = taken + shift_ref[:1, :width] * identity()
        lower_ref[...] = upper.T
        scale = math.sqrt(rows * length * peers)
        coef_ref[:, :width] = inverse * scale
        coef_ref[:, width:] = -dot(inverse, taken) * scale

    def last_body(w_ref, low_ref, high_ref, coef_ref, a1_ref, l1_ref, a2_ref, l2_ref, out_ref, pack_ref):
        for n, ref in enumerate((a1_ref, l1_ref, a2_ref, l2_ref)):
            pack_ref[n] = ref[...]
        for n in range(0, rows, 2):
            side, at = divmod(n, half)
            q_ref = (low_ref, high_ref)[side]
            stacks = [jnp.concatenate([w_ref[n + k], q_ref[at + k]], axis=0) for k in range(2)]
            for m, out in zip((n, n + 1), wide_product(coef_ref[...], stacks, 4)):
                out_ref[m] = out

    swap = [(i, i ^ 1) for i in range(lanes)]
    cuts = [count * n // 3 for n in range(4)]
    groups = [list(range(cuts[n], cuts[n + 1])) for n in range(3)]

    def spread(sent):
        return [exchange(s, "res", entry["pairs"]) for s, entry in zip(sent, rounds)]

    def across(mine, *tokens):
        step = 2
        while step < lanes:
            got = lax.ppermute(mine, "vec", [(i, i ^ step) for i in range(lanes)])
            mine = mine + after(got, *tokens)
            step *= 2
        return mine

    def resend(mine, other):
        y, acc, *sent = call(
            resend_body,
            [chunk, chunk] + [packet] * count,
            [SMEM] * (3 + count) + [VMEM] * 4,
            name="resend",
        )(place, tile_rows, slot_counts, *asked, mine, other, centered, split)
        return y, acc, spread(sent)

    def own(y, *accs):
        return call(
            own_body,
            [chunk] * len(accs),
            [SMEM] * 2 + [VMEM] * (2 + len(accs)),
            name="own",
            aliases={4 + n: n for n in range(len(accs))},
        )(tile_rows, tile_cols, y, split, *accs)

    asked = [exchange(tile_cols, "res", entry["pairs"]) for entry in rounds]
    x, split, acc_a, acc_b = call(
        prepare_body,
        [full, split_shape, chunk, chunk],
        [HBM] * 3,
        [
            pltpu.VMEM(diagonal.shape, F32),
            pltpu.VMEM((slots, length, length), F32),
            pltpu.SemaphoreType.DMA((6,)),
        ],
        name="prepare",
    )(*[pinned(v) for v in (start_block, diagonal, hess_tiles)])
    sent = call(
        send_body, [packet] * (2 * count), [SMEM] * (3 + count) + [VMEM] * 2, name="send"
    )(place, tile_rows, slot_counts, *asked, x, split)
    got_a = spread(sent[:count])
    sent_b = list(sent[count:])
    shift = end_sum(start_sum(jnp.full((8, length), jnp.mean(diagonal), F32), "res"), "res") / peers
    centered = diagonal - shift[:1]
    scaled = jnp.where(place[0] == 0, centered, 0.0)[:, None, :]
    acc_a, acc_b = x[:, :part] * scaled, x[:, part:] * scaled
    acc_a, acc_b = own(x, after(acc_a, sent[0]), acc_b)
    for n in range(2):
        acc_a = join(acc_a, got_a, groups[n])
        turn = groups[0] if n == 1 else []
        acc_a, x, *gated = lax.optimization_barrier((acc_a, x, *[sent_b[p] for p in turn]))
        for p, value in zip(turn, gated):
            sent_b[p] = value
        if n == 0:
            (gram,) = call(gram_body, [square], [VMEM], name="gram")(x)
            start_gram = start_sum(gram, "res")
    acc_a = after(acc_a, start_gram)
    keep_a, give_a = join(acc_a, got_a, groups[2], last=True)
    for p in groups[1] + groups[2]:
        sent_b[p] = after(sent_b[p], keep_a)
    got_b = spread(sent_b)

    core = lax.ppermute(give_a, "vec", swap)
    acc_b = join(acc_b, got_b, groups[0])
    mine_a = keep_a + after(core, acc_b)
    (start_inv,) = call(first_body, [square], [VMEM], name="first")(end_sum(start_gram, "res", mine_a))
    acc_b = join(after(acc_b, start_inv), got_b, groups[1])
    mine_a = across(mine_a, acc_b)
    other_a = lax.ppermute(mine_a, "vec", swap)
    keep_b, give_b = join(acc_b, got_b, groups[2], last=True)
    y_a, acc_a, got_a = resend(mine_a, after(other_a, keep_b))

    core = lax.ppermute(give_b, "vec", swap)
    mine_b = keep_b + after(core, y_a)
    (acc_a,) = own(y_a, after(acc_a, mine_b))
    mine_b = across(mine_b, acc_a)
    other_b = lax.ppermute(mine_b, "vec", swap)
    acc_a = join(after(acc_a, mine_b), got_a, groups[2])
    y_b, acc_b, got_b = resend(mine_b, after(other_b, acc_a))
    acc_a = join(after(acc_a, y_b), got_a, groups[1])
    keep_a, give_a = join(acc_a, got_a, groups[0], last=True)

    core = lax.ppermute(give_a, "vec", swap)
    (acc_b,) = own(after(y_b, keep_a), acc_b)
    acc_b = join(acc_b, got_b, groups[0])
    mine_a = keep_a + after(core, acc_b)
    (gram,) = call(cross_body, [(width, 2 * width)], [VMEM] * 3, name="cross")(x, y_a, after(y_b, mine_a))
    acc_b = join(after(acc_b, gram), got_b, groups[1])
    cross_gram = start_sum(gram, "res")
    keep_b, give_b = join(after(acc_b, cross_gram), got_b, groups[2], last=True)

    core = lax.ppermute(give_b, "vec", swap)
    mine_a = across(mine_a, cross_gram)
    other_a = lax.ppermute(mine_a, "vec", swap)
    cross_gram = end_sum(cross_gram, "res")
    mine_b = keep_b + after(core, mine_a, cross_gram)
    cross1, lower1, coef, gain = call(
        second_body, [square, square, (2 * width, 3 * width), square], [VMEM] * 3, name="second"
    )(after(cross_gram, mine_b), start_inv, shift)
    w_low, q_low, norm_low = blend(0, mine_a, other_a, coef)
    w_high, q_high, norm_high = blend(1, mine_a, other_a, coef)
    mine_b = across(mine_b, norm_low, norm_high)
    other_b = lax.ppermute(mine_b, "vec", swap)
    w, gram = call(
        third_body,
        [full, (width + 8, 2 * width)],
        [SMEM] + [VMEM] * 9,
        [pltpu.VMEM(chunk, F32)],
        name="third",
    )(place, mine_b, other_b, gain, w_low, w_high, q_low, q_high, norm_low, norm_high)
    gram = all_sum(gram, "res")
    cross2, lower2, coef = call(
        fourth_body, [square, square, (width, 2 * width)], [VMEM] * 2, name="fourth"
    )(gram, shift)
    return call(last_body, [full, (4, width, width)], [VMEM] * 8, name="last")(
        w, q_low, q_high, coef, cross1, lower1, cross2, lower2
    )


def solution(mesh):
    in_specs = (
        P(("conf", "res"), None, None),
        P(("conf", "res"), None),
        P(("conf", "res"), "vec", None, None, None),
        P(("conf", "res"), "vec", None),
        P(("conf", "res"), "vec", None),
        P(("conf", "res"), "vec", None),
    )
    out_specs = (P(("conf", "res"), None, None), P("conf", None, None))
    return jax.shard_map(local, mesh=mesh, in_specs=in_specs, out_specs=out_specs, check_vma=False)
```
